128 devices in a mesh: inner: 4 (over x), fsdp: 32 (over z, y, core).
Axes of the slice: x: 4, y: 4, z: 4, core: 2. Of those that a mesh axis runs over, the one named last changes fastest.
Arguments:
- x_in: bfloat16 [16384, 2048], P(('inner', 'fsdp'))
- w_up: bfloat16 [2, 2048, 8192], P(None, ('inner', 'fsdp'))
- w_down: bfloat16 [2, 8192, 2048], P(None, ('inner', 'fsdp'))
- grad_out: bfloat16 [16384, 2048], P(('inner', 'fsdp'))
Outputs:
- output 1: bfloat16 [16384, 2048], P(('inner', 'fsdp'))
- output 2: bfloat16 [16384, 2048], P(('inner', 'fsdp'))
- output 3: float32 [2, 2048, 8192], P(None, ('inner', 'fsdp'))
- output 4: float32 [2, 8192, 2048], P(None, ('inner', 'fsdp'))
All inputs are finite; a program needn't handle non-finite values.
Results may differ from the reference program's by a relative error of at most 0.00497.
Values are sent between devices in bfloat16 or wider.
A program may use at most 1 GiB of HBM per device.

```python
import jax
import jax.numpy as jnp
from jax import lax

TOKENS = 16384
ROW_BLOCK = 128
D_MODEL = 2048
D_FF = 8192
LAYERS = 2


def gelu_parts(pre_act):
    norm_cdf = 0.5 * (1.0 + lax.erf(pre_act * (2.0 ** -0.5)))
    norm_pdf = jnp.exp(-0.5 * pre_act * pre_act) * ((2.0 * jnp.pi) ** -0.5)
    return pre_act * norm_cdf, norm_cdf + pre_act * norm_pdf


def setup_inputs(seed: int = 0) -> dict:
    base_key = jax.random.key(seed)
    key_x, key_up, key_down, key_g = jax.random.split(base_key, 4)
    x_in = jax.random.normal(key_x, (TOKENS, D_MODEL), jnp.float32).astype(jnp.bfloat16)
    w_up = (jax.random.normal(key_up, (LAYERS, D_MODEL, D_FF), jnp.float32) * D_MODEL ** -0.5).astype(jnp.bfloat16)
    w_down = (jax.random.normal(key_down, (LAYERS, D_FF, D_MODEL), jnp.float32) * D_FF ** -0.5).astype(jnp.bfloat16)
    grad_out = jax.random.normal(key_g, (TOKENS, D_MODEL), jnp.float32).astype(jnp.bfloat16)
    return {"x_in": x_in, "w_up": w_up, "w_down": w_down, "grad_out": grad_out}


def block_pass(x_blk, g_blk, w_up, w_down):
    def fwd_step(x_cur, weights):
        up_mat, down_mat = weights
        pre_act = jnp.dot(x_cur, up_mat, preferred_element_type=jnp.float32)
        post_act = gelu_parts(pre_act)[0].astype(jnp.bfloat16)
        branch = jnp.dot(post_act, down_mat, preferred_element_type=jnp.float32)
        return (x_cur.astype(jnp.float32) + branch).astype(jnp.bfloat16), x_cur

    y_blk, layer_inputs = lax.scan(fwd_step, x_blk, (w_up, w_down))

    def bwd_step(g_cur, scan_in):
        x_cur, up_mat, down_mat = scan_in
        pre_act = jnp.dot(x_cur, up_mat, preferred_element_type=jnp.float32)
        post_full, gelu_slope = gelu_parts(pre_act)
        post_act = post_full.astype(jnp.bfloat16)
        d_act = jnp.dot(g_cur, down_mat.T, preferred_element_type=jnp.float32)
        d_pre = (d_act * gelu_slope).astype(jnp.bfloat16)
        back_term = jnp.dot(d_pre, up_mat.T, preferred_element_type=jnp.float32)
        g_next = (g_cur.astype(jnp.float32) + back_term).astype(jnp.bfloat16)
        grad_up = jnp.dot(x_cur.T, d_pre, preferred_element_type=jnp.float32)
        grad_down = jnp.dot(post_act.T, g_cur, preferred_element_type=jnp.float32)
        return g_next, (grad_up, grad_down)

    g_in, layer_grads = lax.scan(bwd_step, g_blk, (layer_inputs, w_up, w_down), reverse=True)
    return y_blk, g_in, layer_grads[0], layer_grads[1]


def reference(x_in, w_up, w_down, grad_out):
    blocks = TOKENS // ROW_BLOCK
    x_blocks = x_in.reshape(blocks, ROW_BLOCK, D_MODEL)
    g_blocks = grad_out.reshape(blocks, ROW_BLOCK, D_MODEL)

    def block_step(running, scan_in):
        y_blk, g_in, grad_up, grad_down = block_pass(scan_in[0], scan_in[1], w_up, w_down)
        return (running[0] + grad_up, running[1] + grad_down), (y_blk, g_in)

    zero_sums = (jnp.zeros((LAYERS, D_MODEL, D_FF), jnp.float32), jnp.zeros((LAYERS, D_FF, D_MODEL), jnp.float32))
    grad_sums, per_block = lax.scan(block_step, zero_sums, (x_blocks, g_blocks))
    y_out = per_block[0].reshape(TOKENS, D_MODEL)
    grad_in = per_block[1].reshape(TOKENS, D_MODEL)
    return (y_out, grad_in, grad_sums[0], grad_sums[1])
```

```python
import functools

import jax
import jax.numpy as jnp
import numpy as np
from jax import lax
from jax.experimental import pallas as pl
from jax.experimental.pallas import tpu as pltpu
from jax.sharding import Mesh, PartitionSpec as P

MESH_ID = pl.DeviceIdType.MESH
ALL = ("x", "z", "y", "c")
F32, BF16 = jnp.float32, jnp.bfloat16
RING, CORES, ARRIVALS = 4, 2, 6
OWN, NXT, OPP, PRV = range(RING)
X0, X1, G1, G0 = range(RING)
HALVES = (0, 1)
N_SEM = 224
N_LOCAL = 112


def gelu_parts(pre_act):
    norm_cdf = 0.5 * (1.0 + lax.erf(pre_act * (2.0 ** -0.5)))
    norm_pdf = jnp.exp(-0.5 * pre_act * pre_act) * ((2.0 * jnp.pi) ** -0.5)
    return pre_act * norm_cdf, norm_cdf + pre_act * norm_pdf


def loop(n, body, init):
    return lax.fori_loop(0, n, body, init)


def dot_nn(left, right):
    return lax.dot_general(left, right, (((1,), (0,)), ((), ())), preferred_element_type=F32)


def dot_nt(left, right):
    return lax.dot_general(left, right, (((1,), (1,)), ((), ())), preferred_element_type=F32)


def dot_tn(left, right):
    return lax.dot_general(left, right, (((0,), (0,)), ((), ())), preferred_element_type=F32)


def kernel(dims, x_in, wu_in, wd_in, g_in,
           y_out, gi_out, gu_out, gd_out,
           xh0, gh1, wuh, wdh, sh0, ah, ra1, rb1, ra2, rb2, uh,
           U, W, XV, GV1, GV0, SV, AV, DV, GPA, GPB, PP, DR, XR, RES, STA, STB,
           ss, rs, ls, credit):
    D, K, TB, UR, DR_ROWS = dims
    HB = TB // 2
    x, z, y, c = (lax.axis_index(a) for a in ALL)
    cp = 1 - c
    S2 = 2 * DR_ROWS
    XD = D // 4
    ZD = D // 16

    def dev(dx=0, dz=0, dy=0, dc=0):
        wrap = lambda v, d, n: v if d == 0 else lax.rem(v + (d % n), n)
        return (wrap(x, dx, 4), wrap(z, dz, 4), wrap(y, dy, 4), wrap(c, dc, 2))

    partner = dev(dc=1)
    rings = {"x": (x, dev(dx=1), dev(dx=-1)), "z": (z, dev(dz=1), dev(dz=-1)), "y": (y, dev(dy=1), dev(dy=-1))}
    off = lambda v, d: v if d == 0 else lax.rem(v + d, 4)

    count = [0]

    def rcopy(src, dst, to):
        k = count[0]
        count[0] += 1
        return pltpu.make_async_remote_copy(src_ref=src, dst_ref=dst, send_sem=ss.at[k], recv_sem=rs.at[k],
                                            device_id=to, device_id_type=MESH_ID)

    lcount = [0]

    def lcopy(src, dst):
        k = lcount[0]
        lcount[0] += 1
        return pltpu.make_async_copy(src, dst, ls.at[k])

    def mo(v, m):
        return pl.multiple_of(v, m)

    class Gather4:
        def __init__(self, axis, src, dst):
            i, right, left = rings[axis]
            lft, rgt = off(i, 3), off(i, 1)
            self.d = [rcopy(src(0), dst(i, 0), right), rcopy(src(1), dst(i, 1), right),
                      rcopy(src(0), dst(i, 0), left), rcopy(src(1), dst(i, 1), left),
                      rcopy(dst(lft, 0), dst(lft, 0), right), rcopy(dst(rgt, 1), dst(rgt, 1), left)]

        def start(self):
            for k in (0, 3, 1, 2):
                self.d[k].start()

        def forward(self):
            self.d[0].wait_recv()
            self.d[4].start()
            self.d[3].wait_recv()
            self.d[5].start()

        def finish(self):
            for k in (1, 2, 4, 5):
                self.d[k].wait_recv()

        def drain(self):
            for d in self.d:
                d.wait_send()

    class Gather8:
        def __init__(self, src, dst):
            self.ring = Gather4("x", src, lambda b, h: dst(b, c, h))
            lft, rgt, opp = off(x, PRV), off(x, NXT), off(x, OPP)
            blocks = [(lft, 0), (rgt, 1), (lft, 1), (rgt, 0), (opp, 0), (opp, 1)]
            self.own = [rcopy(src(h), dst(x, c, h), partner) for h in HALVES]
            self.push = [rcopy(dst(b, c, h), dst(b, c, h), partner) for b, h in blocks]

        def start(self):
            self.ring.start()
            for d in self.own:
                d.start()

        def forward(self):
            self.ring.forward()
            self.push[0].start()
            self.push[1].start()

        def sides(self):
            self.ring.d[1].wait_recv()
            self.push[2].start()
            self.ring.d[2].wait_recv()
            self.push[3].start()

        def last(self):
            self.ring.d[4].wait_recv()
            self.push[4].start()
            self.ring.d[5].wait_recv()
            self.push[5].start()

        def wait_own(self):
            for d in self.own:
                d.wait_recv()

        def wait_push(self, ks):
            for k in ks:
                self.push[k].wait_recv()

        def drain(self):
            self.ring.drain()
            for d in self.own + self.push:
                d.wait_send()

    def add_rows(dst, srcs, rows, step):
        def body(r, carry):
            sl = pl.ds(mo(r * step, step), step)
            if len(dst.shape) == 3:
                for q in range(dst.shape[0]):
                    acc = dst[q, sl, :]
                    for s in srcs:
                        acc = acc + s[q, sl, :]
                    dst[q, sl, :] = acc
            else:
                acc = dst[sl, :]
                for s in srcs:
                    acc = acc + s[sl, :]
                dst[sl, :] = acc
            return carry
        loop(rows // step, body, None)

    barrier = pltpu.get_barrier_semaphore()
    group = [(dx, dc) for dx in range(RING) for dc in range(2) if (dx, dc) != (0, 0)]
    peers = [dev(dx=dx, dc=dc) for dx, dc in group] + [rings["z"][1], rings["z"][2], rings["y"][1], rings["y"][2]]
    for p in peers:
        pl.semaphore_signal(barrier, inc=1, device_id=p, device_id_type=MESH_ID)

    load_u = [[lcopy(wu_in.at[l, :, pl.ds(b * (4 * K // 2), 4 * K // 2)],
                     RES.at[G0, pl.ds((l * 4 + b) * UR, UR), :]) for b in range(RING)] for l in HALVES]
    for l in HALVES:
        for cpy in load_u[l]:
            cpy.start()
    load_d = [lcopy(wd_in.at[l], RES.at[X1, pl.ds(l * DR_ROWS, DR_ROWS), :]) for l in HALVES]
    for cpy in load_d:
        cpy.start()
    load_x = lcopy(x_in, RES.at[X0])
    load_g = lcopy(g_in, RES.at[G1])
    load_x.start()
    load_g.start()
    pl.semaphore_wait(barrier, len(peers))

    half = lambda h: pl.ds(h * HB, HB)
    gx0 = Gather8(lambda h: x_in.at[half(h)], lambda b, k, h: xh0.at[b, k, half(h)])
    gg1 = Gather8(lambda h: g_in.at[half(h)], lambda b, k, h: gh1.at[b, k, half(h)])
    gx0.start()

    hr = DR_ROWS // 2
    gd1 = [Gather4("z", (lambda l: lambda h: wd_in.at[l, pl.ds(h * hr, hr)])(l),
                   (lambda l: lambda b, h: wdh.at[l, y, b, pl.ds(h * hr, hr)])(l)) for l in HALVES]
    gd2 = [Gather4("y", (lambda l: lambda h: wdh.at[l, y, pl.ds(2 * h, 2)])(l),
                   (lambda l: lambda b, h: wdh.at[l, b, pl.ds(2 * h, 2)])(l)) for l in HALVES]
    gu1 = [Gather4("y", (lambda l: lambda h: wuh.at[l, pl.ds(2 * h, 2), z, y])(l),
                   (lambda l: lambda b, h: wuh.at[l, pl.ds(2 * h, 2), z, b])(l)) for l in HALVES]
    gu2 = [Gather4("z", (lambda l: lambda h: wuh.at[l, pl.ds(2 * h, 2), z])(l),
                   (lambda l: lambda b, h: wuh.at[l, pl.ds(2 * h, 2), b])(l)) for l in HALVES]
    gd1[0].start()

    lane = lax.broadcasted_iota(jnp.int32, (UR, S2), 1)
    low = lane < DR_ROWS

    def shuffle_up(l):
        for b in range(RING):
            rows = pl.ds((l * 4 + b) * UR, UR)
            for yy in range(RING):
                for m in HALVES:
                    s0 = RES[G0, rows, pl.ds((2 * m * 4 + yy) * S2, S2)].astype(F32)
                    s1 = RES[G0, rows, pl.ds(((2 * m + 1) * 4 + yy) * S2, S2)].astype(F32)
                    cols = pl.ds((yy * 2 + m) * S2, S2)
                    t0 = jnp.where(low, s0, pltpu.roll(s1, DR_ROWS, 1))
                    t1 = jnp.where(low, pltpu.roll(s0, DR_ROWS, 1), s1)
                    AV[l, pl.ds((b * 2 + 0) * UR, UR), cols] = t0.astype(BF16)
                    AV[l, pl.ds((b * 2 + 1) * UR, UR), cols] = t1.astype(BF16)

    a2a = [[], []]
    own_u = []
    for l in HALVES:
        for cpy in load_u[l]:
            cpy.wait()
        shuffle_up(l)
        for dx, dc in group:
            tx, tc = off(x, dx), (c if dc == 0 else cp)
            src = AV.at[l, pl.ds(mo((tx * 2 + tc) * UR, UR), UR), :]
            dst = wuh.at[l, x, z, y, pl.ds(mo(c * UR, UR), UR), :]
            d = rcopy(src, dst, dev(dx=dx, dc=dc))
            d.start()
            a2a[l].append(d)
        cpy = lcopy(AV.at[l, pl.ds(mo((x * 2 + c) * UR, UR), UR), :], wuh.at[l, x, z, y, pl.ds(mo(c * UR, UR), UR), :])
        cpy.start()
        own_u.append(cpy)
    own_d = []
    for l in HALVES:
        load_d[l].wait()
        cpy = lcopy(RES.at[X1, pl.ds(l * DR_ROWS, DR_ROWS), :], wdh.at[l, y, z])
        cpy.start()
        own_d.append(cpy)
    load_x.wait()
    load_g.wait()
    own_x = lcopy(RES.at[X0], xh0.at[x, c])
    own_x.start()
    own_g = lcopy(RES.at[G1], gh1.at[x, c])
    own_g.start()

    for d in a2a[0]:
        d.wait_recv()
    own_u[0].wait()
    gu1[0].start()
    gd1[0].forward()
    gx0.forward()
    gu1[0].forward()
    gd1[0].finish()
    own_d[0].wait()
    gd2[0].start()
    gu1[0].finish()
    gu2[0].start()
    gx0.sides()
    gg1.start()
    gx0.last()
    gx0.wait_own()
    gx0.wait_push(range(6))
    own_x.wait()
    load_xv = lcopy(xh0, XV)
    load_xv.start()
    gu2[0].forward()
    gd2[0].forward()
    gd1[1].start()
    for d in a2a[1]:
        d.wait_recv()
    own_u[1].wait()
    gu1[1].start()
    gg1.forward()
    gg1.sides()
    gg1.last()
    gu2[0].finish()
    load_w0u = lcopy(wuh.at[0], U)
    load_w0u.start()
    gd2[0].finish()
    load_w0d = lcopy(wdh.at[0], W)
    load_w0d.start()
    for l in HALVES:
        for d in a2a[l]:
            d.wait_send()
    load_xv.wait()
    load_w0u.wait()

    T2 = 2 * TB
    ND = D // 4
    NK = K // 4

    def up_tile(t, n):
        cols = pl.ds(mo(n * NK, NK), NK)
        return dot_nn(XV[t].reshape(T2, D), U[:, :, :, :, cols].reshape(D, NK)), cols

    def hidden0(t):
        def body(n, carry):
            pre, cols = up_tile(t, n)
            act, slope = gelu_parts(pre)
            AV[t, :, cols] = act.astype(BF16)
            SV[t, :, cols] = slope
            return carry
        loop(K // NK, body, None)

    def hidden1(t):
        def body(n, carry):
            pre, cols = up_tile(t, n)
            act, slope = gelu_parts(pre)
            AV[t, :, cols] = act.astype(BF16)
            DV[t, :, cols] = (SV[t, :, cols] * slope).astype(BF16)
            return carry
        loop(K // NK, body, None)

    def dact(gv, t, n):
        return dot_nt(gv[t].reshape(T2, D), W[n].reshape(NK, D))

    def dact1(t):
        def body(n, carry):
            SV[t, :, pl.ds(mo(n * NK, NK), NK)] = dact(GV1, t, n)
            return carry
        loop(RING, body, None)

    def dact0(t):
        def body(n, carry):
            cols = pl.ds(mo(n * NK, NK), NK)
            DV[t, :, cols] = (dact(GV0, t, n) * SV[t, :, cols]).astype(BF16)
            return carry
        loop(RING, body, None)

    def down_part(j):
        t = off(x, j)

        def body(n, carry):
            cols = pl.ds(mo(n * ND, ND), ND)
            PP[j, :, :, cols] = dot_nn(AV[t], W[:, :, :, cols].reshape(K, ND)).reshape(2, TB, ND)
            return carry
        loop(RING, body, None)

    def dx_part(j):
        t = off(x, j)

        def body(n, carry):
            cols = pl.ds(mo(n * ND, ND), ND)
            PP[j, :, :, cols] = dot_nt(DV[t], U[n].reshape(ND, K)).reshape(2, TB, ND)
            return carry
        loop(RING, body, None)

    class Reduce8:
        def __init__(self, part, index):
            self.part, self.index = part, index
            _, right, left = rings["x"]
            self.right, self.left = right, left
            self.pair = [rcopy(PP.at[j, cp], DR.at[j], partner) for j in range(RING)]
            self.m = [rcopy(PP.at[OPP, c, half(0)], XR.at[0], right), rcopy(PP.at[OPP, c, half(1)], XR.at[1], left),
                      rcopy(PP.at[NXT, c, half(1)], XR.at[2], right), rcopy(PP.at[PRV, c, half(0)], XR.at[3], left),
                      rcopy(PP.at[NXT, c, half(0)], XR.at[4], right), rcopy(PP.at[PRV, c, half(1)], XR.at[5], left)]

        def credits(self):
            if self.index:
                for k in range(3):
                    pl.semaphore_wait(credit.at[k], 1)

        def compute(self, j):
            self.part(j)
            self.pair[j].start()

        def combine(self, j):
            self.pair[j].wait_recv()
            add_rows(PP.at[j, c], [DR.at[j]], TB, min(TB, 16))

        def opposite(self):
            self.combine(OPP)
            self.m[0].start()
            self.m[1].start()

        def sides(self, j):
            self.combine(j)
            self.m[2 if j == NXT else 3].start()

        def relay(self):
            self.m[0].wait_recv()
            add_rows(PP.at[NXT, c, half(0)], [XR.at[0]], HB, min(HB, 16))
            self.m[4].start()
            self.m[1].wait_recv()
            add_rows(PP.at[PRV, c, half(1)], [XR.at[1]], HB, min(HB, 16))
            self.m[5].start()

        def finish(self, res, outs):
            for k in (2, 3, 4, 5):
                self.m[k].wait_recv()
            step = min(HB, 16)
            for h, (kl, kr) in enumerate(((4, 3), (2, 5))):
                def body(r, carry):
                    lo = pl.ds(mo(r * step, step), step)
                    sl = pl.ds(mo(h * HB + r * step, step), step)
                    tot = PP[OWN, c, sl, :] + (XR[kl, lo, :] + XR[kr, lo, :])
                    val = (res[sl, :].astype(F32) + tot).astype(BF16)
                    for o in outs:
                        o[sl, :] = val
                    return carry
                loop(HB // step, body, None)
            for d in self.pair + self.m:
                d.wait_send()
            if self.index < 3:
                pl.semaphore_signal(credit.at[0], inc=1, device_id=self.right, device_id_type=MESH_ID)
                pl.semaphore_signal(credit.at[1], inc=1, device_id=self.left, device_id_type=MESH_ID)
                pl.semaphore_signal(credit.at[2], inc=1, device_id=partner, device_id_type=MESH_ID)

    def grad_a(j):
        t = off(z, j)
        for h in HALVES:
            lo = [pl.ds(mo((2 * h + q) * XD + t * ZD, ZD), ZD) for q in HALVES]
            lhs = jnp.concatenate([XV[:, :, :, s].reshape(8 * TB, ZD) for s in lo], axis=1)

            def body(n, carry):
                cols = pl.ds(mo(n * NK, NK), NK)
                out = dot_tn(lhs, DV[:, :, cols].reshape(8 * TB, NK))
                GPA[j, h, :, :, cols] = out.reshape(2, ZD, NK)
                return carry
            loop(K // NK, body, None)

    def grad_b(gv, j):
        t = off(y, j)
        cols_l = pl.ds(mo(t * NK, NK), NK)

        def body(n, carry):
            cols = pl.ds(mo(n * ND, ND), ND)
            out = dot_tn(AV[:, :, cols_l].reshape(8 * TB, NK), gv[:, :, :, cols].reshape(8 * TB, ND))
            GPB[j, :, :, cols] = out.reshape(2, NK // 2, ND)
            return carry
        loop(RING, body, None)

    class Reduce4:
        def __init__(self, axis, part, recv, rows, step):
            _, right, left = rings[axis]
            self.part, self.recv, self.rows, self.step = part, recv, rows, step
            self.m = [rcopy(part(OPP, 0), recv(0), right), rcopy(part(OPP, 1), recv(1), left),
                      rcopy(part(NXT, 1), recv(2), right), rcopy(part(PRV, 0), recv(3), left),
                      rcopy(part(NXT, 0), recv(4), right), rcopy(part(PRV, 1), recv(5), left)]

        def opposite(self):
            self.m[0].start()
            self.m[1].start()

        def sides(self, j):
            self.m[2 if j == NXT else 3].start()

        def relay(self, stage):
            loads = [lcopy(self.recv(0), stage(0)), lcopy(self.recv(1), stage(1))]
            for k in range(2):
                self.m[k].wait_send()
                self.m[k].wait_recv()
                loads[k].start()
            loads[0].wait()
            add_rows(self.part(NXT, 0), [stage(0)], self.rows, self.step)
            self.m[4].start()
            loads[1].wait()
            add_rows(self.part(PRV, 1), [stage(1)], self.rows, self.step)
            self.m[5].start()

        def finish(self, stages):
            for k in (2, 3, 4, 5):
                self.m[k].wait_send()
            for h, (kl, kr) in enumerate(((4, 3), (2, 5))):
                st = stages(h)
                loads = [lcopy(self.recv(kl), st[0]), lcopy(self.recv(kr), st[1])]
                self.m[kl].wait_recv()
                loads[0].start()
                self.m[kr].wait_recv()
                loads[1].start()
                loads[0].wait()
                loads[1].wait()
                add_rows(self.part(0, h), st, self.rows, self.step)

    hq = DR_ROWS // 2

    def make_reduce(l):
        a1 = Reduce4("z", lambda j, h: GPA.at[j, h], lambda k: ra1.at[l, k], ZD, min(ZD, 16))
        b1 = Reduce4("y", lambda j, h: GPB.at[j, h], lambda k: rb1.at[l, k], NK // 2, min(NK // 2, 16))

        def part_a2(j, h):
            return GPA.at[OWN, h, :, pl.ds(mo(off(y, j) * 2 * UR, 2 * UR), 2 * UR), :]

        def part_b2(j, h):
            t = off(z, j)
            return GPB.at[OWN, t // 2, pl.ds(mo(lax.rem(t, 2) * DR_ROWS + h * hq, hq), hq), :]
        a2 = Reduce4("y", part_a2, lambda k: ra2.at[l, k], 2 * UR, min(2 * UR, 16))
        b2 = Reduce4("z", part_b2, lambda k: rb2.at[l, k], hq, min(hq, 16))
        return a1, b1, a2, b2

    def grads_phase2_start(a2, b2):
        for r in (a2, b2):
            r.opposite()
            r.sides(NXT)
            r.sides(PRV)

    st_a = lambda k: STA.at[k]
    st_b = lambda k: STB.at[k]

    def grads_out_start(l):
        sends = []
        for dx, dc in group:
            tx, tc = off(x, dx), (c if dc == 0 else cp)
            src = GPA.at[OWN, tx // 2, lax.rem(tx, 2), pl.ds(mo(y * 2 * UR + tc * UR, UR), UR), :]
            d = rcopy(src, uh.at[l, x, pl.ds(mo(c * UR, UR), UR), :], dev(dx=dx, dc=dc))
            d.start()
            sends.append(d)
        own = lcopy(GPA.at[OWN, x // 2, lax.rem(x, 2), pl.ds(mo(y * 2 * UR + c * UR, UR), UR), :],
                    uh.at[l, x, pl.ds(mo(c * UR, UR), UR), :])
        own.start()
        outs = [lcopy(GPB.at[OWN, z // 2, pl.ds(mo(lax.rem(z, 2) * DR_ROWS + h * hq, hq), hq), :],
                      gd_out.at[l, pl.ds(h * hq, hq), :]) for h in HALVES]
        for o in outs:
            o.start()
        return sends, own, outs

    def grads_out_finish(l, state):
        sends, own, outs = state
        for d in sends:
            d.wait_recv()
        own.wait()
        loads = [lcopy(uh.at[l, b], STA.at[b // 2, b % 2]) for b in range(RING)]
        for ld in loads:
            ld.start()
        writes = []
        for b in range(RING):
            loads[b].wait()
            rows = pl.ds((b % 2) * UR, UR)
            for yy in range(RING):
                for m in HALVES:
                    cols = pl.ds((yy * 2 + m) * S2, S2)
                    t0 = STA[b // 2, b % 2, 0:UR, cols]
                    t1 = STA[b // 2, b % 2, UR:2 * UR, cols]
                    STB[b // 2, rows, pl.ds((2 * m * 4 + yy) * S2, S2)] = jnp.where(low, t0, pltpu.roll(t1, DR_ROWS, 1))
                    STB[b // 2, rows, pl.ds(((2 * m + 1) * 4 + yy) * S2, S2)] = jnp.where(low, pltpu.roll(t0, DR_ROWS, 1), t1)
            wr = lcopy(STB.at[b // 2, rows, :], gu_out.at[l, :, pl.ds(b * 16 * S2, 16 * S2)])
            wr.start()
            writes.append(wr)
        for wr in writes + outs:
            wr.wait()
        for d in sends:
            d.wait_send()

    def each_chip(fn):
        def body(t, carry):
            fn(t)
            return carry
        loop(RING, body, None)

    each_chip(hidden0)
    save_s = lcopy(SV, sh0)
    save_s.start()
    save_a0 = lcopy(AV, ah.at[0])
    save_a0.start()
    load_w0d.wait()

    r = Reduce8(down_part, 0)
    r.credits()
    r.compute(OPP)
    r.compute(NXT)
    r.opposite()
    r.compute(PRV)
    r.sides(NXT)
    r.compute(OWN)
    r.sides(PRV)
    gd1[1].forward()
    gu1[1].forward()
    gd1[1].finish()
    own_d[1].wait()
    gd2[1].start()
    gu1[1].finish()
    gu2[1].start()
    r.relay()
    r.combine(OWN)
    gg1.wait_own()
    gg1.wait_push(range(6))
    own_g.wait()
    load_gv = lcopy(gh1, GV1)
    load_gv.start()
    gu2[1].forward()
    gd2[1].forward()
    load_gv.wait()
    gx1 = Gather8(lambda h: RES.at[X1, half(h)], lambda b, k, h: XV.at[b, k, half(h)])
    r.finish(RES.at[X0], [RES.at[X1], XV.at[x, c]])
    gx1.start()
    gu2[1].finish()
    load_w1u = lcopy(wuh.at[1], U)
    load_w1u.start()
    gd2[1].finish()
    load_w1d = lcopy(wdh.at[1], W)
    load_w1d.start()
    gx1.forward()
    save_s.wait()
    load_w1d.wait()
    dact1(off(x, OWN))
    gx1.sides()
    dact1(off(x, NXT))
    dact1(off(x, PRV))
    load_w1u.wait()
    save_a0.wait()
    gx1.wait_own()
    hidden1(off(x, OWN))
    gx1.last()
    dact1(off(x, OPP))
    load_w0d_again = lcopy(wdh.at[0], W)
    load_w0d_again.start()
    gx1.wait_push((0, 2))
    hidden1(off(x, PRV))
    gx1.wait_push((1, 3))
    hidden1(off(x, NXT))
    gx1.wait_push((4, 5))
    hidden1(off(x, OPP))
    load_s0 = lcopy(sh0, SV)
    load_s0.start()
    save_a1 = lcopy(AV, ah.at[1])
    save_a1.start()

    a1, b1, a2, b2 = make_reduce(1)
    r = Reduce8(dx_part, 1)
    r.credits()
    r.compute(OPP)
    r.compute(NXT)
    r.opposite()
    r.compute(PRV)
    r.sides(NXT)
    r.sides(PRV)
    grad_b(GV1, OPP)
    b1.opposite()
    grad_a(OPP)
    a1.opposite()
    r.compute(OWN)
    load_w0u_again = lcopy(wuh.at[0], U)
    load_w0u_again.start()
    grad_b(GV1, NXT)
    b1.sides(NXT)
    grad_b(GV1, PRV)
    b1.sides(PRV)
    grad_a(NXT)
    a1.sides(NXT)
    grad_a(PRV)
    a1.sides(PRV)
    r.relay()
    r.combine(OWN)
    grad_b(GV1, OWN)
    save_a1.wait()
    load_a0 = lcopy(ah.at[0], AV)
    load_a0.start()
    gx1.drain()
    grad_a(OWN)
    load_x0 = lcopy(xh0, XV)
    load_x0.start()
    b1.relay(lambda k: GPB.at[OPP, k])
    a1.relay(lambda k: GPA.at[OPP, k])
    gg0 = Gather8(lambda h: RES.at[G0, half(h)], lambda b, k, h: GV0.at[b, k, half(h)])
    r.finish(RES.at[G1], [RES.at[G0], GV0.at[x, c]])
    gg0.start()
    load_w0d_again.wait()
    load_s0.wait()
    gg0.forward()
    gg0.wait_own()
    dact0(off(x, OWN))
    gg0.sides()
    gg0.last()
    gg0.wait_push((0, 2))
    dact0(off(x, PRV))
    gg0.wait_push((1, 3))
    dact0(off(x, NXT))
    gg0.wait_push((4, 5))
    dact0(off(x, OPP))
    load_w1d_again = lcopy(wdh.at[1], W)
    load_w1d_again.start()

    load_w0u_again.wait()
    r = Reduce8(dx_part, 2)
    r.credits()
    r.compute(OPP)
    r.compute(NXT)
    r.opposite()
    r.compute(PRV)
    r.sides(NXT)
    r.sides(PRV)
    r.compute(OWN)
    b1.finish(lambda h: [GPB.at[NXT, h], GPB.at[PRV, h]])
    a1.finish(lambda h: [GPA.at[NXT, h], GPA.at[PRV, h]])
    grads_phase2_start(a2, b2)
    load_a0.wait()
    a1n, b1n, a2n, b2n = make_reduce(0)
    grad_b(GV0, OPP)
    b1n.opposite()
    load_x0.wait()
    grad_a(OPP)
    a1n.opposite()
    r.relay()
    r.combine(OWN)
    b2.relay(st_b)
    a2.relay(st_a)
    grad_b(GV0, NXT)
    b1n.sides(NXT)
    grad_b(GV0, PRV)
    b1n.sides(PRV)
    grad_a(NXT)
    a1n.sides(NXT)
    grad_a(PRV)
    a1n.sides(PRV)
    b2.finish(lambda h: [STB.at[0], STB.at[1]])
    a2.finish(lambda h: [STA.at[0], STA.at[1]])
    state1 = grads_out_start(1)
    r.finish(RES.at[G0], [RES.at[X0]])
    write_gi = lcopy(RES.at[X0], gi_out)
    write_gi.start()
    grads_out_finish(1, state1)
    grad_b(GV0, OWN)
    load_a1 = lcopy(ah.at[1], AV)
    load_a1.start()
    grad_a(OWN)
    load_a1.wait()
    load_w1d_again.wait()
    r = Reduce8(down_part, 3)
    r.credits()
    r.compute(OPP)
    r.compute(NXT)
    r.opposite()
    r.compute(PRV)
    r.sides(NXT)
    r.compute(OWN)
    r.sides(PRV)
    b1n.relay(lambda k: GPB.at[OPP, k])
    a1n.relay(lambda k: GPA.at[OPP, k])
    r.relay()
    r.combine(OWN)
    r.finish(RES.at[X1], [RES.at[G1]])
    write_y = lcopy(RES.at[G1], y_out)
    write_y.start()
    b1n.finish(lambda h: [GPB.at[NXT, h], GPB.at[PRV, h]])
    a1n.finish(lambda h: [GPA.at[NXT, h], GPA.at[PRV, h]])
    grads_phase2_start(a2n, b2n)
    b2n.relay(st_b)
    a2n.relay(st_a)
    b2n.finish(lambda h: [STB.at[0], STB.at[1]])
    a2n.finish(lambda h: [STA.at[0], STA.at[1]])
    state0 = grads_out_start(0)
    grads_out_finish(0, state0)
    write_gi.wait()
    write_y.wait()
    for g in gd1 + gd2 + gu1 + gu2 + [gx0, gg1, gg0]:
        g.drain()
    assert count[0] <= N_SEM and lcount[0] <= N_LOCAL


def solution(mesh, interpret=None):
    fine = Mesh(np.asarray(mesh.devices).reshape(4, 4, 4, 2), ALL)
    tok_spec = P(ALL, None)
    weight_spec = P(None, ALL, None)

    def device_step(x_loc, up_loc, down_loc, g_loc):
        layers, ur, ff = up_loc.shape
        dr, dm = down_loc.shape[1:]
        tb = x_loc.shape[0]
        k = ff // 8
        zd = dm // 16
        nk = k // 4
        hbm = lambda shape, dt: jax.ShapeDtypeStruct(shape, dt)
        outs = [
            hbm((tb, dm), BF16), hbm((tb, dm), BF16), hbm((layers, ur, ff), F32), hbm((layers, dr, dm), F32),
            hbm((RING, CORES, tb, dm), BF16), hbm((RING, CORES, tb, dm), BF16),
            hbm((layers, RING, RING, RING, 2 * ur, k), BF16),
            hbm((layers, RING, RING, dr, dm), BF16),
            hbm((RING, 2 * tb, k), F32), hbm((layers, 4, 2 * tb, k), BF16),
            hbm((layers, ARRIVALS, CORES, zd, k), F32), hbm((layers, ARRIVALS, nk // 2, dm), F32),
            hbm((layers, ARRIVALS, CORES, 2 * ur, k), F32), hbm((layers, ARRIVALS, dr // 2, dm), F32),
            hbm((layers, 4, 2 * ur, k), F32),
        ]
        vm = pltpu.VMEM
        scratch = [
            vm((RING, RING, RING, 2 * ur, k), BF16), vm((RING, RING, dr, dm), BF16),
            vm((RING, CORES, tb, dm), BF16), vm((RING, CORES, tb, dm), BF16), vm((RING, CORES, tb, dm), BF16),
            vm((RING, 2 * tb, k), F32), vm((RING, 2 * tb, k), BF16), vm((RING, 2 * tb, k), BF16),
            vm((4, 2, 2, zd, k), F32), vm((4, 2, nk // 2, dm), F32),
            vm((RING, CORES, tb, dm), F32), vm((4, tb, dm), F32), vm((6, tb // 2, dm), F32),
            vm((4, tb, dm), BF16), vm((2, 2, 2 * ur, k), F32), vm((2, dr // 2, dm), F32),
            pltpu.SemaphoreType.DMA((N_SEM,)), pltpu.SemaphoreType.DMA((N_SEM,)), pltpu.SemaphoreType.DMA((N_LOCAL,)),
            pltpu.SemaphoreType.REGULAR((3,)),
        ]
        anyspec = pl.BlockSpec(memory_space=pl.ANY)
        call = pl.pallas_call(
            functools.partial(kernel, (dm, k, tb, ur, dr)),
            out_shape=outs,
            in_specs=[anyspec] * 4,
            out_specs=[anyspec] * len(outs),
            scratch_shapes=scratch,
            compiler_params=pltpu.CompilerParams(collective_id=0, has_side_effects=True, vmem_limit_bytes=67043328),
            name="mlp_stack",
            **({"interpret": interpret} if interpret else {}),
        )
        return tuple(call(x_loc, up_loc, down_loc, g_loc)[:4])

    return jax.shard_map(device_step, mesh=fine, in_specs=(tok_spec, weight_spec, weight_spec, tok_spec),
                         out_specs=(tok_spec, tok_spec, weight_spec, weight_spec), check_vma=False)
```

```python
import functools

import jax
import jax.numpy as jnp
import numpy as np
from jax import lax
from jax.experimental import pallas as pl
from jax.experimental.pallas import tpu as pltpu
from jax.sharding import Mesh, PartitionSpec as P

MESH_ID = pl.DeviceIdType.MESH
ALL = ("x", "z", "y", "c")
F32, BF16 = jnp.float32, jnp.bfloat16
RING, CORES, ARRIVALS = 4, 2, 6
OWN, NXT, OPP, PRV = range(RING)
X0, X1, G1, G0 = range(RING)
HALVES = (0, 1)
N_SEM = 384
N_LOCAL = 116


def gelu_parts(pre_act):
    norm_cdf = 0.5 * (1.0 + lax.erf(pre_act * (2.0 ** -0.5)))
    norm_pdf = jnp.exp(-0.5 * pre_act * pre_act) * ((2.0 * jnp.pi) ** -0.5)
    return pre_act * norm_cdf, norm_cdf + pre_act * norm_pdf


def loop(n, body, init):
    return lax.fori_loop(0, n, body, init)


def dot_nn(left, right):
    return lax.dot_general(left, right, (((1,), (0,)), ((), ())), preferred_element_type=F32)


def dot_nt(left, right):
    return lax.dot_general(left, right, (((1,), (1,)), ((), ())), preferred_element_type=F32)


def dot_tn(left, right):
    return lax.dot_general(left, right, (((0,), (0,)), ((), ())), preferred_element_type=F32)


def kernel(dims, x_in, wu_in, wd_in, g_in,
           y_out, gi_out, gd_out,
           xh0, wuh, wdh, sh0, ah, ra1, rb1, ra2, rb2, uh,
           U, W, XV, GV1, GV0, SV, AV, DV, GPA, GPB, PP, DR, XR, RES, STA, STB,
           ss, rs, ls, credit):
    D, K, TB, UR, DR_ROWS = dims
    HB = TB // 2
    x, z, y, c = (lax.axis_index(a) for a in ALL)
    cp = 1 - c
    S2 = 2 * DR_ROWS
    XD = D // 4
    ZD = D // 16

    def dev(dx=0, dz=0, dy=0, dc=0):
        wrap = lambda v, d, n: v if d == 0 else lax.rem(v + (d % n), n)
        return (wrap(x, dx, 4), wrap(z, dz, 4), wrap(y, dy, 4), wrap(c, dc, 2))

    partner = dev(dc=1)
    rings = {"x": (x, dev(dx=1), dev(dx=-1)), "z": (z, dev(dz=1), dev(dz=-1)), "y": (y, dev(dy=1), dev(dy=-1))}
    off = lambda v, d: v if d == 0 else lax.rem(v + d, 4)

    count = [0]

    def rcopy(src, dst, to):
        k = count[0]
        count[0] += 1
        return pltpu.make_async_remote_copy(src_ref=src, dst_ref=dst, send_sem=ss.at[k], recv_sem=rs.at[k],
                                            device_id=to, device_id_type=MESH_ID)

    lcount = [0]

    def lcopy(src, dst):
        k = lcount[0]
        lcount[0] += 1
        return pltpu.make_async_copy(src, dst, ls.at[k])

    def mo(v, m):
        return pl.multiple_of(v, m)

    class Gather4:
        def __init__(self, axis, src, dst):
            i, right, left = rings[axis]
            lft, rgt = off(i, 3), off(i, 1)
            self.d = [rcopy(src(0), dst(i, 0), right), rcopy(src(1), dst(i, 1), right),
                      rcopy(src(0), dst(i, 0), left), rcopy(src(1), dst(i, 1), left),
                      rcopy(dst(lft, 0), dst(lft, 0), right), rcopy(dst(rgt, 1), dst(rgt, 1), left)]

        def start(self):
            for k in (0, 3, 1, 2):
                self.d[k].start()

        def forward(self):
            self.d[0].wait_recv()
            self.d[4].start()
            self.d[3].wait_recv()
            self.d[5].start()

        def neighbours(self):
            self.d[1].wait_recv()
            self.d[2].wait_recv()

        def opposite(self):
            self.d[4].wait_recv()
            self.d[5].wait_recv()

        def finish(self):
            self.neighbours()
            self.opposite()

        def drain(self):
            for d in self.d:
                d.wait_send()

    class Gather8:
        def __init__(self, src, dst):
            self.ring = Gather4("x", src, lambda b, h: dst(b, c, h))
            lft, rgt, opp = off(x, PRV), off(x, NXT), off(x, OPP)
            blocks = [(lft, 0), (rgt, 1), (lft, 1), (rgt, 0), (opp, 0), (opp, 1)]
            self.own = [rcopy(src(h), dst(x, c, h), partner) for h in HALVES]
            self.push = [rcopy(dst(b, c, h), dst(b, c, h), partner) for b, h in blocks]

        def start(self):
            self.ring.start()
            for d in self.own:
                d.start()

        def forward(self):
            self.ring.forward()
            self.push[0].start()
            self.push[1].start()

        def sides(self):
            self.ring.d[1].wait_recv()
            self.push[2].start()
            self.ring.d[2].wait_recv()
            self.push[3].start()

        def last(self):
            self.ring.d[4].wait_recv()
            self.push[4].start()
            self.ring.d[5].wait_recv()
            self.push[5].start()

        def wait_own(self):
            for d in self.own:
                d.wait_recv()

        def wait_push(self, ks):
            for k in ks:
                self.push[k].wait_recv()

        def drain(self):
            self.ring.drain()
            for d in self.own + self.push:
                d.wait_send()

    def add_rows(dst, srcs, rows, step):
        def body(r, carry):
            sl = pl.ds(mo(r * step, step), step)
            if len(dst.shape) == 3:
                for q in range(dst.shape[0]):
                    acc = dst[q, sl, :]
                    for s in srcs:
                        acc = acc + s[q, sl, :]
                    dst[q, sl, :] = acc
            else:
                acc = dst[sl, :]
                for s in srcs:
                    acc = acc + s[sl, :]
                dst[sl, :] = acc
            return carry
        loop(rows // step, body, None)

    barrier = pltpu.get_barrier_semaphore()
    group = [(dx, dc) for dx in range(RING) for dc in HALVES if dx or dc]
    peers = [dev(dx=dx, dc=dc) for dx, dc in group] + [rings[a][k] for a in "zy" for k in (1, 2)]
    for p in peers:
        pl.semaphore_signal(barrier, inc=1, device_id=p, device_id_type=MESH_ID)

    load_u = [[lcopy(wu_in.at[l, :, pl.ds(b * D, D)], RES.at[G0, pl.ds((l * RING + b) * UR, UR), :])
               for b in range(RING)] for l in HALVES]
    load_d = [lcopy(wd_in.at[l], RES.at[X1, pl.ds(l * DR_ROWS, DR_ROWS), :]) for l in HALVES]
    load_x = lcopy(x_in, RES.at[X0])
    load_g = lcopy(g_in, RES.at[G1])
    own_x = lcopy(x_in, XV.at[x, c])
    own_g = lcopy(g_in, GV1.at[x, c])
    own_d0 = lcopy(wd_in.at[0], W.at[y, z])
    for cpy in load_u[0] + load_u[1] + load_d + [load_x, own_d0, own_x, load_g, own_g]:
        cpy.start()

    low = lax.broadcasted_iota(jnp.int32, (UR, S2), 1) < DR_ROWS
    swap = lambda v: pltpu.roll(v, DR_ROWS, 1)
    for l in HALVES:
        for cpy in load_u[l]:
            cpy.wait()
        for b in range(RING):
            rows = pl.ds((l * RING + b) * UR, UR)
            for yy in range(RING):
                for m in HALVES:
                    s0 = RES[G0, rows, pl.ds((2 * m * RING + yy) * S2, S2)].astype(F32)
                    s1 = RES[G0, rows, pl.ds(((2 * m + 1) * RING + yy) * S2, S2)].astype(F32)
                    cols = pl.ds((yy * 2 + m) * S2, S2)
                    AV[l, 0, pl.ds(2 * b * UR, UR), cols] = jnp.where(low, s0, swap(s1)).astype(BF16)
                    AV[l, 0, pl.ds((2 * b + 1) * UR, UR), cols] = jnp.where(low, swap(s0), s1).astype(BF16)
    for cpy in load_d + [load_x, own_d0]:
        cpy.wait()
    pl.semaphore_wait(barrier, len(peers))

    half = lambda h: pl.ds(h * HB, HB)
    gx0 = Gather8(lambda h: RES.at[X0, half(h)], lambda b, k, h: XV.at[b, k, half(h)])
    gg1 = Gather8(lambda h: RES.at[G1, half(h)], lambda b, k, h: GV1.at[b, k, half(h)])
    up = [U, wuh.at[1]]
    down = [W, wdh.at[1]]
    hr = DR_ROWS // 4

    def down_gathers(l):
        def rows(q, h):
            return pl.ds((2 * q + h) * hr, hr)

        def src(q):
            return lambda h: RES.at[X1, pl.ds(l * DR_ROWS + (2 * q + h) * hr, hr)]
        to = down[l]
        first = [Gather4("z", src(0), lambda b, h: to.at[y, b, rows(0, h)]),
                 Gather4("y", src(1), lambda b, h: to.at[b, z, rows(1, h)])]
        second = [Gather4("y", lambda h: to.at[y, :, rows(0, h)], lambda b, h: to.at[b, :, rows(0, h)]),
                  Gather4("z", lambda h: to.at[:, z, rows(1, h)], lambda b, h: to.at[:, b, rows(1, h)])]
        return first, second

    def up_first(to):
        return [Gather4("y", lambda h: to.at[h, z, y], lambda b, h: to.at[h, z, b]),
                Gather4("z", lambda h: to.at[2 + h, z, y], lambda b, h: to.at[2 + h, b, y])]

    def up_second(to):
        return [Gather4("z", lambda h: to.at[h, z], lambda b, h: to.at[h, b]),
                Gather4("y", lambda h: to.at[2 + h, :, y], lambda b, h: to.at[2 + h, :, b])]

    def up_unit(to, j):
        yj, zj = off(y, j), off(z, j)
        return [Gather4("z", lambda h: to.at[h, z, yj], lambda b, h: to.at[h, b, yj]),
                Gather4("y", lambda h: to.at[2 + h, zj, y], lambda b, h: to.at[2 + h, zj, b])]

    def do(gathers, step):
        for g in gathers:
            getattr(g, step)()

    mine = pl.ds(mo(c * UR, UR), UR)

    def up_exchange(l):
        sends = []
        for dx, dc in group:
            tx, tc = off(x, dx), (cp if dc else c)
            src = AV.at[l, 0, pl.ds(mo((tx * 2 + tc) * UR, UR), UR), :]
            sends.append(rcopy(src, up[l].at[x, z, y, mine, :], dev(dx=dx, dc=dc)))
        for cpy in sends:
            cpy.start()
        return sends

    (d0a, d0b), (d1a, d1b) = down_gathers(0), down_gathers(1)
    u0a, u1a, u1b = up_first(up[0]), up_first(up[1]), up_second(up[1])
    u0u = [up_unit(up[0], j) for j in (OWN, PRV, NXT, OPP)]
    ex0 = up_exchange(0)
    do(d0a, "start")
    gx0.start()
    ex1 = up_exchange(1)
    my_rows = pl.ds(mo((x * 2 + c) * UR, UR), UR)
    own_u1 = lcopy(AV.at[1, 0, my_rows, :], up[1].at[x, z, y, mine, :])
    own_u1.start()
    own_d1 = lcopy(RES.at[X1, pl.ds(DR_ROWS, DR_ROWS), :], down[1].at[y, z])
    own_d1.start()
    U[x, z, y, mine, :] = AV[0, 0, my_rows, :]
    do(d0a, "forward")
    for cpy in ex0:
        cpy.wait_recv()
    do(u0a, "start")
    do(u0u[0], "start")
    do(d0a, "finish")
    do(u0a, "forward")
    do(u0a, "neighbours")
    do(u0u[1], "start")
    do(u0u[2], "start")
    do(u0u[0], "forward")
    do(u0a, "opposite")
    do(u0u[3], "start")
    do(u0u[1], "forward")
    do(u0u[2], "forward")
    gx0.forward()
    do(u0u[3], "forward")
    do(d0b, "start")
    gx0.sides()
    gx0.last()
    load_g.wait()
    gg1.start()
    gx0.wait_own()
    gx0.wait_push(range(len(gx0.push)))
    own_x.wait()
    save_x = lcopy(XV, xh0)
    save_x.start()
    for cpy in ex0 + ex1:
        cpy.wait_send()
    for unit in u0u:
        do(unit, "finish")
    save_u0 = lcopy(U, wuh.at[0])
    save_u0.start()

    T2 = 2 * TB
    ND = D // 4
    NK = K // 4

    def up_tile(t, n):
        cols = pl.ds(mo(n * NK, NK), NK)
        return dot_nn(XV[t].reshape(T2, D), U[:, :, :, :, cols].reshape(D, NK)), cols

    def hidden0(t):
        def body(n, carry):
            pre, cols = up_tile(t, n)
            act, slope = gelu_parts(pre)
            AV[t, :, :, cols] = act.astype(BF16).reshape(2, TB, NK)
            SV[t, :, :, cols] = slope.reshape(2, TB, NK)
            return carry
        loop(K // NK, body, None)

    def hidden1(t):
        def body(n, carry):
            pre, cols = up_tile(t, n)
            act, slope = gelu_parts(pre)
            AV[t, :, :, cols] = act.astype(BF16).reshape(2, TB, NK)
            DV[t, :, cols] = (SV[t, :, :, cols].reshape(T2, NK) * slope).astype(BF16)
            return carry
        loop(K // NK, body, None)

    def dact(gv, t, n):
        return dot_nt(gv[t].reshape(T2, D), W[n].reshape(NK, D))

    def dact1(t):
        def body(n, carry):
            SV[t, :, :, pl.ds(mo(n * NK, NK), NK)] = dact(GV1, t, n).reshape(2, TB, NK)
            return carry
        loop(RING, body, None)

    def dact0(t):
        def body(n, carry):
            cols = pl.ds(mo(n * NK, NK), NK)
            DV[t, :, cols] = (dact(GV0, t, n) * SV[t, :, :, cols].reshape(T2, NK)).astype(BF16)
            return carry
        loop(RING, body, None)

    def down_part(act, j):
        t = off(x, j)

        def body(n, carry):
            cols = pl.ds(mo(n * ND, ND), ND)
            PP[j, :, :, cols] = dot_nn(act[t, :, :, 0:K].reshape(T2, K), W[:, :, :, cols].reshape(K, ND)).reshape(2, TB, ND)
            return carry
        loop(RING, body, None)

    def dx_part(j):
        t = off(x, j)

        def body(n, carry):
            cols = pl.ds(mo(n * ND, ND), ND)
            PP[j, :, :, cols] = dot_nt(DV[t], U[n].reshape(ND, K)).reshape(2, TB, ND)
            return carry
        loop(RING, body, None)

    class Reduce8:
        def __init__(self, part, index, chunks=1):
            self.part, self.index, self.chunks = part, index, chunks
            _, right, left = rings["x"]
            self.right, self.left = right, left
            self.qb = HB // chunks
            self.pair = [rcopy(PP.at[j, cp], DR.at[j], partner) for j in range(RING)]

            def messages(q):
                src = lambda j, h: PP.at[j, c, self.rows(q, h)]
                dst = lambda k: XR.at[k, pl.ds(q * self.qb, self.qb)]
                return [rcopy(src(OPP, 0), dst(0), right), rcopy(src(OPP, 1), dst(1), left),
                        rcopy(src(NXT, 1), dst(2), right), rcopy(src(PRV, 0), dst(3), left),
                        rcopy(src(NXT, 0), dst(4), right), rcopy(src(PRV, 1), dst(5), left)]
            self.m = [messages(q) for q in range(chunks)]

        def rows(self, q, h):
            return pl.ds((2 * q + h) * self.qb, self.qb)

        def credits(self):
            if self.index:
                for k in range(len((self.right, self.left, partner))):
                    pl.semaphore_wait(credit.at[k], 1)

        def compute(self, j):
            self.part(j)
            self.pair[j].start()

        def combine(self, j):
            self.pair[j].wait_recv()
            add_rows(PP.at[j, c], [DR.at[j]], TB, min(TB, 16))

        def opposite(self, q):
            self.m[q][0].start()
            self.m[q][1].start()

        def sides(self, q):
            self.m[q][2].start()
            self.m[q][3].start()

        def relay(self, q):
            for k, j, h in ((0, NXT, 0), (1, PRV, 1)):
                self.m[q][k].wait_recv()
                add_rows(PP.at[j, c, self.rows(q, h)], [XR.at[k, pl.ds(q * self.qb, self.qb)]], self.qb, min(self.qb, 16))
                self.m[q][4 + k].start()

        def finish(self, q, res, outs):
            for d in self.m[q][2:]:
                d.wait_recv()
            step = min(self.qb, 16)
            for h, (kl, kr) in enumerate(((4, 3), (2, 5))):
                def body(r, carry):
                    lo = pl.ds(mo(q * self.qb + r * step, step), step)
                    sl = pl.ds(mo((2 * q + h) * self.qb + r * step, step), step)
                    tot = PP[OWN, c, sl, :] + (XR[kl, lo, :] + XR[kr, lo, :])
                    val = (res[sl, :].astype(F32) + tot).astype(BF16)
                    for o in outs:
                        o[sl, :] = val
                    return carry
                loop(self.qb // step, body, None)

        def release(self):
            for d in self.pair + sum(self.m, []):
                d.wait_send()
            for k, to in enumerate((self.right, self.left, partner)):
                pl.semaphore_signal(credit.at[k], inc=1, device_id=to, device_id_type=MESH_ID)

        def drain(self):
            for d in self.pair + sum(self.m, []):
                d.wait_send()

        def launch(self):
            self.credits()
            self.compute(OPP)
            self.compute(NXT)
            self.combine(OPP)
            self.opposite(0)
            self.compute(PRV)
            self.combine(NXT)
            self.combine(PRV)
            self.sides(0)

    def grad_a(j, dst):
        t = off(z, j)
        for h in HALVES:
            lo = [pl.ds(mo((2 * h + q) * XD + t * ZD, ZD), ZD) for q in HALVES]
            lhs = jnp.concatenate([XV[:, :, :, s].reshape(8 * TB, ZD) for s in lo], axis=1)

            def body(n, carry):
                cols = pl.ds(mo(n * NK, NK), NK)
                dst[h, :, :, cols] = dot_tn(lhs, DV[:, :, cols].reshape(8 * TB, NK)).reshape(2, ZD, NK)
                return carry
            loop(K // NK, body, None)

    def grad_b(gv, j, dst):
        cols_l = pl.ds(mo(off(y, j) * NK, NK), NK)
        for n in HALVES:
            def body(m, carry):
                cols = pl.ds(mo(n * K + m * ND, ND), ND)
                out = dot_tn(AV[:, :, :, cols_l].reshape(8 * TB, NK), gv[:, :, :, cols].reshape(8 * TB, ND))
                dst[:, n, :, pl.ds(mo(m * ND, ND), ND)] = out.reshape(2, NK // 2, ND)
                return carry
            loop(2, body, None)

    class Reduce4:
        def __init__(self, axis, part, recv, stage):
            _, right, left = rings[axis]
            self.part, self.recv, self.stage = part, recv, stage
            self.m = [rcopy(part(OPP, 0), recv(0), right), rcopy(part(OPP, 1), recv(1), left),
                      rcopy(part(NXT, 1), recv(2), right), rcopy(part(PRV, 0), recv(3), left),
                      rcopy(part(NXT, 0), recv(4), right), rcopy(part(PRV, 1), recv(5), left)]
            self.to = [(NXT, 0), (PRV, 1), (OWN, 1), (OWN, 0), (OWN, 0), (OWN, 1)]
            self.loads = [lcopy(recv(k), stage(k)) for k in range(ARRIVALS)]

        def opposite(self):
            self.m[0].start()
            self.m[1].start()

        def sides(self, j):
            self.m[2 if j == NXT else 3].start()

        def fetch(self, k):
            self.m[k].wait_send()
            self.m[k].wait_recv()
            self.loads[k].start()

        def absorb(self, k):
            self.loads[k].wait()
            dst = self.part(*self.to[k])
            add_rows(dst, [self.stage(k)], dst.shape[1], min(dst.shape[1], 16))

    def arrive(reduces, ks):
        for k in ks:
            for r in reduces:
                r.fetch(k)
        for k in ks:
            for r in reduces:
                r.absorb(k)

    def relay(reduces):
        for k in (0, 1):
            for r in reduces:
                r.fetch(k)
        for k in (0, 1):
            for r in reduces:
                r.absorb(k)
                r.m[4 + k].start()

    EARLY, LATE = (2, 3), (4, 5)
    hq = DR_ROWS // 2
    own_grads = [(SV.at[pl.ds(0, 2)], SV.at[pl.ds(2, 2)]), (GPA.at[OWN], GPB.at[OWN])]

    def make_reduce(l, q, chunks):
        own_a, own_b = own_grads[l]
        ca = pl.ds(q * (K // chunks), K // chunks)
        nb = pl.ds(q, 1) if chunks == 2 else pl.ds(0, 2)
        pick = ((OPP, 0), (OPP, 1), (NXT, 1), (PRV, 0), (NXT, 0), (PRV, 1))

        def part_a(j, h):
            return (own_a.at[h, :, :, ca] if j == OWN else GPA.at[j, h, :, :, ca])

        def part_b(j, h):
            return (own_b.at[h, nb] if j == OWN else GPB.at[j, h, nb])

        def part_a2(j, h):
            return own_a.at[h, :, pl.ds(mo(off(y, j) * 2 * UR, 2 * UR), 2 * UR), ca]

        def part_b2(j, h):
            t = off(z, j)
            return own_b.at[t // 2, nb, pl.ds(mo(lax.rem(t, 2) * DR_ROWS + h * hq, hq), hq), :]
        return (Reduce4("z", part_a, lambda k: ra1.at[l, k, :, :, ca], lambda k: part_a(*pick[k])),
                Reduce4("y", part_b, lambda k: rb1.at[l, k, nb], lambda k: part_b(*pick[k])),
                Reduce4("y", part_a2, lambda k: ra2.at[l, k, :, :, ca], lambda k: STA.at[k % 2, :, :, ca]),
                Reduce4("z", part_b2, lambda k: rb2.at[l, k, nb], lambda k: STB.at[k % 2, nb]))

    def second_start(reduces):
        for r in reduces:
            r.opposite()
            r.sides(NXT)
            r.sides(PRV)

    def grads_out_start(l, q, chunks):
        own_a, own_b = own_grads[l]
        ca = pl.ds(q * (K // chunks), K // chunks)

        def rows_of(tx, tc):
            return own_a.at[tx // 2, lax.rem(tx, 2), pl.ds(mo((2 * y + tc) * UR, UR), UR), ca]
        to = uh.at[l, x, mine, ca]
        sends = [rcopy(rows_of(off(x, dx), cp if dc else c), to, dev(dx=dx, dc=dc)) for dx, dc in group]
        local = [lcopy(rows_of(x, c), to)]
        for n in ((q,) if chunks == 2 else HALVES):
            local.append(lcopy(own_b.at[z // 2, n, pl.ds(mo(lax.rem(z, 2) * DR_ROWS, DR_ROWS), DR_ROWS), :],
                               gd_out.at[l, :, pl.ds(n * K, K)]))
        for cpy in sends + local:
            cpy.start()
        return sends, local

    def grads_out_finish(state):
        for cpy in state[0]:
            cpy.wait_recv()
            cpy.wait_send()
        for cpy in state[1]:
            cpy.wait()

    hidden0(0)
    do(d0b, "forward")
    do(d1a, "start")
    for cpy in ex1:
        cpy.wait_recv()
    own_u1.wait()
    own_d1.wait()
    do(u1a, "start")
    hidden0(1)
    hidden0(2)
    gg1.forward()
    hidden0(3)
    save_s = lcopy(SV, sh0)
    save_s.start()
    save_a0 = lcopy(AV, ah.at[0])
    save_a0.start()
    gg1.sides()
    do(d0b, "finish")
    save_d0 = lcopy(W, wdh.at[0])
    save_d0.start()
    save_x.wait()
    gx0.drain()
    do(d0a, "drain")

    r = Reduce8(functools.partial(down_part, AV), 0, 2)
    r.compute(OPP)
    do(d1a, "forward")
    r.compute(NXT)
    r.combine(OPP)
    r.opposite(0)
    r.compute(PRV)
    r.combine(NXT)
    r.combine(PRV)
    r.sides(0)
    do(u1a, "forward")
    gg1.last()
    do(d1a, "finish")
    do(d1b, "start")
    r.compute(OWN)
    do(u1a, "finish")
    r.relay(0)
    r.opposite(1)
    r.sides(1)
    r.combine(OWN)
    do(d1b, "forward")
    do(u1b, "start")

    def token_gathers(slot, buf):
        rows = lambda q, h: pl.ds((2 * q + h) * r.qb, r.qb)
        make = lambda q: Gather8(lambda h: RES.at[slot, rows(q, h)], lambda b, k, h: buf.at[b, k, rows(q, h)])
        return [make(0), make(1)]

    gx1 = token_gathers(X1, XV)
    r.relay(1)
    do(d1a, "drain")
    r.finish(0, RES.at[X0], [RES.at[X1], XV.at[x, c]])
    gx1[0].start()
    gg1.wait_own()
    gg1.wait_push(range(len(gg1.push)))
    own_g.wait()
    save_d0.wait()
    do(d0b, "drain")
    do(d1b, "finish")
    load_w1d = lcopy(wdh.at[1], W)
    load_w1d.start()
    do(u1b, "forward")
    r.finish(1, RES.at[X0], [RES.at[X1], XV.at[x, c]])
    gx1[1].start()
    save_s.wait()
    load_w1d.wait()
    dact1(off(x, OWN))
    gx1[0].forward()
    dact1(off(x, NXT))
    gx1[0].sides()
    r.release()
    dact1(off(x, PRV))
    gx1[1].forward()
    gx1[0].last()
    dact1(off(x, OPP))
    load_w0d_again = lcopy(wdh.at[0], W)
    load_w0d_again.start()
    gx1[1].sides()
    save_u0.wait()
    do(sum(u0u, u0a), "drain")
    do(u1b, "finish")
    load_w1u = lcopy(wuh.at[1], U)
    load_w1u.start()
    load_w1u.wait()
    save_a0.wait()
    do(gx1, "wait_own")
    hidden1(off(x, OWN))
    gx1[1].last()
    for g in gx1:
        g.wait_push((0, 2))
    hidden1(off(x, PRV))
    for g in gx1:
        g.wait_push((1, 3))
    hidden1(off(x, NXT))
    for g in gx1:
        g.wait_push((4, 5))
    hidden1(off(x, OPP))
    load_s0 = lcopy(sh0, SV)
    load_s0.start()
    save_a1 = lcopy(AV, ah.at[1])
    save_a1.start()

    a1, b1, a2, b2 = make_reduce(1, 0, 1)
    grad_b(GV1, OPP, GPB.at[OPP])
    b1.opposite()
    grad_a(OPP, GPA.at[OPP])
    a1.opposite()
    r = Reduce8(dx_part, 1, 2)
    r.launch()
    grad_b(GV1, NXT, GPB.at[NXT])
    b1.sides(NXT)
    grad_b(GV1, PRV, GPB.at[PRV])
    b1.sides(PRV)
    r.relay(0)
    r.opposite(1)
    r.sides(1)
    r.compute(OWN)
    load_w0u_again = lcopy(wuh.at[0], U)
    load_w0u_again.start()
    grad_a(NXT, GPA.at[NXT])
    a1.sides(NXT)
    grad_a(PRV, GPA.at[PRV])
    a1.sides(PRV)
    r.combine(OWN)
    gg0 = token_gathers(G0, GV0)
    r.relay(1)
    r.finish(0, RES.at[G1], [RES.at[G0], GV0.at[x, c]])
    gg0[0].start()
    grad_b(GV1, OWN, GPB.at[OWN])
    save_a1.wait()
    load_a0 = lcopy(ah.at[0], AV)
    load_a0.start()
    gg1.drain()
    load_a1 = lcopy(ah.at[1], GV1.at[:, :, :, 0:K])
    load_a1.start()
    r.finish(1, RES.at[G1], [RES.at[G0], GV0.at[x, c]])
    gg0[1].start()
    gg0[0].forward()
    grad_a(OWN, GPA.at[OWN])
    do(gx1, "drain")
    load_x0 = lcopy(xh0, XV)
    load_x0.start()
    gg0[0].sides()
    relay((b1, a1))
    r.release()
    gg0[1].forward()
    gg0[0].last()
    load_w0d_again.wait()
    load_s0.wait()
    do(gg0, "wait_own")
    dact0(off(x, OWN))
    gg0[1].sides()
    gg0[1].last()
    for g in gg0:
        g.wait_push((0, 2))
    dact0(off(x, PRV))
    for g in gg0:
        g.wait_push((1, 3))
    dact0(off(x, NXT))
    for g in gg0:
        g.wait_push((4, 5))

    a1n, b1n, a2n, b2n = zip(*[make_reduce(0, q, 2) for q in HALVES])
    load_a0.wait()
    grad_b(GV0, OPP, GPB.at[OPP])
    b1n[0].opposite()
    dact0(off(x, OPP))
    load_w1d_again = lcopy(wdh.at[1], W)
    load_w1d_again.start()
    load_x0.wait()
    grad_a(OPP, GPA.at[OPP])
    a1n[0].opposite()
    load_w0u_again.wait()
    r = Reduce8(dx_part, 2)
    r.launch()
    arrive((b1, a1), EARLY + LATE)
    second_start((a2, b2))
    grad_b(GV0, NXT, GPB.at[NXT])
    b1n[0].sides(NXT)
    grad_b(GV0, PRV, GPB.at[PRV])
    b1n[0].sides(PRV)
    grad_a(NXT, GPA.at[NXT])
    a1n[0].sides(NXT)
    grad_a(PRV, GPA.at[PRV])
    a1n[0].sides(PRV)
    relay((b2, a2))
    r.relay(0)
    relay((b1n[0], a1n[0]))
    for red in (b1n[1], a1n[1]):
        red.opposite()
        red.sides(NXT)
        red.sides(PRV)
    r.compute(OWN)
    r.combine(OWN)
    grad_b(GV0, OWN, own_grads[0][1])
    grad_a(OWN, own_grads[0][0])
    r.finish(0, RES.at[G0], [RES.at[X0]])
    r.release()
    write_gi = lcopy(RES.at[X0], gi_out)
    write_gi.start()
    arrive((b1n[0], a1n[0]), EARLY)
    load_a1.wait()
    load_w1d_again.wait()
    r = Reduce8(functools.partial(down_part, GV1), 3)
    r.launch()
    r.compute(OWN)
    arrive((b2, a2), EARLY)
    arrive((b2, a2), LATE)
    state1 = grads_out_start(1, 0, 1)
    r.combine(OWN)
    arrive((b1n[0], a1n[0]), LATE)
    r.relay(0)
    relay((b1n[1], a1n[1]))
    second_start((a2n[0], b2n[0]))
    arrive((b1n[1], a1n[1]), EARLY)
    relay((b2n[0], a2n[0]))
    arrive((b1n[1], a1n[1]), LATE)
    second_start((a2n[1], b2n[1]))
    arrive((b2n[0], a2n[0]), EARLY)
    arrive((b2n[0], a2n[0]), LATE)
    state0 = [grads_out_start(0, 0, 2)]
    relay((b2n[1], a2n[1]))
    r.finish(0, RES.at[X1], [RES.at[G1]])
    write_y = lcopy(RES.at[G1], y_out)
    write_y.start()
    grads_out_finish(state1)
    arrive((b2n[1], a2n[1]), EARLY)
    arrive((b2n[1], a2n[1]), LATE)
    state0.append(grads_out_start(0, 1, 2))
    r.drain()
    do(d1b + u1a + u1b + gg0, "drain")
    write_gi.wait()
    write_y.wait()
    for state in state0:
        grads_out_finish(state)
    assert count[0] <= N_SEM and lcount[0] <= N_LOCAL


def finish_kernel(y_in, gi_in, gu_in, gd_in, y_out, gi_out, gu_out, gd_out, ybuf, gibuf, gubuf, gdbuf, gushuf, sems):
    layers, ur, ff = gu_out.shape
    s2 = ff // 64
    half = s2 // 2
    loads = [pltpu.make_async_copy(a, b, sems.at[0, k])
             for k, (a, b) in enumerate(((gu_in, gubuf), (gd_in, gdbuf), (y_in, ybuf), (gi_in, gibuf)))]
    stores = [pltpu.make_async_copy(a, b, sems.at[1, k])
              for k, (a, b) in enumerate(((gushuf, gu_out), (gdbuf, gd_out), (ybuf, y_out), (gibuf, gi_out)))]
    for cpy in loads:
        cpy.start()
    low = lax.broadcasted_iota(jnp.int32, (ur, s2), 1) < half
    swap = lambda v: pltpu.roll(v, half, 1)
    for k in (1, 2, 3):
        loads[k].wait()
        stores[k].start()
    loads[0].wait()
    for l in range(layers):
        for b in range(RING):
            for yy in range(RING):
                for m in HALVES:
                    cols = pl.ds((yy * 2 + m) * s2, s2)
                    t0, t1 = (gubuf[l, b, pl.ds(k * ur, ur), cols] for k in HALVES)
                    strip = (b * RING + 2 * m) * RING + yy
                    gushuf[l, :, pl.ds(strip * s2, s2)] = jnp.where(low, t0, swap(t1))
                    gushuf[l, :, pl.ds((strip + RING) * s2, s2)] = jnp.where(low, swap(t0), t1)
    stores[0].start()
    for cpy in stores:
        cpy.wait()


def solution(mesh, interpret=None):
    fine = Mesh(np.asarray(mesh.devices).reshape(4, 4, 4, 2), ALL)
    tok_spec = P(ALL, None)
    weight_spec = P(None, ALL, None)

    def device_step(x_loc, up_loc, down_loc, g_loc):
        layers, ur, ff = up_loc.shape
        dr, dm = down_loc.shape[1:]
        tb = x_loc.shape[0]
        k = ff // 8
        zd = dm // 16
        hbm = lambda shape, dt: jax.ShapeDtypeStruct(shape, dt)
        outs = [
            hbm((tb, dm), BF16), hbm((tb, dm), BF16), hbm((layers, dr, dm), F32),
            hbm((RING, CORES, tb, dm), BF16),
            hbm((layers, RING, RING, RING, 2 * ur, k), BF16),
            hbm((layers, RING, RING, dr, dm), BF16),
            hbm((RING, CORES, tb, k), F32), hbm((layers, RING, CORES, tb, k), BF16),
            *[hbm((layers, ARRIVALS, CORES, n, k), F32) for n in (zd, zd, 2 * ur, 2 * ur)],
            hbm((layers, RING, 2 * ur, k), F32),
        ]
        vm = pltpu.VMEM
        scratch = [
            vm((RING, RING, RING, 2 * ur, k), BF16), vm((RING, RING, dr, dm), BF16),
            vm((RING, CORES, tb, dm), BF16), vm((RING, CORES, tb, dm), BF16), vm((RING, CORES, tb, dm), BF16),
            vm((RING, CORES, tb, k), F32), vm((RING, CORES, tb, k), BF16), vm((RING, 2 * tb, k), BF16),
            vm((RING, CORES, CORES, zd, k), F32), vm((RING, CORES, CORES, zd, k), F32),
            vm((RING, CORES, tb, dm), F32), vm((4, tb, dm), F32), vm((6, tb // 2, dm), F32),
            vm((4, tb, dm), BF16), vm((CORES, CORES, 2 * ur, k), F32), vm((CORES, CORES, 2 * ur, k), F32),
            pltpu.SemaphoreType.DMA((N_SEM,)), pltpu.SemaphoreType.DMA((N_SEM,)), pltpu.SemaphoreType.DMA((N_LOCAL,)),
            pltpu.SemaphoreType.REGULAR((3,)),
        ]
        anyspec = pl.BlockSpec(memory_space=pl.ANY)
        call = pl.pallas_call(
            functools.partial(kernel, (dm, k, tb, ur, dr)),
            out_shape=outs,
            in_specs=[anyspec] * 4,
            out_specs=[anyspec] * len(outs),
            scratch_shapes=scratch,
            compiler_params=pltpu.CompilerParams(collective_id=0, has_side_effects=True, vmem_limit_bytes=67043328),
            name="mlp_stack",
            **({"interpret": interpret} if interpret else {}),
        )
        y_raw, gi_raw, gd_raw, *_, gu_raw = call(x_loc, up_loc, down_loc, g_loc)
        raws = (y_raw, gi_raw, gu_raw, gd_raw)
        outs = [hbm((tb, dm), BF16), hbm((tb, dm), BF16), hbm((layers, ur, ff), F32), hbm((layers, dr, dm), F32)]
        return tuple(pl.pallas_call(
            finish_kernel, out_shape=outs, in_specs=[anyspec] * len(outs), out_specs=[anyspec] * len(outs),
            scratch_shapes=[vm(v.shape, v.dtype) for v in raws] + [vm(outs[2].shape, F32), pltpu.SemaphoreType.DMA((2, len(outs)))],
            name="write_out")(*raws))

    return jax.shard_map(device_step, mesh=fine, in_specs=(tok_spec, weight_spec, weight_spec, tok_spec),
                         out_specs=(tok_spec, tok_spec, weight_spec, weight_spec), check_vma=False)
```

```python
import functools

import jax
import jax.numpy as jnp
import numpy as np
from jax import lax
from jax.experimental import pallas as pl
from jax.experimental.pallas import tpu as pltpu
from jax.sharding import Mesh, PartitionSpec as P

MESH_ID = pl.DeviceIdType.MESH
ALL = ("x", "z", "y", "c")
F32, BF16 = jnp.float32, jnp.bfloat16
RING, CORES, ARRIVALS = 4, 2, 6
OWN, NXT, OPP, PRV = range(RING)
X0, X1, G1, G0 = range(RING)
HALVES = (0, 1)
WHOLE, SPLIT2, SPLIT3 = (4,), (2, 2), (1, 1, 2)
N_SEM = 440
N_LOCAL = 120


def gelu_parts(pre_act):
    norm_cdf = 0.5 * (1.0 + lax.erf(pre_act * (2.0 ** -0.5)))
    norm_pdf = jnp.exp(-0.5 * pre_act * pre_act) * ((2.0 * jnp.pi) ** -0.5)
    return pre_act * norm_cdf, norm_cdf + pre_act * norm_pdf


def loop(n, body, init):
    return lax.fori_loop(0, n, body, init)


def dot_nn(left, right):
    return lax.dot_general(left, right, (((1,), (0,)), ((), ())), preferred_element_type=F32)


def dot_nt(left, right):
    return lax.dot_general(left, right, (((1,), (1,)), ((), ())), preferred_element_type=F32)


def dot_tn(left, right):
    return lax.dot_general(left, right, (((0,), (0,)), ((), ())), preferred_element_type=F32)


def kernel(dims, x_in, wu_in, wd_in, g_in,
           y_out, gi_out, gd_out,
           xh0, wuh, wdh, sh0, ah, ra1, rb1, ra2, rb2, uh,
           U, W, XV, GV1, GV0, SV, AV, DV, GPA, GPB, PP, DR, XR, RES, STA, STB,
           ss, rs, ls, credit):
    D, K, TB, UR, DR_ROWS = dims
    HB = TB // 2
    x, z, y, c = (lax.axis_index(a) for a in ALL)
    cp = 1 - c
    S2 = 2 * DR_ROWS
    XD = D // 4
    ZD = D // 16

    def dev(dx=0, dz=0, dy=0, dc=0):
        wrap = lambda v, d, n: v if d == 0 else lax.rem(v + (d % n), n)
        return (wrap(x, dx, 4), wrap(z, dz, 4), wrap(y, dy, 4), wrap(c, dc, 2))

    partner = dev(dc=1)
    rings = {"x": (x, dev(dx=1), dev(dx=-1)), "z": (z, dev(dz=1), dev(dz=-1)), "y": (y, dev(dy=1), dev(dy=-1))}
    off = lambda v, d: v if d == 0 else lax.rem(v + d, 4)

    count = [0]

    def rcopy(src, dst, to):
        k = count[0]
        count[0] += 1
        return pltpu.make_async_remote_copy(src_ref=src, dst_ref=dst, send_sem=ss.at[k], recv_sem=rs.at[k],
                                            device_id=to, device_id_type=MESH_ID)

    lcount = [0]

    def lcopy(src, dst):
        k = lcount[0]
        lcount[0] += 1
        return pltpu.make_async_copy(src, dst, ls.at[k])

    def mo(v, m):
        return pl.multiple_of(v, m)

    class Gather4:
        def __init__(self, axis, src, dst):
            i, right, left = rings[axis]
            lft, rgt = off(i, 3), off(i, 1)
            self.d = [rcopy(src(0), dst(i, 0), right), rcopy(src(1), dst(i, 1), right),
                      rcopy(src(0), dst(i, 0), left), rcopy(src(1), dst(i, 1), left),
                      rcopy(dst(lft, 0), dst(lft, 0), right), rcopy(dst(rgt, 1), dst(rgt, 1), left)]

        def start(self):
            for k in (0, 3, 1, 2):
                self.d[k].start()

        def forward(self):
            self.d[0].wait_recv()
            self.d[4].start()
            self.d[3].wait_recv()
            self.d[5].start()

        def neighbours(self):
            self.d[1].wait_recv()
            self.d[2].wait_recv()

        def opposite(self):
            self.d[4].wait_recv()
            self.d[5].wait_recv()

        def finish(self):
            self.neighbours()
            self.opposite()

        def drain(self):
            for d in self.d:
                d.wait_send()

    class Gather8:
        def __init__(self, src, dst):
            self.ring = Gather4("x", src, lambda b, h: dst(b, c, h))
            lft, rgt, opp = off(x, PRV), off(x, NXT), off(x, OPP)
            blocks = [(lft, 0), (rgt, 1), (lft, 1), (rgt, 0), (opp, 0), (opp, 1)]
            self.own = [rcopy(src(h), dst(x, c, h), partner) for h in HALVES]
            self.push = [rcopy(dst(b, c, h), dst(b, c, h), partner) for b, h in blocks]

        def start(self):
            self.ring.start()
            for d in self.own:
                d.start()

        def forward(self):
            self.ring.forward()
            self.push[0].start()
            self.push[1].start()

        def sides(self):
            self.ring.d[1].wait_recv()
            self.push[2].start()
            self.ring.d[2].wait_recv()
            self.push[3].start()

        def last(self):
            self.ring.d[4].wait_recv()
            self.push[4].start()
            self.ring.d[5].wait_recv()
            self.push[5].start()

        def wait_own(self):
            for d in self.own:
                d.wait_recv()

        def wait_push(self, ks):
            for k in ks:
                self.push[k].wait_recv()

        def drain(self):
            self.ring.drain()
            for d in self.own + self.push:
                d.wait_send()

    def add_rows(dst, srcs, rows, step):
        def body(r, carry):
            sl = pl.ds(mo(r * step, step), step)
            if len(dst.shape) == 3:
                for q in range(dst.shape[0]):
                    acc = dst[q, sl, :]
                    for s in srcs:
                        acc = acc + s[q, sl, :]
                    dst[q, sl, :] = acc
            else:
                acc = dst[sl, :]
                for s in srcs:
                    acc = acc + s[sl, :]
                dst[sl, :] = acc
            return carry
        loop(rows // step, body, None)

    barrier = pltpu.get_barrier_semaphore()
    group = [(dx, dc) for dx in range(RING) for dc in HALVES if dx or dc]
    peers = [dev(dx=dx, dc=dc) for dx, dc in group] + [rings[a][k] for a in "zy" for k in (1, 2)]
    for p in peers:
        pl.semaphore_signal(barrier, inc=1, device_id=p, device_id_type=MESH_ID)

    load_u = [[lcopy(wu_in.at[l, :, pl.ds(b * D, D)], RES.at[G0, pl.ds((l * RING + b) * UR, UR), :])
               for b in range(RING)] for l in HALVES]
    load_d = [lcopy(wd_in.at[l], RES.at[X1, pl.ds(l * DR_ROWS, DR_ROWS), :]) for l in HALVES]
    load_x = lcopy(x_in, RES.at[X0])
    load_g = lcopy(g_in, RES.at[G1])
    own_x = lcopy(x_in, XV.at[x, c])
    own_g = lcopy(g_in, GV1.at[x, c])
    own_d0 = lcopy(wd_in.at[0], W.at[y, z])
    for cpy in load_u[0] + load_u[1] + load_d + [load_x, own_d0, own_x, load_g, own_g]:
        cpy.start()

    low = lax.broadcasted_iota(jnp.int32, (UR, S2), 1) < DR_ROWS
    swap = lambda v: pltpu.roll(v, DR_ROWS, 1)
    for l in HALVES:
        for cpy in load_u[l]:
            cpy.wait()
        for b in range(RING):
            rows = pl.ds((l * RING + b) * UR, UR)
            for yy in range(RING):
                for m in HALVES:
                    s0 = RES[G0, rows, pl.ds((2 * m * RING + yy) * S2, S2)].astype(F32)
                    s1 = RES[G0, rows, pl.ds(((2 * m + 1) * RING + yy) * S2, S2)].astype(F32)
                    cols = pl.ds((yy * 2 + m) * S2, S2)
                    AV[l, 0, pl.ds(2 * b * UR, UR), cols] = jnp.where(low, s0, swap(s1)).astype(BF16)
                    AV[l, 0, pl.ds((2 * b + 1) * UR, UR), cols] = jnp.where(low, swap(s0), s1).astype(BF16)
    for cpy in load_d + [load_x, own_d0]:
        cpy.wait()
    pl.semaphore_wait(barrier, len(peers))

    half = lambda h: pl.ds(h * HB, HB)

    def tile_cols(split, q):
        return pl.ds(sum(split[:q]) * (D // RING), split[q] * (D // RING))

    gx0 = Gather8(lambda h: RES.at[X0, half(h)], lambda b, k, h: XV.at[b, k, half(h)])
    gg1 = Gather8(lambda h: RES.at[G1, half(h)], lambda b, k, h: GV1.at[b, k, half(h)])
    up = [U, wuh.at[1]]
    down = [W, wdh.at[1]]
    hr = DR_ROWS // 4

    def down_gathers(l, split):
        def rows(q, h):
            return pl.ds((2 * q + h) * hr, hr)

        def src(q):
            return lambda h: RES.at[X1, pl.ds(l * DR_ROWS + (2 * q + h) * hr, hr)]
        to = down[l]

        def second(n):
            cs = tile_cols(split, n)
            return [Gather4("y", lambda h: to.at[y, :, rows(0, h), cs], lambda b, h: to.at[b, :, rows(0, h), cs]),
                    Gather4("z", lambda h: to.at[:, z, rows(1, h), cs], lambda b, h: to.at[:, b, rows(1, h), cs])]
        first = [Gather4("z", src(0), lambda b, h: to.at[y, b, rows(0, h)]),
                 Gather4("y", src(1), lambda b, h: to.at[b, z, rows(1, h)])]
        return [first] + [second(n) for n in range(len(split))]

    def up_first(to):
        return [Gather4("y", lambda h: to.at[h, z, y], lambda b, h: to.at[h, z, b]),
                Gather4("z", lambda h: to.at[2 + h, z, y], lambda b, h: to.at[2 + h, b, y])]

    def up_second(to, n):
        cs = pl.ds(n * (K // 2), K // 2)
        return [Gather4("z", lambda h: to.at[h, z, :, :, cs], lambda b, h: to.at[h, b, :, :, cs]),
                Gather4("y", lambda h: to.at[2 + h, :, y, :, cs], lambda b, h: to.at[2 + h, :, b, :, cs])]

    def up_unit(to, j):
        yj, zj = off(y, j), off(z, j)
        return [Gather4("z", lambda h: to.at[h, z, yj], lambda b, h: to.at[h, b, yj]),
                Gather4("y", lambda h: to.at[2 + h, zj, y], lambda b, h: to.at[2 + h, zj, b])]

    def do(gathers, step):
        for g in gathers:
            getattr(g, step)()

    mine = pl.ds(mo(c * UR, UR), UR)

    def up_exchange(l):
        sends = []
        for dx, dc in group:
            tx, tc = off(x, dx), (cp if dc else c)
            src = AV.at[l, 0, pl.ds(mo((tx * 2 + tc) * UR, UR), UR), :]
            sends.append(rcopy(src, up[l].at[x, z, y, mine, :], dev(dx=dx, dc=dc)))
        for cpy in sends:
            cpy.start()
        return sends

    (d0a, d0b, d0c, d0d), (d1a, d1b) = down_gathers(0, SPLIT3), down_gathers(1, WHOLE)
    u0a, u1a = up_first(up[0]), up_first(up[1])
    u1b, u1c = up_second(up[1], 0), up_second(up[1], 1)
    u0u = [up_unit(up[0], j) for j in (OWN, PRV, NXT, OPP)]
    ex0 = up_exchange(0)
    do(d0a, "start")
    gx0.start()
    ex1 = up_exchange(1)
    my_rows = pl.ds(mo((x * 2 + c) * UR, UR), UR)
    own_u1 = lcopy(AV.at[1, 0, my_rows, :], up[1].at[x, z, y, mine, :])
    own_u1.start()
    own_d1 = lcopy(RES.at[X1, pl.ds(DR_ROWS, DR_ROWS), :], down[1].at[y, z])
    own_d1.start()
    U[x, z, y, mine, :] = AV[0, 0, my_rows, :]
    do(d0a, "forward")
    for cpy in ex0:
        cpy.wait_recv()
    do(u0a, "start")
    do(u0u[0], "start")
    do(u0a, "forward")
    do(u0a, "neighbours")
    do(u0u[1], "start")
    do(u0u[2], "start")
    do(u0u[0], "forward")
    do(u0a, "opposite")
    do(u0u[3], "start")
    gx0.forward()
    load_g.wait()
    gg1.start()
    do(u0u[1], "forward")
    do(u0u[2], "forward")
    gx0.sides()
    do(d0a, "finish")
    do(u0u[3], "forward")
    do(d0b, "start")
    gx0.last()
    gx0.wait_own()
    gx0.wait_push(range(len(gx0.push)))
    own_x.wait()
    save_x = lcopy(XV, xh0)
    save_x.start()
    for cpy in ex0 + ex1:
        cpy.wait_send()
    own_u1.wait()
    gg1.forward()
    for unit in u0u:
        do(unit, "finish")
    save_u0 = lcopy(U, wuh.at[0])
    save_u0.start()

    T2 = 2 * TB
    ND = D // 4
    NK = K // 4

    def up_tile(t, n):
        cols = pl.ds(mo(n * NK, NK), NK)
        return dot_nn(XV[t].reshape(T2, D), U[:, :, :, :, cols].reshape(D, NK)), cols

    def hidden0(t):
        for n in range(RING):
            pre, cols = up_tile(t, n)
            act, slope = gelu_parts(pre)
            AV[t, :, :, cols] = act.astype(BF16).reshape(2, TB, NK)
            SV[t, :, :, cols] = slope.reshape(2, TB, NK)

    def hidden1(t, part):
        for n in (2 * part, 2 * part + 1):
            pre, cols = up_tile(t, n)
            act, slope = gelu_parts(pre)
            AV[t, :, :, cols] = act.astype(BF16).reshape(2, TB, NK)
            DV[t, :, cols] = (SV[t, :, :, cols].reshape(T2, NK) * slope).astype(BF16)

    def dact(gv, t, n):
        return dot_nt(gv[t].reshape(T2, D), W[n].reshape(NK, D))

    def dact1(t):
        def body(n, carry):
            SV[t, :, :, pl.ds(mo(n * NK, NK), NK)] = dact(GV1, t, n).reshape(2, TB, NK)
            return carry
        loop(RING, body, None)

    def dact0(t):
        def body(n, carry):
            cols = pl.ds(mo(n * NK, NK), NK)
            DV[t, :, cols] = (dact(GV0, t, n) * SV[t, :, :, cols].reshape(T2, NK)).astype(BF16)
            return carry
        loop(RING, body, None)

    def down_part(act, j, lo, tiles):
        t = lax.rem(x + j, RING)

        def body(n, carry):
            cols = pl.ds(mo((lo + n) * ND, ND), ND)
            PP[j, :, :, cols] = dot_nn(act[t, :, :, 0:K].reshape(T2, K), W[:, :, :, cols].reshape(K, ND)).reshape(2, TB, ND)
            return carry
        loop(tiles, body, None)

    def dx_part(j, lo, tiles):
        t = lax.rem(x + j, RING)

        def body(n, carry):
            cols = pl.ds(mo((lo + n) * ND, ND), ND)
            PP[j, :, :, cols] = dot_nt(DV[t], U[lo + n].reshape(ND, K)).reshape(2, TB, ND)
            return carry
        loop(tiles, body, None)

    class Reduce8:
        def __init__(self, part, index, split):
            self.part, self.index, self.split = part, index, split
            _, right, left = rings["x"]
            self.right, self.left = right, left
            self.pair, self.m = [], []
            for q in range(len(split)):
                cq = self.cols(q)
                self.pair.append((count[0], [rcopy(PP.at[j, cp, :, cq], DR.at[j, :, cq], partner) for j in range(RING)]))
                src = lambda j, h: PP.at[j, c, half(h), cq]
                self.m.append([rcopy(src(OPP, 0), XR.at[0, :, cq], right), rcopy(src(OPP, 1), XR.at[1, :, cq], left),
                               rcopy(src(NXT, 1), XR.at[2, :, cq], right), rcopy(src(PRV, 0), XR.at[3, :, cq], left),
                               rcopy(src(NXT, 0), XR.at[4, :, cq], right), rcopy(src(PRV, 1), XR.at[5, :, cq], left)])

        def cols(self, q):
            return tile_cols(self.split, q)

        def compute(self, j, q):
            self.part(j, sum(self.split[:q]), self.split[q])
            self.pair[q][1][j].start()

        def compute_all(self, q):
            first, cq = self.pair[q][0], self.cols(q)

            def body(i, carry):
                j = lax.rem(i + 1, RING)
                self.part(j, sum(self.split[:q]), self.split[q])
                pltpu.make_async_remote_copy(src_ref=PP.at[j, cp, :, cq], dst_ref=DR.at[j, :, cq],
                                             send_sem=ss.at[first + j], recv_sem=rs.at[first + j],
                                             device_id=partner, device_id_type=MESH_ID).start()
                return carry
            loop(RING, body, None)

        def combine(self, j, q):
            self.pair[q][1][j].wait_recv()
            add_rows(PP.at[j, c, :, self.cols(q)], [DR.at[j, :, self.cols(q)]], TB, min(TB, 16))

        def opposite(self, q):
            self.m[q][0].start()
            self.m[q][1].start()

        def side(self, j, q):
            self.combine(j, q)
            self.m[q][2 if j == NXT else 3].start()

        def send(self, q):
            self.combine(OPP, q)
            self.opposite(q)
            self.side(NXT, q)
            self.side(PRV, q)

        def relay(self, q):
            for k, j, h in ((0, NXT, 0), (1, PRV, 1)):
                self.m[q][k].wait_recv()
                add_rows(PP.at[j, c, half(h), self.cols(q)], [XR.at[k, :, self.cols(q)]], HB, min(HB, 16))
                self.m[q][4 + k].start()

        def finish(self, q, res, outs):
            for d in self.m[q][2:]:
                d.wait_recv()
            step, cq = min(HB, 16), self.cols(q)
            for h, (kl, kr) in enumerate(((4, 3), (2, 5))):
                def body(r, carry):
                    lo = pl.ds(mo(r * step, step), step)
                    sl = pl.ds(mo(h * HB + r * step, step), step)
                    tot = PP[OWN, c, sl, cq] + (XR[kl, lo, cq] + XR[kr, lo, cq])
                    val = (res[sl, cq].astype(F32) + tot).astype(BF16)
                    for o in outs:
                        o[sl, cq] = val
                    return carry
                loop(HB // step, body, None)

        def drain(self):
            for d in sum([p[1] for p in self.pair] + self.m, []):
                d.wait_send()

        def release(self):
            self.drain()
            for k, to in enumerate((self.right, self.left, partner)):
                pl.semaphore_signal(credit.at[k], inc=1, device_id=to, device_id_type=MESH_ID)

        def acquire(self):
            for k in range(len((self.right, self.left, partner))):
                pl.semaphore_wait(credit.at[k], 1)

    def grad_a(j, dst, halves=None):
        t = off(z, j)

        def rows(h, carry):
            lo = [pl.ds(mo((2 * h + q) * XD + t * ZD, ZD), ZD) for q in HALVES]
            lhs = jnp.concatenate([XV[:, :, :, s].reshape(8 * TB, ZD) for s in lo], axis=1)

            def body(n, carry):
                cols = pl.ds(mo(n * ND, ND), ND)
                dst[h, :, :, cols] = dot_tn(lhs, DV[:, :, cols].reshape(8 * TB, ND)).reshape(2, ZD, ND)
                return carry
            return loop(K // ND, body, carry)
        if halves is None:
            loop(2, rows, None)
        else:
            for h in halves:
                rows(h, None)

    def grad_b(gv, j, dst):
        cols_l = pl.ds(mo(off(y, j) * NK, NK), NK)

        def body(m, carry):
            cols = pl.ds(mo(m * ND, ND), ND)
            out = dot_tn(AV[:, :, :, cols_l].reshape(8 * TB, NK), gv[:, :, :, cols].reshape(8 * TB, ND))
            dst[:, m // 2, :, pl.ds(mo(lax.rem(m, 2) * ND, ND), ND)] = out.reshape(2, NK // 2, ND)
            return carry
        loop(RING, body, None)

    class Reduce4:
        def __init__(self, axis, part, recv, stage):
            _, right, left = rings[axis]
            self.part, self.recv, self.stage = part, recv, stage
            self.m = [rcopy(part(OPP, 0), recv(0), right), rcopy(part(OPP, 1), recv(1), left),
                      rcopy(part(NXT, 1), recv(2), right), rcopy(part(PRV, 0), recv(3), left),
                      rcopy(part(NXT, 0), recv(4), right), rcopy(part(PRV, 1), recv(5), left)]
            self.to = [(NXT, 0), (PRV, 1), (OWN, 1), (OWN, 0), (OWN, 0), (OWN, 1)]
            self.loads = [lcopy(recv(k), stage(k)) for k in range(ARRIVALS)]

        def opposite(self):
            self.m[0].start()
            self.m[1].start()

        def sides(self, j):
            self.m[2 if j == NXT else 3].start()

        def fetch(self, k):
            self.m[k].wait_send()
            self.m[k].wait_recv()
            self.loads[k].start()

        def absorb(self, k):
            self.loads[k].wait()
            dst = self.part(*self.to[k])
            add_rows(dst, [self.stage(k)], dst.shape[1], min(dst.shape[1], 16))

    def arrive(reduces, ks):
        for k in ks:
            for r in reduces:
                r.fetch(k)
        for k in ks:
            for r in reduces:
                r.absorb(k)

    def relay(reduces):
        for k in (0, 1):
            for r in reduces:
                r.fetch(k)
        for k in (0, 1):
            for r in reduces:
                r.absorb(k)
                r.m[4 + k].start()

    EARLY, LATE = (2, 3), (4, 5)
    hq = DR_ROWS // 2
    own_grads = [(SV.at[pl.ds(0, 2)], SV.at[pl.ds(2, 2)]), (GPA.at[OWN], GPB.at[OWN])]

    def make_reduce(l, q, chunks):
        own_a, own_b = own_grads[l]
        ca = pl.ds(q * (K // chunks), K // chunks)
        nb = pl.ds(q, 1) if chunks == 2 else pl.ds(0, 2)
        pick = ((OPP, 0), (OPP, 1), (NXT, 1), (PRV, 0), (NXT, 0), (PRV, 1))

        def part_a(j, h):
            return (own_a.at[h, :, :, ca] if j == OWN else GPA.at[j, h, :, :, ca])

        def part_b(j, h):
            return (own_b.at[h, nb] if j == OWN else GPB.at[j, h, nb])

        def part_a2(j, h):
            return own_a.at[h, :, pl.ds(mo(off(y, j) * 2 * UR, 2 * UR), 2 * UR), ca]

        def part_b2(j, h):
            t = off(z, j)
            return own_b.at[t // 2, nb, pl.ds(mo(lax.rem(t, 2) * DR_ROWS + h * hq, hq), hq), :]
        return (Reduce4("z", part_a, lambda k: ra1.at[l, k, :, :, ca], lambda k: part_a(*pick[k])),
                Reduce4("y", part_b, lambda k: rb1.at[l, k, nb], lambda k: part_b(*pick[k])),
                Reduce4("y", part_a2, lambda k: ra2.at[l, k, :, :, ca], lambda k: STA.at[k % 2, :, :, ca]),
                Reduce4("z", part_b2, lambda k: rb2.at[l, k, nb], lambda k: STB.at[k % 2, nb]))

    def second_start(reduces):
        for r in reduces:
            r.opposite()
            r.sides(NXT)
            r.sides(PRV)

    def grads_out_start(l, q, chunks):
        own_a, own_b = own_grads[l]
        ca = pl.ds(q * (K // chunks), K // chunks)

        def rows_of(tx, tc):
            return own_a.at[tx // 2, lax.rem(tx, 2), pl.ds(mo((2 * y + tc) * UR, UR), UR), ca]
        to = uh.at[l, x, mine, ca]
        sends = [rcopy(rows_of(off(x, dx), cp if dc else c), to, dev(dx=dx, dc=dc)) for dx, dc in group]
        local = [lcopy(rows_of(x, c), to)]
        for n in ((q,) if chunks == 2 else HALVES):
            local.append(lcopy(own_b.at[z // 2, n, pl.ds(mo(lax.rem(z, 2) * DR_ROWS, DR_ROWS), DR_ROWS), :],
                               gd_out.at[l, :, pl.ds(n * K, K)]))
        for cpy in sends + local:
            cpy.start()
        return sends, local

    def grads_out_finish(state):
        for cpy in state[0]:
            cpy.wait_recv()
            cpy.wait_send()
        for cpy in state[1]:
            cpy.wait()

    do(d0b, "forward")
    do(d0c, "start")
    gx0.drain()
    do(d0a, "drain")
    save_x.wait()
    r = Reduce8(functools.partial(down_part, AV), 0, SPLIT3)
    hidden0(off(x, OPP))
    do(d0b, "finish")
    r.compute(OPP, 0)
    hidden0(off(x, NXT))
    do(d0c, "forward")
    do(d0d, "start")
    r.compute(NXT, 0)
    r.combine(OPP, 0)
    r.opposite(0)
    hidden0(off(x, PRV))
    r.compute(PRV, 0)
    r.side(NXT, 0)
    gg1.sides()
    hidden0(off(x, OWN))
    r.side(PRV, 0)
    save_s = lcopy(SV, sh0)
    save_s.start()
    save_a0 = lcopy(AV, ah.at[0])
    save_a0.start()
    do(d0d, "forward")
    do(d1a, "start")
    do(d0c, "finish")
    r.compute_all(1)
    r.relay(0)
    r.send(1)
    for cpy in ex1:
        cpy.wait_recv()
    own_d1.wait()
    do(u1a, "start")
    gg1.last()
    do(d0d, "finish")
    save_d0 = lcopy(W, wdh.at[0])
    save_d0.start()
    r.compute_all(2)
    do(d1a, "forward")
    r.relay(1)
    r.send(2)
    do(u1a, "forward")
    r.compute(OWN, 0)
    do(d1a, "finish")
    do(d1b, "start")
    for q in range(len(SPLIT3)):
        r.combine(OWN, q)
    do(u1a, "finish")

    def token_gathers(slot, buf):
        def make(q):
            cq = tile_cols(SPLIT2, q)
            return Gather8(lambda h: RES.at[slot, half(h), cq], lambda b, k, h: buf.at[b, k, half(h), cq])
        return [make(0), make(1)]

    gx1 = token_gathers(X1, XV)
    do(d1a, "drain")
    for q in HALVES:
        r.finish(q, RES.at[X0], [RES.at[X1], XV.at[x, c]])
    gg1.wait_own()
    gg1.wait_push(range(len(gg1.push)))
    own_g.wait()
    do(d1b, "forward")
    do(u1b, "start")
    r.relay(2)
    gx1[0].start()
    save_d0.wait()
    do(d0b + d0c + d0d, "drain")
    do(d1b, "finish")
    load_w1d = lcopy(wdh.at[1], W)
    load_w1d.start()
    r.finish(2, RES.at[X0], [RES.at[X1], XV.at[x, c]])
    gx1[1].start()
    save_s.wait()
    do(u1b, "forward")
    do(u1c, "start")
    gx1[0].forward()
    load_w1d.wait()
    dact1(off(x, OWN))
    r.release()
    dact1(off(x, NXT))
    gx1[0].sides()
    dact1(off(x, PRV))
    save_u0.wait()
    do(sum(u0u, u0a), "drain")
    do(u1b, "finish")

    def load_up(n):
        cs = pl.ds(n * (K // 2), K // 2)
        return lcopy(wuh.at[1, :, :, :, :, cs], U.at[:, :, :, :, cs])
    load_w1u = [load_up(n) for n in HALVES]
    load_w1u[0].start()
    do(u1c, "forward")
    gx1[1].forward()
    dact1(off(x, OPP))
    load_w0d_again = lcopy(wdh.at[0], W)
    load_w0d_again.start()
    save_a0.wait()
    do(gx1, "wait_own")
    load_w1u[0].wait()
    hidden1(off(x, OWN), 0)
    gx1[1].sides()
    gx1[0].last()
    do(u1c, "finish")
    load_w1u[1].start()
    for g in gx1:
        g.wait_push((0, 2))
    hidden1(off(x, PRV), 0)
    gx1[1].last()
    for g in gx1:
        g.wait_push((1, 3))
    hidden1(off(x, NXT), 0)
    load_w1u[1].wait()
    for j in (OWN, PRV, NXT):
        hidden1(off(x, j), 1)
    for g in gx1:
        g.wait_push((4, 5))
    for n in HALVES:
        hidden1(off(x, OPP), n)
    load_s0 = lcopy(sh0, SV)
    load_s0.start()
    save_a1 = lcopy(AV, ah.at[1])
    save_a1.start()

    a1, b1, a2, b2 = make_reduce(1, 0, 1)
    grad_b(GV1, OPP, GPB.at[OPP])
    b1.opposite()
    for h in HALVES:
        grad_a(OPP, GPA.at[OPP], (h,))
        a1.m[h].start()
    r = Reduce8(dx_part, 1, SPLIT2)
    r.acquire()
    r.compute(OPP, 0)
    r.compute(NXT, 0)
    r.combine(OPP, 0)
    r.opposite(0)
    r.compute(PRV, 0)
    r.side(NXT, 0)
    r.side(PRV, 0)
    r.compute_all(1)
    load_w0u_again = lcopy(wuh.at[0], U)
    r.compute(OWN, 0)
    load_w0u_again.start()
    grad_b(GV1, NXT, GPB.at[NXT])
    b1.sides(NXT)
    grad_b(GV1, PRV, GPB.at[PRV])
    b1.sides(PRV)
    r.relay(0)
    r.send(1)
    grad_a(NXT, GPA.at[NXT])
    a1.sides(NXT)
    grad_a(PRV, GPA.at[PRV])
    a1.sides(PRV)
    r.combine(OWN, 0)
    r.combine(OWN, 1)
    gg0 = token_gathers(G0, GV0)
    r.relay(1)
    r.finish(0, RES.at[G1], [RES.at[G0], GV0.at[x, c]])
    gg0[0].start()
    relay((b1, a1))
    grad_b(GV1, OWN, GPB.at[OWN])
    save_a1.wait()
    load_a0 = lcopy(ah.at[0], AV)
    load_a0.start()
    gg1.drain()
    load_a1 = lcopy(ah.at[1], GV1.at[:, :, :, 0:K])
    load_a1.start()
    r.finish(1, RES.at[G1], [RES.at[G0], GV0.at[x, c]])
    gg0[1].start()
    gg0[0].forward()
    grad_a(OWN, GPA.at[OWN])
    do(gx1, "drain")
    load_x0 = lcopy(xh0, XV)
    load_x0.start()
    gg0[0].sides()
    r.release()
    gg0[1].forward()
    gg0[0].last()
    load_w0d_again.wait()
    load_s0.wait()
    do(gg0, "wait_own")
    dact0(off(x, OWN))
    gg0[1].sides()
    gg0[1].last()
    for g in gg0:
        g.wait_push((0, 2))
    dact0(off(x, PRV))
    for g in gg0:
        g.wait_push((1, 3))
    dact0(off(x, NXT))
    for g in gg0:
        g.wait_push((4, 5))

    a1n, b1n, a2n, b2n = zip(*[make_reduce(0, q, 2) for q in HALVES])
    load_a0.wait()
    grad_b(GV0, OPP, GPB.at[OPP])
    b1n[0].opposite()
    dact0(off(x, OPP))
    load_w1d_again = lcopy(wdh.at[1], W)
    load_w1d_again.start()
    load_x0.wait()
    for h in HALVES:
        grad_a(OPP, GPA.at[OPP], (h,))
        a1n[0].m[h].start()
    arrive((b1, a1), EARLY + LATE)
    second_start((a2, b2))
    load_w0u_again.wait()
    r = Reduce8(dx_part, 2, WHOLE)
    r.acquire()
    r.compute_all(0)
    r.send(0)
    grad_b(GV0, NXT, GPB.at[NXT])
    b1n[0].sides(NXT)
    grad_b(GV0, PRV, GPB.at[PRV])
    b1n[0].sides(PRV)
    grad_a(NXT, GPA.at[NXT])
    a1n[0].sides(NXT)
    grad_a(PRV, GPA.at[PRV])
    a1n[0].sides(PRV)
    relay((b2, a2))
    r.relay(0)
    relay((b1n[0], a1n[0]))
    for red in (b1n[1], a1n[1]):
        red.opposite()
        red.sides(NXT)
        red.sides(PRV)
    r.combine(OWN, 0)
    grad_b(GV0, OWN, own_grads[0][1])
    grad_a(OWN, own_grads[0][0])
    r.finish(0, RES.at[G0], [RES.at[X0]])
    r.release()
    write_gi = lcopy(RES.at[X0], gi_out)
    write_gi.start()
    arrive((b1n[0], a1n[0]), EARLY)
    load_a1.wait()
    load_w1d_again.wait()
    r = Reduce8(functools.partial(down_part, GV1), 3, WHOLE)
    r.acquire()
    r.compute_all(0)
    r.send(0)
    arrive((b2, a2), EARLY)
    arrive((b2, a2), LATE)
    state1 = grads_out_start(1, 0, 1)
    r.combine(OWN, 0)
    arrive((b1n[0], a1n[0]), LATE)
    relay((b1n[1], a1n[1]))
    second_start((a2n[0], b2n[0]))
    r.relay(0)
    arrive((b1n[1], a1n[1]), EARLY)
    arrive((b1n[1], a1n[1]), LATE)
    second_start((a2n[1], b2n[1]))
    relay((b2n[0], a2n[0]))
    arrive((b2n[0], a2n[0]), EARLY)
    relay((b2n[1], a2n[1]))
    arrive((b2n[0], a2n[0]), LATE)
    state0 = [grads_out_start(0, 0, 2)]
    r.finish(0, RES.at[X1], [RES.at[G1]])
    write_y = lcopy(RES.at[G1], y_out)
    write_y.start()
    grads_out_finish(state1)
    arrive((b2n[1], a2n[1]), EARLY)
    arrive((b2n[1], a2n[1]), LATE)
    state0.append(grads_out_start(0, 1, 2))
    r.drain()
    do(d1b + u1a + u1b + u1c + gg0, "drain")
    write_gi.wait()
    write_y.wait()
    for state in state0:
        grads_out_finish(state)
    assert count[0] <= N_SEM and lcount[0] <= N_LOCAL


def finish_kernel(y_in, gi_in, gu_in, gd_in, y_out, gi_out, gu_out, gd_out, ybuf, gibuf, gubuf, gdbuf, gushuf, sems):
    layers, ur, ff = gu_out.shape
    s2 = ff // 64
    half = s2 // 2
    loads = [pltpu.make_async_copy(a, b, sems.at[0, k])
             for k, (a, b) in enumerate(((gu_in, gubuf), (gd_in, gdbuf), (y_in, ybuf), (gi_in, gibuf)))]
    stores = [pltpu.make_async_copy(a, b, sems.at[1, k])
              for k, (a, b) in enumerate(((gushuf, gu_out), (gdbuf, gd_out), (ybuf, y_out), (gibuf, gi_out)))]
    for cpy in loads:
        cpy.start()
    low = lax.broadcasted_iota(jnp.int32, (ur, s2), 1) < half
    swap = lambda v: pltpu.roll(v, half, 1)
    for k in (1, 2, 3):
        loads[k].wait()
        stores[k].start()
    loads[0].wait()
    for l in range(layers):
        for b in range(RING):
            for yy in range(RING):
                for m in HALVES:
                    cols = pl.ds((yy * 2 + m) * s2, s2)
                    t0, t1 = (gubuf[l, b, pl.ds(k * ur, ur), cols] for k in HALVES)
                    strip = (b * RING + 2 * m) * RING + yy
                    gushuf[l, :, pl.ds(strip * s2, s2)] = jnp.where(low, t0, swap(t1))
                    gushuf[l, :, pl.ds((strip + RING) * s2, s2)] = jnp.where(low, swap(t0), t1)
    stores[0].start()
    for cpy in stores:
        cpy.wait()


def solution(mesh, interpret=None):
    fine = Mesh(np.asarray(mesh.devices).reshape(4, 4, 4, 2), ALL)
    tok_spec = P(ALL, None)
    weight_spec = P(None, ALL, None)

    def device_step(x_loc, up_loc, down_loc, g_loc):
        layers, ur, ff = up_loc.shape
        dr, dm = down_loc.shape[1:]
        tb = x_loc.shape[0]
        k = ff // 8
        zd = dm // 16
        hbm = lambda shape, dt: jax.ShapeDtypeStruct(shape, dt)
        outs = [
            hbm((tb, dm), BF16), hbm((tb, dm), BF16), hbm((layers, dr, dm), F32),
            hbm((RING, CORES, tb, dm), BF16),
            hbm((layers, RING, RING, RING, 2 * ur, k), BF16),
            hbm((layers, RING, RING, dr, dm), BF16),
            hbm((RING, CORES, tb, k), F32), hbm((layers, RING, CORES, tb, k), BF16),
            *[hbm((layers, ARRIVALS, CORES, n, k), F32) for n in (zd, zd, 2 * ur, 2 * ur)],
            hbm((layers, RING, 2 * ur, k), F32),
        ]
        vm = pltpu.VMEM
        scratch = [
            vm((RING, RING, RING, 2 * ur, k), BF16), vm((RING, RING, dr, dm), BF16),
            vm((RING, CORES, tb, dm), BF16), vm((RING, CORES, tb, dm), BF16), vm((RING, CORES, tb, dm), BF16),
            vm((RING, CORES, tb, k), F32), vm((RING, CORES, tb, k), BF16), vm((RING, 2 * tb, k), BF16),
            vm((RING, CORES, CORES, zd, k), F32), vm((RING, CORES, CORES, zd, k), F32),
            vm((RING, CORES, tb, dm), F32), vm((4, tb, dm), F32), vm((6, tb // 2, dm), F32),
            vm((4, tb, dm), BF16), vm((CORES, CORES, 2 * ur, k), F32), vm((CORES, CORES, 2 * ur, k), F32),
            pltpu.SemaphoreType.DMA((N_SEM,)), pltpu.SemaphoreType.DMA((N_SEM,)), pltpu.SemaphoreType.DMA((N_LOCAL,)),
            pltpu.SemaphoreType.REGULAR((3,)),
        ]
        anyspec = pl.BlockSpec(memory_space=pl.ANY)
        call = pl.pallas_call(
            functools.partial(kernel, (dm, k, tb, ur, dr)),
            out_shape=outs,
            in_specs=[anyspec] * 4,
            out_specs=[anyspec] * len(outs),
            scratch_shapes=scratch,
            compiler_params=pltpu.CompilerParams(collective_id=0, has_side_effects=True, vmem_limit_bytes=67043328),
            name="mlp_stack",
            **({"interpret": interpret} if interpret else {}),
        )
        y_raw, gi_raw, gd_raw, *_, gu_raw = call(x_loc, up_loc, down_loc, g_loc)
        raws = (y_raw, gi_raw, gu_raw, gd_raw)
        outs = [hbm((tb, dm), BF16), hbm((tb, dm), BF16), hbm((layers, ur, ff), F32), hbm((layers, dr, dm), F32)]
        return tuple(pl.pallas_call(
            finish_kernel, out_shape=outs, in_specs=[anyspec] * len(outs), out_specs=[anyspec] * len(outs),
            scratch_shapes=[vm(v.shape, v.dtype) for v in raws] + [vm(outs[2].shape, F32), pltpu.SemaphoreType.DMA((2, len(outs)))],
            name="write_out")(*raws))

    return jax.shard_map(device_step, mesh=fine, in_specs=(tok_spec, weight_spec, weight_spec, tok_spec),
                         out_specs=(tok_spec, tok_spec, weight_spec, weight_spec), check_vma=False)
```

```python
import functools

import jax
import jax.numpy as jnp
import numpy as np
from jax import lax
from jax.experimental import pallas as pl
from jax.experimental.pallas import tpu as pltpu
from jax.sharding import Mesh, PartitionSpec as P

MESH_ID = pl.DeviceIdType.MESH
ALL = ("x", "z", "y", "c")
F32, BF16 = jnp.float32, jnp.bfloat16
RING, CORES, ARRIVALS = 4, 2, 6
OWN, NXT, OPP, PRV = range(RING)
X0, X1, G1, G0 = range(RING)
HALVES = (0, 1)
WHOLE, SPLIT2, SPLIT3 = (4,), (2, 2), (1, 1, 2)
N_RECV, N_SEND, N_LOCAL = 182, 110, 15


def gelu_parts(pre_act):
    norm_cdf = 0.5 * (1.0 + lax.erf(pre_act * (2.0 ** -0.5)))
    norm_pdf = jnp.exp(-0.5 * pre_act * pre_act) * ((2.0 * jnp.pi) ** -0.5)
    return pre_act * norm_cdf, norm_cdf + pre_act * norm_pdf


def loop(n, body, init):
    return lax.fori_loop(0, n, body, init)


def dot_nn(left, right):
    return lax.dot_general(left, right, (((1,), (0,)), ((), ())), preferred_element_type=F32)


def dot_nt(left, right):
    return lax.dot_general(left, right, (((1,), (1,)), ((), ())), preferred_element_type=F32)


def dot_tn(left, right):
    return lax.dot_general(left, right, (((0,), (0,)), ((), ())), preferred_element_type=F32)


def kernel(dims, x_in, wu_in, wd_in, g_in,
           y_out, gi_out, gd_out,
           xh0, wuh, wdh, sh0, ah, ra1, rb1, ra2, rb2, uh,
           U, W, XV, GV1, GV0, SV, AV, DV, GPA, GPB, PP, DR, XR, RES, STA, STB,
           ss, rs, ls, ps, credit):
    D, K, TB, UR, DR_ROWS = dims
    HB = TB // 2
    x, z, y, c = (lax.axis_index(a) for a in ALL)
    cp = 1 - c
    S2 = 2 * DR_ROWS
    XD = D // 4
    ZD = D // 16

    def dev(dx=0, dz=0, dy=0, dc=0):
        wrap = lambda v, d, n: v if d == 0 else lax.rem(v + (d % n), n)
        return (wrap(x, dx, 4), wrap(z, dz, 4), wrap(y, dy, 4), wrap(c, dc, 2))

    partner = dev(dc=1)
    rings = {"x": (x, dev(dx=1), dev(dx=-1)), "z": (z, dev(dz=1), dev(dz=-1)), "y": (y, dev(dy=1), dev(dy=-1))}
    off = lambda v, d: v if d == 0 else lax.rem(v + d, 4)

    used = {"recv": 0, "send": 0, "local": 0}
    free = {"send": [], "local": []}
    keys = []

    def fresh(kind):
        if kind == "recv" and keys:
            return keys.pop()
        used[kind] += 1
        return used[kind] - 1

    def take(kind):
        return free[kind].pop() if free[kind] else fresh(kind)

    def remote(src, dst, send, recv, to):
        return pltpu.make_async_remote_copy(src_ref=src, dst_ref=dst, send_sem=send, recv_sem=recv,
                                            device_id=to, device_id_type=MESH_ID)

    class rcopy:
        def __init__(self, src, dst, to, key=None):
            self.args, self.key = (src, dst, to), fresh("recv") if key is None else key

        def start(self):
            src, dst, to = self.args
            self.sem = take("send")
            self.d = remote(src, dst, ss.at[self.sem], rs.at[self.key], to)
            self.d.start()

        def wait_recv(self):
            self.d.wait_recv()

        def wait_send(self):
            self.d.wait_send()
            free["send"].append(self.sem)

    class lcopy:
        def __init__(self, src, dst):
            self.args = src, dst

        def start(self):
            self.sem = take("local")
            self.d = pltpu.make_async_copy(*self.args, ls.at[self.sem])
            self.d.start()

        def wait(self):
            self.d.wait()
            free["local"].append(self.sem)

    def mo(v, m):
        return pl.multiple_of(v, m)

    class Gather4:
        def __init__(self, axis, src, dst):
            i, right, left = rings[axis]
            lft, rgt = off(i, 3), off(i, 1)
            self.d = [rcopy(src(0), dst(i, 0), right), rcopy(src(1), dst(i, 1), right),
                      rcopy(src(0), dst(i, 0), left), rcopy(src(1), dst(i, 1), left),
                      rcopy(dst(lft, 0), dst(lft, 0), right), rcopy(dst(rgt, 1), dst(rgt, 1), left)]

        def start_first(self):
            self.d[0].start()
            self.d[3].start()

        def start_rest(self):
            self.d[1].start()
            self.d[2].start()

        def start(self):
            self.start_first()
            self.start_rest()

        def forward(self):
            for k in HALVES:
                self.d[3 * k].wait_recv()
                self.d[4 + k].start()

        def neighbours(self):
            self.d[1].wait_recv()
            self.d[2].wait_recv()

        def opposite(self):
            self.d[4].wait_recv()
            self.d[5].wait_recv()

        def finish(self):
            self.neighbours()
            self.opposite()

        def drain(self):
            for d in self.d:
                d.wait_send()

    class Gather8:
        def __init__(self, src, dst):
            self.ring = Gather4("x", src, lambda b, h: dst(b, c, h))
            lft, rgt, opp = off(x, PRV), off(x, NXT), off(x, OPP)
            blocks = [(lft, 0), (rgt, 1), (lft, 1), (rgt, 0), (opp, 0), (opp, 1)]
            self.own = [rcopy(src(h), dst(x, c, h), partner) for h in HALVES]
            self.push = [rcopy(dst(b, c, h), dst(b, c, h), partner) for b, h in blocks]

        def start(self):
            self.ring.start()
            for d in self.own:
                d.start()

        def forward(self):
            self.ring.forward()
            self.push[0].start()
            self.push[1].start()

        def sides(self):
            self.ring.d[1].wait_recv()
            self.push[2].start()
            self.ring.d[2].wait_recv()
            self.push[3].start()

        def last(self):
            self.ring.d[4].wait_recv()
            self.push[4].start()
            self.ring.d[5].wait_recv()
            self.push[5].start()

        def wait_own(self):
            for d in self.own:
                d.wait_recv()

        def wait_push(self, ks):
            for k in ks:
                self.push[k].wait_recv()

        def drain(self):
            self.ring.drain()
            for d in self.own + self.push:
                d.wait_send()

    def add_rows(dst, srcs, rows, step):
        def body(r, carry):
            sl = pl.ds(mo(r * step, step), step)
            if len(dst.shape) == 3:
                for q in range(dst.shape[0]):
                    acc = dst[q, sl, :]
                    for s in srcs:
                        acc = acc + s[q, sl, :]
                    dst[q, sl, :] = acc
            else:
                acc = dst[sl, :]
                for s in srcs:
                    acc = acc + s[sl, :]
                dst[sl, :] = acc
            return carry
        loop(rows // step, body, None)

    barrier = pltpu.get_barrier_semaphore()
    group = [(dx, dc) for dx in range(RING) for dc in HALVES if dx or dc]
    peers = [dev(dx=dx, dc=dc) for dx, dc in group] + [rings[a][k] for a in "zy" for k in (1, 2)]
    for p in peers:
        pl.semaphore_signal(barrier, inc=1, device_id=p, device_id_type=MESH_ID)

    load_u = [[lcopy(wu_in.at[l, :, pl.ds(b * D, D)], RES.at[G0, pl.ds((l * RING + b) * UR, UR), :])
               for b in range(RING)] for l in HALVES]
    load_d = [lcopy(wd_in.at[l], RES.at[X1, pl.ds(l * DR_ROWS, DR_ROWS), :]) for l in HALVES]
    load_x = lcopy(x_in, RES.at[X0])
    load_g = lcopy(g_in, RES.at[G1])
    own_x = lcopy(x_in, XV.at[x, c])
    own_g = lcopy(g_in, GV1.at[x, c])
    own_d0 = lcopy(wd_in.at[0], W.at[y, z])
    for cpy in load_u[0] + load_u[1] + load_d + [load_x, own_d0, own_x, load_g, own_g]:
        cpy.start()

    low = lax.broadcasted_iota(jnp.int32, (UR, S2), 1) < DR_ROWS
    swap = lambda v: pltpu.roll(v, DR_ROWS, 1)
    for l in HALVES:
        for cpy in load_u[l]:
            cpy.wait()
        for b in range(RING):
            rows = pl.ds((l * RING + b) * UR, UR)
            for yy in range(RING):
                for m in HALVES:
                    s0 = RES[G0, rows, pl.ds((2 * m * RING + yy) * S2, S2)].astype(F32)
                    s1 = RES[G0, rows, pl.ds(((2 * m + 1) * RING + yy) * S2, S2)].astype(F32)
                    cols = pl.ds((yy * 2 + m) * S2, S2)
                    AV[l, 0, pl.ds(2 * b * UR, UR), cols] = jnp.where(low, s0, swap(s1)).astype(BF16)
                    AV[l, 0, pl.ds((2 * b + 1) * UR, UR), cols] = jnp.where(low, swap(s0), s1).astype(BF16)
    for cpy in load_d + [load_x, own_d0]:
        cpy.wait()
    pl.semaphore_wait(barrier, len(peers))

    half = lambda h: pl.ds(h * HB, HB)

    def tile_cols(split, q):
        return pl.ds(sum(split[:q]) * (D // RING), split[q] * (D // RING))

    gx0 = Gather8(lambda h: RES.at[X0, half(h)], lambda b, k, h: XV.at[b, k, half(h)])
    gg1 = Gather8(lambda h: RES.at[G1, half(h)], lambda b, k, h: GV1.at[b, k, half(h)])
    up = [U, wuh.at[1]]
    down = [W, wdh.at[1]]
    hr = DR_ROWS // 4

    def quarter(q, h):
        return pl.ds((2 * q + h) * hr, hr)

    def down_first(l):
        to = down[l]
        src = lambda q: lambda h: RES.at[X1, pl.ds(l * DR_ROWS + (2 * q + h) * hr, hr)]
        return [Gather4("z", src(0), lambda b, h: to.at[y, b, quarter(0, h)]),
                Gather4("y", src(1), lambda b, h: to.at[b, z, quarter(1, h)])]

    def down_second(l, split, n):
        to, cs = down[l], tile_cols(split, n)
        return [Gather4("y", lambda h: to.at[y, :, quarter(0, h), cs], lambda b, h: to.at[b, :, quarter(0, h), cs]),
                Gather4("z", lambda h: to.at[:, z, quarter(1, h), cs], lambda b, h: to.at[:, b, quarter(1, h), cs])]

    def up_first(to):
        return [Gather4("y", lambda h: to.at[h, z, y], lambda b, h: to.at[h, z, b]),
                Gather4("z", lambda h: to.at[2 + h, z, y], lambda b, h: to.at[2 + h, b, y])]

    def hidden_cols(n):
        return pl.ds(sum(SPLIT2[:n]) * (K // RING), SPLIT2[n] * (K // RING))

    def up_second(to, n):
        cs = hidden_cols(n)
        return [Gather4("z", lambda h: to.at[h, z, :, :, cs], lambda b, h: to.at[h, b, :, :, cs]),
                Gather4("y", lambda h: to.at[2 + h, :, y, :, cs], lambda b, h: to.at[2 + h, :, b, :, cs])]

    def up_unit(to, j):
        yj, zj = off(y, j), off(z, j)
        return [Gather4("z", lambda h: to.at[h, z, yj], lambda b, h: to.at[h, b, yj]),
                Gather4("y", lambda h: to.at[2 + h, zj, y], lambda b, h: to.at[2 + h, zj, b])]

    def do(gathers, step):
        for g in gathers:
            getattr(g, step)()

    mine = pl.ds(mo(c * UR, UR), UR)

    def up_exchange(l):
        sends = []
        for dx, dc in group:
            tx, tc = off(x, dx), (cp if dc else c)
            src = AV.at[l, 0, pl.ds(mo((tx * 2 + tc) * UR, UR), UR), :]
            sends.append(rcopy(src, up[l].at[x, z, y, mine, :], dev(dx=dx, dc=dc)))
        for cpy in sends:
            cpy.start()
        return sends

    def keys_of(gathers):
        return [d.key for g in gathers for d in g.d]

    d0a, d0b, d0c = down_first(0), down_second(0, SPLIT3, 0), down_second(0, SPLIT3, 1)
    u0a, u0u = up_first(up[0]), [up_unit(up[0], j) for j in (OWN, PRV, NXT, OPP)]
    keys.extend(keys_of(u0a))
    d0d = down_second(0, SPLIT3, 2)
    keys.extend(keys_of(d0a))
    d1a = down_first(1)
    keys.extend(keys_of(sum(u0u, [])))
    d1b, u1a = down_second(1, WHOLE, 0), up_first(up[1])
    u1b, u1c = up_second(up[1], 0), up_second(up[1], 1)
    ex0 = up_exchange(0)
    do(d0a, "start")
    gx0.start()
    ex1 = up_exchange(1)
    my_rows = pl.ds(mo((x * 2 + c) * UR, UR), UR)
    own_u1 = lcopy(AV.at[1, 0, my_rows, :], up[1].at[x, z, y, mine, :])
    own_u1.start()
    own_d1 = lcopy(RES.at[X1, pl.ds(DR_ROWS, DR_ROWS), :], down[1].at[y, z])
    own_d1.start()
    U[x, z, y, mine, :] = AV[0, 0, my_rows, :]
    do(d0a, "forward")
    for cpy in ex0:
        cpy.wait_recv()
    do(u0a, "start")
    do(u0u[0], "start")
    do(u0a, "forward")
    gx0.forward()
    load_g.wait()
    gg1.start()
    do(u0a, "neighbours")
    do(u0u[1], "start")
    do(u0u[2], "start")
    do(u0u[0], "forward")
    do(u0a, "opposite")
    do(u0u[3], "start")
    do(d0a, "finish")
    do(u0u[1], "forward")
    do(u0u[2], "forward")
    do(d0b, "start_first")
    gx0.sides()
    for cpy in ex0 + ex1:
        cpy.wait_send()
    own_u1.wait()
    do(u0u[3], "forward")
    do(u0a + d0a, "drain")
    do(d0b, "start_rest")
    do(d0c, "start_first")
    gg1.forward()
    do(d0b, "forward")
    do(d0c, "start_rest")
    do(d1a, "start")
    gx0.last()
    gx0.wait_own()
    gx0.wait_push(range(len(gx0.push)))
    own_x.wait()
    save_x = lcopy(XV, xh0)
    save_x.start()
    gx0.drain()
    for unit in u0u:
        do(unit, "finish")
    save_u0 = lcopy(U, wuh.at[0])
    save_u0.start()

    T2 = 2 * TB
    ND = D // 4
    NK = K // 4

    def up_tile(t, n):
        cols = pl.ds(mo(n * NK, NK), NK)
        return dot_nn(XV[t].reshape(T2, D), U[:, :, :, :, cols].reshape(D, NK)), cols

    def hidden0(t):
        for n in range(RING):
            pre, cols = up_tile(t, n)
            act, slope = gelu_parts(pre)
            AV[t, :, :, cols] = act.astype(BF16).reshape(2, TB, NK)
            SV[t, :, :, cols] = slope.reshape(2, TB, NK)

    def hidden1(t, part):
        for n in range(sum(SPLIT2[:part]), sum(SPLIT2[:part + 1])):
            pre, cols = up_tile(t, n)
            act, slope = gelu_parts(pre)
            AV[t, :, :, cols] = act.astype(BF16).reshape(2, TB, NK)
            DV[t, :, cols] = (SV[t, :, :, cols].reshape(T2, NK) * slope).astype(BF16)

    def dact(gv, t, n):
        return dot_nt(gv[t].reshape(T2, D), W[n].reshape(NK, D))

    def dact1(t):
        def body(n, carry):
            SV[t, :, :, pl.ds(mo(n * NK, NK), NK)] = dact(GV1, t, n).reshape(2, TB, NK)
            return carry
        loop(RING, body, None)

    def dact0(t):
        def body(n, carry):
            cols = pl.ds(mo(n * NK, NK), NK)
            DV[t, :, cols] = (dact(GV0, t, n) * SV[t, :, :, cols].reshape(T2, NK)).astype(BF16)
            return carry
        loop(RING, body, None)

    def down_part(act, j, lo, tiles):
        t = lax.rem(x + j, RING)

        def body(n, carry):
            cols = pl.ds(mo((lo + n) * ND, ND), ND)
            PP[j, :, :, cols] = dot_nn(act[t, :, :, 0:K].reshape(T2, K), W[:, :, :, cols].reshape(K, ND)).reshape(2, TB, ND)
            return carry
        loop(tiles, body, None)

    def dx_part(j, lo, tiles):
        t = lax.rem(x + j, RING)

        def body(n, carry):
            cols = pl.ds(mo((lo + n) * ND, ND), ND)
            PP[j, :, :, cols] = dot_nt(DV[t], U[lo + n].reshape(ND, K)).reshape(2, TB, ND)
            return carry
        loop(tiles, body, None)

    class Reduce8:
        def __init__(self, part, index, split, old=()):
            self.part, self.index, self.split = part, index, split
            keys.extend(old)
            _, right, left = rings["x"]
            self.right, self.left = right, left
            self.pair, self.m, self.first = [], [], []
            for q in range(len(split)):
                cq = self.cols(q)
                first = sorted(fresh("recv") for j in range(RING))
                self.pair.append([self.swap(j, q, first[0]) for j in range(RING)])
                self.first.append(first[0])
                src = lambda j, h: PP.at[j, c, half(h), cq]
                self.m.append([rcopy(src(OPP, 0), XR.at[0, :, cq], right), rcopy(src(OPP, 1), XR.at[1, :, cq], left),
                               rcopy(src(NXT, 1), XR.at[2, :, cq], right), rcopy(src(PRV, 0), XR.at[3, :, cq], left),
                               rcopy(src(NXT, 0), XR.at[4, :, cq], right), rcopy(src(PRV, 1), XR.at[5, :, cq], left)])
            keys.clear()

        def cols(self, q):
            return tile_cols(self.split, q)

        def swap(self, j, q, first):
            cq = self.cols(q)
            return remote(PP.at[j, cp, :, cq], DR.at[j, :, cq], ps.at[q * RING + j], rs.at[first + j], partner)

        def compute(self, j, q):
            self.part(j, sum(self.split[:q]), self.split[q])
            self.pair[q][j].start()

        def compute_all(self, q):
            def body(i, carry):
                j = lax.rem(i + 1, RING)
                self.part(j, sum(self.split[:q]), self.split[q])
                self.swap(j, q, self.first[q]).start()
                return carry
            loop(RING, body, None)

        def combine(self, j, q):
            self.pair[q][j].wait_recv()
            add_rows(PP.at[j, c, :, self.cols(q)], [DR.at[j, :, self.cols(q)]], TB, min(TB, 16))

        def opposite(self, q):
            self.m[q][0].start()
            self.m[q][1].start()

        def side(self, j, q):
            self.combine(j, q)
            self.m[q][2 if j == NXT else 3].start()

        def send(self, q):
            self.combine(OPP, q)
            self.opposite(q)
            self.side(NXT, q)
            self.side(PRV, q)

        def relay(self, q):
            for k, j, h in ((0, NXT, 0), (1, PRV, 1)):
                self.m[q][k].wait_recv()
                add_rows(PP.at[j, c, half(h), self.cols(q)], [XR.at[k, :, self.cols(q)]], HB, min(HB, 16))
                self.m[q][4 + k].start()

        def finish(self, q, res, outs):
            for d in self.m[q][2:]:
                d.wait_recv()
            step, cq = min(HB, 16), self.cols(q)
            for h, (kl, kr) in enumerate(((4, 3), (2, 5))):
                def body(r, carry):
                    lo = pl.ds(mo(r * step, step), step)
                    sl = pl.ds(mo(h * HB + r * step, step), step)
                    tot = PP[OWN, c, sl, cq] + (XR[kl, lo, cq] + XR[kr, lo, cq])
                    val = (res[sl, cq].astype(F32) + tot).astype(BF16)
                    for o in outs:
                        o[sl, cq] = val
                    return carry
                loop(HB // step, body, None)

        def drain(self):
            for d in sum(self.pair + self.m, []):
                d.wait_send()

        def release(self):
            self.drain()
            for k, to in enumerate((self.right, self.left, partner)):
                pl.semaphore_signal(credit.at[k], inc=1, device_id=to, device_id_type=MESH_ID)

        def acquire(self):
            for k in range(len((self.right, self.left, partner))):
                pl.semaphore_wait(credit.at[k], 1)

    def grad_a(j, dst, halves=None):
        t = off(z, j)

        def rows(h, carry):
            lo = [pl.ds(mo((2 * h + q) * XD + t * ZD, ZD), ZD) for q in HALVES]
            lhs = jnp.concatenate([XV[:, :, :, s].reshape(8 * TB, ZD) for s in lo], axis=1)

            def body(n, carry):
                cols = pl.ds(mo(n * ND, ND), ND)
                dst[h, :, :, cols] = dot_tn(lhs, DV[:, :, cols].reshape(8 * TB, ND)).reshape(2, ZD, ND)
                return carry
            return loop(K // ND, body, carry)
        if halves is None:
            loop(2, rows, None)
        else:
            for h in halves:
                rows(h, None)

    def grad_b(gv, j, dst):
        cols_l = pl.ds(mo(off(y, j) * NK, NK), NK)

        def body(m, carry):
            cols = pl.ds(mo(m * ND, ND), ND)
            out = dot_tn(AV[:, :, :, cols_l].reshape(8 * TB, NK), gv[:, :, :, cols].reshape(8 * TB, ND))
            dst[:, m // 2, :, pl.ds(mo(lax.rem(m, 2) * ND, ND), ND)] = out.reshape(2, NK // 2, ND)
            return carry
        loop(RING, body, None)

    grad_keys = [keys_of(sum(u0u, u0a) + d0a), [d.key for d in ex0 + ex1] + keys_of(d0b + d0c)]

    class Reduce4:
        def __init__(self, l, axis, part, recv, stage):
            _, right, left = rings[axis]
            self.part, self.recv, self.stage = part, recv, stage
            which = ((OPP, 0), (OPP, 1), (NXT, 1), (PRV, 0), (NXT, 0), (PRV, 1))
            self.m = [rcopy(part(*which[k]), recv(k), left if k % 2 else right, grad_keys[l].pop())
                      for k in range(ARRIVALS)]
            self.to = [(NXT, 0), (PRV, 1), (OWN, 1), (OWN, 0), (OWN, 0), (OWN, 1)]
            self.loads = [lcopy(recv(k), stage(k)) for k in range(ARRIVALS)] if stage else None

        def opposite(self):
            self.m[0].start()
            self.m[1].start()

        def sides(self, j):
            self.m[2 if j == NXT else 3].start()

        def fetch(self, k):
            self.m[k].wait_send()
            self.m[k].wait_recv()
            if self.loads:
                self.loads[k].start()

        def absorb(self, k):
            if self.loads:
                self.loads[k].wait()
            dst = self.part(*self.to[k])
            add_rows(dst, [(self.stage or self.recv)(k)], dst.shape[1], min(dst.shape[1], 16))

    def arrive(reduces, ks):
        for k in ks:
            for r in reduces:
                r.fetch(k)
        for k in ks:
            for r in reduces:
                r.absorb(k)

    def relay(reduces):
        for k in (0, 1):
            for r in reduces:
                r.fetch(k)
        for k in (0, 1):
            for r in reduces:
                r.absorb(k)
                r.m[4 + k].start()

    EARLY, LATE = (2, 3), (4, 5)
    hq = DR_ROWS // 2
    own_grads = [(SV.at[pl.ds(0, 2)], SV.at[pl.ds(2, 2)]), (GPA.at[OWN], GPB.at[OWN])]

    def make_reduce(l, q, chunks):
        own_a, own_b = own_grads[l]
        ca = pl.ds(q * (K // chunks), K // chunks)
        nb = pl.ds(q, 1) if chunks == 2 else pl.ds(0, 2)
        pick = ((OPP, 0), (OPP, 1), (NXT, 1), (PRV, 0), (NXT, 0), (PRV, 1))

        def part_a(j, h):
            return (own_a.at[h, :, :, ca] if j == OWN else GPA.at[j, h, :, :, ca])

        def part_b(j, h):
            return (own_b.at[h, nb] if j == OWN else GPB.at[j, h, nb])

        def part_a2(j, h):
            return own_a.at[h, :, pl.ds(mo(off(y, j) * 2 * UR, 2 * UR), 2 * UR), ca]

        def part_b2(j, h):
            t = off(z, j)
            return own_b.at[t // 2, nb, pl.ds(mo(lax.rem(t, 2) * DR_ROWS + h * hq, hq), hq), :]
        first = (Reduce4(l, "z", part_a, lambda k: ra1.at[l, k, :, :, ca], lambda k: part_a(*pick[k])),
                 Reduce4(l, "y", part_b, lambda k: rb1.at[l, k, nb], lambda k: part_b(*pick[k])))
        if q:
            def third(k, rows):
                return pl.ds((k // 2) * rows, rows)
            return first + (Reduce4(l, "y", part_a2, lambda k: GPA.at[OWN, k % 2, :, third(k, 2 * UR), ca], None),
                            Reduce4(l, "z", part_b2, lambda k: GPB.at[OWN, k % 2, nb, third(k, hq), :], None))
        return first + (Reduce4(l, "y", part_a2, lambda k: ra2.at[l, k, :, :, ca], lambda k: STA.at[k % 2, :, :, ca]),
                        Reduce4(l, "z", part_b2, lambda k: rb2.at[l, k, nb], lambda k: STB.at[k % 2, nb]))

    def second_start(reduces):
        for r in reduces:
            r.opposite()
            r.sides(NXT)
            r.sides(PRV)

    def grads_out_start(l, q, chunks):
        own_a, own_b = own_grads[l]
        ca = pl.ds(q * (K // chunks), K // chunks)

        def rows_of(tx, tc):
            return own_a.at[tx // 2, lax.rem(tx, 2), pl.ds(mo((2 * y + tc) * UR, UR), UR), ca]
        to = uh.at[l, x, mine, ca]
        sends = [rcopy(rows_of(off(x, dx), cp if dc else c), to, dev(dx=dx, dc=dc), grad_keys[l].pop()) for dx, dc in group]
        local = [lcopy(rows_of(x, c), to)]
        for n in ((q,) if chunks == 2 else HALVES):
            local.append(lcopy(own_b.at[z // 2, n, pl.ds(mo(lax.rem(z, 2) * DR_ROWS, DR_ROWS), DR_ROWS), :],
                               gd_out.at[l, :, pl.ds(n * K, K)]))
        for cpy in sends + local:
            cpy.start()
        return sends, local

    def grads_out_finish(state):
        for cpy in state[0]:
            cpy.wait_recv()
            cpy.wait_send()
        for cpy in state[1]:
            cpy.wait()

    r = Reduce8(functools.partial(down_part, AV), 0, SPLIT3)
    r_keys = sorted([d.key for m in r.m for d in m] + [f + j for f in r.first for j in range(RING)])
    hidden0(off(x, OPP))
    hidden0(off(x, NXT))
    do(d0b, "finish")
    r.compute(OPP, 0)
    r.compute(NXT, 0)
    do(d0c, "forward")
    do(d0d, "start")
    r.combine(OPP, 0)
    r.opposite(0)
    do(sum(u0u, []), "drain")
    hidden0(off(x, PRV))
    r.compute(PRV, 0)
    r.side(NXT, 0)
    do(d1a, "forward")
    hidden0(off(x, OWN))
    r.side(PRV, 0)
    save_s = lcopy(SV, sh0)
    save_s.start()
    save_a0 = lcopy(AV, ah.at[0])
    save_a0.start()
    gg1.sides()
    do(d0c, "finish")
    r.compute_all(1)
    r.relay(0)
    do(d0d, "forward")
    for cpy in ex1:
        cpy.wait_recv()
    own_d1.wait()
    do(u1a, "start")
    r.send(1)
    do(d1a, "finish")
    do(d1b, "start")
    gg1.last()
    save_x.wait()
    do(d0d, "finish")
    save_d0 = lcopy(W, wdh.at[0])
    save_d0.start()
    r.compute(OPP, 2)
    r.relay(1)
    do(u1a, "forward")
    r.compute(NXT, 2)
    r.combine(OPP, 2)
    r.opposite(2)
    r.compute(PRV, 2)
    r.side(NXT, 2)
    r.compute(OWN, 2)
    r.side(PRV, 2)
    r.compute(OWN, 0)
    for q in range(len(SPLIT3)):
        r.combine(OWN, q)

    def gather_keys(gathers):
        return [d.key for g in gathers for d in g.ring.d + g.own + g.push]

    def token_gathers(slot, buf):
        def make(q):
            cq = tile_cols(SPLIT2, q)
            return Gather8(lambda h: RES.at[slot, half(h), cq], lambda b, k, h: buf.at[b, k, half(h), cq])
        return [make(0), make(1)]

    keys.extend(gather_keys((gx0,)))
    gx1 = token_gathers(X1, XV)
    do(d1a, "drain")
    do(d1b, "forward")
    for q in HALVES:
        r.finish(q, RES.at[X0], [RES.at[X1], XV.at[x, c]])
    r.relay(2)
    gx1[0].start()
    do(u1a, "finish")
    do(u1b, "start")
    do(u1c, "start_first")
    gg1.wait_own()
    gg1.wait_push(range(len(gg1.push)))
    own_g.wait()
    save_d0.wait()
    do(d0b + d0c + d0d, "drain")
    gg1.drain()
    do(d1b, "finish")
    load_w1d = lcopy(wdh.at[1], W)
    load_w1d.start()
    r.finish(2, RES.at[X0], [RES.at[X1], XV.at[x, c]])
    gx1[1].start()
    save_s.wait()
    do(u1b, "forward")
    do(u1c, "start_rest")
    load_w1d.wait()
    dact1(off(x, OWN))
    gx1[0].forward()
    r.release()
    dact1(off(x, NXT))
    gx1[0].sides()
    dact1(off(x, PRV))
    do(u1c, "forward")
    save_u0.wait()
    do(u1b, "finish")

    def load_up(n):
        cs = hidden_cols(n)
        return lcopy(wuh.at[1, :, :, :, :, cs], U.at[:, :, :, :, cs])
    load_w1u = [load_up(n) for n in HALVES]
    load_w1u[0].start()
    dact1(off(x, OPP))
    load_w0d_again = lcopy(wdh.at[0], W)
    load_w0d_again.start()
    save_a0.wait()
    do(gx1, "wait_own")
    load_w1u[0].wait()
    hidden1(off(x, OWN), 0)
    gx1[1].forward()
    gx1[0].last()
    gx1[1].sides()
    do(u1c, "finish")
    load_w1u[1].start()
    for g in gx1:
        g.wait_push((0, 2))
    hidden1(off(x, PRV), 0)
    for g in gx1:
        g.wait_push((1, 3))
    hidden1(off(x, NXT), 0)
    load_w1u[1].wait()
    hidden1(off(x, OWN), 1)
    gx1[1].last()
    hidden1(off(x, PRV), 1)
    hidden1(off(x, NXT), 1)
    for g in gx1:
        g.wait_push((4, 5))
    for n in HALVES:
        hidden1(off(x, OPP), n)
    load_s0 = lcopy(sh0, SV)
    load_s0.start()
    save_a1 = lcopy(AV, ah.at[1])
    save_a1.start()

    a1, b1, a2, b2 = make_reduce(1, 0, 1)
    grad_b(GV1, OPP, GPB.at[OPP])
    b1.opposite()
    for h in HALVES:
        grad_a(OPP, GPA.at[OPP], (h,))
        a1.m[h].start()
    r = Reduce8(dx_part, 1, SPLIT2, r_keys)
    r.acquire()
    r.compute(OPP, 0)
    r.compute(NXT, 0)
    r.combine(OPP, 0)
    r.opposite(0)
    r.compute(PRV, 0)
    r.side(NXT, 0)
    r.side(PRV, 0)
    r.compute_all(1)
    load_w0u_again = lcopy(wuh.at[0], U)
    r.compute(OWN, 0)
    load_w0u_again.start()
    grad_b(GV1, NXT, GPB.at[NXT])
    b1.sides(NXT)
    grad_b(GV1, PRV, GPB.at[PRV])
    b1.sides(PRV)
    r.relay(0)
    r.send(1)
    grad_a(NXT, GPA.at[NXT])
    a1.sides(NXT)
    grad_a(PRV, GPA.at[PRV])
    a1.sides(PRV)
    r.combine(OWN, 0)
    r.combine(OWN, 1)
    keys.extend(gather_keys(gx1))
    gg0 = token_gathers(G0, GV0)
    r.relay(1)
    r.finish(0, RES.at[G1], [RES.at[G0], GV0.at[x, c]])
    gg0[0].start()
    relay((b1, a1))
    grad_b(GV1, OWN, GPB.at[OWN])
    save_a1.wait()
    load_a0 = lcopy(ah.at[0], AV)
    load_a0.start()
    do(d1b + u1a + u1b + u1c, "drain")
    load_a1 = lcopy(ah.at[1], GV1.at[:, :, :, 0:K])
    load_a1.start()
    r.finish(1, RES.at[G1], [RES.at[G0], GV0.at[x, c]])
    gg0[1].start()
    gg0[0].forward()
    grad_a(OWN, GPA.at[OWN])
    do(gx1, "drain")
    load_x0 = lcopy(xh0, XV)
    load_x0.start()
    gg0[0].sides()
    r.release()
    gg0[1].forward()
    gg0[0].last()
    load_w0d_again.wait()
    load_s0.wait()
    do(gg0, "wait_own")
    dact0(off(x, OWN))
    gg0[1].sides()
    gg0[1].last()
    for g in gg0:
        g.wait_push((0, 2))
    dact0(off(x, PRV))
    for g in gg0:
        g.wait_push((1, 3))
    dact0(off(x, NXT))
    for g in gg0:
        g.wait_push((4, 5))

    a1n, b1n, a2n, b2n = zip(*[make_reduce(0, q, 2) for q in HALVES])
    load_a0.wait()
    grad_b(GV0, OPP, GPB.at[OPP])
    b1n[0].opposite()
    dact0(off(x, OPP))
    load_w1d_again = lcopy(wdh.at[1], W)
    load_w1d_again.start()
    load_x0.wait()
    for h in HALVES:
        grad_a(OPP, GPA.at[OPP], (h,))
        a1n[0].m[h].start()
    arrive((b1, a1), EARLY + LATE)
    second_start((a2, b2))
    load_w0u_again.wait()
    r = Reduce8(dx_part, 2, WHOLE, r_keys)
    r.acquire()
    r.compute_all(0)
    r.send(0)
    grad_b(GV0, NXT, GPB.at[NXT])
    b1n[0].sides(NXT)
    grad_b(GV0, PRV, GPB.at[PRV])
    b1n[0].sides(PRV)
    grad_a(NXT, GPA.at[NXT])
    a1n[0].sides(NXT)
    grad_a(PRV, GPA.at[PRV])
    a1n[0].sides(PRV)
    relay((b2, a2))
    r.relay(0)
    relay((b1n[0], a1n[0]))
    for red in (b1n[1], a1n[1]):
        red.opposite()
        red.sides(NXT)
        red.sides(PRV)
    r.combine(OWN, 0)
    grad_b(GV0, OWN, own_grads[0][1])
    grad_a(OWN, own_grads[0][0])
    r.finish(0, RES.at[G0], [RES.at[X0]])
    r.release()
    write_gi = lcopy(RES.at[X0], gi_out)
    write_gi.start()
    arrive((b1n[0], a1n[0]), EARLY)
    load_a1.wait()
    load_w1d_again.wait()
    r = Reduce8(functools.partial(down_part, GV1), 3, WHOLE, r_keys)
    r.acquire()
    r.compute_all(0)
    r.send(0)
    arrive((b2, a2), EARLY)
    arrive((b2, a2), LATE)
    state1 = grads_out_start(1, 0, 1)
    r.combine(OWN, 0)
    arrive((b1n[0], a1n[0]), LATE)
    grads_out_finish(state1)
    relay((b1n[1], a1n[1]))
    second_start((a2n[0], b2n[0]))
    r.relay(0)
    arrive((b1n[1], a1n[1]), EARLY)
    arrive((b1n[1], a1n[1]), LATE)
    second_start((a2n[1], b2n[1]))
    relay((b2n[0], a2n[0]))
    arrive((b2n[0], a2n[0]), EARLY)
    relay((b2n[1], a2n[1]))
    arrive((b2n[1], a2n[1]), EARLY)
    arrive((b2n[0], a2n[0]), LATE)
    state0 = [grads_out_start(0, 0, 2)]
    r.finish(0, RES.at[X1], [RES.at[G1]])
    write_y = lcopy(RES.at[G1], y_out)
    write_y.start()
    arrive((b2n[1], a2n[1]), LATE)
    state0.append(grads_out_start(0, 1, 2))
    r.drain()
    do(gg0, "drain")
    write_gi.wait()
    write_y.wait()
    for state in state0:
        grads_out_finish(state)
    assert used["recv"] <= N_RECV and used["send"] <= N_SEND and used["local"] <= N_LOCAL


def finish_kernel(y_in, gi_in, gu_in, gd_in, y_out, gi_out, gu_out, gd_out, ybuf, gibuf, gubuf, gdbuf, gushuf, sems):
    layers, ur, ff = gu_out.shape
    s2 = ff // 64
    half = s2 // 2
    loads = [pltpu.make_async_copy(a, b, sems.at[0, k])
             for k, (a, b) in enumerate(((gu_in, gubuf), (gd_in, gdbuf), (y_in, ybuf), (gi_in, gibuf)))]
    stores = [pltpu.make_async_copy(a, b, sems.at[1, k])
              for k, (a, b) in enumerate(((gushuf, gu_out), (gdbuf, gd_out), (ybuf, y_out), (gibuf, gi_out)))]
    for cpy in loads:
        cpy.start()
    low = lax.broadcasted_iota(jnp.int32, (ur, s2), 1) < half
    swap = lambda v: pltpu.roll(v, half, 1)
    loads[0].wait()
    for l in range(layers):
        for b in range(RING):
            for yy in range(RING):
                for m in HALVES:
                    cols = pl.ds((yy * 2 + m) * s2, s2)
                    t0, t1 = (gubuf[l, b, pl.ds(k * ur, ur), cols] for k in HALVES)
                    strip = (b * RING + 2 * m) * RING + yy
                    gushuf[l, :, pl.ds(strip * s2, s2)] = jnp.where(low, t0, swap(t1))
                    gushuf[l, :, pl.ds((strip + RING) * s2, s2)] = jnp.where(low, swap(t0), t1)
    stores[0].start()
    for k in (1, 2, 3):
        loads[k].wait()
        stores[k].start()
    for cpy in stores:
        cpy.wait()


def solution(mesh, interpret=None):
    fine = Mesh(np.asarray(mesh.devices).reshape(4, 4, 4, 2), ALL)
    tok_spec = P(ALL, None)
    weight_spec = P(None, ALL, None)

    def device_step(x_loc, up_loc, down_loc, g_loc):
        layers, ur, ff = up_loc.shape
        dr, dm = down_loc.shape[1:]
        tb = x_loc.shape[0]
        k = ff // 8
        zd = dm // 16
        hbm = lambda shape, dt: jax.ShapeDtypeStruct(shape, dt)
        outs = [
            hbm((tb, dm), BF16), hbm((tb, dm), BF16), hbm((layers, dr, dm), F32),
            hbm((RING, CORES, tb, dm), BF16),
            hbm((layers, RING, RING, RING, 2 * ur, k), BF16),
            hbm((layers, RING, RING, dr, dm), BF16),
            hbm((RING, CORES, tb, k), F32), hbm((layers, RING, CORES, tb, k), BF16),
            *[hbm((layers, ARRIVALS, CORES, n, k), F32) for n in (zd, zd, 2 * ur, 2 * ur)],
            hbm((layers, RING, 2 * ur, k), F32),
        ]
        vm = pltpu.VMEM
        scratch = [
            vm((RING, RING, RING, 2 * ur, k), BF16), vm((RING, RING, dr, dm), BF16),
            vm((RING, CORES, tb, dm), BF16), vm((RING, CORES, tb, dm), BF16), vm((RING, CORES, tb, dm), BF16),
            vm((RING, CORES, tb, k), F32), vm((RING, CORES, tb, k), BF16), vm((RING, 2 * tb, k), BF16),
            vm((RING, CORES, CORES, zd, k), F32), vm((RING, CORES, CORES, zd, k), F32),
            vm((RING, CORES, tb, dm), F32), vm((4, tb, dm), F32), vm((6, tb // 2, dm), F32),
            vm((4, tb, dm), BF16), vm((CORES, CORES, 2 * ur, k), F32), vm((CORES, CORES, 2 * ur, k), F32),
            *[pltpu.SemaphoreType.DMA((n,)) for n in (N_SEND, N_RECV, N_LOCAL, len(SPLIT3) * RING)],
            pltpu.SemaphoreType.REGULAR((3,)),
        ]
        anyspec = pl.BlockSpec(memory_space=pl.ANY)
        call = pl.pallas_call(
            functools.partial(kernel, (dm, k, tb, ur, dr)),
            out_shape=outs,
            in_specs=[anyspec] * 4,
            out_specs=[anyspec] * len(outs),
            scratch_shapes=scratch,
            compiler_params=pltpu.CompilerParams(collective_id=0, has_side_effects=True, vmem_limit_bytes=67043328),
            name="mlp_stack",
            **({"interpret": interpret} if interpret else {}),
        )
        y_raw, gi_raw, gd_raw, *_, gu_raw = call(x_loc, up_loc, down_loc, g_loc)
        raws = (y_raw, gi_raw, gu_raw, gd_raw)
        outs = [hbm((tb, dm), BF16), hbm((tb, dm), BF16), hbm((layers, ur, ff), F32), hbm((layers, dr, dm), F32)]
        return tuple(pl.pallas_call(
            finish_kernel, out_shape=outs, in_specs=[anyspec] * len(outs), out_specs=[anyspec] * len(outs),
            scratch_shapes=[vm(v.shape, v.dtype) for v in raws] + [vm(outs[2].shape, F32), pltpu.SemaphoreType.DMA((2, len(outs)))],
            name="write_out")(*raws))

    return jax.shard_map(device_step, mesh=fine, in_specs=(tok_spec, weight_spec, weight_spec, tok_spec),
                         out_specs=(tok_spec, tok_spec, weight_spec, weight_spec), check_vma=False)
```

```python
import functools

import jax
import jax.numpy as jnp
import numpy as np
from jax import lax
from jax.experimental import pallas as pl
from jax.experimental.pallas import tpu as pltpu
from jax.sharding import Mesh, PartitionSpec as P

MESH_ID = pl.DeviceIdType.MESH
ALL = ("x", "z", "y", "c")
F32, BF16 = jnp.float32, jnp.bfloat16
RING, CORES, ARRIVALS = 4, 2, 6
OWN, NXT, OPP, PRV = range(RING)
X0, X1, G1, G0 = range(RING)
HALVES = (0, 1)
WHOLE, SPLIT2, SPLIT3 = (4,), (2, 2), (1, 1, 2)
N_RECV, N_SEND, N_LOCAL = 182, 110, 15


def gelu_parts(pre_act):
    norm_cdf = 0.5 * (1.0 + lax.erf(pre_act * (2.0 ** -0.5)))
    norm_pdf = jnp.exp(-0.5 * pre_act * pre_act) * ((2.0 * jnp.pi) ** -0.5)
    return pre_act * norm_cdf, norm_cdf + pre_act * norm_pdf


def loop(n, body, init):
    return lax.fori_loop(0, n, body, init)


def dot_nn(left, right):
    return lax.dot_general(left, right, (((1,), (0,)), ((), ())), preferred_element_type=F32)


def dot_nt(left, right):
    return lax.dot_general(left, right, (((1,), (1,)), ((), ())), preferred_element_type=F32)


def dot_tn(left, right):
    return lax.dot_general(left, right, (((0,), (0,)), ((), ())), preferred_element_type=F32)


def kernel(dims, x_in, wu_in, wd_in, g_in,
           y_out, gi_out, gd_out,
           xh0, wuh, wdh, sh0, ah, ra1, rb1, ra2, rb2, uh,
           U, W, XV, GV1, GV0, SV, AV, DV, GPA, GPB, PP, DR, XR, RES, STA, STB,
           ss, rs, ls, ps, credit):
    D, K, TB, UR, DR_ROWS = dims
    HB = TB // 2
    x, z, y, c = (lax.axis_index(a) for a in ALL)
    cp = 1 - c
    S2 = 2 * DR_ROWS
    XD = D // 4
    ZD = D // 16

    def dev(dx=0, dz=0, dy=0, dc=0):
        wrap = lambda v, d, n: v if d == 0 else lax.rem(v + (d % n), n)
        return (wrap(x, dx, 4), wrap(z, dz, 4), wrap(y, dy, 4), wrap(c, dc, 2))

    partner = dev(dc=1)
    rings = {"x": (x, dev(dx=1), dev(dx=-1)), "z": (z, dev(dz=1), dev(dz=-1)), "y": (y, dev(dy=1), dev(dy=-1))}
    off = lambda v, d: v if d == 0 else lax.rem(v + d, 4)

    used = {"recv": 0, "send": 0, "local": 0}
    free = {"send": [], "local": []}
    keys = []

    def fresh(kind):
        if kind == "recv" and keys:
            return keys.pop()
        used[kind] += 1
        return used[kind] - 1

    def take(kind):
        return free[kind].pop() if free[kind] else fresh(kind)

    def remote(src, dst, send, recv, to):
        return pltpu.make_async_remote_copy(src_ref=src, dst_ref=dst, send_sem=send, recv_sem=recv,
                                            device_id=to, device_id_type=MESH_ID)

    class rcopy:
        def __init__(self, src, dst, to, key=None):
            self.args, self.key = (src, dst, to), fresh("recv") if key is None else key

        def start(self):
            src, dst, to = self.args
            self.sem = take("send")
            self.d = remote(src, dst, ss.at[self.sem], rs.at[self.key], to)
            self.d.start()

        def wait_recv(self):
            self.d.wait_recv()

        def wait_send(self):
            self.d.wait_send()
            free["send"].append(self.sem)

    class lcopy:
        def __init__(self, src, dst):
            self.args = src, dst

        def start(self):
            self.sem = take("local")
            self.d = pltpu.make_async_copy(*self.args, ls.at[self.sem])
            self.d.start()

        def wait(self):
            self.d.wait()
            free["local"].append(self.sem)

    def mo(v, m):
        return pl.multiple_of(v, m)

    class Gather4:
        def __init__(self, axis, src, dst):
            i, right, left = rings[axis]
            lft, rgt = off(i, 3), off(i, 1)
            self.d = [rcopy(src(0), dst(i, 0), right), rcopy(src(1), dst(i, 1), right),
                      rcopy(src(0), dst(i, 0), left), rcopy(src(1), dst(i, 1), left),
                      rcopy(dst(lft, 0), dst(lft, 0), right), rcopy(dst(rgt, 1), dst(rgt, 1), left)]

        def start_first(self):
            self.d[0].start()
            self.d[3].start()

        def start_rest(self):
            self.d[1].start()
            self.d[2].start()

        def start(self):
            self.start_first()
            self.start_rest()

        def forward(self):
            for k in HALVES:
                self.d[3 * k].wait_recv()
                self.d[4 + k].start()

        def neighbours(self):
            self.d[1].wait_recv()
            self.d[2].wait_recv()

        def opposite(self):
            self.d[4].wait_recv()
            self.d[5].wait_recv()

        def finish(self):
            self.neighbours()
            self.opposite()

        def drain(self):
            for d in self.d:
                d.wait_send()

    class Gather8:
        def __init__(self, src, dst):
            self.ring = Gather4("x", src, lambda b, h: dst(b, c, h))
            lft, rgt, opp = off(x, PRV), off(x, NXT), off(x, OPP)
            blocks = [(lft, 0), (rgt, 1), (lft, 1), (rgt, 0), (opp, 0), (opp, 1)]
            self.own = [rcopy(src(h), dst(x, c, h), partner) for h in HALVES]
            self.push = [rcopy(dst(b, c, h), dst(b, c, h), partner) for b, h in blocks]

        def start(self):
            self.ring.start()
            for d in self.own:
                d.start()

        def forward(self):
            self.ring.forward()
            self.push[0].start()
            self.push[1].start()

        def sides(self):
            self.ring.d[1].wait_recv()
            self.push[2].start()
            self.ring.d[2].wait_recv()
            self.push[3].start()

        def last(self):
            self.ring.d[4].wait_recv()
            self.push[4].start()
            self.ring.d[5].wait_recv()
            self.push[5].start()

        def wait_own(self):
            for d in self.own:
                d.wait_recv()

        def wait_push(self, ks):
            for k in ks:
                self.push[k].wait_recv()

        def drain(self):
            self.ring.drain()
            for d in self.own + self.push:
                d.wait_send()

    def add_rows(dst, srcs, rows, step):
        def body(r, carry):
            sl = pl.ds(mo(r * step, step), step)
            if len(dst.shape) == 3:
                for q in range(dst.shape[0]):
                    acc = dst[q, sl, :]
                    for s in srcs:
                        acc = acc + s[q, sl, :]
                    dst[q, sl, :] = acc
            else:
                acc = dst[sl, :]
                for s in srcs:
                    acc = acc + s[sl, :]
                dst[sl, :] = acc
            return carry
        loop(rows // step, body, None)

    barrier = pltpu.get_barrier_semaphore()
    group = [(dx, dc) for dx in range(RING) for dc in HALVES if dx or dc]
    peers = [dev(dx=dx, dc=dc) for dx, dc in group] + [rings[a][k] for a in "zy" for k in (1, 2)]
    for p in peers:
        pl.semaphore_signal(barrier, inc=1, device_id=p, device_id_type=MESH_ID)

    load_u = [[lcopy(wu_in.at[l, :, pl.ds(b * D, D)], RES.at[G0, pl.ds((l * RING + b) * UR, UR), :])
               for b in range(RING)] for l in HALVES]
    load_d = [lcopy(wd_in.at[l], RES.at[X1, pl.ds(l * DR_ROWS, DR_ROWS), :]) for l in HALVES]
    load_x = lcopy(x_in, RES.at[X0])
    load_g = lcopy(g_in, RES.at[G1])
    own_x = lcopy(x_in, XV.at[x, c])
    own_g = lcopy(g_in, GV1.at[x, c])
    own_d0 = lcopy(wd_in.at[0], W.at[y, z])
    for cpy in load_u[0] + load_u[1] + load_d + [load_x, own_d0, own_x, load_g, own_g]:
        cpy.start()

    low = lax.broadcasted_iota(jnp.int32, (UR, S2), 1) < DR_ROWS
    swap = lambda v: pltpu.roll(v, DR_ROWS, 1)
    for l in HALVES:
        for cpy in load_u[l]:
            cpy.wait()
        for b in range(RING):
            rows = pl.ds((l * RING + b) * UR, UR)
            for yy in range(RING):
                for m in HALVES:
                    s0 = RES[G0, rows, pl.ds((2 * m * RING + yy) * S2, S2)].astype(F32)
                    s1 = RES[G0, rows, pl.ds(((2 * m + 1) * RING + yy) * S2, S2)].astype(F32)
                    cols = pl.ds((yy * 2 + m) * S2, S2)
                    AV[l, 0, pl.ds(2 * b * UR, UR), cols] = jnp.where(low, s0, swap(s1)).astype(BF16)
                    AV[l, 0, pl.ds((2 * b + 1) * UR, UR), cols] = jnp.where(low, swap(s0), s1).astype(BF16)
    for cpy in load_d + [load_x, own_d0]:
        cpy.wait()
    pl.semaphore_wait(barrier, len(peers))

    half = lambda h: pl.ds(h * HB, HB)

    def tile_cols(split, q):
        return pl.ds(sum(split[:q]) * (D // RING), split[q] * (D // RING))

    gx0 = Gather8(lambda h: RES.at[X0, half(h)], lambda b, k, h: XV.at[b, k, half(h)])
    gg1 = Gather8(lambda h: RES.at[G1, half(h)], lambda b, k, h: GV1.at[b, k, half(h)])
    up = [U, wuh.at[1]]
    down = [W, wdh.at[1]]
    hr = DR_ROWS // 4

    def quarter(q, h):
        return pl.ds((2 * q + h) * hr, hr)

    def down_first(l):
        to = down[l]
        src = lambda q: lambda h: RES.at[X1, pl.ds(l * DR_ROWS + (2 * q + h) * hr, hr)]
        return [Gather4("z", src(0), lambda b, h: to.at[y, b, quarter(0, h)]),
                Gather4("y", src(1), lambda b, h: to.at[b, z, quarter(1, h)])]

    def down_second(l, split, n):
        to, cs = down[l], tile_cols(split, n)
        return [Gather4("y", lambda h: to.at[y, :, quarter(0, h), cs], lambda b, h: to.at[b, :, quarter(0, h), cs]),
                Gather4("z", lambda h: to.at[:, z, quarter(1, h), cs], lambda b, h: to.at[:, b, quarter(1, h), cs])]

    def up_first(to):
        return [Gather4("y", lambda h: to.at[h, z, y], lambda b, h: to.at[h, z, b]),
                Gather4("z", lambda h: to.at[2 + h, z, y], lambda b, h: to.at[2 + h, b, y])]

    def hidden_cols(n):
        return pl.ds(sum(SPLIT2[:n]) * (K // RING), SPLIT2[n] * (K // RING))

    def up_second(to, n):
        cs = hidden_cols(n)
        return [Gather4("z", lambda h: to.at[h, z, :, :, cs], lambda b, h: to.at[h, b, :, :, cs]),
                Gather4("y", lambda h: to.at[2 + h, :, y, :, cs], lambda b, h: to.at[2 + h, :, b, :, cs])]

    def up_unit(to, j):
        yj, zj = off(y, j), off(z, j)
        return [Gather4("z", lambda h: to.at[h, z, yj], lambda b, h: to.at[h, b, yj]),
                Gather4("y", lambda h: to.at[2 + h, zj, y], lambda b, h: to.at[2 + h, zj, b])]

    def do(gathers, step):
        for g in gathers:
            getattr(g, step)()

    mine = pl.ds(mo(c * UR, UR), UR)

    def up_exchange(l):
        sends = []
        for dx, dc in group:
            tx, tc = off(x, dx), (cp if dc else c)
            src = AV.at[l, 0, pl.ds(mo((tx * 2 + tc) * UR, UR), UR), :]
            sends.append(rcopy(src, up[l].at[x, z, y, mine, :], dev(dx=dx, dc=dc)))
        for cpy in sends:
            cpy.start()
        return sends

    def keys_of(gathers):
        return [d.key for g in gathers for d in g.d]

    d0a, d0b, d0c = down_first(0), down_second(0, SPLIT3, 0), down_second(0, SPLIT3, 1)
    u0a, u0u = up_first(up[0]), [up_unit(up[0], j) for j in (OWN, PRV, NXT, OPP)]
    keys.extend(keys_of(u0a))
    d0d = down_second(0, SPLIT3, 2)
    keys.extend(keys_of(d0a))
    d1a = down_first(1)
    keys.extend(keys_of(sum(u0u, [])))
    d1b, u1a = down_second(1, WHOLE, 0), up_first(up[1])
    u1b, u1c = up_second(up[1], 0), up_second(up[1], 1)
    ex0 = up_exchange(0)
    do(d0a, "start")
    gx0.start()
    ex1 = up_exchange(1)
    my_rows = pl.ds(mo((x * 2 + c) * UR, UR), UR)
    own_u1 = lcopy(AV.at[1, 0, my_rows, :], up[1].at[x, z, y, mine, :])
    own_u1.start()
    own_d1 = lcopy(RES.at[X1, pl.ds(DR_ROWS, DR_ROWS), :], down[1].at[y, z])
    own_d1.start()
    U[x, z, y, mine, :] = AV[0, 0, my_rows, :]
    do(d0a, "forward")
    for cpy in ex0:
        cpy.wait_recv()
    do(u0a, "start")
    do(u0u[0], "start")
    do(u0a, "forward")
    gx0.forward()
    load_g.wait()
    gg1.start()
    do(u0a, "neighbours")
    do(u0u[1], "start")
    do(u0u[2], "start")
    do(u0u[0], "forward")
    do(u0a, "opposite")
    do(u0u[3], "start")
    do(d0a, "finish")
    do(u0u[1], "forward")
    do(u0u[2], "forward")
    do(d0b, "start_first")
    gx0.sides()
    for cpy in ex0 + ex1:
        cpy.wait_send()
    own_u1.wait()
    do(u0u[3], "forward")
    do(u0a + d0a, "drain")
    do(d0b, "start_rest")
    do(d0c, "start_first")
    gg1.forward()
    do(d0b, "forward")
    do(d0c, "start_rest")
    do(d1a, "start")
    gx0.last()
    gx0.wait_own()
    gx0.wait_push(range(len(gx0.push)))
    own_x.wait()
    save_x = lcopy(XV, xh0)
    save_x.start()
    gx0.drain()
    for unit in u0u:
        do(unit, "finish")
    save_u0 = lcopy(U, wuh.at[0])
    save_u0.start()

    T2 = 2 * TB
    ND = D // 4
    NK = K // 4

    def up_tile(t, n):
        cols = pl.ds(mo(n * NK, NK), NK)
        return dot_nn(XV[t].reshape(T2, D), U[:, :, :, :, cols].reshape(D, NK)), cols

    def hidden0(t):
        for n in range(RING):
            pre, cols = up_tile(t, n)
            act, slope = gelu_parts(pre)
            AV[t, :, :, cols] = act.astype(BF16).reshape(2, TB, NK)
            SV[t, :, :, cols] = slope.reshape(2, TB, NK)

    def hidden1(t, part):
        for n in range(sum(SPLIT2[:part]), sum(SPLIT2[:part + 1])):
            pre, cols = up_tile(t, n)
            act, slope = gelu_parts(pre)
            AV[t, :, :, cols] = act.astype(BF16).reshape(2, TB, NK)
            DV[t, :, cols] = (SV[t, :, :, cols].reshape(T2, NK) * slope).astype(BF16)

    def dact(gv, t, n):
        return dot_nt(gv[t].reshape(T2, D), W[n].reshape(NK, D))

    def dact1(t):
        def body(n, carry):
            SV[t, :, :, pl.ds(mo(n * NK, NK), NK)] = dact(GV1, t, n).reshape(2, TB, NK)
            return carry
        loop(RING, body, None)

    def dact0(t):
        def body(n, carry):
            cols = pl.ds(mo(n * NK, NK), NK)
            DV[t, :, cols] = (dact(GV0, t, n) * SV[t, :, :, cols].reshape(T2, NK)).astype(BF16)
            return carry
        loop(RING, body, None)

    def down_part(act, j, lo, tiles):
        t = lax.rem(x + j, RING)

        def body(n, carry):
            cols = pl.ds(mo((lo + n) * ND, ND), ND)
            PP[j, :, :, cols] = dot_nn(act[t, :, :, 0:K].reshape(T2, K), W[:, :, :, cols].reshape(K, ND)).reshape(2, TB, ND)
            return carry
        loop(tiles, body, None)

    def dx_part(j, lo, tiles):
        t = lax.rem(x + j, RING)

        def body(n, carry):
            cols = pl.ds(mo((lo + n) * ND, ND), ND)
            PP[j, :, :, cols] = dot_nt(DV[t], U[lo + n].reshape(ND, K)).reshape(2, TB, ND)
            return carry
        loop(tiles, body, None)

    class Reduce8:
        def __init__(self, part, index, split, old=()):
            self.part, self.index, self.split = part, index, split
            keys.extend(old)
            _, right, left = rings["x"]
            self.right, self.left = right, left
            self.pair, self.m, self.first = [], [], []
            for q in range(len(split)):
                cq = self.cols(q)
                first = sorted(fresh("recv") for j in range(RING))
                self.pair.append([self.swap(j, q, first[0]) for j in range(RING)])
                self.first.append(first[0])
                src = lambda j, h: PP.at[j, c, half(h), cq]
                self.m.append([rcopy(src(OPP, 0), XR.at[0, :, cq], right), rcopy(src(OPP, 1), XR.at[1, :, cq], left),
                               rcopy(src(NXT, 1), XR.at[2, :, cq], right), rcopy(src(PRV, 0), XR.at[3, :, cq], left),
                               rcopy(src(NXT, 0), XR.at[4, :, cq], right), rcopy(src(PRV, 1), XR.at[5, :, cq], left)])
            keys.clear()

        def cols(self, q):
            return tile_cols(self.split, q)

        def swap(self, j, q, first):
            cq = self.cols(q)
            return remote(PP.at[j, cp, :, cq], DR.at[j, :, cq], ps.at[q * RING + j], rs.at[first + j], partner)

        def compute(self, j, q):
            self.part(j, sum(self.split[:q]), self.split[q])
            self.pair[q][j].start()

        def compute_all(self, q):
            def body(i, carry):
                j = lax.rem(i + 1, RING)
                self.part(j, sum(self.split[:q]), self.split[q])
                self.swap(j, q, self.first[q]).start()
                return carry
            loop(RING, body, None)

        def combine(self, j, q):
            self.pair[q][j].wait_recv()
            add_rows(PP.at[j, c, :, self.cols(q)], [DR.at[j, :, self.cols(q)]], TB, min(TB, 16))

        def opposite(self, q):
            self.m[q][0].start()
            self.m[q][1].start()

        def side(self, j, q):
            self.combine(j, q)
            self.m[q][2 if j == NXT else 3].start()

        def send(self, q):
            self.combine(OPP, q)
            self.opposite(q)
            self.side(NXT, q)
            self.side(PRV, q)

        def relay(self, q):
            for k, j, h in ((0, NXT, 0), (1, PRV, 1)):
                self.m[q][k].wait_recv()
                add_rows(PP.at[j, c, half(h), self.cols(q)], [XR.at[k, :, self.cols(q)]], HB, min(HB, 16))
                self.m[q][4 + k].start()

        def finish(self, q, res, outs):
            for d in self.m[q][2:]:
                d.wait_recv()
            step, cq = min(HB, 16), self.cols(q)
            for h, (kl, kr) in enumerate(((4, 3), (2, 5))):
                def body(r, carry):
                    lo = pl.ds(mo(r * step, step), step)
                    sl = pl.ds(mo(h * HB + r * step, step), step)
                    tot = PP[OWN, c, sl, cq] + (XR[kl, lo, cq] + XR[kr, lo, cq])
                    val = (res[sl, cq].astype(F32) + tot).astype(BF16)
                    for o in outs:
                        o[sl, cq] = val
                    return carry
                loop(HB // step, body, None)

        def drain(self):
            for d in sum(self.pair + self.m, []):
                d.wait_send()

        def release(self):
            self.drain()
            for k, to in enumerate((self.right, self.left, partner)):
                pl.semaphore_signal(credit.at[k], inc=1, device_id=to, device_id_type=MESH_ID)

        def acquire(self):
            for k in range(len((self.right, self.left, partner))):
                pl.semaphore_wait(credit.at[k], 1)

    def grad_a(j, dst, halves=None):
        t = off(z, j)

        def rows(h, carry):
            lo = [pl.ds(mo((2 * h + q) * XD + t * ZD, ZD), ZD) for q in HALVES]
            lhs = jnp.concatenate([XV[:, :, :, s].reshape(8 * TB, ZD) for s in lo], axis=1)

            def body(n, carry):
                cols = pl.ds(mo(n * ND, ND), ND)
                dst[h, :, :, cols] = dot_tn(lhs, DV[:, :, cols].reshape(8 * TB, ND)).reshape(2, ZD, ND)
                return carry
            return loop(K // ND, body, carry)
        if halves is None:
            loop(2, rows, None)
        else:
            for h in halves:
                rows(h, None)

    def grad_b(gv, j, dst):
        cols_l = pl.ds(mo(off(y, j) * NK, NK), NK)

        def body(m, carry):
            cols = pl.ds(mo(m * ND, ND), ND)
            out = dot_tn(AV[:, :, :, cols_l].reshape(8 * TB, NK), gv[:, :, :, cols].reshape(8 * TB, ND))
            dst[:, m // 2, :, pl.ds(mo(lax.rem(m, 2) * ND, ND), ND)] = out.reshape(2, NK // 2, ND)
            return carry
        loop(RING, body, None)

    grad_keys = [keys_of(sum(u0u, u0a) + d0a), [d.key for d in ex0 + ex1] + keys_of(d0b + d0c)]

    class Reduce4:
        def __init__(self, l, axis, part, recv, stage):
            _, right, left = rings[axis]
            self.part, self.recv, self.stage = part, recv, stage
            which = ((OPP, 0), (OPP, 1), (NXT, 1), (PRV, 0), (NXT, 0), (PRV, 1))
            self.m = [rcopy(part(*which[k]), recv(k), left if k % 2 else right, grad_keys[l].pop())
                      for k in range(ARRIVALS)]
            self.to = [(NXT, 0), (PRV, 1), (OWN, 1), (OWN, 0), (OWN, 0), (OWN, 1)]
            self.loads = [lcopy(recv(k), stage(k)) for k in range(ARRIVALS)] if stage else None

        def opposite(self):
            self.m[0].start()
            self.m[1].start()

        def sides(self, j):
            self.m[2 if j == NXT else 3].start()

        def fetch(self, k):
            self.m[k].wait_send()
            self.m[k].wait_recv()
            if self.loads:
                self.loads[k].start()

        def absorb(self, k):
            if self.loads:
                self.loads[k].wait()
            dst = self.part(*self.to[k])
            add_rows(dst, [(self.stage or self.recv)(k)], dst.shape[1], min(dst.shape[1], 16))

    def arrive(reduces, ks):
        for k in ks:
            for r in reduces:
                r.fetch(k)
        for k in ks:
            for r in reduces:
                r.absorb(k)

    def relay(reduces):
        for k in (0, 1):
            for r in reduces:
                r.fetch(k)
        for k in (0, 1):
            for r in reduces:
                r.absorb(k)
                r.m[4 + k].start()

    EARLY, LATE = (2, 3), (4, 5)
    hq = DR_ROWS // 2
    own_grads = [(SV.at[pl.ds(0, 2)], SV.at[pl.ds(2, 2)]), (GPA.at[OWN], GPB.at[OWN])]

    def make_reduce(l, q, chunks):
        own_a, own_b = own_grads[l]
        ca = pl.ds(q * (K // chunks), K // chunks)
        nb = pl.ds(q, 1) if chunks == 2 else pl.ds(0, 2)
        pick = ((OPP, 0), (OPP, 1), (NXT, 1), (PRV, 0), (NXT, 0), (PRV, 1))

        def part_a(j, h):
            return (own_a.at[h, :, :, ca] if j == OWN else GPA.at[j, h, :, :, ca])

        def part_b(j, h):
            return (own_b.at[h, nb] if j == OWN else GPB.at[j, h, nb])

        def part_a2(j, h):
            return own_a.at[h, :, pl.ds(mo(off(y, j) * 2 * UR, 2 * UR), 2 * UR), ca]

        def part_b2(j, h):
            t = off(z, j)
            return own_b.at[t // 2, nb, pl.ds(mo(lax.rem(t, 2) * DR_ROWS + h * hq, hq), hq), :]
        first = (Reduce4(l, "z", part_a, lambda k: ra1.at[l, k, :, :, ca], lambda k: part_a(*pick[k])),
                 Reduce4(l, "y", part_b, lambda k: rb1.at[l, k, nb], lambda k: part_b(*pick[k])))
        if q:
            def third(k, rows):
                return pl.ds((k // 2) * rows, rows)
            return first + (Reduce4(l, "y", part_a2, lambda k: GPA.at[OWN, k % 2, :, third(k, 2 * UR), ca], None),
                            Reduce4(l, "z", part_b2, lambda k: GPB.at[OWN, k % 2, nb, third(k, hq), :], None))
        return first + (Reduce4(l, "y", part_a2, lambda k: ra2.at[l, k, :, :, ca], lambda k: STA.at[k % 2, :, :, ca]),
                        Reduce4(l, "z", part_b2, lambda k: rb2.at[l, k, nb], lambda k: STB.at[k % 2, nb]))

    def second_start(reduces):
        for r in reduces:
            r.opposite()
            r.sides(NXT)
            r.sides(PRV)

    def grads_out_start(l, q, chunks):
        own_a, own_b = own_grads[l]
        ca = pl.ds(q * (K // chunks), K // chunks)

        def rows_of(tx, tc):
            return own_a.at[tx // 2, lax.rem(tx, 2), pl.ds(mo((2 * y + tc) * UR, UR), UR), ca]
        to = uh.at[l, x, mine, ca]
        sends = [rcopy(rows_of(off(x, dx), cp if dc else c), to, dev(dx=dx, dc=dc), grad_keys[l].pop()) for dx, dc in group]
        local = [lcopy(rows_of(x, c), to)]
        for n in ((q,) if chunks == 2 else HALVES):
            local.append(lcopy(own_b.at[z // 2, n, pl.ds(mo(lax.rem(z, 2) * DR_ROWS, DR_ROWS), DR_ROWS), :],
                               gd_out.at[l, :, pl.ds(n * K, K)]))
        for cpy in sends + local:
            cpy.start()
        return sends, local

    def grads_out_finish(state):
        for cpy in state[0]:
            cpy.wait_recv()
            cpy.wait_send()
        for cpy in state[1]:
            cpy.wait()

    r = Reduce8(functools.partial(down_part, AV), 0, SPLIT3)
    r_keys = sorted([d.key for m in r.m for d in m] + [f + j for f in r.first for j in range(RING)])
    hidden0(off(x, OPP))
    hidden0(off(x, NXT))
    do(d0b, "finish")
    r.compute(OPP, 0)
    r.compute(NXT, 0)
    do(d0c, "forward")
    do(d0d, "start")
    r.combine(OPP, 0)
    r.opposite(0)
    do(sum(u0u, []), "drain")
    hidden0(off(x, PRV))
    r.compute(PRV, 0)
    r.side(NXT, 0)
    do(d1a, "forward")
    hidden0(off(x, OWN))
    r.side(PRV, 0)
    save_s = lcopy(SV, sh0)
    save_s.start()
    save_a0 = lcopy(AV, ah.at[0])
    save_a0.start()
    gg1.sides()
    do(d0c, "finish")
    r.compute_all(1)
    r.relay(0)
    do(d0d, "forward")
    for cpy in ex1:
        cpy.wait_recv()
    own_d1.wait()
    do(u1a, "start")
    r.send(1)
    do(d1a, "finish")
    do(d1b, "start")
    gg1.last()
    save_x.wait()
    do(d0d, "finish")
    save_d0 = lcopy(W, wdh.at[0])
    save_d0.start()
    r.compute(OPP, 2)
    r.relay(1)
    do(u1a, "forward")
    r.compute(NXT, 2)
    r.combine(OPP, 2)
    r.opposite(2)
    r.compute(PRV, 2)
    r.side(NXT, 2)
    r.compute(OWN, 2)
    r.side(PRV, 2)
    r.compute(OWN, 0)
    for q in range(len(SPLIT3)):
        r.combine(OWN, q)

    def gather_keys(gathers):
        return [d.key for g in gathers for d in g.ring.d + g.own + g.push]

    def token_gathers(slot, buf):
        def make(q):
            cq = tile_cols(SPLIT2, q)
            return Gather8(lambda h: RES.at[slot, half(h), cq], lambda b, k, h: buf.at[b, k, half(h), cq])
        return [make(0), make(1)]

    keys.extend(gather_keys((gx0,)))
    gx1 = token_gathers(X1, XV)
    do(d1a, "drain")
    do(d1b, "forward")
    for q in HALVES:
        r.finish(q, RES.at[X0], [RES.at[X1], XV.at[x, c]])
    r.relay(2)
    gx1[0].start()
    do(u1a, "finish")
    do(u1b, "start")
    do(u1c, "start_first")
    gg1.wait_own()
    gg1.wait_push(range(len(gg1.push)))
    own_g.wait()
    save_d0.wait()
    do(d0b + d0c + d0d, "drain")
    gg1.drain()
    do(d1b, "finish")
    load_w1d = lcopy(wdh.at[1], W)
    load_w1d.start()
    r.finish(2, RES.at[X0], [RES.at[X1], XV.at[x, c]])
    gx1[1].start()
    save_s.wait()
    do(u1b, "forward")
    do(u1c, "start_rest")
    load_w1d.wait()
    dact1(off(x, OWN))
    gx1[0].forward()
    r.release()
    dact1(off(x, NXT))
    gx1[0].sides()
    dact1(off(x, PRV))
    do(u1c, "forward")
    save_u0.wait()
    do(u1b, "finish")

    def load_up(n):
        cs = hidden_cols(n)
        return lcopy(wuh.at[1, :, :, :, :, cs], U.at[:, :, :, :, cs])
    load_w1u = [load_up(n) for n in HALVES]
    load_w1u[0].start()
    dact1(off(x, OPP))
    load_w0d_again = lcopy(wdh.at[0], W)
    load_w0d_again.start()
    save_a0.wait()
    do(gx1, "wait_own")
    load_w1u[0].wait()
    hidden1(off(x, OWN), 0)
    gx1[1].forward()
    gx1[0].last()
    gx1[1].sides()
    do(u1c, "finish")
    load_w1u[1].start()
    for g in gx1:
        g.wait_push((0, 2))
    hidden1(off(x, PRV), 0)
    for g in gx1:
        g.wait_push((1, 3))
    hidden1(off(x, NXT), 0)
    load_w1u[1].wait()
    hidden1(off(x, OWN), 1)
    gx1[1].last()
    hidden1(off(x, PRV), 1)
    hidden1(off(x, NXT), 1)
    for g in gx1:
        g.wait_push((4, 5))
    for n in HALVES:
        hidden1(off(x, OPP), n)
    load_s0 = lcopy(sh0, SV)
    load_s0.start()
    save_a1 = lcopy(AV, ah.at[1])
    save_a1.start()

    a1, b1, a2, b2 = make_reduce(1, 0, 1)
    grad_b(GV1, OPP, GPB.at[OPP])
    b1.opposite()
    for h in HALVES:
        grad_a(OPP, GPA.at[OPP], (h,))
        a1.m[h].start()
    r = Reduce8(dx_part, 1, SPLIT2, r_keys)
    r.acquire()
    r.compute(OPP, 0)
    r.compute(NXT, 0)
    r.combine(OPP, 0)
    r.opposite(0)
    r.compute(PRV, 0)
    r.side(NXT, 0)
    r.side(PRV, 0)
    r.compute_all(1)
    load_w0u_again = lcopy(wuh.at[0], U)
    r.compute(OWN, 0)
    load_w0u_again.start()
    grad_b(GV1, NXT, GPB.at[NXT])
    b1.sides(NXT)
    grad_b(GV1, PRV, GPB.at[PRV])
    b1.sides(PRV)
    r.relay(0)
    r.send(1)
    grad_a(NXT, GPA.at[NXT])
    a1.sides(NXT)
    grad_a(PRV, GPA.at[PRV])
    a1.sides(PRV)
    r.combine(OWN, 0)
    r.combine(OWN, 1)
    keys.extend(gather_keys(gx1))
    gg0 = token_gathers(G0, GV0)
    r.relay(1)
    r.finish(0, RES.at[G1], [RES.at[G0], GV0.at[x, c]])
    gg0[0].start()
    relay((b1, a1))
    grad_b(GV1, OWN, GPB.at[OWN])
    save_a1.wait()
    load_a0 = lcopy(ah.at[0], AV)
    load_a0.start()
    do(d1b + u1a + u1b + u1c, "drain")
    load_a1 = lcopy(ah.at[1], GV1.at[:, :, :, 0:K])
    load_a1.start()
    r.finish(1, RES.at[G1], [RES.at[G0], GV0.at[x, c]])
    gg0[1].start()
    gg0[0].forward()
    grad_a(OWN, GPA.at[OWN])
    do(gx1, "drain")
    load_x0 = lcopy(xh0, XV)
    load_x0.start()
    gg0[0].sides()
    r.release()
    gg0[1].forward()
    gg0[0].last()
    load_w0d_again.wait()
    load_s0.wait()
    do(gg0, "wait_own")
    dact0(off(x, OWN))
    gg0[1].sides()
    gg0[1].last()
    for g in gg0:
        g.wait_push((0, 2))
    dact0(off(x, PRV))
    for g in gg0:
        g.wait_push((1, 3))
    dact0(off(x, NXT))
    for g in gg0:
        g.wait_push((4, 5))

    a1n, b1n, a2n, b2n = zip(*[make_reduce(0, q, 2) for q in HALVES])
    load_a0.wait()
    grad_b(GV0, OPP, GPB.at[OPP])
    b1n[0].opposite()
    dact0(off(x, OPP))
    load_w1d_again = lcopy(wdh.at[1], W)
    load_w1d_again.start()
    load_x0.wait()
    for h in HALVES:
        grad_a(OPP, GPA.at[OPP], (h,))
        a1n[0].m[h].start()
    arrive((b1, a1), EARLY + LATE)
    second_start((a2, b2))
    load_w0u_again.wait()
    r = Reduce8(dx_part, 2, WHOLE, r_keys)
    r.acquire()
    r.compute_all(0)
    r.send(0)
    grad_b(GV0, NXT, GPB.at[NXT])
    b1n[0].sides(NXT)
    grad_b(GV0, PRV, GPB.at[PRV])
    b1n[0].sides(PRV)
    grad_a(NXT, GPA.at[NXT])
    a1n[0].sides(NXT)
    grad_a(PRV, GPA.at[PRV])
    a1n[0].sides(PRV)
    relay((b2, a2))
    r.relay(0)
    relay((b1n[0], a1n[0]))
    for red in (b1n[1], a1n[1]):
        red.opposite()
        red.sides(NXT)
        red.sides(PRV)
    r.combine(OWN, 0)
    grad_b(GV0, OWN, own_grads[0][1])
    grad_a(OWN, own_grads[0][0])
    r.finish(0, RES.at[G0], [RES.at[X0]])
    r.release()
    write_gi = lcopy(RES.at[X0], gi_out)
    write_gi.start()
    arrive((b1n[0], a1n[0]), EARLY)
    arrive((b2, a2), EARLY)
    arrive((b2, a2), LATE)
    state1 = grads_out_start(1, 0, 1)
    load_a1.wait()
    load_w1d_again.wait()
    r = Reduce8(functools.partial(down_part, GV1), 3, WHOLE, r_keys)
    r.acquire()
    r.compute_all(0)
    r.send(0)
    r.combine(OWN, 0)
    arrive((b1n[0], a1n[0]), LATE)
    grads_out_finish(state1)
    relay((b1n[1], a1n[1]))
    second_start((a2n[0], b2n[0]))
    r.relay(0)
    arrive((b1n[1], a1n[1]), EARLY)
    arrive((b1n[1], a1n[1]), LATE)
    second_start((a2n[1], b2n[1]))
    relay((b2n[0], a2n[0]))
    arrive((b2n[0], a2n[0]), EARLY)
    relay((b2n[1], a2n[1]))
    arrive((b2n[1], a2n[1]), EARLY)
    arrive((b2n[0], a2n[0]), LATE)
    state0 = [grads_out_start(0, 0, 2)]
    r.finish(0, RES.at[X1], [RES.at[G1]])
    write_y = lcopy(RES.at[G1], y_out)
    write_y.start()
    arrive((b2n[1], a2n[1]), LATE)
    state0.append(grads_out_start(0, 1, 2))
    r.drain()
    do(gg0, "drain")
    write_gi.wait()
    write_y.wait()
    for state in state0:
        grads_out_finish(state)
    assert used["recv"] <= N_RECV and used["send"] <= N_SEND and used["local"] <= N_LOCAL


def finish_kernel(y_in, gi_in, gu_in, gd_in, y_out, gi_out, gu_out, gd_out, ybuf, gibuf, gubuf, gdbuf, gushuf, sems):
    layers, ur, ff = gu_out.shape
    s2 = ff // 64
    half = s2 // 2
    loads = [pltpu.make_async_copy(a, b, sems.at[0, k])
             for k, (a, b) in enumerate(((gu_in, gubuf), (gd_in, gdbuf), (y_in, ybuf), (gi_in, gibuf)))]
    stores = [pltpu.make_async_copy(a, b, sems.at[1, k])
              for k, (a, b) in enumerate(((gushuf, gu_out), (gdbuf, gd_out), (ybuf, y_out), (gibuf, gi_out)))]
    for cpy in loads:
        cpy.start()
    low = lax.broadcasted_iota(jnp.int32, (ur, s2), 1) < half
    swap = lambda v: pltpu.roll(v, half, 1)
    loads[0].wait()
    for l in range(layers):
        for b in range(RING):
            for yy in range(RING):
                for m in HALVES:
                    cols = pl.ds((yy * 2 + m) * s2, s2)
                    t0, t1 = (gubuf[l, b, pl.ds(k * ur, ur), cols] for k in HALVES)
                    strip = (b * RING + 2 * m) * RING + yy
                    gushuf[l, :, pl.ds(strip * s2, s2)] = jnp.where(low, t0, swap(t1))
                    gushuf[l, :, pl.ds((strip + RING) * s2, s2)] = jnp.where(low, swap(t0), t1)
    stores[0].start()
    for k in (1, 2, 3):
        loads[k].wait()
        stores[k].start()
    for cpy in stores:
        cpy.wait()


def solution(mesh, interpret=None):
    fine = Mesh(np.asarray(mesh.devices).reshape(4, 4, 4, 2), ALL)
    tok_spec = P(ALL, None)
    weight_spec = P(None, ALL, None)

    def device_step(x_loc, up_loc, down_loc, g_loc):
        layers, ur, ff = up_loc.shape
        dr, dm = down_loc.shape[1:]
        tb = x_loc.shape[0]
        k = ff // 8
        zd = dm // 16
        hbm = lambda shape, dt: jax.ShapeDtypeStruct(shape, dt)
        outs = [
            hbm((tb, dm), BF16), hbm((tb, dm), BF16), hbm((layers, dr, dm), F32),
            hbm((RING, CORES, tb, dm), BF16),
            hbm((layers, RING, RING, RING, 2 * ur, k), BF16),
            hbm((layers, RING, RING, dr, dm), BF16),
            hbm((RING, CORES, tb, k), F32), hbm((layers, RING, CORES, tb, k), BF16),
            *[hbm((layers, ARRIVALS, CORES, n, k), F32) for n in (zd, zd, 2 * ur, 2 * ur)],
            hbm((layers, RING, 2 * ur, k), F32),
        ]
        vm = pltpu.VMEM
        scratch = [
            vm((RING, RING, RING, 2 * ur, k), BF16), vm((RING, RING, dr, dm), BF16),
            vm((RING, CORES, tb, dm), BF16), vm((RING, CORES, tb, dm), BF16), vm((RING, CORES, tb, dm), BF16),
            vm((RING, CORES, tb, k), F32), vm((RING, CORES, tb, k), BF16), vm((RING, 2 * tb, k), BF16),
            vm((RING, CORES, CORES, zd, k), F32), vm((RING, CORES, CORES, zd, k), F32),
            vm((RING, CORES, tb, dm), F32), vm((4, tb, dm), F32), vm((6, tb // 2, dm), F32),
            vm((4, tb, dm), BF16), vm((CORES, CORES, 2 * ur, k), F32), vm((CORES, CORES, 2 * ur, k), F32),
            *[pltpu.SemaphoreType.DMA((n,)) for n in (N_SEND, N_RECV, N_LOCAL, len(SPLIT3) * RING)],
            pltpu.SemaphoreType.REGULAR((3,)),
        ]
        anyspec = pl.BlockSpec(memory_space=pl.ANY)
        call = pl.pallas_call(
            functools.partial(kernel, (dm, k, tb, ur, dr)),
            out_shape=outs,
            in_specs=[anyspec] * 4,
            out_specs=[anyspec] * len(outs),
            scratch_shapes=scratch,
            compiler_params=pltpu.CompilerParams(collective_id=0, has_side_effects=True, vmem_limit_bytes=67043328),
            name="mlp_stack",
            **({"interpret": interpret} if interpret else {}),
        )
        y_raw, gi_raw, gd_raw, *_, gu_raw = call(x_loc, up_loc, down_loc, g_loc)
        raws = (y_raw, gi_raw, gu_raw, gd_raw)
        outs = [hbm((tb, dm), BF16), hbm((tb, dm), BF16), hbm((layers, ur, ff), F32), hbm((layers, dr, dm), F32)]
        return tuple(pl.pallas_call(
            finish_kernel, out_shape=outs, in_specs=[anyspec] * len(outs), out_specs=[anyspec] * len(outs),
            scratch_shapes=[vm(v.shape, v.dtype) for v in raws] + [vm(outs[2].shape, F32), pltpu.SemaphoreType.DMA((2, len(outs)))],
            name="write_out")(*raws))

    return jax.shard_map(device_step, mesh=fine, in_specs=(tok_spec, weight_spec, weight_spec, tok_spec),
                         out_specs=(tok_spec, tok_spec, weight_spec, weight_spec), check_vma=False)
```

```python
import functools

import jax
import jax.numpy as jnp
import numpy as np
from jax import lax
from jax.experimental import pallas as pl
from jax.experimental.pallas import tpu as pltpu
from jax.sharding import Mesh, PartitionSpec as P

MESH_ID = pl.DeviceIdType.MESH
ALL = ("x", "z", "y", "c")
F32, BF16 = jnp.float32, jnp.bfloat16
RING, CORES, ARRIVALS = 4, 2, 6
OWN, NXT, OPP, PRV = range(RING)
X0, X1, G1, G0 = range(RING)
HALVES = (0, 1)
WHOLE, SPLIT2, SPLIT3 = (4,), (2, 2), (1, 1, 2)
PIECES = ((OPP, 0), (OPP, 1), (NXT, 1), (PRV, 0), (NXT, 0), (PRV, 1))
TARGETS = ((NXT, 0), (PRV, 1), (OWN, 1), (OWN, 0), (OWN, 0), (OWN, 1))
EARLY, LATE = (2, 3), (4, 5)
PUSHES = {PRV: (0, 2), NXT: (1, 3), OPP: (4, 5)}
N_RECV, N_SEND, N_LOCAL = 187, 110, 15


def gelu_parts(pre_act):
    norm_cdf = 0.5 * (1.0 + lax.erf(pre_act * (2.0 ** -0.5)))
    norm_pdf = jnp.exp(-0.5 * pre_act * pre_act) * ((2.0 * jnp.pi) ** -0.5)
    return pre_act * norm_cdf, norm_cdf + pre_act * norm_pdf


def loop(n, body, init):
    return lax.fori_loop(0, n, body, init)


def dot_nn(left, right):
    return lax.dot_general(left, right, (((1,), (0,)), ((), ())), preferred_element_type=F32)


def dot_nt(left, right):
    return lax.dot_general(left, right, (((1,), (1,)), ((), ())), preferred_element_type=F32)


def dot_tn(left, right):
    return lax.dot_general(left, right, (((0,), (0,)), ((), ())), preferred_element_type=F32)


def kernel(dims, x_in, wu_in, wd_in, g_in,
           y_out, gi_out, gd_out,
           xh0, wuh, wdh, sh0, ah, ra1, rb1, ra2, rb2, uh,
           U, W, XV, GV1, GV0, SV, AV, DV, GPA, GPB, PP, DR, XR, RES, STA, STB,
           ss, rs, ls, ps, credit):
    D, K, TB, UR, DR_ROWS = dims
    HB = TB // 2
    x, z, y, c = (lax.axis_index(a) for a in ALL)
    cp = 1 - c
    S2 = 2 * DR_ROWS
    XD = D // 4
    ZD = D // 16

    def dev(dx=0, dz=0, dy=0, dc=0):
        wrap = lambda v, d, n: v if d == 0 else lax.rem(v + (d % n), n)
        return (wrap(x, dx, 4), wrap(z, dz, 4), wrap(y, dy, 4), wrap(c, dc, 2))

    partner = dev(dc=1)
    rings = {"x": (x, dev(dx=1), dev(dx=-1)), "z": (z, dev(dz=1), dev(dz=-1)), "y": (y, dev(dy=1), dev(dy=-1))}
    off = lambda v, d: v if d == 0 else lax.rem(v + d, 4)

    used = {"recv": 0, "send": 0, "local": 0}
    free = {"send": [], "local": []}
    keys = []

    def fresh(kind):
        if kind == "recv" and keys:
            return keys.pop()
        used[kind] += 1
        return used[kind] - 1

    def take(kind):
        return free[kind].pop() if free[kind] else fresh(kind)

    def remote(src, dst, send, recv, to):
        return pltpu.make_async_remote_copy(src_ref=src, dst_ref=dst, send_sem=send, recv_sem=recv,
                                            device_id=to, device_id_type=MESH_ID)

    class rcopy:
        def __init__(self, src, dst, to, key=None):
            self.args, self.key = (src, dst, to), fresh("recv") if key is None else key

        def start(self):
            src, dst, to = self.args
            self.sem = take("send")
            self.d = remote(src, dst, ss.at[self.sem], rs.at[self.key], to)
            self.d.start()

        def wait_recv(self):
            self.d.wait_recv()

        def wait_send(self):
            self.d.wait_send()
            free["send"].append(self.sem)

    class lcopy:
        def __init__(self, src, dst):
            self.args = src, dst

        def start(self):
            self.sem = take("local")
            self.d = pltpu.make_async_copy(*self.args, ls.at[self.sem])
            self.d.start()

        def wait(self):
            self.d.wait()
            free["local"].append(self.sem)

    def mo(v, m):
        return pl.multiple_of(v, m)

    class Gather4:
        def __init__(self, axis, src, dst):
            i, right, left = rings[axis]
            lft, rgt = off(i, 3), off(i, 1)
            self.d = [rcopy(src(0), dst(i, 0), right), rcopy(src(1), dst(i, 1), right),
                      rcopy(src(0), dst(i, 0), left), rcopy(src(1), dst(i, 1), left),
                      rcopy(dst(lft, 0), dst(lft, 0), right), rcopy(dst(rgt, 1), dst(rgt, 1), left)]

        def start_first(self):
            self.d[0].start()
            self.d[3].start()

        def start_rest(self):
            self.d[1].start()
            self.d[2].start()

        def start(self):
            self.start_first()
            self.start_rest()

        def forward(self):
            for k in HALVES:
                self.d[3 * k].wait_recv()
                self.d[4 + k].start()

        def neighbours(self):
            self.d[1].wait_recv()
            self.d[2].wait_recv()

        def opposite(self):
            self.d[4].wait_recv()
            self.d[5].wait_recv()

        def finish(self):
            self.neighbours()
            self.opposite()

        def drain(self):
            for d in self.d:
                d.wait_send()

    class Gather8:
        def __init__(self, src, dst):
            self.ring = Gather4("x", src, lambda b, h: dst(b, c, h))
            lft, rgt, opp = off(x, PRV), off(x, NXT), off(x, OPP)
            blocks = [(lft, 0), (rgt, 1), (lft, 1), (rgt, 0), (opp, 0), (opp, 1)]
            self.own = [rcopy(src(h), dst(x, c, h), partner) for h in HALVES]
            self.push = [rcopy(dst(b, c, h), dst(b, c, h), partner) for b, h in blocks]

        def start(self):
            self.ring.start()
            for d in self.own:
                d.start()

        def forward(self):
            self.ring.forward()
            self.push[0].start()
            self.push[1].start()

        def sides(self):
            self.ring.d[1].wait_recv()
            self.push[2].start()
            self.ring.d[2].wait_recv()
            self.push[3].start()

        def last(self):
            self.ring.d[4].wait_recv()
            self.push[4].start()
            self.ring.d[5].wait_recv()
            self.push[5].start()

        def wait_own(self):
            for d in self.own:
                d.wait_recv()

        def wait_push(self, ks):
            for k in ks:
                self.push[k].wait_recv()

        def drain(self):
            self.ring.drain()
            for d in self.own + self.push:
                d.wait_send()

    def add_rows(dst, srcs, rows, step):
        def body(r, carry):
            sl = pl.ds(mo(r * step, step), step)
            if len(dst.shape) == 3:
                for q in range(dst.shape[0]):
                    acc = dst[q, sl, :]
                    for s in srcs:
                        acc = acc + s[q, sl, :]
                    dst[q, sl, :] = acc
            else:
                acc = dst[sl, :]
                for s in srcs:
                    acc = acc + s[sl, :]
                dst[sl, :] = acc
            return carry
        loop(rows // step, body, None)

    barrier = pltpu.get_barrier_semaphore()
    group = [(dx, dc) for dx in (OPP, NXT, PRV, OWN) for dc in HALVES if dx or dc]
    peers = [dev(dx=dx, dc=dc) for dx, dc in group] + [rings[a][k] for a in "zy" for k in (1, 2)]
    for p in peers:
        pl.semaphore_signal(barrier, inc=1, device_id=p, device_id_type=MESH_ID)

    load_u = [[lcopy(wu_in.at[l, :, pl.ds(b * D, D)], RES.at[G0, pl.ds((l * RING + b) * UR, UR), :])
               for b in range(RING)] for l in HALVES]
    load_d = [lcopy(wd_in.at[l], RES.at[X1, pl.ds(l * DR_ROWS, DR_ROWS), :]) for l in HALVES]
    load_x = lcopy(x_in, RES.at[X0])
    load_g = lcopy(g_in, RES.at[G1])
    own_x = lcopy(x_in, XV.at[x, c])
    own_g = lcopy(g_in, GV1.at[x, c])
    own_d0 = lcopy(wd_in.at[0], W.at[y, z])
    for cpy in load_u[0] + load_u[1] + load_d + [load_x, own_d0, own_x, load_g, own_g]:
        cpy.start()

    low = lax.broadcasted_iota(jnp.int32, (UR, S2), 1) < DR_ROWS
    swap = lambda v: pltpu.roll(v, DR_ROWS, 1)
    for l in HALVES:
        for cpy in load_u[l]:
            cpy.wait()
        for b in range(RING):
            rows = pl.ds((l * RING + b) * UR, UR)
            for yy in range(RING):
                for m in HALVES:
                    s0 = RES[G0, rows, pl.ds((2 * m * RING + yy) * S2, S2)].astype(F32)
                    s1 = RES[G0, rows, pl.ds(((2 * m + 1) * RING + yy) * S2, S2)].astype(F32)
                    cols = pl.ds((yy * 2 + m) * S2, S2)
                    AV[l, 0, pl.ds(2 * b * UR, UR), cols] = jnp.where(low, s0, swap(s1)).astype(BF16)
                    AV[l, 0, pl.ds((2 * b + 1) * UR, UR), cols] = jnp.where(low, swap(s0), s1).astype(BF16)
    for cpy in load_d + [load_x, own_d0]:
        cpy.wait()
    pl.semaphore_wait(barrier, len(peers))

    half = lambda h: pl.ds(h * HB, HB)

    def tile_cols(split, q):
        return pl.ds(sum(split[:q]) * (D // RING), split[q] * (D // RING))

    gx0 = Gather8(lambda h: RES.at[X0, half(h)], lambda b, k, h: XV.at[b, k, half(h)])
    gg1 = Gather8(lambda h: RES.at[G1, half(h)], lambda b, k, h: GV1.at[b, k, half(h)])
    up = [U, wuh.at[1]]
    down = [W, wdh.at[1]]
    hr = DR_ROWS // 4

    def quarter(q, h):
        return pl.ds((2 * q + h) * hr, hr)

    def down_first(l):
        to = down[l]
        src = lambda q: lambda h: RES.at[X1, pl.ds(l * DR_ROWS + (2 * q + h) * hr, hr)]
        return [Gather4("z", src(0), lambda b, h: to.at[y, b, quarter(0, h)]),
                Gather4("y", src(1), lambda b, h: to.at[b, z, quarter(1, h)])]

    def down_second(l, split, n):
        to, cs = down[l], tile_cols(split, n)
        return [Gather4("y", lambda h: to.at[y, :, quarter(0, h), cs], lambda b, h: to.at[b, :, quarter(0, h), cs]),
                Gather4("z", lambda h: to.at[:, z, quarter(1, h), cs], lambda b, h: to.at[:, b, quarter(1, h), cs])]

    def up_first(to):
        return [Gather4("y", lambda h: to.at[h, z, y], lambda b, h: to.at[h, z, b]),
                Gather4("z", lambda h: to.at[2 + h, z, y], lambda b, h: to.at[2 + h, b, y])]

    def hidden_cols(n):
        return pl.ds(sum(SPLIT2[:n]) * (K // RING), SPLIT2[n] * (K // RING))

    def up_second(to, n):
        cs = hidden_cols(n)
        return [Gather4("z", lambda h: to.at[h, z, :, :, cs], lambda b, h: to.at[h, b, :, :, cs]),
                Gather4("y", lambda h: to.at[2 + h, :, y, :, cs], lambda b, h: to.at[2 + h, :, b, :, cs])]

    def up_unit(to, j):
        yj, zj = off(y, j), off(z, j)
        return [Gather4("z", lambda h: to.at[h, z, yj], lambda b, h: to.at[h, b, yj]),
                Gather4("y", lambda h: to.at[2 + h, zj, y], lambda b, h: to.at[2 + h, zj, b])]

    def do(gathers, step):
        for g in gathers:
            getattr(g, step)()

    mine = pl.ds(mo(c * UR, UR), UR)

    def up_exchange(l):
        sends = []
        for dx, dc in group:
            tx, tc = off(x, dx), (cp if dc else c)
            src = AV.at[l, 0, pl.ds(mo((tx * 2 + tc) * UR, UR), UR), :]
            sends.append(rcopy(src, up[l].at[x, z, y, mine, :], dev(dx=dx, dc=dc)))
        for cpy in sends:
            cpy.start()
        return sends

    def keys_of(gathers):
        return [d.key for g in gathers for d in g.d]

    d0a, d0b, d0c = down_first(0), down_second(0, SPLIT3, 0), down_second(0, SPLIT3, 1)
    u0a, u0u = up_first(up[0]), [up_unit(up[0], j) for j in (OWN, PRV, NXT, OPP)]
    keys.extend(keys_of(u0a))
    d0d = down_second(0, SPLIT3, 2)
    keys.extend(keys_of(d0a))
    d1a = down_first(1)
    keys.extend(keys_of(sum(u0u, [])))
    d1b, u1a = down_second(1, WHOLE, 0), up_first(up[1])
    u1b, u1c = up_second(up[1], 0), up_second(up[1], 1)
    ex0 = up_exchange(0)
    do(d0a, "start")
    gx0.start()
    ex1 = up_exchange(1)
    my_rows = pl.ds(mo((x * 2 + c) * UR, UR), UR)
    own_u1 = lcopy(AV.at[1, 0, my_rows, :], up[1].at[x, z, y, mine, :])
    own_u1.start()
    own_d1 = lcopy(RES.at[X1, pl.ds(DR_ROWS, DR_ROWS), :], down[1].at[y, z])
    own_d1.start()
    U[x, z, y, mine, :] = AV[0, 0, my_rows, :]
    do(d0a, "forward")
    for cpy in ex0:
        cpy.wait_recv()
    do(u0a, "start")
    do(u0u[0], "start")
    do(u0a, "forward")
    gx0.forward()
    load_g.wait()
    gg1.start()
    do(u0a, "neighbours")
    do(u0u[1], "start")
    do(u0u[2], "start")
    do(u0u[0], "forward")
    do(u0a, "opposite")
    do(u0u[3], "start")
    do(d0a, "finish")
    do(u0u[1], "forward")
    do(u0u[2], "forward")
    do(d0b, "start_first")
    gx0.sides()
    for cpy in ex0 + ex1:
        cpy.wait_send()
    own_u1.wait()
    do(u0u[3], "forward")
    do(u0a + d0a, "drain")
    do(d0b, "start_rest")
    do(d0c, "start_first")
    gg1.forward()
    do(d0b, "forward")
    do(d0c, "start_rest")
    do(d1a, "start")
    gx0.last()
    gx0.wait_own()
    gx0.wait_push(range(len(gx0.push)))
    own_x.wait()
    save_x = lcopy(XV, xh0)
    save_x.start()
    gx0.drain()
    for unit in u0u:
        do(unit, "finish")
    save_u0 = lcopy(U, wuh.at[0])
    save_u0.start()

    T2 = 2 * TB
    ND = D // 4
    NK = K // 4

    def up_tile(t, n):
        cols = pl.ds(mo(n * NK, NK), NK)
        return dot_nn(XV[t].reshape(T2, D), U[:, :, :, :, cols].reshape(D, NK)), cols

    def hidden0(t):
        for n in range(RING):
            pre, cols = up_tile(t, n)
            act, slope = gelu_parts(pre)
            AV[t, :, :, cols] = act.astype(BF16).reshape(2, TB, NK)
            SV[t, :, :, cols] = slope.reshape(2, TB, NK)

    def hidden1(t, part):
        for n in range(sum(SPLIT2[:part]), sum(SPLIT2[:part + 1])):
            pre, cols = up_tile(t, n)
            act, slope = gelu_parts(pre)
            AV[t, :, :, cols] = act.astype(BF16).reshape(2, TB, NK)
            DV[t, :, cols] = (SV[t, :, :, cols].reshape(T2, NK) * slope).astype(BF16)

    def dact(gv, t, n):
        return dot_nt(gv[t].reshape(T2, D), W[n].reshape(NK, D))

    def dact1(t):
        def body(n, carry):
            SV[t, :, :, pl.ds(mo(n * NK, NK), NK)] = dact(GV1, t, n).reshape(2, TB, NK)
            return carry
        loop(RING, body, None)

    def dact0(t):
        def body(n, carry):
            cols = pl.ds(mo(n * NK, NK), NK)
            DV[t, :, cols] = (dact(GV0, t, n) * SV[t, :, :, cols].reshape(T2, NK)).astype(BF16)
            return carry
        loop(RING, body, None)

    def down_part(act, j, lo, tiles):
        t = lax.rem(x + j, RING)

        def body(n, carry):
            cols = pl.ds(mo((lo + n) * ND, ND), ND)
            PP[j, :, :, cols] = dot_nn(act[t, :, :, 0:K].reshape(T2, K), W[:, :, :, cols].reshape(K, ND)).reshape(2, TB, ND)
            return carry
        loop(tiles, body, None)

    def dx_part(j, lo, tiles):
        t = lax.rem(x + j, RING)

        def body(n, carry):
            cols = pl.ds(mo((lo + n) * ND, ND), ND)
            PP[j, :, :, cols] = dot_nt(DV[t], U[lo + n].reshape(ND, K)).reshape(2, TB, ND)
            return carry
        loop(tiles, body, None)

    class Reduce8:
        def __init__(self, part, index, split, old=()):
            self.part, self.index, self.split = part, index, split
            keys.extend(old)
            _, right, left = rings["x"]
            self.right, self.left = right, left
            self.pair, self.m, self.first = [], [], []
            for q in range(len(split)):
                cq = self.cols(q)
                first = sorted(fresh("recv") for j in range(RING))
                self.pair.append([self.swap(j, q, first[0]) for j in range(RING)])
                self.first.append(first[0])
                src = lambda j, h: PP.at[j, c, half(h), cq]
                self.m.append([rcopy(src(*PIECES[k]), XR.at[k, :, cq], left if k % 2 else right) for k in range(ARRIVALS)])
            keys.clear()

        def cols(self, q):
            return tile_cols(self.split, q)

        def swap(self, j, q, first):
            cq = self.cols(q)
            return remote(PP.at[j, cp, :, cq], DR.at[j, :, cq], ps.at[q * RING + j], rs.at[first + j], partner)

        def compute(self, j, q):
            self.part(j, sum(self.split[:q]), self.split[q])
            self.pair[q][j].start()

        def compute_all(self, q):
            def body(i, carry):
                j = lax.rem(i + 1, RING)
                self.part(j, sum(self.split[:q]), self.split[q])
                self.swap(j, q, self.first[q]).start()
                return carry
            loop(RING, body, None)

        def combine(self, j, q):
            self.pair[q][j].wait_recv()
            add_rows(PP.at[j, c, :, self.cols(q)], [DR.at[j, :, self.cols(q)]], TB, min(TB, 16))

        def opposite(self, q):
            self.m[q][0].start()
            self.m[q][1].start()

        def side(self, j, q):
            self.combine(j, q)
            self.m[q][2 if j == NXT else 3].start()

        def send(self, q):
            self.combine(OPP, q)
            self.opposite(q)
            self.side(NXT, q)
            self.side(PRV, q)

        def relay(self, q):
            for k, j, h in ((0, NXT, 0), (1, PRV, 1)):
                self.m[q][k].wait_recv()
                add_rows(PP.at[j, c, half(h), self.cols(q)], [XR.at[k, :, self.cols(q)]], HB, min(HB, 16))
                self.m[q][4 + k].start()

        def finish(self, q, res, outs):
            for d in self.m[q][2:]:
                d.wait_recv()
            step, cq = min(HB, 16), self.cols(q)
            for h, (kl, kr) in enumerate(((4, 3), (2, 5))):
                def body(r, carry):
                    lo = pl.ds(mo(r * step, step), step)
                    sl = pl.ds(mo(h * HB + r * step, step), step)
                    tot = PP[OWN, c, sl, cq] + (XR[kl, lo, cq] + XR[kr, lo, cq])
                    val = (res[sl, cq].astype(F32) + tot).astype(BF16)
                    for o in outs:
                        o[sl, cq] = val
                    return carry
                loop(HB // step, body, None)

        def drain(self):
            for d in sum(self.pair + self.m, []):
                d.wait_send()

        def release(self):
            self.drain()
            for k, to in enumerate((self.right, self.left, partner)):
                pl.semaphore_signal(credit.at[k], inc=1, device_id=to, device_id_type=MESH_ID)

        def acquire(self):
            for k in range(len((self.right, self.left, partner))):
                pl.semaphore_wait(credit.at[k], 1)

    def grad_a(j, dst, halves=None):
        t = off(z, j)

        def rows(h, carry):
            lo = [pl.ds(mo((2 * h + q) * XD + t * ZD, ZD), ZD) for q in HALVES]
            lhs = jnp.concatenate([XV[:, :, :, s].reshape(8 * TB, ZD) for s in lo], axis=1)

            def body(n, carry):
                cols = pl.ds(mo(n * ND, ND), ND)
                dst[h, :, :, cols] = dot_tn(lhs, DV[:, :, cols].reshape(8 * TB, ND)).reshape(2, ZD, ND)
                return carry
            return loop(K // ND, body, carry)
        if halves is None:
            loop(2, rows, None)
        else:
            for h in halves:
                rows(h, None)

    def grad_b(gv, j, dst, lo=0, tiles=RING):
        cols_l = pl.ds(mo(off(y, j) * NK, NK), NK)

        def body(i, carry):
            m = lo + i
            cols = pl.ds(mo(m * ND, ND), ND)
            out = dot_tn(AV[:, :, :, cols_l].reshape(8 * TB, NK), gv[:, :, :, cols].reshape(8 * TB, ND))
            dst[:, m // 2, :, pl.ds(mo(lax.rem(m, 2) * ND, ND), ND)] = out.reshape(2, NK // 2, ND)
            return carry
        loop(tiles, body, None)

    grad_keys = [keys_of(sum(u0u, u0a) + d0a), [d.key for d in ex0 + ex1] + keys_of(d0b + d0c)]

    def grad_key(l):
        return grad_keys[l].pop() if grad_keys[l] else fresh("recv")

    class Reduce4:
        def __init__(self, l, axis, part, recv, stage):
            _, right, left = rings[axis]
            self.part, self.recv, self.stage = part, recv, stage
            self.m = [rcopy(part(*PIECES[k]), recv(k), left if k % 2 else right, grad_key(l))
                      for k in range(ARRIVALS)]
            self.loads = [lcopy(recv(k), stage(k)) for k in range(ARRIVALS)] if stage else None

        def opposite(self):
            self.m[0].start()
            self.m[1].start()

        def sides(self, j):
            self.m[2 if j == NXT else 3].start()

        def fetch(self, k):
            self.m[k].wait_send()
            self.m[k].wait_recv()
            if self.loads:
                self.loads[k].start()

        def absorb(self, k):
            if self.loads:
                self.loads[k].wait()
            dst = self.part(*TARGETS[k])
            add_rows(dst, [(self.stage or self.recv)(k)], dst.shape[1], min(dst.shape[1], 16))

    def arrive(reduces, ks):
        for k in ks:
            for r in reduces:
                r.fetch(k)
        for k in ks:
            for r in reduces:
                r.absorb(k)

    def relay(reduces):
        for k in (0, 1):
            for r in reduces:
                r.fetch(k)
        for k in (0, 1):
            for r in reduces:
                r.absorb(k)
                r.m[4 + k].start()

    hq = DR_ROWS // 2
    own_grads = [(SV.at[pl.ds(0, 2)], SV.at[pl.ds(2, 2)]), (GPA.at[OWN], GPB.at[OWN])]

    def third(k, rows):
        return pl.ds((k // 2) * rows, rows)

    def reduce_a(l, q, chunks):
        own = own_grads[l][0]
        ca = pl.ds(q * (K // chunks), K // chunks)

        def part(j, h):
            return (own if j == OWN else GPA.at[j]).at[h, :, :, ca]

        def part2(j, h):
            return own.at[h, :, pl.ds(mo(off(y, j) * 2 * UR, 2 * UR), 2 * UR), ca]
        if l < q:
            second = lambda k: GPA.at[OWN, k % 2, :, third(k, 2 * UR), ca], None
        else:
            second = lambda k: ra2.at[l, k, :, :, ca], lambda k: STA.at[k % 2, :, :, ca]
        return (Reduce4(l, "z", part, lambda k: ra1.at[l, k, :, :, ca], lambda k: part(*PIECES[k])),
                Reduce4(l, "y", part2, *second))

    def reduce_b(l, q):
        own, nb = own_grads[l][1], pl.ds(q, 1)

        def part(j, h):
            return (own if j == OWN else GPB.at[j]).at[h, nb]

        def part2(j, h):
            t = off(z, j)
            return own.at[t // 2, nb, pl.ds(mo(lax.rem(t, 2) * DR_ROWS + h * hq, hq), hq), :]
        if l < q:
            second = lambda k: GPB.at[OWN, k % 2, nb, third(k, hq), :], None
        else:
            second = lambda k: rb2.at[l, k, nb], lambda k: STB.at[k % 2, nb]
        return (Reduce4(l, "y", part, lambda k: rb1.at[l, k, nb], lambda k: part(*PIECES[k])),
                Reduce4(l, "z", part2, *second))

    def sides(reduces, j):
        for r in reduces:
            r.sides(j)

    def second_start(reduces):
        for r in reduces:
            r.opposite()
            r.sides(NXT)
            r.sides(PRV)

    def up_out(l, q, chunks):
        own = own_grads[l][0]
        ca = pl.ds(q * (K // chunks), K // chunks)

        def rows_of(tx, tc):
            return own.at[tx // 2, lax.rem(tx, 2), pl.ds(mo((2 * y + tc) * UR, UR), UR), ca]
        to = uh.at[l, x, mine, ca]
        sends = [rcopy(rows_of(off(x, dx), cp if dc else c), to, dev(dx=dx, dc=dc), grad_key(l)) for dx, dc in group]
        local = [lcopy(rows_of(x, c), to)]
        for cpy in sends + local:
            cpy.start()
        return sends, local

    def down_out(l, n):
        cpy = lcopy(own_grads[l][1].at[z // 2, n, pl.ds(mo(lax.rem(z, 2) * DR_ROWS, DR_ROWS), DR_ROWS), :],
                    gd_out.at[l, :, pl.ds(n * K, K)])
        cpy.start()
        return [], [cpy]

    def grads_out_finish(state):
        for cpy in state[0]:
            cpy.wait_recv()
            cpy.wait_send()
        for cpy in state[1]:
            cpy.wait()

    r = Reduce8(functools.partial(down_part, AV), 0, SPLIT3)
    r_keys = sorted([d.key for m in r.m for d in m] + [f + j for f in r.first for j in range(RING)])
    hidden0(off(x, OPP))
    hidden0(off(x, NXT))
    do(d0b, "finish")
    r.compute(OPP, 0)
    r.compute(NXT, 0)
    do(d0c, "forward")
    do(d0d, "start")
    r.combine(OPP, 0)
    r.opposite(0)
    do(sum(u0u, []), "drain")
    hidden0(off(x, PRV))
    r.compute(PRV, 0)
    r.side(NXT, 0)
    do(d1a, "forward")
    hidden0(off(x, OWN))
    r.side(PRV, 0)
    save_s = lcopy(SV, sh0)
    save_s.start()
    save_a0 = lcopy(AV, ah.at[0])
    save_a0.start()
    gg1.sides()
    do(d0c, "finish")
    r.compute_all(1)
    r.relay(0)
    do(d0d, "forward")
    for cpy in ex1:
        cpy.wait_recv()
    own_d1.wait()
    do(u1a, "start")
    r.send(1)
    do(d1a, "finish")
    do(d1b, "start")
    gg1.last()
    save_x.wait()
    do(d0d, "finish")
    save_d0 = lcopy(W, wdh.at[0])
    save_d0.start()
    r.compute(OPP, 2)
    r.relay(1)
    do(u1a, "forward")
    r.compute(NXT, 2)
    r.combine(OPP, 2)
    r.opposite(2)
    r.compute(PRV, 2)
    r.side(NXT, 2)
    r.compute(OWN, 2)
    r.side(PRV, 2)
    r.compute(OWN, 0)
    for q in range(len(SPLIT3)):
        r.combine(OWN, q)

    def gather_keys(gathers):
        return [d.key for g in gathers for d in g.ring.d + g.own + g.push]

    def token_gathers(slot, buf):
        def make(q):
            cq = tile_cols(SPLIT2, q)
            return Gather8(lambda h: RES.at[slot, half(h), cq], lambda b, k, h: buf.at[b, k, half(h), cq])
        return [make(0), make(1)]

    keys.extend(gather_keys((gx0,)))
    gx1 = token_gathers(X1, XV)
    do(d1a, "drain")
    do(d1b, "forward")
    for q in HALVES:
        r.finish(q, RES.at[X0], [RES.at[X1], XV.at[x, c]])
    r.relay(2)
    gx1[0].start()
    do(u1a, "finish")
    do(u1b, "start")
    do(u1c, "start_first")
    gg1.wait_own()
    gg1.wait_push(range(len(gg1.push)))
    own_g.wait()
    save_d0.wait()
    do(d0b + d0c + d0d, "drain")
    gg1.drain()
    do(d1b, "finish")
    load_w1d = lcopy(wdh.at[1], W)
    load_w1d.start()
    r.finish(2, RES.at[X0], [RES.at[X1], XV.at[x, c]])
    gx1[1].start()
    save_s.wait()
    do(u1b, "forward")
    do(u1c, "start_rest")
    load_w1d.wait()
    dact1(off(x, OWN))
    gx1[0].forward()
    r.release()
    dact1(off(x, NXT))
    gx1[0].sides()
    dact1(off(x, PRV))
    do(u1c, "forward")
    save_u0.wait()
    do(u1b, "finish")

    def load_up(n):
        cs = hidden_cols(n)
        return lcopy(wuh.at[1, :, :, :, :, cs], U.at[:, :, :, :, cs])
    load_w1u = [load_up(n) for n in HALVES]
    load_w1u[0].start()
    dact1(off(x, OPP))
    load_w0d_again = lcopy(wdh.at[0], W)
    load_w0d_again.start()
    save_a0.wait()
    do(gx1, "wait_own")
    load_w1u[0].wait()
    hidden1(off(x, OWN), 0)
    do(gx1[1:], "forward")
    do(gx1[1:], "sides")
    for j in (PRV, NXT):
        for g in gx1:
            g.wait_push(PUSHES[j])
        hidden1(off(x, j), 0)
    gx1[0].last()
    do(u1c, "finish")
    load_w1u[1].start()
    load_w1u[1].wait()
    hidden1(off(x, OWN), 1)
    gx1[1].last()
    hidden1(off(x, PRV), 1)
    hidden1(off(x, NXT), 1)
    for g in gx1:
        g.wait_push(PUSHES[OPP])
    for n in HALVES:
        hidden1(off(x, OPP), n)
    load_s0 = lcopy(sh0, SV)
    load_s0.start()
    save_a1 = lcopy(AV, ah.at[1])
    save_a1.start()

    (a1, a2), (b1, b2) = reduce_a(1, 0, 1), zip(*[reduce_b(1, q) for q in HALVES])
    first1, second1 = (*b1, a1), (*b2, a2)
    grad_b(GV1, OPP, GPB.at[OPP], 0, 2)
    b1[0].opposite()
    for h in HALVES:
        grad_a(OPP, GPA.at[OPP], (h,))
        a1.m[h].start()
    grad_b(GV1, OPP, GPB.at[OPP], 2, 2)
    b1[1].opposite()
    r = Reduce8(dx_part, 1, SPLIT2, r_keys)
    r.acquire()
    r.compute(OPP, 0)
    r.compute(NXT, 0)
    r.combine(OPP, 0)
    r.opposite(0)
    r.compute(PRV, 0)
    r.side(NXT, 0)
    r.side(PRV, 0)
    r.compute_all(1)
    load_w0u_again = lcopy(wuh.at[0], U)
    r.compute(OWN, 0)
    load_w0u_again.start()
    grad_b(GV1, NXT, GPB.at[NXT])
    sides(b1, NXT)
    grad_b(GV1, PRV, GPB.at[PRV])
    sides(b1, PRV)
    r.relay(0)
    r.send(1)
    grad_a(NXT, GPA.at[NXT])
    a1.sides(NXT)
    grad_a(PRV, GPA.at[PRV])
    a1.sides(PRV)
    r.combine(OWN, 0)
    r.combine(OWN, 1)
    keys.extend(gather_keys(gx1))
    gg0 = token_gathers(G0, GV0)
    r.relay(1)
    r.finish(0, RES.at[G1], [RES.at[G0], GV0.at[x, c]])
    gg0[0].start()
    relay(first1)
    grad_b(GV1, OWN, GPB.at[OWN])
    save_a1.wait()
    load_a0 = lcopy(ah.at[0], AV)
    load_a0.start()
    do(d1b + u1a + u1b + u1c, "drain")
    load_a1 = lcopy(ah.at[1], GV1.at[:, :, :, 0:K])
    load_a1.start()
    r.finish(1, RES.at[G1], [RES.at[G0], GV0.at[x, c]])
    gg0[1].start()
    gg0[0].forward()
    grad_a(OWN, GPA.at[OWN])
    do(gx1, "drain")
    load_x0 = lcopy(xh0, XV)
    load_x0.start()
    gg0[0].sides()
    r.release()
    gg0[1].forward()
    gg0[0].last()
    load_w0d_again.wait()
    load_s0.wait()
    do(gg0, "wait_own")
    dact0(off(x, OWN))
    gg0[1].sides()
    gg0[1].last()
    for g in gg0:
        g.wait_push(PUSHES[PRV])
    dact0(off(x, PRV))
    for g in gg0:
        g.wait_push(PUSHES[NXT])
    dact0(off(x, NXT))
    for g in gg0:
        g.wait_push(PUSHES[OPP])

    (a1n, a2n), (b1n, b2n) = zip(*[reduce_a(0, q, 2) for q in HALVES]), zip(*[reduce_b(0, q) for q in HALVES])
    load_a0.wait()
    grad_b(GV0, OPP, GPB.at[OPP])
    b1n[0].opposite()
    dact0(off(x, OPP))
    load_w1d_again = lcopy(wdh.at[1], W)
    load_w1d_again.start()
    load_x0.wait()
    for h in HALVES:
        grad_a(OPP, GPA.at[OPP], (h,))
        a1n[0].m[h].start()
    arrive(first1, EARLY + LATE)
    second_start(second1)
    load_w0u_again.wait()
    r = Reduce8(dx_part, 2, WHOLE, r_keys)
    r.acquire()
    r.compute_all(0)
    r.send(0)
    grad_b(GV0, NXT, GPB.at[NXT])
    b1n[0].sides(NXT)
    grad_b(GV0, PRV, GPB.at[PRV])
    b1n[0].sides(PRV)
    grad_a(NXT, GPA.at[NXT])
    a1n[0].sides(NXT)
    grad_a(PRV, GPA.at[PRV])
    a1n[0].sides(PRV)
    relay(second1)
    r.relay(0)
    relay((b1n[0], a1n[0]))
    for red in (b1n[1], a1n[1]):
        red.opposite()
        red.sides(NXT)
        red.sides(PRV)
    r.combine(OWN, 0)
    grad_b(GV0, OWN, own_grads[0][1])
    grad_a(OWN, own_grads[0][0])
    r.finish(0, RES.at[G0], [RES.at[X0]])
    r.release()
    write_gi = lcopy(RES.at[X0], gi_out)
    write_gi.start()
    arrive((b1n[0], a1n[0]), EARLY)
    arrive(second1, EARLY)
    arrive(second1, LATE)
    state1 = [up_out(1, 0, 1)] + [down_out(1, n) for n in HALVES]
    load_a1.wait()
    load_w1d_again.wait()
    r = Reduce8(functools.partial(down_part, GV1), 3, WHOLE, r_keys)
    r.acquire()
    r.compute_all(0)
    r.send(0)
    r.combine(OWN, 0)
    arrive((b1n[0], a1n[0]), LATE)
    for state in state1:
        grads_out_finish(state)
    relay((b1n[1], a1n[1]))
    second_start((a2n[0], b2n[0]))
    r.relay(0)
    arrive((b1n[1], a1n[1]), EARLY)
    arrive((b1n[1], a1n[1]), LATE)
    last = (a2n[1], b2n[1])
    for red in last:
        red.opposite()
    relay((b2n[0], a2n[0]))
    sides(last, NXT)
    sides(last, PRV)
    arrive((b2n[0], a2n[0]), EARLY)
    relay((b2n[1], a2n[1]))
    arrive((a2n[0],), LATE)
    state0 = [up_out(0, 0, 2)]
    arrive((b2n[0],), LATE)
    state0.append(down_out(0, 0))
    arrive((a2n[1], b2n[1]), EARLY)
    r.finish(0, RES.at[X1], [RES.at[G1]])
    write_y = lcopy(RES.at[G1], y_out)
    write_y.start()
    arrive((a2n[1],), LATE)
    state0.append(up_out(0, 1, 2))
    arrive((b2n[1],), LATE)
    state0.append(down_out(0, 1))
    r.drain()
    do(gg0, "drain")
    write_gi.wait()
    write_y.wait()
    for state in state0:
        grads_out_finish(state)
    assert used["recv"] <= N_RECV and used["send"] <= N_SEND and used["local"] <= N_LOCAL


def finish_kernel(y_in, gi_in, gu_in, gd_in, y_out, gi_out, gu_out, gd_out, ybuf, gibuf, gubuf, gdbuf, gushuf, sems):
    layers, ur, ff = gu_out.shape
    s2 = ff // 64
    half = s2 // 2
    loads = [pltpu.make_async_copy(a, b, sems.at[0, k])
             for k, (a, b) in enumerate(((gu_in, gubuf), (gd_in, gdbuf), (y_in, ybuf), (gi_in, gibuf)))]
    stores = [pltpu.make_async_copy(a, b, sems.at[1, k])
              for k, (a, b) in enumerate(((gushuf, gu_out), (gdbuf, gd_out), (ybuf, y_out), (gibuf, gi_out)))]
    for cpy in loads:
        cpy.start()
    low = lax.broadcasted_iota(jnp.int32, (ur, s2), 1) < half
    swap = lambda v: pltpu.roll(v, half, 1)
    loads[0].wait()
    for l in range(layers):
        for b in range(RING):
            for yy in range(RING):
                for m in HALVES:
                    cols = pl.ds((yy * 2 + m) * s2, s2)
                    t0, t1 = (gubuf[l, b, pl.ds(k * ur, ur), cols] for k in HALVES)
                    strip = (b * RING + 2 * m) * RING + yy
                    gushuf[l, :, pl.ds(strip * s2, s2)] = jnp.where(low, t0, swap(t1))
                    gushuf[l, :, pl.ds((strip + RING) * s2, s2)] = jnp.where(low, swap(t0), t1)
    stores[0].start()
    for k in range(1, len(loads)):
        loads[k].wait()
        stores[k].start()
    for cpy in stores:
        cpy.wait()


def solution(mesh, interpret=None):
    fine = Mesh(np.asarray(mesh.devices).reshape(4, 4, 4, 2), ALL)
    tok_spec = P(ALL, None)
    weight_spec = P(None, ALL, None)

    def device_step(x_loc, up_loc, down_loc, g_loc):
        layers, ur, ff = up_loc.shape
        dr, dm = down_loc.shape[1:]
        tb = x_loc.shape[0]
        k = ff // 8
        zd = dm // 16
        hbm = lambda shape, dt: jax.ShapeDtypeStruct(shape, dt)
        outs = [
            hbm((tb, dm), BF16), hbm((tb, dm), BF16), hbm((layers, dr, dm), F32),
            hbm((RING, CORES, tb, dm), BF16),
            hbm((layers, RING, RING, RING, 2 * ur, k), BF16),
            hbm((layers, RING, RING, dr, dm), BF16),
            hbm((RING, CORES, tb, k), F32), hbm((layers, RING, CORES, tb, k), BF16),
            *[hbm((layers, ARRIVALS, CORES, n, k), F32) for n in (zd, zd, 2 * ur, 2 * ur)],
            hbm((layers, RING, 2 * ur, k), F32),
        ]
        vm = pltpu.VMEM
        scratch = [
            vm((RING, RING, RING, 2 * ur, k), BF16), vm((RING, RING, dr, dm), BF16),
            vm((RING, CORES, tb, dm), BF16), vm((RING, CORES, tb, dm), BF16), vm((RING, CORES, tb, dm), BF16),
            vm((RING, CORES, tb, k), F32), vm((RING, CORES, tb, k), BF16), vm((RING, 2 * tb, k), BF16),
            vm((RING, CORES, CORES, zd, k), F32), vm((RING, CORES, CORES, zd, k), F32),
            vm((RING, CORES, tb, dm), F32), vm((4, tb, dm), F32), vm((6, tb // 2, dm), F32),
            vm((4, tb, dm), BF16), vm((CORES, CORES, 2 * ur, k), F32), vm((CORES, CORES, 2 * ur, k), F32),
            *[pltpu.SemaphoreType.DMA((n,)) for n in (N_SEND, N_RECV, N_LOCAL, len(SPLIT3) * RING)],
            pltpu.SemaphoreType.REGULAR((3,)),
        ]
        anyspec = pl.BlockSpec(memory_space=pl.ANY)
        call = pl.pallas_call(
            functools.partial(kernel, (dm, k, tb, ur, dr)),
            out_shape=outs,
            in_specs=[anyspec] * 4,
            out_specs=[anyspec] * len(outs),
            scratch_shapes=scratch,
            compiler_params=pltpu.CompilerParams(collective_id=0, has_side_effects=True, vmem_limit_bytes=67043328),
            name="mlp_stack",
            **({"interpret": interpret} if interpret else {}),
        )
        y_raw, gi_raw, gd_raw, *_, gu_raw = call(x_loc, up_loc, down_loc, g_loc)
        raws = (y_raw, gi_raw, gu_raw, gd_raw)
        outs = [hbm((tb, dm), BF16), hbm((tb, dm), BF16), hbm((layers, ur, ff), F32), hbm((layers, dr, dm), F32)]
        return tuple(pl.pallas_call(
            finish_kernel, out_shape=outs, in_specs=[anyspec] * len(outs), out_specs=[anyspec] * len(outs),
            scratch_shapes=[vm(v.shape, v.dtype) for v in raws] + [vm(outs[2].shape, F32), pltpu.SemaphoreType.DMA((2, len(outs)))],
            name="write_out")(*raws))

    return jax.shard_map(device_step, mesh=fine, in_specs=(tok_spec, weight_spec, weight_spec, tok_spec),
                         out_specs=(tok_spec, tok_spec, weight_spec, weight_spec), check_vma=False)
```

```python
import functools

import jax
import jax.numpy as jnp
import numpy as np
from jax import lax
from jax.experimental import pallas as pl
from jax.experimental.pallas import tpu as pltpu
from jax.sharding import Mesh, PartitionSpec as P

MESH_ID = pl.DeviceIdType.MESH
ALL = ("x", "z", "y", "c")
F32, BF16 = jnp.float32, jnp.bfloat16
RING, CORES, ARRIVALS = 4, 2, 6
OWN, NXT, OPP, PRV = range(RING)
X0, X1, G1, G0 = range(RING)
HALVES = (0, 1)
WHOLE, SPLIT2, SPLIT3 = (4,), (2, 2), (1, 1, 2)
PIECES = ((OPP, 0), (OPP, 1), (NXT, 1), (PRV, 0), (NXT, 0), (PRV, 1))
TARGETS = ((NXT, 0), (PRV, 1), (OWN, 1), (OWN, 0), (OWN, 0), (OWN, 1))
EARLY, LATE = (2, 3), (4, 5)
PUSHES = {PRV: (0, 2), NXT: (1, 3), OPP: (4, 5)}
N_RECV, N_SEND, N_LOCAL = 206, 110, 19


def gelu_parts(pre_act):
    norm_cdf = 0.5 * (1.0 + lax.erf(pre_act * (2.0 ** -0.5)))
    norm_pdf = jnp.exp(-0.5 * pre_act * pre_act) * ((2.0 * jnp.pi) ** -0.5)
    return pre_act * norm_cdf, norm_cdf + pre_act * norm_pdf


def loop(n, body, init):
    return lax.fori_loop(0, n, body, init)


def dot_nn(left, right):
    return lax.dot_general(left, right, (((1,), (0,)), ((), ())), preferred_element_type=F32)


def dot_nt(left, right):
    return lax.dot_general(left, right, (((1,), (1,)), ((), ())), preferred_element_type=F32)


def dot_tn(left, right):
    return lax.dot_general(left, right, (((0,), (0,)), ((), ())), preferred_element_type=F32)


def kernel(dims, x_in, wu_in, wd_in, g_in,
           y_out, gi_out, gd_out,
           xh0, wuh, wdh, sh0, ah, ra1, rb1, ra2, rb2, uh,
           U, W, XV, GV1, GV0, SV, AV, DV, GPA, GPB, PP, DR, XR, RES, STA, STB,
           ss, rs, ls, ps, credit):
    D, K, TB, UR, DR_ROWS = dims
    HB = TB // 2
    x, z, y, c = (lax.axis_index(a) for a in ALL)
    cp = 1 - c
    S2 = 2 * DR_ROWS
    XD = D // 4
    ZD = D // 16

    def dev(dx=0, dz=0, dy=0, dc=0):
        wrap = lambda v, d, n: v if d == 0 else lax.rem(v + (d % n), n)
        return (wrap(x, dx, 4), wrap(z, dz, 4), wrap(y, dy, 4), wrap(c, dc, 2))

    partner = dev(dc=1)
    rings = {"x": (x, dev(dx=1), dev(dx=-1)), "z": (z, dev(dz=1), dev(dz=-1)), "y": (y, dev(dy=1), dev(dy=-1))}
    off = lambda v, d: v if d == 0 else lax.rem(v + d, 4)

    used = {"recv": 0, "send": 0, "local": 0}
    free = {"send": [], "local": []}
    keys = []

    def fresh(kind):
        if kind == "recv" and keys:
            return keys.pop()
        used[kind] += 1
        return used[kind] - 1

    def take(kind):
        return free[kind].pop() if free[kind] else fresh(kind)

    def remote(src, dst, send, recv, to):
        return pltpu.make_async_remote_copy(src_ref=src, dst_ref=dst, send_sem=send, recv_sem=recv,
                                            device_id=to, device_id_type=MESH_ID)

    class rcopy:
        def __init__(self, src, dst, to, key=None):
            self.args, self.key = (src, dst, to), fresh("recv") if key is None else key

        def start(self):
            src, dst, to = self.args
            self.sem = take("send")
            self.d = remote(src, dst, ss.at[self.sem], rs.at[self.key], to)
            self.d.start()

        def wait_recv(self):
            self.d.wait_recv()

        def wait_send(self):
            self.d.wait_send()
            free["send"].append(self.sem)

    class lcopy:
        def __init__(self, src, dst):
            self.args = src, dst

        def start(self):
            self.sem = take("local")
            self.d = pltpu.make_async_copy(*self.args, ls.at[self.sem])
            self.d.start()

        def wait(self):
            self.d.wait()
            free["local"].append(self.sem)

    def mo(v, m):
        return pl.multiple_of(v, m)

    class Gather4:
        def __init__(self, axis, src, dst):
            i, right, left = rings[axis]
            lft, rgt = off(i, 3), off(i, 1)
            self.d = [rcopy(src(0), dst(i, 0), right), rcopy(src(1), dst(i, 1), right),
                      rcopy(src(0), dst(i, 0), left), rcopy(src(1), dst(i, 1), left),
                      rcopy(dst(lft, 0), dst(lft, 0), right), rcopy(dst(rgt, 1), dst(rgt, 1), left)]

        def start_first(self):
            self.d[0].start()
            self.d[3].start()

        def start_rest(self):
            self.d[1].start()
            self.d[2].start()

        def start(self):
            self.start_first()
            self.start_rest()

        def forward(self):
            for k in HALVES:
                self.d[3 * k].wait_recv()
                self.d[4 + k].start()

        def neighbours(self):
            self.d[1].wait_recv()
            self.d[2].wait_recv()

        def opposite(self):
            self.d[4].wait_recv()
            self.d[5].wait_recv()

        def finish(self):
            self.neighbours()
            self.opposite()

        def drain(self):
            for d in self.d:
                d.wait_send()

    class Gather8:
        def __init__(self, src, dst):
            self.ring = Gather4("x", src, lambda b, h: dst(b, c, h))
            lft, rgt, opp = off(x, PRV), off(x, NXT), off(x, OPP)
            blocks = [(lft, 0), (rgt, 1), (lft, 1), (rgt, 0), (opp, 0), (opp, 1)]
            self.own = [rcopy(src(h), dst(x, c, h), partner) for h in HALVES]
            self.push = [rcopy(dst(b, c, h), dst(b, c, h), partner) for b, h in blocks]

        def start(self):
            self.ring.start()
            for d in self.own:
                d.start()

        def forward(self):
            self.ring.forward()
            self.push[0].start()
            self.push[1].start()

        def sides(self):
            self.ring.d[1].wait_recv()
            self.push[2].start()
            self.ring.d[2].wait_recv()
            self.push[3].start()

        def last(self):
            self.ring.d[4].wait_recv()
            self.push[4].start()
            self.ring.d[5].wait_recv()
            self.push[5].start()

        def wait_own(self):
            for d in self.own:
                d.wait_recv()

        def wait_push(self, ks):
            for k in ks:
                self.push[k].wait_recv()

        def drain(self):
            self.ring.drain()
            for d in self.own + self.push:
                d.wait_send()

    def add_rows(dst, srcs, rows, step):
        def body(r, carry):
            sl = pl.ds(mo(r * step, step), step)
            if len(dst.shape) == 3:
                for q in range(dst.shape[0]):
                    acc = dst[q, sl, :]
                    for s in srcs:
                        acc = acc + s[q, sl, :]
                    dst[q, sl, :] = acc
            else:
                acc = dst[sl, :]
                for s in srcs:
                    acc = acc + s[sl, :]
                dst[sl, :] = acc
            return carry
        loop(rows // step, body, None)

    barrier = pltpu.get_barrier_semaphore()
    group = [(dx, dc) for dx in (OPP, NXT, PRV, OWN) for dc in HALVES if dx or dc]
    peers = [dev(dx=dx, dc=dc) for dx, dc in group] + [rings[a][k] for a in "zy" for k in (1, 2)]
    for p in peers:
        pl.semaphore_signal(barrier, inc=1, device_id=p, device_id_type=MESH_ID)

    load_u = [[lcopy(wu_in.at[l, :, pl.ds(b * D, D)], RES.at[G0, pl.ds((l * RING + b) * UR, UR), :])
               for b in range(RING)] for l in HALVES]
    load_d = [lcopy(wd_in.at[l], RES.at[X1, pl.ds(l * DR_ROWS, DR_ROWS), :]) for l in HALVES]
    load_x = lcopy(x_in, RES.at[X0])
    load_g = lcopy(g_in, RES.at[G1])
    own_x = lcopy(x_in, XV.at[x, c])
    own_g = lcopy(g_in, GV1.at[x, c])
    own_d0 = lcopy(wd_in.at[0], W.at[y, z])
    for cpy in load_u[0] + load_u[1] + load_d + [load_x, own_d0, own_x, load_g, own_g]:
        cpy.start()

    low = lax.broadcasted_iota(jnp.int32, (UR, S2), 1) < DR_ROWS
    swap = lambda v: pltpu.roll(v, DR_ROWS, 1)
    for l in HALVES:
        for cpy in load_u[l]:
            cpy.wait()
        for b in range(RING):
            rows = pl.ds((l * RING + b) * UR, UR)
            for yy in range(RING):
                for m in HALVES:
                    s0 = RES[G0, rows, pl.ds((2 * m * RING + yy) * S2, S2)].astype(F32)
                    s1 = RES[G0, rows, pl.ds(((2 * m + 1) * RING + yy) * S2, S2)].astype(F32)
                    cols = pl.ds((yy * 2 + m) * S2, S2)
                    AV[l, 0, pl.ds(2 * b * UR, UR), cols] = jnp.where(low, s0, swap(s1)).astype(BF16)
                    AV[l, 0, pl.ds((2 * b + 1) * UR, UR), cols] = jnp.where(low, swap(s0), s1).astype(BF16)
    for cpy in load_d + [load_x, own_d0]:
        cpy.wait()
    pl.semaphore_wait(barrier, len(peers))

    half = lambda h: pl.ds(h * HB, HB)

    def tile_cols(split, q):
        return pl.ds(sum(split[:q]) * (D // RING), split[q] * (D // RING))

    gx0 = Gather8(lambda h: RES.at[X0, half(h)], lambda b, k, h: XV.at[b, k, half(h)])
    gg1 = Gather8(lambda h: RES.at[G1, half(h)], lambda b, k, h: GV1.at[b, k, half(h)])
    up = [U, wuh.at[1]]
    down = [W, wdh.at[1]]
    hr = DR_ROWS // 4

    def quarter(q, h):
        return pl.ds((2 * q + h) * hr, hr)

    def down_first(l):
        to = down[l]
        src = lambda q: lambda h: RES.at[X1, pl.ds(l * DR_ROWS + (2 * q + h) * hr, hr)]
        return [Gather4("z", src(0), lambda b, h: to.at[y, b, quarter(0, h)]),
                Gather4("y", src(1), lambda b, h: to.at[b, z, quarter(1, h)])]

    def down_second(l, split, n):
        to, cs = down[l], tile_cols(split, n)
        return [Gather4("y", lambda h: to.at[y, :, quarter(0, h), cs], lambda b, h: to.at[b, :, quarter(0, h), cs]),
                Gather4("z", lambda h: to.at[:, z, quarter(1, h), cs], lambda b, h: to.at[:, b, quarter(1, h), cs])]

    def up_first(to):
        return [Gather4("y", lambda h: to.at[h, z, y], lambda b, h: to.at[h, z, b]),
                Gather4("z", lambda h: to.at[2 + h, z, y], lambda b, h: to.at[2 + h, b, y])]

    def hidden_cols(n):
        return pl.ds(sum(SPLIT2[:n]) * (K // RING), SPLIT2[n] * (K // RING))

    def up_second(n):
        cs, src = hidden_cols(n), up[1]
        return [Gather4("z", lambda h: src.at[h, z, :, :, cs], lambda b, h: U.at[h, b, :, :, cs]),
                Gather4("y", lambda h: src.at[2 + h, :, y, :, cs], lambda b, h: U.at[2 + h, :, b, :, cs])]

    def up_unit(to, j):
        yj, zj = off(y, j), off(z, j)
        return [Gather4("z", lambda h: to.at[h, z, yj], lambda b, h: to.at[h, b, yj]),
                Gather4("y", lambda h: to.at[2 + h, zj, y], lambda b, h: to.at[2 + h, zj, b])]

    def do(gathers, step):
        for g in gathers:
            getattr(g, step)()

    mine = pl.ds(mo(c * UR, UR), UR)

    def up_exchange(l):
        sends = []
        for dx, dc in group:
            tx, tc = off(x, dx), (cp if dc else c)
            src = AV.at[l, 0, pl.ds(mo((tx * 2 + tc) * UR, UR), UR), :]
            sends.append(rcopy(src, up[l].at[x, z, y, mine, :], dev(dx=dx, dc=dc)))
        for cpy in sends:
            cpy.start()
        return sends

    def keys_of(gathers):
        return [d.key for g in gathers for d in g.d]

    d0a, d0b, d0c = down_first(0), down_second(0, SPLIT3, 0), down_second(0, SPLIT3, 1)
    u0a, u0u = up_first(up[0]), [up_unit(up[0], j) for j in (OWN, PRV, NXT, OPP)]
    keys.extend(keys_of(u0a))
    d0d = down_second(0, SPLIT3, 2)
    keys.extend(keys_of(d0a))
    d1a = down_first(1)
    keys.extend(keys_of(sum(u0u, [])))
    d1b, u1a = down_second(1, WHOLE, 0), up_first(up[1])
    u1b, u1c = up_second(0), up_second(1)
    ex0 = up_exchange(0)
    do(d0a, "start")
    gx0.start()
    ex1 = up_exchange(1)
    my_rows = pl.ds(mo((x * 2 + c) * UR, UR), UR)
    own_u1 = lcopy(AV.at[1, 0, my_rows, :], up[1].at[x, z, y, mine, :])
    own_u1.start()
    own_d1 = lcopy(RES.at[X1, pl.ds(DR_ROWS, DR_ROWS), :], down[1].at[y, z])
    own_d1.start()
    U[x, z, y, mine, :] = AV[0, 0, my_rows, :]
    do(d0a, "forward")
    for cpy in ex0:
        cpy.wait_recv()
    do(u0a, "start")
    do(u0u[0], "start")
    do(u0a, "forward")
    gx0.forward()
    load_g.wait()
    gg1.start()
    do(u0a, "neighbours")
    do(u0u[1], "start")
    do(u0u[2], "start")
    do(u0u[0], "forward")
    do(u0a, "opposite")
    do(u0u[3], "start")
    do(d0a, "finish")
    do(u0u[1], "forward")
    do(u0u[2], "forward")
    do(d0b, "start_first")
    gx0.sides()
    for cpy in ex0 + ex1:
        cpy.wait_send()
    own_u1.wait()
    do(u0u[3], "forward")
    do(u0a + d0a, "drain")
    do(d0b, "start_rest")
    do(d0c, "start_first")
    gg1.forward()
    do(d0b, "forward")
    do(d0c, "start_rest")
    do(d1a, "start")
    gx0.last()
    gx0.wait_own()
    gx0.wait_push(range(len(gx0.push)))
    own_x.wait()
    save_x = lcopy(XV, xh0)
    save_x.start()
    gx0.drain()
    for unit in u0u:
        do(unit, "finish")
    save_u0 = lcopy(U, wuh.at[0])
    save_u0.start()

    T2 = 2 * TB
    ND = D // 4
    NK = K // 4

    def up_tile(t, n):
        cols = pl.ds(mo(n * NK, NK), NK)
        return dot_nn(XV[t].reshape(T2, D), U[:, :, :, :, cols].reshape(D, NK)), cols

    def hidden0(t):
        for n in range(RING):
            pre, cols = up_tile(t, n)
            act, slope = gelu_parts(pre)
            AV[t, :, :, cols] = act.astype(BF16).reshape(2, TB, NK)
            SV[t, :, :, cols] = slope.reshape(2, TB, NK)

    def hidden1_tile(t, n):
        pre, cols = up_tile(t, n)
        act, slope = gelu_parts(pre)
        AV[t, :, :, cols] = act.astype(BF16).reshape(2, TB, NK)
        DV[t, :, cols] = (SV[t, :, :, cols].reshape(T2, NK) * slope).astype(BF16)

    def hidden1(t, part):
        for n in range(sum(SPLIT2[:part]), sum(SPLIT2[:part + 1])):
            hidden1_tile(t, n)

    def dact(gv, t, n):
        return dot_nt(gv[t].reshape(T2, D), W[n].reshape(NK, D))

    def dact1(t):
        def body(n, carry):
            SV[t, :, :, pl.ds(mo(n * NK, NK), NK)] = dact(GV1, t, n).reshape(2, TB, NK)
            return carry
        loop(RING, body, None)

    def dact0(t):
        def body(n, carry):
            cols = pl.ds(mo(n * NK, NK), NK)
            DV[t, :, cols] = (dact(GV0, t, n) * SV[t, :, :, cols].reshape(T2, NK)).astype(BF16)
            return carry
        loop(RING, body, None)

    def down_part(act, j, lo, tiles):
        t = lax.rem(x + j, RING)

        def body(n, carry):
            cols = pl.ds(mo((lo + n) * ND, ND), ND)
            PP[j, :, :, cols] = dot_nn(act[t, :, :, 0:K].reshape(T2, K), W[:, :, :, cols].reshape(K, ND)).reshape(2, TB, ND)
            return carry
        loop(tiles, body, None)

    def dx_part(j, lo, tiles):
        t = lax.rem(x + j, RING)

        def body(n, carry):
            cols = pl.ds(mo((lo + n) * ND, ND), ND)
            PP[j, :, :, cols] = dot_nt(DV[t], U[lo + n].reshape(ND, K)).reshape(2, TB, ND)
            return carry
        loop(tiles, body, None)

    class Reduce8:
        def __init__(self, part, index, split, old=()):
            self.part, self.index, self.split = part, index, split
            keys.extend(old)
            _, right, left = rings["x"]
            self.right, self.left = right, left
            self.pair, self.m, self.first = [], [], []
            for q in range(len(split)):
                cq = self.cols(q)
                first = sorted(fresh("recv") for j in range(RING))
                self.pair.append([self.swap(j, q, first[0]) for j in range(RING)])
                self.first.append(first[0])
                src = lambda j, h: PP.at[j, c, half(h), cq]
                self.m.append([rcopy(src(*PIECES[k]), XR.at[k, :, cq], left if k % 2 else right) for k in range(ARRIVALS)])
            keys.clear()

        def cols(self, q):
            return tile_cols(self.split, q)

        def swap(self, j, q, first):
            cq = self.cols(q)
            return remote(PP.at[j, cp, :, cq], DR.at[j, :, cq], ps.at[q * RING + j], rs.at[first + j], partner)

        def compute(self, j, q):
            self.part(j, sum(self.split[:q]), self.split[q])
            self.pair[q][j].start()

        def compute_all(self, q):
            def body(i, carry):
                j = lax.rem(i + 1, RING)
                self.part(j, sum(self.split[:q]), self.split[q])
                self.swap(j, q, self.first[q]).start()
                return carry
            loop(RING, body, None)

        def combine(self, j, q):
            self.pair[q][j].wait_recv()
            add_rows(PP.at[j, c, :, self.cols(q)], [DR.at[j, :, self.cols(q)]], TB, min(TB, 16))

        def opposite(self, q):
            self.m[q][0].start()
            self.m[q][1].start()

        def side(self, j, q):
            self.combine(j, q)
            self.m[q][2 if j == NXT else 3].start()

        def send(self, q):
            self.combine(OPP, q)
            self.opposite(q)
            self.side(NXT, q)
            self.side(PRV, q)

        def relay(self, q):
            for k, j, h in ((0, NXT, 0), (1, PRV, 1)):
                self.m[q][k].wait_recv()
                add_rows(PP.at[j, c, half(h), self.cols(q)], [XR.at[k, :, self.cols(q)]], HB, min(HB, 16))
                self.m[q][4 + k].start()

        def finish(self, q, res, outs):
            for d in self.m[q][2:]:
                d.wait_recv()
            step, cq = min(HB, 16), self.cols(q)
            for h, (kl, kr) in enumerate(((4, 3), (2, 5))):
                def body(r, carry):
                    lo = pl.ds(mo(r * step, step), step)
                    sl = pl.ds(mo(h * HB + r * step, step), step)
                    tot = PP[OWN, c, sl, cq] + (XR[kl, lo, cq] + XR[kr, lo, cq])
                    val = (res[sl, cq].astype(F32) + tot).astype(BF16)
                    for o in outs:
                        o[sl, cq] = val
                    return carry
                loop(HB // step, body, None)

        def drain(self):
            for d in sum(self.pair + self.m, []):
                d.wait_send()

        def release(self):
            self.drain()
            for k, to in enumerate((self.right, self.left, partner)):
                pl.semaphore_signal(credit.at[k], inc=1, device_id=to, device_id_type=MESH_ID)

        def acquire(self):
            for k in range(len((self.right, self.left, partner))):
                pl.semaphore_wait(credit.at[k], 1)

    def grad_a(j, dst, halves=None, q=None):
        t = off(z, j)

        def rows(h, carry):
            lo = [pl.ds(mo((2 * h + q) * XD + t * ZD, ZD), ZD) for q in HALVES]
            lhs = jnp.concatenate([XV[:, :, :, s].reshape(8 * TB, ZD) for s in lo], axis=1)

            def body(n, carry):
                cols = pl.ds(mo(n * ND, ND), ND)
                dst[h, :, :, cols] = dot_tn(lhs, DV[:, :, cols].reshape(8 * TB, ND)).reshape(2, ZD, ND)
                return carry
            return loop(K // ND, body, carry) if q is None else body(q, carry)
        if halves is None:
            loop(2, rows, None)
        else:
            for h in halves:
                rows(h, None)

    def grad_b(gv, j, dst, lo=0, tiles=RING):
        cols_l = pl.ds(mo(off(y, j) * NK, NK), NK)

        def body(i, carry):
            m = lo + i
            cols = pl.ds(mo(m * ND, ND), ND)
            out = dot_tn(AV[:, :, :, cols_l].reshape(8 * TB, NK), gv[:, :, :, cols].reshape(8 * TB, ND))
            dst[:, m // 2, :, pl.ds(mo(lax.rem(m, 2) * ND, ND), ND)] = out.reshape(2, NK // 2, ND)
            return carry
        loop(tiles, body, None)

    grad_keys = [keys_of(sum(u0u, u0a) + d0a), [d.key for d in ex0 + ex1] + keys_of(d0b + d0c)]

    def grad_key(l):
        return grad_keys[l].pop() if grad_keys[l] else fresh("recv")

    class Reduce4:
        def __init__(self, l, axis, part, recv, stage):
            _, right, left = rings[axis]
            self.part, self.recv, self.stage = part, recv, stage
            self.m = [rcopy(part(*PIECES[k]), recv(k), left if k % 2 else right, grad_key(l))
                      for k in range(ARRIVALS)]
            self.loads = [lcopy(recv(k), stage(k)) for k in range(ARRIVALS)] if stage else None

        def opposite(self):
            self.m[0].start()
            self.m[1].start()

        def sides(self, j):
            self.m[2 if j == NXT else 3].start()

        def fetch(self, k):
            self.m[k].wait_send()
            self.m[k].wait_recv()
            if self.loads:
                self.loads[k].start()

        def absorb(self, k):
            if self.loads:
                self.loads[k].wait()
            dst = self.part(*TARGETS[k])
            add_rows(dst, [(self.stage or self.recv)(k)], dst.shape[1], min(dst.shape[1], 16))

    def arrive(reduces, ks):
        for k in ks:
            for r in reduces:
                r.fetch(k)
        for k in ks:
            for r in reduces:
                r.absorb(k)

    def relay(reduces):
        for k in (0, 1):
            for r in reduces:
                r.fetch(k)
        for k in (0, 1):
            for r in reduces:
                r.absorb(k)
                r.m[4 + k].start()

    hq = DR_ROWS // 2
    own_grads = [(SV.at[pl.ds(0, 2)], SV.at[pl.ds(2, 2)]), (GPA.at[OWN], GPB.at[OWN])]

    def third(k, rows):
        return pl.ds((k // 2) * rows, rows)

    def reduce_a(l, q, chunks):
        own = own_grads[l][0]
        ca = pl.ds(q * (K // chunks), K // chunks)

        def part(j, h):
            return (own if j == OWN else GPA.at[j]).at[h, :, :, ca]

        def part2(j, h):
            return own.at[h, :, pl.ds(mo(off(y, j) * 2 * UR, 2 * UR), 2 * UR), ca]
        if l < q:
            second = lambda k: GPA.at[OWN, k % 2, :, third(k, 2 * UR), ca], None
        else:
            second = lambda k: ra2.at[l, k, :, :, ca], lambda k: STA.at[k % 2, :, :, ca]
        return (Reduce4(l, "z", part, lambda k: ra1.at[l, k, :, :, ca], lambda k: part(*PIECES[k])),
                Reduce4(l, "y", part2, *second))

    def reduce_b(l, q):
        own, nb = own_grads[l][1], pl.ds(q, 1)

        def part(j, h):
            return (own if j == OWN else GPB.at[j]).at[h, nb]

        def part2(j, h):
            t = off(z, j)
            return own.at[t // 2, nb, pl.ds(mo(lax.rem(t, 2) * DR_ROWS + h * hq, hq), hq), :]
        if l < q:
            second = lambda k: GPB.at[OWN, k % 2, nb, third(k, hq), :], None
        else:
            second = lambda k: rb2.at[l, k, nb], lambda k: STB.at[k % 2, nb]
        return (Reduce4(l, "y", part, lambda k: rb1.at[l, k, nb], lambda k: part(*PIECES[k])),
                Reduce4(l, "z", part2, *second))

    def sides(reduces, j):
        for r in reduces:
            r.sides(j)

    def second_start(reduces):
        for r in reduces:
            r.opposite()
            r.sides(NXT)
            r.sides(PRV)

    def up_out(l, q, chunks):
        own = own_grads[l][0]
        ca = pl.ds(q * (K // chunks), K // chunks)

        def rows_of(tx, tc):
            return own.at[tx // 2, lax.rem(tx, 2), pl.ds(mo((2 * y + tc) * UR, UR), UR), ca]
        to = uh.at[l, x, mine, ca]
        sends = [rcopy(rows_of(off(x, dx), cp if dc else c), to, dev(dx=dx, dc=dc), grad_key(l)) for dx, dc in group]
        local = [lcopy(rows_of(x, c), to)]
        for cpy in sends + local:
            cpy.start()
        return sends, local

    def down_out(l, n):
        cpy = lcopy(own_grads[l][1].at[z // 2, n, pl.ds(mo(lax.rem(z, 2) * DR_ROWS, DR_ROWS), DR_ROWS), :],
                    gd_out.at[l, :, pl.ds(n * K, K)])
        cpy.start()
        return [], [cpy]

    def grads_out_finish(state):
        for cpy in state[0]:
            cpy.wait_recv()
            cpy.wait_send()
        for cpy in state[1]:
            cpy.wait()

    r = Reduce8(functools.partial(down_part, AV), 0, SPLIT3)
    r_keys = sorted([d.key for m in r.m for d in m] + [f + j for f in r.first for j in range(RING)])
    hidden0(off(x, OPP))
    hidden0(off(x, NXT))
    do(d0b, "finish")
    r.compute(OPP, 0)
    r.compute(NXT, 0)
    do(d0c, "forward")
    do(d0d, "start")
    r.combine(OPP, 0)
    r.opposite(0)
    do(sum(u0u, []), "drain")
    hidden0(off(x, PRV))
    r.compute(PRV, 0)
    r.side(NXT, 0)
    do(d1a, "forward")
    hidden0(off(x, OWN))
    r.side(PRV, 0)
    save_s = lcopy(SV, sh0)
    save_s.start()
    save_a0 = lcopy(AV, ah.at[0])
    save_a0.start()
    gg1.sides()
    do(d0c, "finish")
    r.compute_all(1)
    r.relay(0)
    do(d0d, "forward")
    for cpy in ex1:
        cpy.wait_recv()
    own_d1.wait()
    do(u1a, "start")
    r.send(1)
    do(d1a, "finish")
    do(d1b, "start")
    gg1.last()
    save_x.wait()
    do(d0d, "finish")
    save_d0 = lcopy(W, wdh.at[0])
    save_d0.start()
    r.compute(OPP, 2)
    r.relay(1)
    save_u0.wait()
    do(u1a, "forward")
    r.compute(NXT, 2)
    r.combine(OPP, 2)
    r.opposite(2)
    r.compute(PRV, 2)
    r.side(NXT, 2)
    r.compute(OWN, 2)
    r.side(PRV, 2)
    r.compute(OWN, 0)
    for q in range(len(SPLIT3)):
        r.combine(OWN, q)

    def gather_keys(gathers):
        return [d.key for g in gathers for d in g.ring.d + g.own + g.push]

    def token_gathers(slot, buf):
        def make(q):
            cq = tile_cols(SPLIT2, q)
            return Gather8(lambda h: RES.at[slot, half(h), cq], lambda b, k, h: buf.at[b, k, half(h), cq])
        return [make(0), make(1)]

    keys.extend(gather_keys((gx0,)))
    gx1 = token_gathers(X1, XV)
    do(d1a, "drain")
    do(d1b, "forward")
    for q in HALVES:
        r.finish(q, RES.at[X0], [RES.at[X1], XV.at[x, c]])
    r.relay(2)
    gx1[0].start()
    do(u1a, "finish")
    do(u1b, "start")
    do(u1c, "start_first")
    pair, rest = pl.ds(0, 2), pl.ds(2, 2)
    own_up = [lcopy(up[1].at[pair, z], U.at[pair, z]), lcopy(up[1].at[rest, :, y], U.at[rest, :, y])]
    for cpy in own_up:
        cpy.start()
    gg1.wait_own()
    gg1.wait_push(range(len(gg1.push)))
    own_g.wait()
    save_d0.wait()
    do(d0b + d0c + d0d, "drain")
    gg1.drain()
    do(d1b, "finish")
    load_w1d = lcopy(wdh.at[1], W)
    load_w1d.start()
    r.finish(2, RES.at[X0], [RES.at[X1], XV.at[x, c]])
    gx1[1].start()
    save_s.wait()
    do(u1b, "forward")
    do(u1c, "start_rest")
    load_w1d.wait()
    dact1(off(x, OWN))
    gx1[0].forward()
    r.release()
    dact1(off(x, NXT))
    gx1[0].sides()
    dact1(off(x, PRV))
    do(u1c, "forward")
    do(u1b, "finish")
    dact1(off(x, OPP))
    load_w0d_again = lcopy(wdh.at[0], W)
    load_w0d_again.start()
    save_a0.wait()
    do(gx1, "wait_own")
    for cpy in own_up:
        cpy.wait()
    hidden1(off(x, OWN), 0)
    do(gx1[1:], "forward")
    do(gx1[1:], "sides")
    for j in (PRV, NXT):
        for g in gx1:
            g.wait_push(PUSHES[j])
        hidden1(off(x, j), 0)
    gx1[0].last()
    do(u1c, "finish")
    hidden1(off(x, OWN), 1)
    hidden1(off(x, PRV), 1)
    gx1[1].last()
    hidden1(off(x, NXT), 1)
    for g in gx1:
        g.wait_push(PUSHES[OPP])
    hidden1_tile(off(x, OPP), off(y, OPP))

    (a1, a2), (b1, b2) = zip(*[reduce_a(1, q, 2) for q in HALVES]), zip(*[reduce_b(1, q) for q in HALVES])
    first1, second1 = b1 + a1, b2 + a2
    grad_b(GV1, OPP, GPB.at[OPP], 0, 2)
    b1[0].opposite()
    for n in (PRV, OWN, NXT):
        hidden1_tile(off(x, OPP), off(y, n))
    for q in HALVES:
        for h in HALVES:
            grad_a(OPP, GPA.at[OPP], (h,), q)
            a1[q].m[h].start()
    load_s0 = lcopy(sh0, SV)
    load_s0.start()
    save_a1 = lcopy(AV, ah.at[1])
    save_a1.start()
    grad_b(GV1, OPP, GPB.at[OPP], 2, 2)
    b1[1].opposite()
    r = Reduce8(dx_part, 1, SPLIT2, r_keys)
    r.acquire()
    r.compute(OPP, 0)
    r.compute(NXT, 0)
    r.combine(OPP, 0)
    r.opposite(0)
    r.compute(PRV, 0)
    r.side(NXT, 0)
    r.side(PRV, 0)
    r.compute_all(1)
    load_w0u_again = lcopy(wuh.at[0], U)
    r.compute(OWN, 0)
    do(u1b + u1c, "drain")
    load_w0u_again.start()
    grad_b(GV1, NXT, GPB.at[NXT])
    sides(b1, NXT)
    grad_b(GV1, PRV, GPB.at[PRV])
    sides(b1, PRV)
    r.relay(0)
    r.send(1)
    grad_a(NXT, GPA.at[NXT])
    sides(a1, NXT)
    grad_a(PRV, GPA.at[PRV])
    sides(a1, PRV)
    r.combine(OWN, 0)
    r.combine(OWN, 1)
    keys.extend(gather_keys(gx1))
    gg0 = token_gathers(G0, GV0)
    r.relay(1)
    r.finish(0, RES.at[G1], [RES.at[G0], GV0.at[x, c]])
    gg0[0].start()
    relay(first1)
    grad_b(GV1, OWN, GPB.at[OWN])
    save_a1.wait()
    load_a0 = lcopy(ah.at[0], AV)
    load_a0.start()
    do(d1b + u1a, "drain")
    load_a1 = lcopy(ah.at[1], GV1.at[:, :, :, 0:K])
    load_a1.start()
    r.finish(1, RES.at[G1], [RES.at[G0], GV0.at[x, c]])
    gg0[1].start()
    gg0[0].forward()
    grad_a(OWN, GPA.at[OWN])
    do(gx1, "drain")
    load_x0 = lcopy(xh0, XV)
    load_x0.start()
    gg0[0].sides()
    r.release()
    gg0[1].forward()
    gg0[0].last()
    load_w0d_again.wait()
    load_s0.wait()
    do(gg0, "wait_own")
    dact0(off(x, OWN))
    gg0[1].sides()
    gg0[1].last()
    for g in gg0:
        g.wait_push(PUSHES[PRV])
    dact0(off(x, PRV))
    for g in gg0:
        g.wait_push(PUSHES[NXT])
    dact0(off(x, NXT))
    for g in gg0:
        g.wait_push(PUSHES[OPP])

    (a1n, a2n), (b1n, b2n) = zip(*[reduce_a(0, q, 2) for q in HALVES]), zip(*[reduce_b(0, q) for q in HALVES])
    load_a0.wait()
    grad_b(GV0, OPP, GPB.at[OPP])
    b1n[0].opposite()
    dact0(off(x, OPP))
    load_w1d_again = lcopy(wdh.at[1], W)
    load_w1d_again.start()
    load_x0.wait()
    for h in HALVES:
        grad_a(OPP, GPA.at[OPP], (h,))
        a1n[0].m[h].start()
    arrive(first1, EARLY + LATE)
    second_start(second1)
    load_w0u_again.wait()
    r = Reduce8(dx_part, 2, WHOLE, r_keys)
    r.acquire()
    r.compute_all(0)
    r.send(0)
    grad_b(GV0, NXT, GPB.at[NXT])
    b1n[0].sides(NXT)
    grad_b(GV0, PRV, GPB.at[PRV])
    b1n[0].sides(PRV)
    grad_a(NXT, GPA.at[NXT])
    a1n[0].sides(NXT)
    grad_a(PRV, GPA.at[PRV])
    a1n[0].sides(PRV)
    relay(second1)
    r.relay(0)
    relay((b1n[0], a1n[0]))
    for red in (b1n[1], a1n[1]):
        red.opposite()
        red.sides(NXT)
        red.sides(PRV)
    r.combine(OWN, 0)
    grad_b(GV0, OWN, own_grads[0][1])
    grad_a(OWN, own_grads[0][0])
    r.finish(0, RES.at[G0], [RES.at[X0]])
    r.release()
    write_gi = lcopy(RES.at[X0], gi_out)
    write_gi.start()
    arrive((b1n[0], a1n[0]), EARLY)
    arrive(second1, EARLY)
    arrive(second1, LATE)
    state1 = [up_out(1, q, 2) for q in HALVES] + [down_out(1, n) for n in HALVES]
    load_a1.wait()
    load_w1d_again.wait()
    r = Reduce8(functools.partial(down_part, GV1), 3, WHOLE, r_keys)
    r.acquire()
    r.compute_all(0)
    r.send(0)
    r.combine(OWN, 0)
    arrive((b1n[0], a1n[0]), LATE)
    for state in state1:
        grads_out_finish(state)
    relay((b1n[1], a1n[1]))
    second_start((a2n[0], b2n[0]))
    r.relay(0)
    arrive((b1n[1], a1n[1]), EARLY)
    arrive((b1n[1], a1n[1]), LATE)
    last = (a2n[1], b2n[1])
    for red in last:
        red.opposite()
    relay((b2n[0], a2n[0]))
    sides(last, NXT)
    sides(last, PRV)
    arrive((b2n[0], a2n[0]), EARLY)
    relay((b2n[1], a2n[1]))
    arrive((a2n[0],), LATE)
    state0 = [up_out(0, 0, 2)]
    arrive((a2n[1], b2n[1]), EARLY)
    arrive((a2n[1],), LATE)
    state0.append(up_out(0, 1, 2))
    for q in HALVES:
        arrive((b2n[q],), LATE)
        state0.append(down_out(0, q))
    r.finish(0, RES.at[X1], [RES.at[G1]])
    write_y = lcopy(RES.at[G1], y_out)
    write_y.start()
    r.drain()
    do(gg0, "drain")
    write_gi.wait()
    write_y.wait()
    for state in state0:
        grads_out_finish(state)
    assert used["recv"] <= N_RECV and used["send"] <= N_SEND and used["local"] <= N_LOCAL


def finish_kernel(y_in, gi_in, gu_in, gd_in, y_out, gi_out, gu_out, gd_out, ybuf, gibuf, gubuf, gdbuf, gushuf, sems):
    layers, ur, ff = gu_out.shape
    s2 = ff // 64
    half = s2 // 2
    loads = [pltpu.make_async_copy(a, b, sems.at[0, k])
             for k, (a, b) in enumerate(((gu_in, gubuf), (gd_in, gdbuf), (y_in, ybuf), (gi_in, gibuf)))]
    stores = [pltpu.make_async_copy(a, b, sems.at[1, k])
              for k, (a, b) in enumerate(((gushuf, gu_out), (gdbuf, gd_out), (ybuf, y_out), (gibuf, gi_out)))]
    for cpy in loads:
        cpy.start()
    low = lax.broadcasted_iota(jnp.int32, (ur, s2), 1) < half
    swap = lambda v: pltpu.roll(v, half, 1)
    loads[0].wait()
    for l in range(layers):
        for b in range(RING):
            for yy in range(RING):
                for m in HALVES:
                    cols = pl.ds((yy * 2 + m) * s2, s2)
                    t0, t1 = (gubuf[l, b, pl.ds(k * ur, ur), cols] for k in HALVES)
                    strip = (b * RING + 2 * m) * RING + yy
                    gushuf[l, :, pl.ds(strip * s2, s2)] = jnp.where(low, t0, swap(t1))
                    gushuf[l, :, pl.ds((strip + RING) * s2, s2)] = jnp.where(low, swap(t0), t1)
    stores[0].start()
    for k in range(1, len(loads)):
        loads[k].wait()
        stores[k].start()
    for cpy in stores:
        cpy.wait()


def solution(mesh, interpret=None):
    fine = Mesh(np.asarray(mesh.devices).reshape(4, 4, 4, 2), ALL)
    tok_spec = P(ALL, None)
    weight_spec = P(None, ALL, None)

    def device_step(x_loc, up_loc, down_loc, g_loc):
        layers, ur, ff = up_loc.shape
        dr, dm = down_loc.shape[1:]
        tb = x_loc.shape[0]
        k = ff // 8
        zd = dm // 16
        hbm = lambda shape, dt: jax.ShapeDtypeStruct(shape, dt)
        outs = [
            hbm((tb, dm), BF16), hbm((tb, dm), BF16), hbm((layers, dr, dm), F32),
            hbm((RING, CORES, tb, dm), BF16),
            hbm((layers, RING, RING, RING, 2 * ur, k), BF16),
            hbm((layers, RING, RING, dr, dm), BF16),
            hbm((RING, CORES, tb, k), F32), hbm((layers, RING, CORES, tb, k), BF16),
            *[hbm((layers, ARRIVALS, CORES, n, k), F32) for n in (zd, zd, 2 * ur, 2 * ur)],
            hbm((layers, RING, 2 * ur, k), F32),
        ]
        vm = pltpu.VMEM
        scratch = [
            vm((RING, RING, RING, 2 * ur, k), BF16), vm((RING, RING, dr, dm), BF16),
            vm((RING, CORES, tb, dm), BF16), vm((RING, CORES, tb, dm), BF16), vm((RING, CORES, tb, dm), BF16),
            vm((RING, CORES, tb, k), F32), vm((RING, CORES, tb, k), BF16), vm((RING, 2 * tb, k), BF16),
            vm((RING, CORES, CORES, zd, k), F32), vm((RING, CORES, CORES, zd, k), F32),
            vm((RING, CORES, tb, dm), F32), vm((4, tb, dm), F32), vm((6, tb // 2, dm), F32),
            vm((4, tb, dm), BF16), vm((CORES, CORES, 2 * ur, k), F32), vm((CORES, CORES, 2 * ur, k), F32),
            *[pltpu.SemaphoreType.DMA((n,)) for n in (N_SEND, N_RECV, N_LOCAL, len(SPLIT3) * RING)],
            pltpu.SemaphoreType.REGULAR((3,)),
        ]
        anyspec = pl.BlockSpec(memory_space=pl.ANY)
        call = pl.pallas_call(
            functools.partial(kernel, (dm, k, tb, ur, dr)),
            out_shape=outs,
            in_specs=[anyspec] * 4,
            out_specs=[anyspec] * len(outs),
            scratch_shapes=scratch,
            compiler_params=pltpu.CompilerParams(collective_id=0, has_side_effects=True, vmem_limit_bytes=67043328),
            name="mlp_stack",
            **({"interpret": interpret} if interpret else {}),
        )
        y_raw, gi_raw, gd_raw, *_, gu_raw = call(x_loc, up_loc, down_loc, g_loc)
        raws = (y_raw, gi_raw, gu_raw, gd_raw)
        outs = [hbm((tb, dm), BF16), hbm((tb, dm), BF16), hbm((layers, ur, ff), F32), hbm((layers, dr, dm), F32)]
        return tuple(pl.pallas_call(
            finish_kernel, out_shape=outs, in_specs=[anyspec] * len(outs), out_specs=[anyspec] * len(outs),
            scratch_shapes=[vm(v.shape, v.dtype) for v in raws] + [vm(outs[2].shape, F32), pltpu.SemaphoreType.DMA((2, len(outs)))],
            name="write_out")(*raws))

    return jax.shard_map(device_step, mesh=fine, in_specs=(tok_spec, weight_spec, weight_spec, tok_spec),
                         out_specs=(tok_spec, tok_spec, weight_spec, weight_spec), check_vma=False)
```

```python
import functools

import jax
import jax.numpy as jnp
import numpy as np
from jax import lax
from jax.experimental import pallas as pl
from jax.experimental.pallas import tpu as pltpu
from jax.sharding import Mesh, PartitionSpec as P

MESH_ID = pl.DeviceIdType.MESH
ALL = ("x", "z", "y", "c")
F32, BF16 = jnp.float32, jnp.bfloat16
RING, CORES, ARRIVALS = 4, 2, 6
OWN, NXT, OPP, PRV = range(RING)
X0, X1, G1, G0 = range(RING)
HALVES = (0, 1)
WHOLE, SPLIT2, SPLIT3 = (4,), (2, 2), (1, 1, 2)
PIECES = ((OPP, 0), (OPP, 1), (NXT, 1), (PRV, 0), (NXT, 0), (PRV, 1))
TARGETS = ((NXT, 0), (PRV, 1), (OWN, 1), (OWN, 0), (OWN, 0), (OWN, 1))
EARLY, LATE = (2, 3), (4, 5)
PUSHES = {PRV: (0, 2), NXT: (1, 3), OPP: (4, 5)}
N_RECV, N_SEND, N_LOCAL = 206, 110, 19


def gelu_parts(pre_act):
    norm_cdf = 0.5 * (1.0 + lax.erf(pre_act * (2.0 ** -0.5)))
    norm_pdf = jnp.exp(-0.5 * pre_act * pre_act) * ((2.0 * jnp.pi) ** -0.5)
    return pre_act * norm_cdf, norm_cdf + pre_act * norm_pdf


def loop(n, body, init):
    return lax.fori_loop(0, n, body, init)


def dot_nn(left, right):
    return lax.dot_general(left, right, (((1,), (0,)), ((), ())), preferred_element_type=F32)


def dot_nt(left, right):
    return lax.dot_general(left, right, (((1,), (1,)), ((), ())), preferred_element_type=F32)


def dot_tn(left, right):
    return lax.dot_general(left, right, (((0,), (0,)), ((), ())), preferred_element_type=F32)


def kernel(dims, x_in, wu_in, wd_in, g_in,
           y_out, gi_out, gd_out,
           xh0, wuh, wdh, sh0, ah, ra1, rb1, ra2, rb2, uh,
           U, W, XV, GV1, GV0, SV, AV, DV, GPA, GPB, PP, DR, XR, RES, STA, STB,
           ss, rs, ls, ps, credit):
    D, K, TB, UR, DR_ROWS = dims
    HB = TB // 2
    x, z, y, c = (lax.axis_index(a) for a in ALL)
    cp = 1 - c
    S2 = 2 * DR_ROWS
    XD = D // 4
    ZD = D // 16

    def dev(dx=0, dz=0, dy=0, dc=0):
        wrap = lambda v, d, n: v if d == 0 else lax.rem(v + (d % n), n)
        return (wrap(x, dx, 4), wrap(z, dz, 4), wrap(y, dy, 4), wrap(c, dc, 2))

    partner = dev(dc=1)
    rings = {"x": (x, dev(dx=1), dev(dx=-1)), "z": (z, dev(dz=1), dev(dz=-1)), "y": (y, dev(dy=1), dev(dy=-1))}
    off = lambda v, d: v if d == 0 else lax.rem(v + d, 4)

    used = {"recv": 0, "send": 0, "local": 0}
    free = {"send": [], "local": []}
    keys = []

    def fresh(kind):
        if kind == "recv" and keys:
            return keys.pop()
        used[kind] += 1
        return used[kind] - 1

    def take(kind):
        return free[kind].pop() if free[kind] else fresh(kind)

    def remote(src, dst, send, recv, to):
        return pltpu.make_async_remote_copy(src_ref=src, dst_ref=dst, send_sem=send, recv_sem=recv,
                                            device_id=to, device_id_type=MESH_ID)

    class rcopy:
        def __init__(self, src, dst, to, key=None):
            self.args, self.key = (src, dst, to), fresh("recv") if key is None else key

        def start(self):
            src, dst, to = self.args
            self.sem = take("send")
            self.d = remote(src, dst, ss.at[self.sem], rs.at[self.key], to)
            self.d.start()

        def wait_recv(self):
            self.d.wait_recv()

        def wait_send(self):
            self.d.wait_send()
            free["send"].append(self.sem)

    class lcopy:
        def __init__(self, src, dst):
            self.args = src, dst

        def start(self):
            self.sem = take("local")
            self.d = pltpu.make_async_copy(*self.args, ls.at[self.sem])
            self.d.start()

        def wait(self):
            self.d.wait()
            free["local"].append(self.sem)

    def mo(v, m):
        return pl.multiple_of(v, m)

    class Gather4:
        def __init__(self, axis, src, dst):
            i, right, left = rings[axis]
            lft, rgt = off(i, 3), off(i, 1)
            self.d = [rcopy(src(0), dst(i, 0), right), rcopy(src(1), dst(i, 1), right),
                      rcopy(src(0), dst(i, 0), left), rcopy(src(1), dst(i, 1), left),
                      rcopy(dst(lft, 0), dst(lft, 0), right), rcopy(dst(rgt, 1), dst(rgt, 1), left)]

        def start_first(self):
            self.d[0].start()
            self.d[3].start()

        def start_rest(self):
            self.d[1].start()
            self.d[2].start()

        def start(self):
            self.start_first()
            self.start_rest()

        def forward(self):
            for k in HALVES:
                self.d[3 * k].wait_recv()
                self.d[4 + k].start()

        def neighbours(self):
            self.d[1].wait_recv()
            self.d[2].wait_recv()

        def opposite(self):
            self.d[4].wait_recv()
            self.d[5].wait_recv()

        def finish(self):
            self.neighbours()
            self.opposite()

        def drain(self):
            for d in self.d:
                d.wait_send()

    class Gather8:
        def __init__(self, src, dst):
            self.ring = Gather4("x", src, lambda b, h: dst(b, c, h))
            lft, rgt, opp = off(x, PRV), off(x, NXT), off(x, OPP)
            blocks = [(lft, 0), (rgt, 1), (lft, 1), (rgt, 0), (opp, 0), (opp, 1)]
            self.own = [rcopy(src(h), dst(x, c, h), partner) for h in HALVES]
            self.push = [rcopy(dst(b, c, h), dst(b, c, h), partner) for b, h in blocks]

        def start(self):
            self.ring.start()
            for d in self.own:
                d.start()

        def forward(self):
            self.ring.forward()
            self.push[0].start()
            self.push[1].start()

        def sides(self):
            self.ring.d[1].wait_recv()
            self.push[2].start()
            self.ring.d[2].wait_recv()
            self.push[3].start()

        def last(self):
            self.ring.d[4].wait_recv()
            self.push[4].start()
            self.ring.d[5].wait_recv()
            self.push[5].start()

        def wait_own(self):
            for d in self.own:
                d.wait_recv()

        def wait_push(self, ks):
            for k in ks:
                self.push[k].wait_recv()

        def drain(self):
            self.ring.drain()
            for d in self.own + self.push:
                d.wait_send()

    def add_rows(dst, srcs, rows, step):
        def body(r, carry):
            sl = pl.ds(mo(r * step, step), step)
            if len(dst.shape) == 3:
                for q in range(dst.shape[0]):
                    acc = dst[q, sl, :]
                    for s in srcs:
                        acc = acc + s[q, sl, :]
                    dst[q, sl, :] = acc
            else:
                acc = dst[sl, :]
                for s in srcs:
                    acc = acc + s[sl, :]
                dst[sl, :] = acc
            return carry
        loop(rows // step, body, None)

    barrier = pltpu.get_barrier_semaphore()
    group = [(dx, dc) for dx in (OPP, NXT, PRV, OWN) for dc in HALVES if dx or dc]
    peers = [dev(dx=dx, dc=dc) for dx, dc in group] + [rings[a][k] for a in "zy" for k in (1, 2)]
    for p in peers:
        pl.semaphore_signal(barrier, inc=1, device_id=p, device_id_type=MESH_ID)

    load_u = [[lcopy(wu_in.at[l, :, pl.ds(b * D, D)], RES.at[G0, pl.ds((l * RING + b) * UR, UR), :])
               for b in range(RING)] for l in HALVES]
    load_d = [lcopy(wd_in.at[l], RES.at[X1, pl.ds(l * DR_ROWS, DR_ROWS), :]) for l in HALVES]
    load_x = lcopy(x_in, RES.at[X0])
    load_g = lcopy(g_in, RES.at[G1])
    own_x = lcopy(x_in, XV.at[x, c])
    own_g = lcopy(g_in, GV1.at[x, c])
    own_d0 = lcopy(wd_in.at[0], W.at[y, z])
    for cpy in load_u[0] + load_u[1] + load_d + [load_x, own_d0, own_x, load_g, own_g]:
        cpy.start()

    low = lax.broadcasted_iota(jnp.int32, (UR, S2), 1) < DR_ROWS
    swap = lambda v: pltpu.roll(v, DR_ROWS, 1)
    for l in HALVES:
        for cpy in load_u[l]:
            cpy.wait()
        for b in range(RING):
            rows = pl.ds((l * RING + b) * UR, UR)
            for yy in range(RING):
                for m in HALVES:
                    s0 = RES[G0, rows, pl.ds((2 * m * RING + yy) * S2, S2)].astype(F32)
                    s1 = RES[G0, rows, pl.ds(((2 * m + 1) * RING + yy) * S2, S2)].astype(F32)
                    cols = pl.ds((yy * 2 + m) * S2, S2)
                    AV[l, 0, pl.ds(2 * b * UR, UR), cols] = jnp.where(low, s0, swap(s1)).astype(BF16)
                    AV[l, 0, pl.ds((2 * b + 1) * UR, UR), cols] = jnp.where(low, swap(s0), s1).astype(BF16)
    for cpy in load_d + [load_x, own_d0]:
        cpy.wait()
    pl.semaphore_wait(barrier, len(peers))

    half = lambda h: pl.ds(h * HB, HB)

    def tile_cols(split, q):
        return pl.ds(sum(split[:q]) * (D // RING), split[q] * (D // RING))

    gx0 = Gather8(lambda h: RES.at[X0, half(h)], lambda b, k, h: XV.at[b, k, half(h)])
    gg1 = Gather8(lambda h: RES.at[G1, half(h)], lambda b, k, h: GV1.at[b, k, half(h)])
    up = [U, wuh.at[1]]
    down = [W, wdh.at[1]]
    hr = DR_ROWS // 4

    def quarter(q, h):
        return pl.ds((2 * q + h) * hr, hr)

    def down_first(l):
        to = down[l]
        src = lambda q: lambda h: RES.at[X1, pl.ds(l * DR_ROWS + (2 * q + h) * hr, hr)]
        return [Gather4("z", src(0), lambda b, h: to.at[y, b, quarter(0, h)]),
                Gather4("y", src(1), lambda b, h: to.at[b, z, quarter(1, h)])]

    def down_second(l, split, n):
        to, cs = down[l], tile_cols(split, n)
        return [Gather4("y", lambda h: to.at[y, :, quarter(0, h), cs], lambda b, h: to.at[b, :, quarter(0, h), cs]),
                Gather4("z", lambda h: to.at[:, z, quarter(1, h), cs], lambda b, h: to.at[:, b, quarter(1, h), cs])]

    def up_first(to):
        return [Gather4("y", lambda h: to.at[h, z, y], lambda b, h: to.at[h, z, b]),
                Gather4("z", lambda h: to.at[2 + h, z, y], lambda b, h: to.at[2 + h, b, y])]

    def hidden_cols(n):
        return pl.ds(sum(SPLIT2[:n]) * (K // RING), SPLIT2[n] * (K // RING))

    def up_second(n):
        cs, src = hidden_cols(n), up[1]
        return [Gather4("z", lambda h: src.at[h, z, :, :, cs], lambda b, h: U.at[h, b, :, :, cs]),
                Gather4("y", lambda h: src.at[2 + h, :, y, :, cs], lambda b, h: U.at[2 + h, :, b, :, cs])]

    def up_unit(to, j):
        yj, zj = off(y, j), off(z, j)
        return [Gather4("z", lambda h: to.at[h, z, yj], lambda b, h: to.at[h, b, yj]),
                Gather4("y", lambda h: to.at[2 + h, zj, y], lambda b, h: to.at[2 + h, zj, b])]

    def do(gathers, step):
        for g in gathers:
            getattr(g, step)()

    mine = pl.ds(mo(c * UR, UR), UR)

    def up_exchange(l):
        sends = []
        for dx, dc in group:
            tx, tc = off(x, dx), (cp if dc else c)
            src = AV.at[l, 0, pl.ds(mo((tx * 2 + tc) * UR, UR), UR), :]
            sends.append(rcopy(src, up[l].at[x, z, y, mine, :], dev(dx=dx, dc=dc)))
        for cpy in sends:
            cpy.start()
        return sends

    def keys_of(gathers):
        return [d.key for g in gathers for d in g.d]

    d0a, d0b, d0c = down_first(0), down_second(0, SPLIT3, 0), down_second(0, SPLIT3, 1)
    u0a, u0u = up_first(up[0]), [up_unit(up[0], j) for j in (OWN, PRV, NXT, OPP)]
    keys.extend(keys_of(u0a))
    d0d = down_second(0, SPLIT3, 2)
    keys.extend(keys_of(d0a))
    d1a = down_first(1)
    keys.extend(keys_of(sum(u0u, [])))
    d1b, u1a = down_second(1, WHOLE, 0), up_first(up[1])
    u1b, u1c = up_second(0), up_second(1)
    ex0 = up_exchange(0)
    do(d0a, "start")
    gx0.start()
    ex1 = up_exchange(1)
    my_rows = pl.ds(mo((x * 2 + c) * UR, UR), UR)
    own_u1 = lcopy(AV.at[1, 0, my_rows, :], up[1].at[x, z, y, mine, :])
    own_u1.start()
    own_d1 = lcopy(RES.at[X1, pl.ds(DR_ROWS, DR_ROWS), :], down[1].at[y, z])
    own_d1.start()
    U[x, z, y, mine, :] = AV[0, 0, my_rows, :]
    do(d0a, "forward")
    for cpy in ex0:
        cpy.wait_recv()
    do(u0a, "start")
    do(u0u[0], "start")
    do(u0a, "forward")
    gx0.forward()
    load_g.wait()
    gg1.start()
    do(u0a, "neighbours")
    do(u0u[1], "start")
    do(u0u[2], "start")
    do(u0u[0], "forward")
    do(u0a, "opposite")
    do(u0u[3], "start")
    do(d0a, "finish")
    do(u0u[1], "forward")
    do(u0u[2], "forward")
    do(d0b, "start_first")
    gx0.sides()
    for cpy in ex0 + ex1:
        cpy.wait_send()
    own_u1.wait()
    do(u0u[3], "forward")
    do(u0a + d0a, "drain")
    do(d0b, "start_rest")
    do(d0c, "start_first")
    gg1.forward()
    do(d0b, "forward")
    do(d0c, "start_rest")
    do(d1a, "start")
    gx0.last()
    gx0.wait_own()
    gx0.wait_push(range(len(gx0.push)))
    own_x.wait()
    save_x = lcopy(XV, xh0)
    save_x.start()
    gx0.drain()
    for unit in u0u:
        do(unit, "finish")
    save_u0 = lcopy(U, wuh.at[0])
    save_u0.start()

    T2 = 2 * TB
    ND = D // 4
    NK = K // 4

    def up_tile(t, n):
        cols = pl.ds(mo(n * NK, NK), NK)
        return dot_nn(XV[t].reshape(T2, D), U[:, :, :, :, cols].reshape(D, NK)), cols

    def hidden0(t):
        for n in range(RING):
            pre, cols = up_tile(t, n)
            act, slope = gelu_parts(pre)
            AV[t, :, :, cols] = act.astype(BF16).reshape(2, TB, NK)
            SV[t, :, :, cols] = slope.reshape(2, TB, NK)

    def hidden1_tile(t, n):
        pre, cols = up_tile(t, n)
        act, slope = gelu_parts(pre)
        AV[t, :, :, cols] = act.astype(BF16).reshape(2, TB, NK)
        DV[t, :, cols] = (SV[t, :, :, cols].reshape(T2, NK) * slope).astype(BF16)

    def hidden1(t, part):
        for n in range(sum(SPLIT2[:part]), sum(SPLIT2[:part + 1])):
            hidden1_tile(t, n)

    def dact(gv, t, n):
        return dot_nt(gv[t].reshape(T2, D), W[n].reshape(NK, D))

    def dact1(t):
        def body(n, carry):
            SV[t, :, :, pl.ds(mo(n * NK, NK), NK)] = dact(GV1, t, n).reshape(2, TB, NK)
            return carry
        loop(RING, body, None)

    def dact0(t):
        def body(n, carry):
            cols = pl.ds(mo(n * NK, NK), NK)
            DV[t, :, cols] = (dact(GV0, t, n) * SV[t, :, :, cols].reshape(T2, NK)).astype(BF16)
            return carry
        loop(RING, body, None)

    def down_part(act, j, lo, tiles):
        t = lax.rem(x + j, RING)

        def body(n, carry):
            cols = pl.ds(mo((lo + n) * ND, ND), ND)
            PP[j, :, :, cols] = dot_nn(act[t, :, :, 0:K].reshape(T2, K), W[:, :, :, cols].reshape(K, ND)).reshape(2, TB, ND)
            return carry
        loop(tiles, body, None)

    def dx_part(j, lo, tiles):
        t = lax.rem(x + j, RING)

        def body(n, carry):
            cols = pl.ds(mo((lo + n) * ND, ND), ND)
            PP[j, :, :, cols] = dot_nt(DV[t], U[lo + n].reshape(ND, K)).reshape(2, TB, ND)
            return carry
        loop(tiles, body, None)

    class Reduce8:
        def __init__(self, part, index, split, old=()):
            self.part, self.index, self.split = part, index, split
            keys.extend(old)
            _, right, left = rings["x"]
            self.right, self.left = right, left
            self.pair, self.m, self.first = [], [], []
            for q in range(len(split)):
                cq = self.cols(q)
                first = sorted(fresh("recv") for j in range(RING))
                self.pair.append([self.swap(j, q, first[0]) for j in range(RING)])
                self.first.append(first[0])
                src = lambda j, h: PP.at[j, c, half(h), cq]
                self.m.append([rcopy(src(*PIECES[k]), XR.at[k, :, cq], left if k % 2 else right) for k in range(ARRIVALS)])
            keys.clear()

        def cols(self, q):
            return tile_cols(self.split, q)

        def swap(self, j, q, first):
            cq = self.cols(q)
            return remote(PP.at[j, cp, :, cq], DR.at[j, :, cq], ps.at[q * RING + j], rs.at[first + j], partner)

        def compute(self, j, q):
            self.part(j, sum(self.split[:q]), self.split[q])
            self.pair[q][j].start()

        def compute_all(self, q):
            def body(i, carry):
                j = lax.rem(i + 1, RING)
                self.part(j, sum(self.split[:q]), self.split[q])
                self.swap(j, q, self.first[q]).start()
                return carry
            loop(RING, body, None)

        def combine(self, j, q):
            self.pair[q][j].wait_recv()
            add_rows(PP.at[j, c, :, self.cols(q)], [DR.at[j, :, self.cols(q)]], TB, min(TB, 16))

        def opposite(self, q):
            self.m[q][0].start()
            self.m[q][1].start()

        def side(self, j, q):
            self.combine(j, q)
            self.m[q][2 if j == NXT else 3].start()

        def send(self, q):
            self.combine(OPP, q)
            self.opposite(q)
            self.side(NXT, q)
            self.side(PRV, q)

        def relay(self, q):
            for k, j, h in ((0, NXT, 0), (1, PRV, 1)):
                self.m[q][k].wait_recv()
                add_rows(PP.at[j, c, half(h), self.cols(q)], [XR.at[k, :, self.cols(q)]], HB, min(HB, 16))
                self.m[q][4 + k].start()

        def finish(self, q, res, outs):
            for d in self.m[q][2:]:
                d.wait_recv()
            step, cq = min(HB, 16), self.cols(q)
            for h, (kl, kr) in enumerate(((4, 3), (2, 5))):
                def body(r, carry):
                    lo = pl.ds(mo(r * step, step), step)
                    sl = pl.ds(mo(h * HB + r * step, step), step)
                    tot = PP[OWN, c, sl, cq] + (XR[kl, lo, cq] + XR[kr, lo, cq])
                    val = (res[sl, cq].astype(F32) + tot).astype(BF16)
                    for o in outs:
                        o[sl, cq] = val
                    return carry
                loop(HB // step, body, None)

        def drain(self):
            for d in sum(self.pair + self.m, []):
                d.wait_send()

        def release(self):
            self.drain()
            for k, to in enumerate((self.right, self.left, partner)):
                pl.semaphore_signal(credit.at[k], inc=1, device_id=to, device_id_type=MESH_ID)

        def acquire(self):
            for k in range(len((self.right, self.left, partner))):
                pl.semaphore_wait(credit.at[k], 1)

    def grad_a(j, dst, halves=None, q=None):
        t = off(z, j)

        def rows(h, carry):
            lo = [pl.ds(mo((2 * h + q) * XD + t * ZD, ZD), ZD) for q in HALVES]
            lhs = jnp.concatenate([XV[:, :, :, s].reshape(8 * TB, ZD) for s in lo], axis=1)

            def body(n, carry):
                cols = pl.ds(mo(n * ND, ND), ND)
                dst[h, :, :, cols] = dot_tn(lhs, DV[:, :, cols].reshape(8 * TB, ND)).reshape(2, ZD, ND)
                return carry
            return loop(K // ND, body, carry) if q is None else body(q, carry)
        if halves is None:
            loop(2, rows, None)
        else:
            for h in halves:
                rows(h, None)

    def grad_b(gv, j, dst, lo=0, tiles=RING):
        cols_l = pl.ds(mo(off(y, j) * NK, NK), NK)

        def body(i, carry):
            m = lo + i
            cols = pl.ds(mo(m * ND, ND), ND)
            out = dot_tn(AV[:, :, :, cols_l].reshape(8 * TB, NK), gv[:, :, :, cols].reshape(8 * TB, ND))
            dst[:, m // 2, :, pl.ds(mo(lax.rem(m, 2) * ND, ND), ND)] = out.reshape(2, NK // 2, ND)
            return carry
        loop(tiles, body, None)

    grad_keys = [keys_of(sum(u0u, u0a) + d0a), [d.key for d in ex0 + ex1] + keys_of(d0b + d0c)]

    def grad_key(l):
        return grad_keys[l].pop() if grad_keys[l] else fresh("recv")

    class Reduce4:
        def __init__(self, l, axis, part, recv, stage):
            _, right, left = rings[axis]
            self.part, self.recv, self.stage = part, recv, stage
            self.m = [rcopy(part(*PIECES[k]), recv(k), left if k % 2 else right, grad_key(l))
                      for k in range(ARRIVALS)]
            self.loads = [lcopy(recv(k), stage(k)) for k in range(ARRIVALS)] if stage else None

        def opposite(self):
            self.m[0].start()
            self.m[1].start()

        def sides(self, j):
            self.m[2 if j == NXT else 3].start()

        def fetch(self, k):
            self.m[k].wait_send()
            self.m[k].wait_recv()
            if self.loads:
                self.loads[k].start()

        def absorb(self, k):
            if self.loads:
                self.loads[k].wait()
            dst = self.part(*TARGETS[k])
            add_rows(dst, [(self.stage or self.recv)(k)], dst.shape[1], min(dst.shape[1], 16))

    def arrive(reduces, ks):
        for k in ks:
            for r in reduces:
                r.fetch(k)
        for k in ks:
            for r in reduces:
                r.absorb(k)

    def relay(reduces):
        for k in (0, 1):
            for r in reduces:
                r.fetch(k)
        for k in (0, 1):
            for r in reduces:
                r.absorb(k)
                r.m[4 + k].start()

    hq = DR_ROWS // 2
    own_grads = [(SV.at[pl.ds(0, 2)], SV.at[pl.ds(2, 2)]), (GPA.at[OWN], GPB.at[OWN])]

    def third(k, rows):
        return pl.ds((k // 2) * rows, rows)

    def reduce_a(l, q, chunks):
        own = own_grads[l][0]
        ca = pl.ds(q * (K // chunks), K // chunks)

        def part(j, h):
            return (own if j == OWN else GPA.at[j]).at[h, :, :, ca]

        def part2(j, h):
            return own.at[h, :, pl.ds(mo(off(y, j) * 2 * UR, 2 * UR), 2 * UR), ca]
        if l < q:
            second = lambda k: GPA.at[OWN, k % 2, :, third(k, 2 * UR), ca], None
        else:
            second = lambda k: ra2.at[l, k, :, :, ca], lambda k: STA.at[k % 2, :, :, ca]
        return (Reduce4(l, "z", part, lambda k: ra1.at[l, k, :, :, ca], lambda k: part(*PIECES[k])),
                Reduce4(l, "y", part2, *second))

    def reduce_b(l, q):
        own, nb = own_grads[l][1], pl.ds(q, 1)

        def part(j, h):
            return (own if j == OWN else GPB.at[j]).at[h, nb]

        def part2(j, h):
            t = off(z, j)
            return own.at[t // 2, nb, pl.ds(mo(lax.rem(t, 2) * DR_ROWS + h * hq, hq), hq), :]
        if l < q:
            second = lambda k: GPB.at[OWN, k % 2, nb, third(k, hq), :], None
        else:
            second = lambda k: rb2.at[l, k, nb], lambda k: STB.at[k % 2, nb]
        return (Reduce4(l, "y", part, lambda k: rb1.at[l, k, nb], lambda k: part(*PIECES[k])),
                Reduce4(l, "z", part2, *second))

    def sides(reduces, j):
        for r in reduces:
            r.sides(j)

    def second_start(reduces):
        for r in reduces:
            r.opposite()
            r.sides(NXT)
            r.sides(PRV)

    def up_out(l, q, chunks):
        own = own_grads[l][0]
        ca = pl.ds(q * (K // chunks), K // chunks)

        def rows_of(tx, tc):
            return own.at[tx // 2, lax.rem(tx, 2), pl.ds(mo((2 * y + tc) * UR, UR), UR), ca]
        to = uh.at[l, x, mine, ca]
        sends = [rcopy(rows_of(off(x, dx), cp if dc else c), to, dev(dx=dx, dc=dc), grad_key(l)) for dx, dc in group]
        local = [lcopy(rows_of(x, c), to)]
        for cpy in sends + local:
            cpy.start()
        return sends, local

    def down_out(l, n):
        cpy = lcopy(own_grads[l][1].at[z // 2, n, pl.ds(mo(lax.rem(z, 2) * DR_ROWS, DR_ROWS), DR_ROWS), :],
                    gd_out.at[l, :, pl.ds(n * K, K)])
        cpy.start()
        return [], [cpy]

    def grads_out_finish(state):
        for cpy in state[0]:
            cpy.wait_recv()
            cpy.wait_send()
        for cpy in state[1]:
            cpy.wait()

    r = Reduce8(functools.partial(down_part, AV), 0, SPLIT3)
    r_keys = sorted([d.key for m in r.m for d in m] + [f + j for f in r.first for j in range(RING)])
    hidden0(off(x, OPP))
    hidden0(off(x, NXT))
    do(d0b, "finish")
    r.compute(OPP, 0)
    r.compute(NXT, 0)
    do(d0c, "forward")
    do(d0d, "start")
    r.combine(OPP, 0)
    r.opposite(0)
    do(sum(u0u, []), "drain")
    hidden0(off(x, PRV))
    r.compute(PRV, 0)
    r.side(NXT, 0)
    do(d1a, "forward")
    hidden0(off(x, OWN))
    r.side(PRV, 0)
    save_s = lcopy(SV, sh0)
    save_s.start()
    save_a0 = lcopy(AV, ah.at[0])
    save_a0.start()
    gg1.sides()
    do(d0c, "finish")
    r.compute_all(1)
    r.relay(0)
    do(d0d, "forward")
    for cpy in ex1:
        cpy.wait_recv()
    own_d1.wait()
    do(u1a, "start")
    r.send(1)
    do(d1a, "finish")
    do(d1b, "start")
    gg1.last()
    save_x.wait()
    do(d0d, "finish")
    save_d0 = lcopy(W, wdh.at[0])
    save_d0.start()
    r.compute(OPP, 2)
    r.relay(1)
    save_u0.wait()
    do(u1a, "forward")
    r.compute(NXT, 2)
    r.combine(OPP, 2)
    r.opposite(2)
    r.compute(PRV, 2)
    r.side(NXT, 2)
    r.compute(OWN, 2)
    r.side(PRV, 2)
    r.compute(OWN, 0)
    for q in range(len(SPLIT3)):
        r.combine(OWN, q)

    def gather_keys(gathers):
        return [d.key for g in gathers for d in g.ring.d + g.own + g.push]

    def token_gathers(slot, buf):
        def make(q):
            cq = tile_cols(SPLIT2, q)
            return Gather8(lambda h: RES.at[slot, half(h), cq], lambda b, k, h: buf.at[b, k, half(h), cq])
        return [make(0), make(1)]

    keys.extend(gather_keys((gx0,)))
    gx1 = token_gathers(X1, XV)
    do(d1a, "drain")
    do(d1b, "forward")
    for q in HALVES:
        r.finish(q, RES.at[X0], [RES.at[X1], XV.at[x, c]])
    r.relay(2)
    gx1[0].start()
    do(u1a, "finish")
    do(u1b, "start")
    do(u1c, "start_first")
    pair, rest = pl.ds(0, 2), pl.ds(2, 2)
    own_up = [lcopy(up[1].at[pair, z], U.at[pair, z]), lcopy(up[1].at[rest, :, y], U.at[rest, :, y])]
    for cpy in own_up:
        cpy.start()
    gg1.wait_own()
    gg1.wait_push(range(len(gg1.push)))
    own_g.wait()
    save_d0.wait()
    do(d0b + d0c + d0d, "drain")
    gg1.drain()
    do(d1b, "finish")
    load_w1d = lcopy(wdh.at[1], W)
    load_w1d.start()
    r.finish(2, RES.at[X0], [RES.at[X1], XV.at[x, c]])
    gx1[1].start()
    save_s.wait()
    do(u1b, "forward")
    do(u1c, "start_rest")
    load_w1d.wait()
    dact1(off(x, OWN))
    gx1[0].forward()
    r.release()
    dact1(off(x, NXT))
    gx1[0].sides()
    dact1(off(x, PRV))
    do(u1c, "forward")
    do(u1b, "finish")
    dact1(off(x, OPP))
    load_w0d_again = lcopy(wdh.at[0], W)
    load_w0d_again.start()
    save_a0.wait()
    do(gx1, "wait_own")
    for cpy in own_up:
        cpy.wait()
    hidden1(off(x, OWN), 0)
    do(gx1[1:], "forward")
    do(gx1[1:], "sides")
    for j in (PRV, NXT):
        for g in gx1:
            g.wait_push(PUSHES[j])
        hidden1(off(x, j), 0)
    gx1[0].last()
    do(u1c, "finish")
    hidden1(off(x, OWN), 1)
    hidden1(off(x, PRV), 1)
    gx1[1].last()
    hidden1(off(x, NXT), 1)
    for g in gx1:
        g.wait_push(PUSHES[OPP])
    hidden1_tile(off(x, OPP), off(y, OPP))

    (a1, a2), (b1, b2) = zip(*[reduce_a(1, q, 2) for q in HALVES]), zip(*[reduce_b(1, q) for q in HALVES])
    first1, second1 = b1 + a1, b2 + a2
    grad_b(GV1, OPP, GPB.at[OPP], 0, 2)
    b1[0].opposite()
    for n in (PRV, OWN, NXT):
        hidden1_tile(off(x, OPP), off(y, n))
    for q in HALVES:
        for h in HALVES:
            grad_a(OPP, GPA.at[OPP], (h,), q)
            a1[q].m[h].start()
    load_s0 = lcopy(sh0, SV)
    load_s0.start()
    save_a1 = lcopy(AV, ah.at[1])
    save_a1.start()
    grad_b(GV1, OPP, GPB.at[OPP], 2, 2)
    b1[1].opposite()
    r = Reduce8(dx_part, 1, SPLIT2, r_keys)
    r.acquire()
    r.compute(OPP, 0)
    r.compute(NXT, 0)
    r.combine(OPP, 0)
    r.opposite(0)
    r.compute(PRV, 0)
    r.side(NXT, 0)
    r.side(PRV, 0)
    r.compute_all(1)
    load_w0u_again = lcopy(wuh.at[0], U)
    r.compute(OWN, 0)
    do(u1b + u1c, "drain")
    load_w0u_again.start()
    grad_b(GV1, NXT, GPB.at[NXT])
    sides(b1, NXT)
    grad_b(GV1, PRV, GPB.at[PRV])
    sides(b1, PRV)
    r.relay(0)
    r.send(1)
    grad_a(NXT, GPA.at[NXT])
    sides(a1, NXT)
    grad_a(PRV, GPA.at[PRV])
    sides(a1, PRV)
    r.combine(OWN, 0)
    r.combine(OWN, 1)
    keys.extend(gather_keys(gx1))
    gg0 = token_gathers(G0, GV0)
    r.relay(1)
    r.finish(0, RES.at[G1], [RES.at[G0], GV0.at[x, c]])
    gg0[0].start()
    relay(first1)
    grad_b(GV1, OWN, GPB.at[OWN])
    save_a1.wait()
    load_a0 = lcopy(ah.at[0], AV)
    load_a0.start()
    do(d1b + u1a, "drain")
    load_a1 = lcopy(ah.at[1], GV1.at[:, :, :, 0:K])
    load_a1.start()
    r.finish(1, RES.at[G1], [RES.at[G0], GV0.at[x, c]])
    gg0[1].start()
    gg0[0].forward()
    grad_a(OWN, GPA.at[OWN])
    do(gx1, "drain")
    load_x0 = lcopy(xh0, XV)
    load_x0.start()
    gg0[0].sides()
    r.release()
    gg0[1].forward()
    gg0[0].last()
    load_w0d_again.wait()
    load_s0.wait()
    do(gg0, "wait_own")
    dact0(off(x, OWN))
    gg0[1].sides()
    gg0[1].last()
    for g in gg0:
        g.wait_push(PUSHES[PRV])
    dact0(off(x, PRV))
    for g in gg0:
        g.wait_push(PUSHES[NXT])
    dact0(off(x, NXT))
    for g in gg0:
        g.wait_push(PUSHES[OPP])

    (a1n, a2n), (b1n, b2n) = zip(*[reduce_a(0, q, 2) for q in HALVES]), zip(*[reduce_b(0, q) for q in HALVES])
    load_a0.wait()
    grad_b(GV0, OPP, GPB.at[OPP])
    b1n[0].opposite()
    dact0(off(x, OPP))
    load_w1d_again = lcopy(wdh.at[1], W)
    load_w1d_again.start()
    load_x0.wait()
    for h in HALVES:
        grad_a(OPP, GPA.at[OPP], (h,))
        a1n[0].m[h].start()
    arrive(first1, EARLY + LATE)
    second_start(second1)
    load_w0u_again.wait()
    r = Reduce8(dx_part, 2, WHOLE, r_keys)
    r.acquire()
    r.compute_all(0)
    r.send(0)
    grad_b(GV0, NXT, GPB.at[NXT])
    b1n[0].sides(NXT)
    grad_b(GV0, PRV, GPB.at[PRV])
    b1n[0].sides(PRV)
    grad_a(NXT, GPA.at[NXT])
    a1n[0].sides(NXT)
    grad_a(PRV, GPA.at[PRV])
    a1n[0].sides(PRV)
    relay(second1)
    r.relay(0)
    relay((b1n[0], a1n[0]))
    for red in (b1n[1], a1n[1]):
        red.opposite()
        red.sides(NXT)
        red.sides(PRV)
    r.combine(OWN, 0)
    grad_b(GV0, OWN, own_grads[0][1])
    grad_a(OWN, own_grads[0][0])
    r.finish(0, RES.at[G0], [RES.at[X0]])
    r.release()
    write_gi = lcopy(RES.at[X0], gi_out)
    write_gi.start()
    arrive((b1n[0], a1n[0]), EARLY)
    arrive(second1, EARLY)
    arrive(second1, LATE)
    state1 = [up_out(1, q, 2) for q in HALVES] + [down_out(1, n) for n in HALVES]
    load_a1.wait()
    load_w1d_again.wait()
    r = Reduce8(functools.partial(down_part, GV1), 3, WHOLE, r_keys)
    r.acquire()
    r.compute_all(0)
    r.send(0)
    r.combine(OWN, 0)
    arrive((b1n[0], a1n[0]), LATE)
    for state in state1:
        grads_out_finish(state)
    relay((b1n[1], a1n[1]))
    second_start((a2n[0], b2n[0]))
    r.relay(0)
    arrive((b1n[1], a1n[1]), EARLY)

    def start(red):
        red.opposite()
        sides((red,), NXT)
        sides((red,), PRV)
    arrive((b1n[1],), LATE)
    relay((a2n[0],))
    arrive((a1n[1],), LATE)
    start(a2n[1])
    start(b2n[1])
    arrive((a2n[0],), EARLY)
    relay((b2n[0],))
    arrive((a2n[0],), LATE)
    state0 = [up_out(0, 0, 2)]
    relay((a2n[1],))
    arrive((b2n[0],), EARLY)
    relay((b2n[1],))
    arrive((a2n[1],), EARLY)
    arrive((a2n[1],), LATE)
    state0.append(up_out(0, 1, 2))
    arrive((b2n[1],), EARLY)
    for q in HALVES:
        arrive((b2n[q],), LATE)
        state0.append(down_out(0, q))
    r.finish(0, RES.at[X1], [RES.at[G1]])
    write_y = lcopy(RES.at[G1], y_out)
    write_y.start()
    r.drain()
    do(gg0, "drain")
    write_gi.wait()
    write_y.wait()
    for state in state0:
        grads_out_finish(state)
    assert used["recv"] <= N_RECV and used["send"] <= N_SEND and used["local"] <= N_LOCAL


def finish_kernel(y_in, gi_in, gu_in, gd_in, y_out, gi_out, gu_out, gd_out, ybuf, gibuf, gubuf, gdbuf, gushuf, sems):
    layers, ur, ff = gu_out.shape
    s2 = ff // 64
    half = s2 // 2
    loads = [pltpu.make_async_copy(a, b, sems.at[0, k])
             for k, (a, b) in enumerate(((gu_in, gubuf), (gd_in, gdbuf), (y_in, ybuf), (gi_in, gibuf)))]
    stores = [pltpu.make_async_copy(a, b, sems.at[1, k])
              for k, (a, b) in enumerate(((gushuf, gu_out), (gdbuf, gd_out), (ybuf, y_out), (gibuf, gi_out)))]
    for cpy in loads:
        cpy.start()
    low = lax.broadcasted_iota(jnp.int32, (ur, s2), 1) < half
    swap = lambda v: pltpu.roll(v, half, 1)
    loads[0].wait()
    for l in range(layers):
        for b in range(RING):
            for yy in range(RING):
                for m in HALVES:
                    cols = pl.ds((yy * 2 + m) * s2, s2)
                    t0, t1 = (gubuf[l, b, pl.ds(k * ur, ur), cols] for k in HALVES)
                    strip = (b * RING + 2 * m) * RING + yy
                    gushuf[l, :, pl.ds(strip * s2, s2)] = jnp.where(low, t0, swap(t1))
                    gushuf[l, :, pl.ds((strip + RING) * s2, s2)] = jnp.where(low, swap(t0), t1)
    stores[0].start()
    for k in range(1, len(loads)):
        loads[k].wait()
        stores[k].start()
    for cpy in stores:
        cpy.wait()


def solution(mesh, interpret=None):
    fine = Mesh(np.asarray(mesh.devices).reshape(4, 4, 4, 2), ALL)
    tok_spec = P(ALL, None)
    weight_spec = P(None, ALL, None)

    def device_step(x_loc, up_loc, down_loc, g_loc):
        layers, ur, ff = up_loc.shape
        dr, dm = down_loc.shape[1:]
        tb = x_loc.shape[0]
        k = ff // 8
        zd = dm // 16
        hbm = lambda shape, dt: jax.ShapeDtypeStruct(shape, dt)
        outs = [
            hbm((tb, dm), BF16), hbm((tb, dm), BF16), hbm((layers, dr, dm), F32),
            hbm((RING, CORES, tb, dm), BF16),
            hbm((layers, RING, RING, RING, 2 * ur, k), BF16),
            hbm((layers, RING, RING, dr, dm), BF16),
            hbm((RING, CORES, tb, k), F32), hbm((layers, RING, CORES, tb, k), BF16),
            *[hbm((layers, ARRIVALS, CORES, n, k), F32) for n in (zd, zd, 2 * ur, 2 * ur)],
            hbm((layers, RING, 2 * ur, k), F32),
        ]
        vm = pltpu.VMEM
        scratch = [
            vm((RING, RING, RING, 2 * ur, k), BF16), vm((RING, RING, dr, dm), BF16),
            vm((RING, CORES, tb, dm), BF16), vm((RING, CORES, tb, dm), BF16), vm((RING, CORES, tb, dm), BF16),
            vm((RING, CORES, tb, k), F32), vm((RING, CORES, tb, k), BF16), vm((RING, 2 * tb, k), BF16),
            vm((RING, CORES, CORES, zd, k), F32), vm((RING, CORES, CORES, zd, k), F32),
            vm((RING, CORES, tb, dm), F32), vm((4, tb, dm), F32), vm((6, tb // 2, dm), F32),
            vm((4, tb, dm), BF16), vm((CORES, CORES, 2 * ur, k), F32), vm((CORES, CORES, 2 * ur, k), F32),
            *[pltpu.SemaphoreType.DMA((n,)) for n in (N_SEND, N_RECV, N_LOCAL, len(SPLIT3) * RING)],
            pltpu.SemaphoreType.REGULAR((3,)),
        ]
        anyspec = pl.BlockSpec(memory_space=pl.ANY)
        call = pl.pallas_call(
            functools.partial(kernel, (dm, k, tb, ur, dr)),
            out_shape=outs,
            in_specs=[anyspec] * 4,
            out_specs=[anyspec] * len(outs),
            scratch_shapes=scratch,
            compiler_params=pltpu.CompilerParams(collective_id=0, has_side_effects=True, vmem_limit_bytes=67043328),
            name="mlp_stack",
            **({"interpret": interpret} if interpret else {}),
        )
        y_raw, gi_raw, gd_raw, *_, gu_raw = call(x_loc, up_loc, down_loc, g_loc)
        raws = (y_raw, gi_raw, gu_raw, gd_raw)
        outs = [hbm((tb, dm), BF16), hbm((tb, dm), BF16), hbm((layers, ur, ff), F32), hbm((layers, dr, dm), F32)]
        return tuple(pl.pallas_call(
            finish_kernel, out_shape=outs, in_specs=[anyspec] * len(outs), out_specs=[anyspec] * len(outs),
            scratch_shapes=[vm(v.shape, v.dtype) for v in raws] + [vm(outs[2].shape, F32), pltpu.SemaphoreType.DMA((2, len(outs)))],
            name="write_out")(*raws))

    return jax.shard_map(device_step, mesh=fine, in_specs=(tok_spec, weight_spec, weight_spec, tok_spec),
                         out_specs=(tok_spec, tok_spec, weight_spec, weight_spec), check_vma=False)
```

```python
import functools

import jax
import jax.numpy as jnp
import numpy as np
from jax import lax
from jax.experimental import pallas as pl
from jax.experimental.pallas import tpu as pltpu
from jax.sharding import Mesh, PartitionSpec as P

MESH_ID = pl.DeviceIdType.MESH
ALL = ("x", "z", "y", "c")
F32, BF16 = jnp.float32, jnp.bfloat16
RING, CORES, ARRIVALS = 4, 2, 6
OWN, NXT, OPP, PRV = range(RING)
X0, X1, G1, G0 = range(RING)
HALVES = (0, 1)
WHOLE, SPLIT2, SPLIT3 = (4,), (2, 2), (1, 1, 2)
PIECES = ((OPP, 0), (OPP, 1), (NXT, 1), (PRV, 0), (NXT, 0), (PRV, 1))
TARGETS = ((NXT, 0), (PRV, 1), (OWN, 1), (OWN, 0), (OWN, 0), (OWN, 1))
EARLY, LATE = (2, 3), (4, 5)
PUSHES = {PRV: (0, 2), NXT: (1, 3), OPP: (4, 5)}
N_RECV, N_SEND, N_LOCAL = 192, 90, 19


def gelu_parts(pre_act):
    norm_cdf = 0.5 * (1.0 + lax.erf(pre_act * (2.0 ** -0.5)))
    norm_pdf = jnp.exp(-0.5 * pre_act * pre_act) * ((2.0 * jnp.pi) ** -0.5)
    return pre_act * norm_cdf, norm_cdf + pre_act * norm_pdf


def loop(n, body, init):
    return lax.fori_loop(0, n, body, init)


def dot_nn(left, right):
    return lax.dot_general(left, right, (((1,), (0,)), ((), ())), preferred_element_type=F32)


def dot_nt(left, right):
    return lax.dot_general(left, right, (((1,), (1,)), ((), ())), preferred_element_type=F32)


def dot_tn(left, right):
    return lax.dot_general(left, right, (((0,), (0,)), ((), ())), preferred_element_type=F32)


def kernel(dims, x_in, wu_in, wd_in, g_in,
           y_out, gi_out, gd_out,
           xh0, wuh, wdh, sh0, ah, ra1, rb1, ra2, rb2, uh,
           U, W, XV, GV1, GV0, SV, AV, DV, GPA, GPB, PP, DR, XR, RES, STA, STB,
           ss, rs, ls, ps, credit):
    D, K, TB, UR, DR_ROWS = dims
    HB = TB // 2
    x, z, y, c = (lax.axis_index(a) for a in ALL)
    cp = 1 - c
    S2 = 2 * DR_ROWS
    XD = D // 4
    ZD = D // 16

    def dev(dx=0, dz=0, dy=0, dc=0):
        wrap = lambda v, d, n: v if d == 0 else lax.rem(v + (d % n), n)
        return (wrap(x, dx, 4), wrap(z, dz, 4), wrap(y, dy, 4), wrap(c, dc, 2))

    partner = dev(dc=1)
    rings = {"x": (x, dev(dx=1), dev(dx=-1)), "z": (z, dev(dz=1), dev(dz=-1)), "y": (y, dev(dy=1), dev(dy=-1))}
    off = lambda v, d: v if d == 0 else lax.rem(v + d, 4)

    used = {"recv": 0, "send": 0, "local": 0}
    free = {"send": [], "local": []}
    keys = []

    def fresh(kind):
        if kind == "recv" and keys:
            return keys.pop()
        used[kind] += 1
        return used[kind] - 1

    def take(kind):
        return free[kind].pop() if free[kind] else fresh(kind)

    def remote(src, dst, send, recv, to):
        return pltpu.make_async_remote_copy(src_ref=src, dst_ref=dst, send_sem=send, recv_sem=recv,
                                            device_id=to, device_id_type=MESH_ID)

    class rcopy:
        def __init__(self, src, dst, to, key=None):
            self.args, self.key = (src, dst, to), fresh("recv") if key is None else key

        def start(self):
            src, dst, to = self.args
            self.sem = take("send")
            self.d = remote(src, dst, ss.at[self.sem], rs.at[self.key], to)
            self.d.start()

        def wait_recv(self):
            self.d.wait_recv()

        def wait_send(self):
            self.d.wait_send()
            free["send"].append(self.sem)

    class lcopy:
        def __init__(self, src, dst):
            self.args = src, dst

        def start(self):
            self.sem = take("local")
            self.d = pltpu.make_async_copy(*self.args, ls.at[self.sem])
            self.d.start()

        def wait(self):
            self.d.wait()
            free["local"].append(self.sem)

    def mo(v, m):
        return pl.multiple_of(v, m)

    class Gather4:
        def __init__(self, axis, src, dst):
            i, right, left = rings[axis]
            lft, rgt = off(i, 3), off(i, 1)
            self.d = [rcopy(src(0), dst(i, 0), right), rcopy(src(1), dst(i, 1), right),
                      rcopy(src(0), dst(i, 0), left), rcopy(src(1), dst(i, 1), left),
                      rcopy(dst(lft, 0), dst(lft, 0), right), rcopy(dst(rgt, 1), dst(rgt, 1), left)]

        def start_first(self):
            self.d[0].start()
            self.d[3].start()

        def start_rest(self):
            self.d[1].start()
            self.d[2].start()

        def start(self):
            self.start_first()
            self.start_rest()

        def forward(self):
            for k in HALVES:
                self.d[3 * k].wait_recv()
                self.d[4 + k].start()

        def neighbours(self):
            self.d[1].wait_recv()
            self.d[2].wait_recv()

        def opposite(self):
            self.d[4].wait_recv()
            self.d[5].wait_recv()

        def finish(self):
            self.neighbours()
            self.opposite()

        def drain(self):
            for d in self.d:
                d.wait_send()

    class Gather8:
        def __init__(self, src, dst):
            self.ring = Gather4("x", src, lambda b, h: dst(b, c, h))
            lft, rgt, opp = off(x, PRV), off(x, NXT), off(x, OPP)
            blocks = [(lft, 0), (rgt, 1), (lft, 1), (rgt, 0), (opp, 0), (opp, 1)]
            self.own = [rcopy(src(h), dst(x, c, h), partner) for h in HALVES]
            self.push = [rcopy(dst(b, c, h), dst(b, c, h), partner) for b, h in blocks]

        def start(self):
            self.ring.start()
            for d in self.own:
                d.start()

        def forward(self):
            self.ring.forward()
            self.push[0].start()
            self.push[1].start()

        def sides(self):
            self.ring.d[1].wait_recv()
            self.push[2].start()
            self.ring.d[2].wait_recv()
            self.push[3].start()

        def last(self):
            self.ring.d[4].wait_recv()
            self.push[4].start()
            self.ring.d[5].wait_recv()
            self.push[5].start()

        def wait_own(self):
            for d in self.own:
                d.wait_recv()

        def wait_push(self, ks):
            for k in ks:
                self.push[k].wait_recv()

        def drain(self):
            self.ring.drain()
            for d in self.own + self.push:
                d.wait_send()

    def add_rows(dst, srcs, rows, step):
        def body(r, carry):
            sl = pl.ds(mo(r * step, step), step)
            if len(dst.shape) == 3:
                for q in range(dst.shape[0]):
                    acc = dst[q, sl, :]
                    for s in srcs:
                        acc = acc + s[q, sl, :]
                    dst[q, sl, :] = acc
            else:
                acc = dst[sl, :]
                for s in srcs:
                    acc = acc + s[sl, :]
                dst[sl, :] = acc
            return carry
        loop(rows // step, body, None)

    barrier = pltpu.get_barrier_semaphore()
    group = [(dx, dc) for dx in (OPP, NXT, PRV, OWN) for dc in HALVES if dx or dc]
    peers = [dev(dx=dx, dc=dc) for dx, dc in group] + [rings[a][k] for a in "zy" for k in (1, 2)]
    for p in peers:
        pl.semaphore_signal(barrier, inc=1, device_id=p, device_id_type=MESH_ID)

    load_u = [[lcopy(wu_in.at[l, :, pl.ds(b * D, D)], RES.at[G0, pl.ds((l * RING + b) * UR, UR), :])
               for b in range(RING)] for l in HALVES]
    load_d = [lcopy(wd_in.at[l], RES.at[X1, pl.ds(l * DR_ROWS, DR_ROWS), :]) for l in HALVES]
    load_x = lcopy(x_in, RES.at[X0])
    load_g = lcopy(g_in, RES.at[G1])
    own_x = lcopy(x_in, XV.at[x, c])
    own_g = lcopy(g_in, GV1.at[x, c])
    own_d0 = lcopy(wd_in.at[0], W.at[y, z])
    for cpy in load_u[0] + load_u[1] + load_d + [load_x, own_d0, own_x, load_g, own_g]:
        cpy.start()

    low = lax.broadcasted_iota(jnp.int32, (UR, S2), 1) < DR_ROWS
    swap = lambda v: pltpu.roll(v, DR_ROWS, 1)
    for l in HALVES:
        for cpy in load_u[l]:
            cpy.wait()
        for b in range(RING):
            rows = pl.ds((l * RING + b) * UR, UR)
            for yy in range(RING):
                for m in HALVES:
                    s0 = RES[G0, rows, pl.ds((2 * m * RING + yy) * S2, S2)].astype(F32)
                    s1 = RES[G0, rows, pl.ds(((2 * m + 1) * RING + yy) * S2, S2)].astype(F32)
                    cols = pl.ds((yy * 2 + m) * S2, S2)
                    AV[l, 0, pl.ds(2 * b * UR, UR), cols] = jnp.where(low, s0, swap(s1)).astype(BF16)
                    AV[l, 0, pl.ds((2 * b + 1) * UR, UR), cols] = jnp.where(low, swap(s0), s1).astype(BF16)
    for cpy in load_d + [load_x, own_d0]:
        cpy.wait()
    pl.semaphore_wait(barrier, len(peers))

    half = lambda h: pl.ds(h * HB, HB)

    def tile_cols(split, q):
        return pl.ds(sum(split[:q]) * (D // RING), split[q] * (D // RING))

    gx0 = Gather8(lambda h: RES.at[X0, half(h)], lambda b, k, h: XV.at[b, k, half(h)])
    gg1 = Gather8(lambda h: RES.at[G1, half(h)], lambda b, k, h: GV1.at[b, k, half(h)])
    up = [U, wuh.at[1]]
    down = [W, wdh.at[1]]
    hr = DR_ROWS // 4

    def quarter(q, h):
        return pl.ds((2 * q + h) * hr, hr)

    def down_first(l):
        to = down[l]
        src = lambda q: lambda h: RES.at[X1, pl.ds(l * DR_ROWS + (2 * q + h) * hr, hr)]
        return [Gather4("z", src(0), lambda b, h: to.at[y, b, quarter(0, h)]),
                Gather4("y", src(1), lambda b, h: to.at[b, z, quarter(1, h)])]

    def down_second(l, split, n):
        to, cs = down[l], tile_cols(split, n)
        return [Gather4("y", lambda h: to.at[y, :, quarter(0, h), cs], lambda b, h: to.at[b, :, quarter(0, h), cs]),
                Gather4("z", lambda h: to.at[:, z, quarter(1, h), cs], lambda b, h: to.at[:, b, quarter(1, h), cs])]

    def up_first(to):
        return [Gather4("y", lambda h: to.at[h, z, y], lambda b, h: to.at[h, z, b]),
                Gather4("z", lambda h: to.at[2 + h, z, y], lambda b, h: to.at[2 + h, b, y])]

    def hidden_cols(n):
        return pl.ds(sum(SPLIT2[:n]) * (K // RING), SPLIT2[n] * (K // RING))

    def up_second(n):
        cs, src = hidden_cols(n), up[1]
        return [Gather4("z", lambda h: src.at[h, z, :, :, cs], lambda b, h: U.at[h, b, :, :, cs]),
                Gather4("y", lambda h: src.at[2 + h, :, y, :, cs], lambda b, h: U.at[2 + h, :, b, :, cs])]

    def up_unit(to, j):
        yj, zj = off(y, j), off(z, j)
        return [Gather4("z", lambda h: to.at[h, z, yj], lambda b, h: to.at[h, b, yj]),
                Gather4("y", lambda h: to.at[2 + h, zj, y], lambda b, h: to.at[2 + h, zj, b])]

    def do(gathers, step):
        for g in gathers:
            getattr(g, step)()

    mine = pl.ds(mo(c * UR, UR), UR)

    def up_exchange(l):
        sends = []
        for dx, dc in group:
            tx, tc = off(x, dx), (cp if dc else c)
            src = AV.at[l, 0, pl.ds(mo((tx * 2 + tc) * UR, UR), UR), :]
            sends.append(rcopy(src, up[l].at[x, z, y, mine, :], dev(dx=dx, dc=dc)))
        for cpy in sends:
            cpy.start()
        return sends

    def keys_of(gathers):
        return [d.key for g in gathers for d in g.d]

    d0a, d0b, d0c = down_first(0), down_second(0, SPLIT3, 0), down_second(0, SPLIT3, 1)
    u0a, u0u = up_first(up[0]), [up_unit(up[0], j) for j in (OWN, PRV, NXT, OPP)]
    keys.extend(keys_of(u0a))
    d0d = down_second(0, SPLIT3, 2)
    keys.extend(keys_of(d0a))
    d1a = down_first(1)
    keys.extend(keys_of(sum(u0u, [])))
    d1b, u1a = down_second(1, WHOLE, 0), up_first(up[1])
    u1b, u1c = up_second(0), up_second(1)
    ex0 = up_exchange(0)
    do(d0a, "start")
    gx0.start()
    ex1 = up_exchange(1)
    my_rows = pl.ds(mo((x * 2 + c) * UR, UR), UR)
    own_u1 = lcopy(AV.at[1, 0, my_rows, :], up[1].at[x, z, y, mine, :])
    own_u1.start()
    own_d1 = lcopy(RES.at[X1, pl.ds(DR_ROWS, DR_ROWS), :], down[1].at[y, z])
    own_d1.start()
    U[x, z, y, mine, :] = AV[0, 0, my_rows, :]
    do(d0a, "forward")
    for cpy in ex0:
        cpy.wait_recv()
    do(u0a, "start")
    do(u0u[0], "start")
    do(u0a, "forward")
    gx0.forward()
    load_g.wait()
    gg1.start()
    do(u0a, "neighbours")
    do(u0u[1], "start")
    do(u0u[2], "start")
    do(u0u[0], "forward")
    do(u0a, "opposite")
    do(u0u[3], "start")
    do(d0a, "finish")
    do(d0a + u0a, "drain")
    do(u0u[1], "forward")
    do(u0u[2], "forward")
    do(d0b, "start_first")
    gx0.sides()
    for cpy in ex0 + ex1:
        cpy.wait_send()
    own_u1.wait()
    do(u0u[3], "forward")
    do(u0u[0] + u0u[1], "drain")
    do(d0b, "start_rest")
    do(d0c, "start_first")
    gg1.forward()
    do(d0b, "forward")
    do(d0c, "start_rest")
    do(d1a, "start")
    gx0.last()
    gx0.wait_own()
    gx0.wait_push(range(len(gx0.push)))
    own_x.wait()
    save_x = lcopy(XV, xh0)
    save_x.start()
    gx0.drain()
    for unit in u0u:
        do(unit, "finish")
    save_u0 = lcopy(U, wuh.at[0])
    save_u0.start()

    T2 = 2 * TB
    ND = D // 4
    NK = K // 4

    def up_tile(t, n):
        cols = pl.ds(mo(n * NK, NK), NK)
        return dot_nn(XV[t].reshape(T2, D), U[:, :, :, :, cols].reshape(D, NK)), cols

    def hidden0(t):
        for n in range(RING):
            pre, cols = up_tile(t, n)
            act, slope = gelu_parts(pre)
            AV[t, :, :, cols] = act.astype(BF16).reshape(2, TB, NK)
            SV[t, :, :, cols] = slope.reshape(2, TB, NK)

    def hidden1_tile(t, n):
        pre, cols = up_tile(t, n)
        act, slope = gelu_parts(pre)
        AV[t, :, :, cols] = act.astype(BF16).reshape(2, TB, NK)
        DV[t, :, cols] = (SV[t, :, :, cols].reshape(T2, NK) * slope).astype(BF16)

    def hidden1(t, part):
        for n in range(sum(SPLIT2[:part]), sum(SPLIT2[:part + 1])):
            hidden1_tile(t, n)

    def dact(gv, t, n):
        return dot_nt(gv[t].reshape(T2, D), W[n].reshape(NK, D))

    def dact1(t):
        def body(n, carry):
            SV[t, :, :, pl.ds(mo(n * NK, NK), NK)] = dact(GV1, t, n).reshape(2, TB, NK)
            return carry
        loop(RING, body, None)

    def dact0(t):
        def body(n, carry):
            cols = pl.ds(mo(n * NK, NK), NK)
            DV[t, :, cols] = (dact(GV0, t, n) * SV[t, :, :, cols].reshape(T2, NK)).astype(BF16)
            return carry
        loop(RING, body, None)

    def down_part(act, j, lo, tiles):
        t = lax.rem(x + j, RING)

        def body(n, carry):
            cols = pl.ds(mo((lo + n) * ND, ND), ND)
            PP[j, :, :, cols] = dot_nn(act[t, :, :, 0:K].reshape(T2, K), W[:, :, :, cols].reshape(K, ND)).reshape(2, TB, ND)
            return carry
        loop(tiles, body, None)

    def dx_part(j, lo, tiles):
        t = lax.rem(x + j, RING)

        def body(n, carry):
            cols = pl.ds(mo((lo + n) * ND, ND), ND)
            PP[j, :, :, cols] = dot_nt(DV[t], U[lo + n].reshape(ND, K)).reshape(2, TB, ND)
            return carry
        loop(tiles, body, None)

    class Reduce8:
        def __init__(self, part, index, split, old=()):
            self.part, self.index, self.split = part, index, split
            keys.extend(old)
            _, right, left = rings["x"]
            self.right, self.left = right, left
            self.pair, self.m, self.first = [], [], []
            for q in range(len(split)):
                cq = self.cols(q)
                first = sorted(fresh("recv") for j in range(RING))
                self.pair.append([self.swap(j, q, first[0]) for j in range(RING)])
                self.first.append(first[0])
                src = lambda j, h: PP.at[j, c, half(h), cq]
                self.m.append([rcopy(src(*PIECES[k]), XR.at[k, :, cq], left if k % 2 else right) for k in range(ARRIVALS)])
            keys.clear()

        def cols(self, q):
            return tile_cols(self.split, q)

        def swap(self, j, q, first):
            cq = self.cols(q)
            return remote(PP.at[j, cp, :, cq], DR.at[j, :, cq], ps.at[q * RING + j], rs.at[first + j], partner)

        def compute(self, j, q):
            self.part(j, sum(self.split[:q]), self.split[q])
            self.pair[q][j].start()

        def compute_all(self, q):
            def body(i, carry):
                j = lax.rem(i + 1, RING)
                self.part(j, sum(self.split[:q]), self.split[q])
                self.swap(j, q, self.first[q]).start()
                return carry
            loop(RING, body, None)

        def combine(self, j, q):
            self.pair[q][j].wait_recv()
            add_rows(PP.at[j, c, :, self.cols(q)], [DR.at[j, :, self.cols(q)]], TB, min(TB, 16))

        def opposite(self, q):
            self.m[q][0].start()
            self.m[q][1].start()

        def side(self, j, q):
            self.combine(j, q)
            self.m[q][2 if j == NXT else 3].start()

        def send(self, q):
            self.combine(OPP, q)
            self.opposite(q)
            self.side(NXT, q)
            self.side(PRV, q)

        def relay(self, q):
            for k, j, h in ((0, NXT, 0), (1, PRV, 1)):
                self.m[q][k].wait_recv()
                add_rows(PP.at[j, c, half(h), self.cols(q)], [XR.at[k, :, self.cols(q)]], HB, min(HB, 16))
                self.m[q][4 + k].start()

        def finish(self, q, res, outs):
            for d in self.m[q][2:]:
                d.wait_recv()
            step, cq = min(HB, 16), self.cols(q)
            for h, (kl, kr) in enumerate(((4, 3), (2, 5))):
                def body(r, carry):
                    lo = pl.ds(mo(r * step, step), step)
                    sl = pl.ds(mo(h * HB + r * step, step), step)
                    tot = PP[OWN, c, sl, cq] + (XR[kl, lo, cq] + XR[kr, lo, cq])
                    val = (res[sl, cq].astype(F32) + tot).astype(BF16)
                    for o in outs:
                        o[sl, cq] = val
                    return carry
                loop(HB // step, body, None)

        def drain(self):
            for d in sum(self.pair + self.m, []):
                d.wait_send()

        def release(self):
            self.drain()
            for k, to in enumerate((self.right, self.left, partner)):
                pl.semaphore_signal(credit.at[k], inc=1, device_id=to, device_id_type=MESH_ID)

        def acquire(self):
            for k in range(len((self.right, self.left, partner))):
                pl.semaphore_wait(credit.at[k], 1)

    def grad_a(j, dst, halves=None, q=None):
        t = off(z, j)

        def rows(h, carry):
            lo = [pl.ds(mo((2 * h + q) * XD + t * ZD, ZD), ZD) for q in HALVES]
            lhs = jnp.concatenate([XV[:, :, :, s].reshape(8 * TB, ZD) for s in lo], axis=1)

            cols, width = (pl.ds(0, K), K) if q is None else (pl.ds(q * ND, ND), ND)
            dst[h, :, :, cols] = dot_tn(lhs, DV[:, :, cols].reshape(8 * TB, width)).reshape(2, ZD, width)
            return carry
        if halves is None:
            loop(2, rows, None)
        else:
            for h in halves:
                rows(h, None)

    def grad_b(gv, j, dst, n=None):
        cols_l = pl.ds(mo(off(y, j) * NK, NK), NK)

        def body(n, carry):
            out = dot_tn(AV[:, :, :, cols_l].reshape(8 * TB, NK), gv[:, :, :, pl.ds(mo(n * K, K), K)].reshape(8 * TB, K))
            dst[:, n] = out.reshape(2, NK // 2, K)
            return carry
        if n is None:
            loop(2, body, None)
        else:
            body(n, None)

    grad_keys = [keys_of(sum(u0u, u0a) + d0a), [d.key for d in ex0 + ex1 + gg1.own + gg1.push] + keys_of(d0b + d0c + [gg1.ring])]

    def grad_key(l):
        return grad_keys[l].pop() if grad_keys[l] else fresh("recv")

    class Reduce4:
        def __init__(self, l, axis, part, recv, stage):
            _, right, left = rings[axis]
            self.part, self.recv, self.stage = part, recv, stage
            self.m = [rcopy(part(*PIECES[k]), recv(k), left if k % 2 else right, grad_key(l))
                      for k in range(ARRIVALS)]
            self.loads = [lcopy(recv(k), stage(k)) for k in range(ARRIVALS)] if stage else None

        def opposite(self):
            self.m[0].start()
            self.m[1].start()

        def sides(self, j):
            self.m[2 if j == NXT else 3].start()

        def fetch(self, k):
            self.m[k].wait_send()
            self.m[k].wait_recv()
            if self.loads:
                self.loads[k].start()

        def absorb(self, k):
            if self.loads:
                self.loads[k].wait()
            dst = self.part(*TARGETS[k])
            add_rows(dst, [(self.stage or self.recv)(k)], dst.shape[1], min(dst.shape[1], 16))

    def arrive(reduces, ks):
        for k in ks:
            for r in reduces:
                r.fetch(k)
        for k in ks:
            for r in reduces:
                r.absorb(k)

    def relay(reduces):
        for k in (0, 1):
            for r in reduces:
                r.fetch(k)
        for k in (0, 1):
            for r in reduces:
                r.absorb(k)
                r.m[4 + k].start()

    hq = DR_ROWS // 2
    own_grads = [(SV.at[pl.ds(0, 2)], SV.at[pl.ds(2, 2)]), (GPA.at[OWN], GPB.at[OWN])]

    def third(k, rows):
        return pl.ds((k // 2) * rows, rows)

    def reduce_a(l, q, chunks):
        own = own_grads[l][0]
        ca = pl.ds(q * (K // chunks), K // chunks)

        def part(j, h):
            return (own if j == OWN else GPA.at[j]).at[h, :, :, ca]

        def part2(j, h):
            return own.at[h, :, pl.ds(mo(off(y, j) * 2 * UR, 2 * UR), 2 * UR), ca]
        if l < q:
            second = lambda k: GPA.at[OWN, k % 2, :, third(k, 2 * UR), ca], None
        else:
            second = lambda k: ra2.at[l, k, :, :, ca], lambda k: STA.at[k % 2, :, :, ca]
        return (Reduce4(l, "z", part, lambda k: ra1.at[l, k, :, :, ca], lambda k: part(*PIECES[k])),
                Reduce4(l, "y", part2, *second))

    def reduce_b(l, q):
        own, nb = own_grads[l][1], pl.ds(q, 1)

        def part(j, h):
            return (own if j == OWN else GPB.at[j]).at[h, nb]

        def part2(j, h):
            t = off(z, j)
            return own.at[t // 2, nb, pl.ds(mo(lax.rem(t, 2) * DR_ROWS + h * hq, hq), hq), :]
        if l < q:
            second = lambda k: GPB.at[OWN, k % 2, nb, third(k, hq), :], None
        else:
            second = lambda k: rb2.at[l, k, nb], lambda k: STB.at[k % 2, nb]
        return (Reduce4(l, "y", part, lambda k: rb1.at[l, k, nb], lambda k: part(*PIECES[k])),
                Reduce4(l, "z", part2, *second))

    def sides(reduces, j):
        for r in reduces:
            r.sides(j)

    def second_start(reduces):
        for r in reduces:
            r.opposite()
            r.sides(NXT)
            r.sides(PRV)

    def up_out(l, q, chunks):
        own = own_grads[l][0]
        ca = pl.ds(q * (K // chunks), K // chunks)

        def rows_of(tx, tc):
            return own.at[tx // 2, lax.rem(tx, 2), pl.ds(mo((2 * y + tc) * UR, UR), UR), ca]
        to = uh.at[l, x, mine, ca]
        sends = [rcopy(rows_of(off(x, dx), cp if dc else c), to, dev(dx=dx, dc=dc), grad_key(l)) for dx, dc in group]
        local = [lcopy(rows_of(x, c), to)]
        for cpy in sends + local:
            cpy.start()
        return sends, local

    def down_out(l, n):
        cpy = lcopy(own_grads[l][1].at[z // 2, n, pl.ds(mo(lax.rem(z, 2) * DR_ROWS, DR_ROWS), DR_ROWS), :],
                    gd_out.at[l, :, pl.ds(n * K, K)])
        cpy.start()
        return [], [cpy]

    def grads_out_finish(state):
        for cpy in state[0]:
            cpy.wait_recv()
            cpy.wait_send()
        for cpy in state[1]:
            cpy.wait()

    r = Reduce8(functools.partial(down_part, AV), 0, SPLIT3)
    r_keys = sorted([d.key for m in r.m for d in m] + [f + j for f in r.first for j in range(RING)])
    hidden0(off(x, OPP))
    hidden0(off(x, NXT))
    do(d0b, "finish")
    r.compute(OPP, 0)
    r.compute(NXT, 0)
    do(d0c, "forward")
    do(d0d, "start")
    r.combine(OPP, 0)
    r.opposite(0)
    do(u0u[2] + u0u[3], "drain")
    hidden0(off(x, PRV))
    r.compute(PRV, 0)
    r.side(NXT, 0)
    do(d1a, "forward")
    hidden0(off(x, OWN))
    r.side(PRV, 0)
    save_s = lcopy(SV, sh0)
    save_s.start()
    save_a0 = lcopy(AV, ah.at[0])
    save_a0.start()
    gg1.sides()
    do(d0c, "finish")
    r.compute_all(1)
    r.relay(0)
    do(d0d, "forward")
    for cpy in ex1:
        cpy.wait_recv()
    own_d1.wait()
    do(u1a, "start")
    r.send(1)
    do(d1a, "finish")
    do(d1b, "start")
    gg1.last()
    save_x.wait()
    do(d0d, "finish")
    do(d0b + d0c, "drain")
    save_d0 = lcopy(W, wdh.at[0])
    save_d0.start()
    r.compute(OPP, 2)
    r.relay(1)
    save_u0.wait()
    do(u1a, "forward")
    r.compute(NXT, 2)
    r.combine(OPP, 2)
    r.opposite(2)
    r.compute(PRV, 2)
    r.side(NXT, 2)
    r.compute(OWN, 2)
    r.side(PRV, 2)
    r.compute(OWN, 0)
    for q in range(len(SPLIT3)):
        r.combine(OWN, q)

    def gather_keys(gathers):
        return [d.key for g in gathers for d in g.ring.d + g.own + g.push]

    def token_gathers(slot, buf):
        def make(q):
            cq = tile_cols(SPLIT2, q)
            return Gather8(lambda h: RES.at[slot, half(h), cq], lambda b, k, h: buf.at[b, k, half(h), cq])
        return [make(0), make(1)]

    keys.extend(gather_keys((gx0,)))
    gx1 = token_gathers(X1, XV)
    do(d1a, "drain")
    do(d1b, "forward")
    for q in HALVES:
        r.finish(q, RES.at[X0], [RES.at[X1], XV.at[x, c]])
    r.relay(2)
    gx1[0].start()
    do(u1a, "finish")
    do(u1b, "start")
    do(u1c, "start_first")
    pair, rest = pl.ds(0, 2), pl.ds(2, 2)
    own_up = [lcopy(up[1].at[pair, z], U.at[pair, z]), lcopy(up[1].at[rest, :, y], U.at[rest, :, y])]
    for cpy in own_up:
        cpy.start()
    gg1.wait_own()
    gg1.wait_push(range(len(gg1.push)))
    own_g.wait()
    save_d0.wait()
    do(d0d + u1a, "drain")
    gg1.drain()
    do(d1b, "finish")
    load_w1d = lcopy(wdh.at[1], W)
    load_w1d.start()
    r.finish(2, RES.at[X0], [RES.at[X1], XV.at[x, c]])
    gx1[1].start()
    save_s.wait()
    do(u1b, "forward")
    do(u1c, "start_rest")
    load_w1d.wait()
    dact1(off(x, OWN))
    gx1[0].forward()
    r.release()
    dact1(off(x, NXT))
    gx1[0].sides()
    dact1(off(x, PRV))
    do(u1c, "forward")
    do(u1b, "finish")
    dact1(off(x, OPP))
    load_w0d_again = lcopy(wdh.at[0], W)
    load_w0d_again.start()
    save_a0.wait()
    do(gx1, "wait_own")
    for cpy in own_up:
        cpy.wait()
    hidden1(off(x, OWN), 0)
    do(gx1[1:], "forward")
    do(gx1[1:], "sides")
    for j in (PRV, NXT):
        for g in gx1:
            g.wait_push(PUSHES[j])
        hidden1(off(x, j), 0)
    gx1[0].last()
    do(u1c, "finish")
    hidden1(off(x, OWN), 1)
    hidden1(off(x, PRV), 1)
    gx1[1].last()
    hidden1(off(x, NXT), 1)
    for g in gx1:
        g.wait_push(PUSHES[OPP])
    hidden1_tile(off(x, OPP), off(y, OPP))

    (a1, a2), (b1, b2) = zip(*[reduce_a(1, q, 2) for q in HALVES]), zip(*[reduce_b(1, q) for q in HALVES])
    first1, second1 = b1 + a1, b2 + a2
    grad_b(GV1, OPP, GPB.at[OPP], 0)
    b1[0].opposite()
    for n in (PRV, OWN, NXT):
        hidden1_tile(off(x, OPP), off(y, n))
    for q in HALVES:
        for h in HALVES:
            grad_a(OPP, GPA.at[OPP], (h,), q)
            a1[q].m[h].start()
    load_s0 = lcopy(sh0, SV)
    load_s0.start()
    save_a1 = lcopy(AV, ah.at[1])
    save_a1.start()
    grad_b(GV1, OPP, GPB.at[OPP], 1)
    b1[1].opposite()
    r = Reduce8(dx_part, 1, SPLIT2, r_keys)
    r.acquire()
    r.compute(OPP, 0)
    r.compute(NXT, 0)
    r.combine(OPP, 0)
    r.opposite(0)
    r.compute(PRV, 0)
    r.side(NXT, 0)
    r.side(PRV, 0)
    r.compute_all(1)
    load_w0u_again = lcopy(wuh.at[0], U)
    r.compute(OWN, 0)
    do(u1b + u1c, "drain")
    load_w0u_again.start()
    grad_b(GV1, NXT, GPB.at[NXT])
    sides(b1, NXT)
    grad_b(GV1, PRV, GPB.at[PRV])
    sides(b1, PRV)
    r.relay(0)
    r.send(1)
    grad_a(NXT, GPA.at[NXT])
    sides(a1, NXT)
    grad_a(PRV, GPA.at[PRV])
    sides(a1, PRV)
    r.combine(OWN, 0)
    r.combine(OWN, 1)
    keys.extend(gather_keys(gx1))
    gg0 = token_gathers(G0, GV0)
    r.relay(1)
    r.finish(0, RES.at[G1], [RES.at[G0], GV0.at[x, c]])
    gg0[0].start()
    relay(first1)
    grad_b(GV1, OWN, GPB.at[OWN])
    save_a1.wait()
    load_a0 = lcopy(ah.at[0], AV)
    load_a0.start()
    do(d1b, "drain")
    load_a1 = lcopy(ah.at[1], GV1.at[:, :, :, 0:K])
    load_a1.start()
    r.finish(1, RES.at[G1], [RES.at[G0], GV0.at[x, c]])
    gg0[1].start()
    gg0[0].forward()
    grad_a(OWN, GPA.at[OWN])
    do(gx1, "drain")
    load_x0 = lcopy(xh0, XV)
    load_x0.start()
    gg0[0].sides()
    r.release()
    gg0[1].forward()
    gg0[0].last()
    load_w0d_again.wait()
    load_s0.wait()
    do(gg0, "wait_own")
    dact0(off(x, OWN))
    gg0[1].sides()
    gg0[1].last()
    for g in gg0:
        g.wait_push(PUSHES[PRV])
    dact0(off(x, PRV))
    for g in gg0:
        g.wait_push(PUSHES[NXT])
    dact0(off(x, NXT))
    for g in gg0:
        g.wait_push(PUSHES[OPP])

    (a1n, a2n), (b1n, b2n) = zip(*[reduce_a(0, q, 2) for q in HALVES]), zip(*[reduce_b(0, q) for q in HALVES])
    load_a0.wait()
    grad_b(GV0, OPP, GPB.at[OPP])
    b1n[0].opposite()
    dact0(off(x, OPP))
    load_w1d_again = lcopy(wdh.at[1], W)
    load_w1d_again.start()
    load_x0.wait()
    for h in HALVES:
        grad_a(OPP, GPA.at[OPP], (h,))
        a1n[0].m[h].start()
    arrive(first1, EARLY + LATE)
    second_start(second1)
    load_w0u_again.wait()
    r = Reduce8(dx_part, 2, WHOLE, r_keys)
    r.acquire()
    r.compute_all(0)
    r.send(0)
    grad_b(GV0, NXT, GPB.at[NXT])
    b1n[0].sides(NXT)
    grad_b(GV0, PRV, GPB.at[PRV])
    b1n[0].sides(PRV)
    grad_a(NXT, GPA.at[NXT])
    a1n[0].sides(NXT)
    grad_a(PRV, GPA.at[PRV])
    a1n[0].sides(PRV)
    relay(second1)
    r.relay(0)
    relay((b1n[0], a1n[0]))
    for red in (b1n[1], a1n[1]):
        red.opposite()
        red.sides(NXT)
        red.sides(PRV)
    r.combine(OWN, 0)
    grad_b(GV0, OWN, own_grads[0][1])
    grad_a(OWN, own_grads[0][0])
    r.finish(0, RES.at[G0], [RES.at[X0]])
    r.release()
    write_gi = lcopy(RES.at[X0], gi_out)
    write_gi.start()
    arrive((b1n[0], a1n[0]), EARLY)
    arrive(second1, EARLY)
    arrive(second1, LATE)
    state1 = [up_out(1, q, 2) for q in HALVES] + [down_out(1, n) for n in HALVES]
    load_a1.wait()
    load_w1d_again.wait()
    r = Reduce8(functools.partial(down_part, GV1), 3, WHOLE, r_keys)
    r.acquire()
    r.compute_all(0)
    r.send(0)
    r.combine(OWN, 0)
    arrive((b1n[0], a1n[0]), LATE)
    for state in state1:
        grads_out_finish(state)
    relay((b1n[1], a1n[1]))
    second_start((a2n[0], b2n[0]))
    r.relay(0)
    arrive((b1n[1], a1n[1]), EARLY)

    def start(red):
        red.opposite()
        sides((red,), NXT)
        sides((red,), PRV)
    arrive((b1n[1],), LATE)
    relay((a2n[0],))
    arrive((a1n[1],), LATE)
    start(a2n[1])
    start(b2n[1])
    arrive((a2n[0],), EARLY)
    relay((b2n[0],))
    arrive((a2n[0],), LATE)
    state0 = [up_out(0, 0, 2)]
    relay((a2n[1],))
    arrive((b2n[0],), EARLY)
    relay((b2n[1],))
    arrive((a2n[1],), EARLY)
    arrive((a2n[1],), LATE)
    state0.append(up_out(0, 1, 2))
    arrive((b2n[1],), EARLY)
    for q in HALVES:
        arrive((b2n[q],), LATE)
        state0.append(down_out(0, q))
    r.finish(0, RES.at[X1], [RES.at[G1]])
    write_y = lcopy(RES.at[G1], y_out)
    write_y.start()
    r.drain()
    do(gg0, "drain")
    write_gi.wait()
    write_y.wait()
    for state in state0:
        grads_out_finish(state)
    assert used["recv"] <= N_RECV and used["send"] <= N_SEND and used["local"] <= N_LOCAL


def finish_kernel(y_in, gi_in, gu_in, gd_in, y_out, gi_out, gu_out, gd_out, ybuf, gibuf, gubuf, gdbuf, gushuf, sems):
    layers, ur, ff = gu_out.shape
    s2 = ff // 64
    half = s2 // 2
    pairs = [((gu_in.at[l], gubuf.at[l]), (gushuf.at[l], gu_out.at[l])) for l in range(layers)]
    pairs += [((a, b), (b, o)) for a, b, o in ((gd_in, gdbuf, gd_out), (y_in, ybuf, y_out), (gi_in, gibuf, gi_out))]
    loads = [pltpu.make_async_copy(*p, sems.at[0, k]) for k, (p, _) in enumerate(pairs)]
    stores = [pltpu.make_async_copy(*p, sems.at[1, k]) for k, (_, p) in enumerate(pairs)]
    for cpy in loads:
        cpy.start()
    low = lax.broadcasted_iota(jnp.int32, (ur, s2), 1) < half
    swap = lambda v: pltpu.roll(v, half, 1)
    for l, (load, store) in enumerate(zip(loads, stores)):
        load.wait()
        for b in range(RING if l < layers else 0):
            for yy in range(RING):
                for m in HALVES:
                    cols = pl.ds((yy * 2 + m) * s2, s2)
                    t0, t1 = (gubuf[l, b, pl.ds(k * ur, ur), cols] for k in HALVES)
                    strip = (b * RING + 2 * m) * RING + yy
                    gushuf[l, :, pl.ds(strip * s2, s2)] = jnp.where(low, t0, swap(t1))
                    gushuf[l, :, pl.ds((strip + RING) * s2, s2)] = jnp.where(low, swap(t0), t1)
        store.start()
    for cpy in stores:
        cpy.wait()


def solution(mesh, interpret=None):
    fine = Mesh(np.asarray(mesh.devices).reshape(4, 4, 4, 2), ALL)
    tok_spec = P(ALL, None)
    weight_spec = P(None, ALL, None)

    def device_step(x_loc, up_loc, down_loc, g_loc):
        layers, ur, ff = up_loc.shape
        dr, dm = down_loc.shape[1:]
        tb = x_loc.shape[0]
        k = ff // 8
        zd = dm // 16
        hbm = lambda shape, dt: jax.ShapeDtypeStruct(shape, dt)
        outs = [
            hbm((tb, dm), BF16), hbm((tb, dm), BF16), hbm((layers, dr, dm), F32),
            hbm((RING, CORES, tb, dm), BF16),
            hbm((layers, RING, RING, RING, 2 * ur, k), BF16),
            hbm((layers, RING, RING, dr, dm), BF16),
            hbm((RING, CORES, tb, k), F32), hbm((layers, RING, CORES, tb, k), BF16),
            *[hbm((layers, ARRIVALS, CORES, n, k), F32) for n in (zd, zd, 2 * ur, 2 * ur)],
            hbm((layers, RING, 2 * ur, k), F32),
        ]
        vm = pltpu.VMEM
        scratch = [
            vm((RING, RING, RING, 2 * ur, k), BF16), vm((RING, RING, dr, dm), BF16),
            vm((RING, CORES, tb, dm), BF16), vm((RING, CORES, tb, dm), BF16), vm((RING, CORES, tb, dm), BF16),
            vm((RING, CORES, tb, k), F32), vm((RING, CORES, tb, k), BF16), vm((RING, 2 * tb, k), BF16),
            vm((RING, CORES, CORES, zd, k), F32), vm((RING, CORES, CORES, zd, k), F32),
            vm((RING, CORES, tb, dm), F32), vm((4, tb, dm), F32), vm((6, tb // 2, dm), F32),
            vm((4, tb, dm), BF16), vm((CORES, CORES, 2 * ur, k), F32), vm((CORES, CORES, 2 * ur, k), F32),
            *[pltpu.SemaphoreType.DMA((n,)) for n in (N_SEND, N_RECV, N_LOCAL, len(SPLIT3) * RING)],
            pltpu.SemaphoreType.REGULAR((3,)),
        ]
        anyspec = pl.BlockSpec(memory_space=pl.ANY)
        call = pl.pallas_call(
            functools.partial(kernel, (dm, k, tb, ur, dr)),
            out_shape=outs,
            in_specs=[anyspec] * 4,
            out_specs=[anyspec] * len(outs),
            scratch_shapes=scratch,
            compiler_params=pltpu.CompilerParams(collective_id=0, has_side_effects=True, vmem_limit_bytes=67043328),
            name="mlp_stack",
            **({"interpret": interpret} if interpret else {}),
        )
        y_raw, gi_raw, gd_raw, *_, gu_raw = call(x_loc, up_loc, down_loc, g_loc)
        raws = (y_raw, gi_raw, gu_raw, gd_raw)
        outs = [hbm((tb, dm), BF16), hbm((tb, dm), BF16), hbm((layers, ur, ff), F32), hbm((layers, dr, dm), F32)]
        return tuple(pl.pallas_call(
            finish_kernel, out_shape=outs, in_specs=[anyspec] * len(outs), out_specs=[anyspec] * len(outs),
            scratch_shapes=[vm(v.shape, v.dtype) for v in raws] + [vm(outs[2].shape, F32), pltpu.SemaphoreType.DMA((2, layers + len(outs)))],
            name="write_out")(*raws))

    return jax.shard_map(device_step, mesh=fine, in_specs=(tok_spec, weight_spec, weight_spec, tok_spec),
                         out_specs=(tok_spec, tok_spec, weight_spec, weight_spec), check_vma=False)
```

```python
import functools

import jax
import jax.numpy as jnp
import numpy as np
from jax import lax
from jax.experimental import pallas as pl
from jax.experimental.pallas import tpu as pltpu
from jax.sharding import Mesh, PartitionSpec as P

MESH_ID = pl.DeviceIdType.MESH
ALL = ("x", "z", "y", "c")
F32, BF16 = jnp.float32, jnp.bfloat16
RING, CORES, ARRIVALS = 4, 2, 6
OWN, NXT, OPP, PRV = range(RING)
X0, X1, G1, G0 = range(RING)
HALVES = (0, 1)
WHOLE, SPLIT2, SPLIT3 = (4,), (2, 2), (1, 1, 2)
PIECES = ((OPP, 0), (OPP, 1), (NXT, 1), (PRV, 0), (NXT, 0), (PRV, 1))
TARGETS = ((NXT, 0), (PRV, 1), (OWN, 1), (OWN, 0), (OWN, 0), (OWN, 1))
EARLY, LATE = (2, 3), (4, 5)
PUSHES = {PRV: (0, 2), NXT: (1, 3), OPP: (4, 5)}
N_RECV, N_SEND, N_LOCAL = 192, 90, 19


def gelu_parts(pre_act):
    norm_cdf = 0.5 * (1.0 + lax.erf(pre_act * (2.0 ** -0.5)))
    norm_pdf = jnp.exp(-0.5 * pre_act * pre_act) * ((2.0 * jnp.pi) ** -0.5)
    return pre_act * norm_cdf, norm_cdf + pre_act * norm_pdf


def loop(n, body, init):
    return lax.fori_loop(0, n, body, init)


def dot_nn(left, right):
    return lax.dot_general(left, right, (((1,), (0,)), ((), ())), preferred_element_type=F32)


def dot_nt(left, right):
    return lax.dot_general(left, right, (((1,), (1,)), ((), ())), preferred_element_type=F32)


def dot_tn(left, right):
    return lax.dot_general(left, right, (((0,), (0,)), ((), ())), preferred_element_type=F32)


def kernel(dims, x_in, wu_in, wd_in, g_in,
           y_out, gi_out, gd_out,
           xh0, wuh, wdh, sh0, ah, ra1, rb1, ra2, rb2, uh,
           U, W, XV, GV1, GV0, SV, AV, DV, GPA, GPB, PP, DR, XR, RES, STA, STB,
           ss, rs, ls, ps, credit):
    D, K, TB, UR, DR_ROWS = dims
    HB = TB // 2
    x, z, y, c = (lax.axis_index(a) for a in ALL)
    cp = 1 - c
    S2 = 2 * DR_ROWS
    XD = D // 4
    ZD = D // 16

    def dev(dx=0, dz=0, dy=0, dc=0):
        wrap = lambda v, d, n: v if d == 0 else lax.rem(v + (d % n), n)
        return (wrap(x, dx, 4), wrap(z, dz, 4), wrap(y, dy, 4), wrap(c, dc, 2))

    partner = dev(dc=1)
    rings = {"x": (x, dev(dx=1), dev(dx=-1)), "z": (z, dev(dz=1), dev(dz=-1)), "y": (y, dev(dy=1), dev(dy=-1))}
    off = lambda v, d: v if d == 0 else lax.rem(v + d, 4)

    used = {"recv": 0, "send": 0, "local": 0}
    free = {"send": [], "local": []}
    keys = []

    def fresh(kind):
        if kind == "recv" and keys:
            return keys.pop()
        used[kind] += 1
        return used[kind] - 1

    def take(kind):
        return free[kind].pop() if free[kind] else fresh(kind)

    def remote(src, dst, send, recv, to):
        return pltpu.make_async_remote_copy(src_ref=src, dst_ref=dst, send_sem=send, recv_sem=recv,
                                            device_id=to, device_id_type=MESH_ID)

    class rcopy:
        def __init__(self, src, dst, to, key=None):
            self.args, self.key = (src, dst, to), fresh("recv") if key is None else key

        def start(self):
            src, dst, to = self.args
            self.sem = take("send")
            self.d = remote(src, dst, ss.at[self.sem], rs.at[self.key], to)
            self.d.start()

        def wait_recv(self):
            self.d.wait_recv()

        def wait_send(self):
            self.d.wait_send()
            free["send"].append(self.sem)

    class lcopy:
        def __init__(self, src, dst):
            self.args = src, dst

        def start(self):
            self.sem = take("local")
            self.d = pltpu.make_async_copy(*self.args, ls.at[self.sem])
            self.d.start()

        def wait(self):
            self.d.wait()
            free["local"].append(self.sem)

    def mo(v, m):
        return pl.multiple_of(v, m)

    class Gather4:
        def __init__(self, axis, src, dst):
            i, right, left = rings[axis]
            lft, rgt = off(i, 3), off(i, 1)
            self.d = [rcopy(src(0), dst(i, 0), right), rcopy(src(1), dst(i, 1), right),
                      rcopy(src(0), dst(i, 0), left), rcopy(src(1), dst(i, 1), left),
                      rcopy(dst(lft, 0), dst(lft, 0), right), rcopy(dst(rgt, 1), dst(rgt, 1), left)]

        def start_first(self):
            self.d[0].start()
            self.d[3].start()

        def start_rest(self):
            self.d[1].start()
            self.d[2].start()

        def start(self):
            self.start_first()
            self.start_rest()

        def forward(self):
            for k in HALVES:
                self.d[3 * k].wait_recv()
                self.d[4 + k].start()

        def neighbours(self):
            self.d[1].wait_recv()
            self.d[2].wait_recv()

        def opposite(self):
            self.d[4].wait_recv()
            self.d[5].wait_recv()

        def finish(self):
            self.neighbours()
            self.opposite()

        def drain(self):
            for d in self.d:
                d.wait_send()

    class Gather8:
        def __init__(self, src, dst):
            self.ring = Gather4("x", src, lambda b, h: dst(b, c, h))
            lft, rgt, opp = off(x, PRV), off(x, NXT), off(x, OPP)
            blocks = [(lft, 0), (rgt, 1), (lft, 1), (rgt, 0), (opp, 0), (opp, 1)]
            self.own = [rcopy(src(h), dst(x, c, h), partner) for h in HALVES]
            self.push = [rcopy(dst(b, c, h), dst(b, c, h), partner) for b, h in blocks]

        def start(self):
            self.ring.start()
            for d in self.own:
                d.start()

        def forward(self):
            self.ring.forward()
            self.push[0].start()
            self.push[1].start()

        def sides(self):
            self.ring.d[1].wait_recv()
            self.push[2].start()
            self.ring.d[2].wait_recv()
            self.push[3].start()

        def last(self):
            self.ring.d[4].wait_recv()
            self.push[4].start()
            self.ring.d[5].wait_recv()
            self.push[5].start()

        def wait_own(self):
            for d in self.own:
                d.wait_recv()

        def wait_push(self, ks):
            for k in ks:
                self.push[k].wait_recv()

        def drain(self):
            self.ring.drain()
            for d in self.own + self.push:
                d.wait_send()

    def add_rows(dst, srcs, rows, step):
        def body(r, carry):
            sl = pl.ds(mo(r * step, step), step)
            if len(dst.shape) == 3:
                for q in range(dst.shape[0]):
                    acc = dst[q, sl, :]
                    for s in srcs:
                        acc = acc + s[q, sl, :]
                    dst[q, sl, :] = acc
            else:
                acc = dst[sl, :]
                for s in srcs:
                    acc = acc + s[sl, :]
                dst[sl, :] = acc
            return carry
        loop(rows // step, body, None)

    barrier = pltpu.get_barrier_semaphore()
    group = [(dx, dc) for dx in (OPP, NXT, PRV, OWN) for dc in HALVES if dx or dc]
    peers = [dev(dx=dx, dc=dc) for dx, dc in group] + [rings[a][k] for a in "zy" for k in (1, 2)]
    for p in peers:
        pl.semaphore_signal(barrier, inc=1, device_id=p, device_id_type=MESH_ID)

    load_u = [[lcopy(wu_in.at[l, :, pl.ds(b * D, D)], RES.at[G0, pl.ds((l * RING + b) * UR, UR), :])
               for b in range(RING)] for l in HALVES]
    load_d = [lcopy(wd_in.at[l], RES.at[X1, pl.ds(l * DR_ROWS, DR_ROWS), :]) for l in HALVES]
    load_x = lcopy(x_in, RES.at[X0])
    load_g = lcopy(g_in, RES.at[G1])
    own_x = lcopy(x_in, XV.at[x, c])
    own_g = lcopy(g_in, GV1.at[x, c])
    own_d0 = lcopy(wd_in.at[0], W.at[y, z])
    for cpy in load_u[0] + load_u[1] + load_d + [load_x, own_d0, own_x, load_g, own_g]:
        cpy.start()

    low = lax.broadcasted_iota(jnp.int32, (UR, S2), 1) < DR_ROWS
    swap = lambda v: pltpu.roll(v, DR_ROWS, 1)
    for l in HALVES:
        for cpy in load_u[l]:
            cpy.wait()
        for b in range(RING):
            rows = pl.ds((l * RING + b) * UR, UR)
            for yy in range(RING):
                for m in HALVES:
                    s0 = RES[G0, rows, pl.ds((2 * m * RING + yy) * S2, S2)].astype(F32)
                    s1 = RES[G0, rows, pl.ds(((2 * m + 1) * RING + yy) * S2, S2)].astype(F32)
                    cols = pl.ds((yy * 2 + m) * S2, S2)
                    AV[l, 0, pl.ds(2 * b * UR, UR), cols] = jnp.where(low, s0, swap(s1)).astype(BF16)
                    AV[l, 0, pl.ds((2 * b + 1) * UR, UR), cols] = jnp.where(low, swap(s0), s1).astype(BF16)
    for cpy in load_d + [load_x, own_d0]:
        cpy.wait()
    pl.semaphore_wait(barrier, len(peers))

    half = lambda h: pl.ds(h * HB, HB)

    def tile_cols(split, q):
        return pl.ds(sum(split[:q]) * (D // RING), split[q] * (D // RING))

    gx0 = Gather8(lambda h: RES.at[X0, half(h)], lambda b, k, h: XV.at[b, k, half(h)])
    gg1 = Gather8(lambda h: RES.at[G1, half(h)], lambda b, k, h: GV1.at[b, k, half(h)])
    up = [U, wuh.at[1]]
    down = [W, wdh.at[1]]
    hr = DR_ROWS // 4

    def quarter(q, h):
        return pl.ds((2 * q + h) * hr, hr)

    def down_first(l):
        to = down[l]
        src = lambda q: lambda h: RES.at[X1, pl.ds(l * DR_ROWS + (2 * q + h) * hr, hr)]
        return [Gather4("z", src(0), lambda b, h: to.at[y, b, quarter(0, h)]),
                Gather4("y", src(1), lambda b, h: to.at[b, z, quarter(1, h)])]

    def down_second(l, split, n):
        to, cs = down[l], tile_cols(split, n)
        return [Gather4("y", lambda h: to.at[y, :, quarter(0, h), cs], lambda b, h: to.at[b, :, quarter(0, h), cs]),
                Gather4("z", lambda h: to.at[:, z, quarter(1, h), cs], lambda b, h: to.at[:, b, quarter(1, h), cs])]

    def up_first(to):
        return [Gather4("y", lambda h: to.at[h, z, y], lambda b, h: to.at[h, z, b]),
                Gather4("z", lambda h: to.at[2 + h, z, y], lambda b, h: to.at[2 + h, b, y])]

    def hidden_cols(n):
        return pl.ds(sum(SPLIT2[:n]) * (K // RING), SPLIT2[n] * (K // RING))

    def up_second(n):
        cs, src = hidden_cols(n), up[1]
        return [Gather4("z", lambda h: src.at[h, z, :, :, cs], lambda b, h: U.at[h, b, :, :, cs]),
                Gather4("y", lambda h: src.at[2 + h, :, y, :, cs], lambda b, h: U.at[2 + h, :, b, :, cs])]

    def up_unit(to, j):
        yj, zj = off(y, j), off(z, j)
        return [Gather4("z", lambda h: to.at[h, z, yj], lambda b, h: to.at[h, b, yj]),
                Gather4("y", lambda h: to.at[2 + h, zj, y], lambda b, h: to.at[2 + h, zj, b])]

    def do(gathers, step):
        for g in gathers:
            getattr(g, step)()

    mine = pl.ds(mo(c * UR, UR), UR)

    def up_exchange(l):
        sends = []
        for dx, dc in group:
            tx, tc = off(x, dx), (cp if dc else c)
            src = AV.at[l, 0, pl.ds(mo((tx * 2 + tc) * UR, UR), UR), :]
            sends.append(rcopy(src, up[l].at[x, z, y, mine, :], dev(dx=dx, dc=dc)))
        for cpy in sends:
            cpy.start()
        return sends

    def keys_of(gathers):
        return [d.key for g in gathers for d in g.d]

    d0a, d0b, d0c = down_first(0), down_second(0, SPLIT3, 0), down_second(0, SPLIT3, 1)
    u0a, u0u = up_first(up[0]), [up_unit(up[0], j) for j in (OWN, PRV, NXT, OPP)]
    keys.extend(keys_of(u0a))
    d0d = down_second(0, SPLIT3, 2)
    keys.extend(keys_of(d0a))
    d1a = down_first(1)
    keys.extend(keys_of(sum(u0u, [])))
    d1b, u1a = down_second(1, WHOLE, 0), up_first(up[1])
    u1b, u1c = up_second(0), up_second(1)
    ex0 = up_exchange(0)
    do(d0a, "start")
    gx0.start()
    ex1 = up_exchange(1)
    my_rows = pl.ds(mo((x * 2 + c) * UR, UR), UR)
    own_u1 = lcopy(AV.at[1, 0, my_rows, :], up[1].at[x, z, y, mine, :])
    own_u1.start()
    own_d1 = lcopy(RES.at[X1, pl.ds(DR_ROWS, DR_ROWS), :], down[1].at[y, z])
    own_d1.start()
    U[x, z, y, mine, :] = AV[0, 0, my_rows, :]
    do(d0a, "forward")
    for cpy in ex0:
        cpy.wait_recv()
    do(u0a, "start")
    do(u0u[0], "start")
    do(u0a, "forward")
    gx0.forward()
    load_g.wait()
    gg1.start()
    do(u0a, "neighbours")
    do(u0u[1], "start")
    do(u0u[2], "start")
    do(u0u[0], "forward")
    do(u0a, "opposite")
    do(u0u[3], "start")
    do(d0a, "finish")
    do(d0a + u0a, "drain")
    do(u0u[1], "forward")
    do(u0u[2], "forward")
    do(d0b, "start_first")
    gx0.sides()
    for cpy in ex0 + ex1:
        cpy.wait_send()
    own_u1.wait()
    do(u0u[3], "forward")
    do(u0u[0] + u0u[1], "drain")
    do(d0b, "start_rest")
    do(d0c, "start_first")
    gg1.forward()
    do(d0b, "forward")
    do(d0c, "start_rest")
    do(d1a, "start")
    gx0.last()
    gx0.wait_own()
    gx0.wait_push(range(len(gx0.push)))
    own_x.wait()
    save_x = lcopy(XV, xh0)
    save_x.start()
    gx0.drain()
    for unit in u0u:
        do(unit, "finish")
    save_u0 = lcopy(U, wuh.at[0])
    save_u0.start()

    T2 = 2 * TB
    ND = D // 4
    NK = K // 4

    def up_tile(t, n):
        cols = pl.ds(mo(n * NK, NK), NK)
        return dot_nn(XV[t].reshape(T2, D), U[:, :, :, :, cols].reshape(D, NK)), cols

    def hidden0(t):
        for n in range(RING):
            pre, cols = up_tile(t, n)
            act, slope = gelu_parts(pre)
            AV[t, :, :, cols] = act.astype(BF16).reshape(2, TB, NK)
            SV[t, :, :, cols] = slope.reshape(2, TB, NK)

    def hidden1_tile(t, n):
        pre, cols = up_tile(t, n)
        act, slope = gelu_parts(pre)
        AV[t, :, :, cols] = act.astype(BF16).reshape(2, TB, NK)
        DV[t, :, cols] = (SV[t, :, :, cols].reshape(T2, NK) * slope).astype(BF16)

    def hidden1(t, part):
        for n in range(sum(SPLIT2[:part]), sum(SPLIT2[:part + 1])):
            hidden1_tile(t, n)

    def dact(gv, t, n):
        return dot_nt(gv[t].reshape(T2, D), W[n].reshape(NK, D))

    def dact1(t):
        def body(n, carry):
            SV[t, :, :, pl.ds(mo(n * NK, NK), NK)] = dact(GV1, t, n).reshape(2, TB, NK)
            return carry
        loop(RING, body, None)

    def dact0(t):
        def body(n, carry):
            cols = pl.ds(mo(n * NK, NK), NK)
            DV[t, :, cols] = (dact(GV0, t, n) * SV[t, :, :, cols].reshape(T2, NK)).astype(BF16)
            return carry
        loop(RING, body, None)

    def down_part(act, j, lo, tiles):
        t = lax.rem(x + j, RING)

        def body(n, carry):
            cols = pl.ds(mo((lo + n) * ND, ND), ND)
            PP[j, :, :, cols] = dot_nn(act[t, :, :, 0:K].reshape(T2, K), W[:, :, :, cols].reshape(K, ND)).reshape(2, TB, ND)
            return carry
        loop(tiles, body, None)

    def dx_part(j, lo, tiles):
        t = lax.rem(x + j, RING)

        def body(n, carry):
            cols = pl.ds(mo((lo + n) * ND, ND), ND)
            PP[j, :, :, cols] = dot_nt(DV[t], U[lo + n].reshape(ND, K)).reshape(2, TB, ND)
            return carry
        loop(tiles, body, None)

    class Reduce8:
        def __init__(self, part, index, split, old=()):
            self.part, self.index, self.split = part, index, split
            keys.extend(old)
            _, right, left = rings["x"]
            self.right, self.left = right, left
            self.pair, self.m, self.first = [], [], []
            for q in range(len(split)):
                cq = self.cols(q)
                first = sorted(fresh("recv") for j in range(RING))
                self.pair.append([self.swap(j, q, first[0]) for j in range(RING)])
                self.first.append(first[0])
                src = lambda j, h: PP.at[j, c, half(h), cq]
                self.m.append([rcopy(src(*PIECES[k]), XR.at[k, :, cq], left if k % 2 else right) for k in range(ARRIVALS)])
            keys.clear()

        def cols(self, q):
            return tile_cols(self.split, q)

        def swap(self, j, q, first):
            cq = self.cols(q)
            return remote(PP.at[j, cp, :, cq], DR.at[j, :, cq], ps.at[q * RING + j], rs.at[first + j], partner)

        def compute(self, j, q):
            self.part(j, sum(self.split[:q]), self.split[q])
            self.pair[q][j].start()

        def compute_all(self, q):
            def body(i, carry):
                j = lax.rem(i + 1, RING)
                self.part(j, sum(self.split[:q]), self.split[q])
                self.swap(j, q, self.first[q]).start()
                return carry
            loop(RING, body, None)

        def combine(self, j, q):
            self.pair[q][j].wait_recv()
            add_rows(PP.at[j, c, :, self.cols(q)], [DR.at[j, :, self.cols(q)]], TB, min(TB, 16))

        def opposite(self, q):
            self.m[q][0].start()
            self.m[q][1].start()

        def side(self, j, q):
            self.combine(j, q)
            self.m[q][2 if j == NXT else 3].start()

        def send(self, q):
            self.combine(OPP, q)
            self.opposite(q)
            self.side(NXT, q)
            self.side(PRV, q)

        def relay(self, q):
            for k, j, h in ((0, NXT, 0), (1, PRV, 1)):
                self.m[q][k].wait_recv()
                add_rows(PP.at[j, c, half(h), self.cols(q)], [XR.at[k, :, self.cols(q)]], HB, min(HB, 16))
                self.m[q][4 + k].start()

        def finish(self, q, res, outs):
            for d in self.m[q][2:]:
                d.wait_recv()
            step, cq = min(HB, 16), self.cols(q)
            for h, (kl, kr) in enumerate(((4, 3), (2, 5))):
                def body(r, carry):
                    lo = pl.ds(mo(r * step, step), step)
                    sl = pl.ds(mo(h * HB + r * step, step), step)
                    tot = PP[OWN, c, sl, cq] + (XR[kl, lo, cq] + XR[kr, lo, cq])
                    val = (res[sl, cq].astype(F32) + tot).astype(BF16)
                    for o in outs:
                        o[sl, cq] = val
                    return carry
                loop(HB // step, body, None)

        def drain(self):
            for d in sum(self.pair + self.m, []):
                d.wait_send()

        def release(self):
            self.drain()
            for k, to in enumerate((self.right, self.left, partner)):
                pl.semaphore_signal(credit.at[k], inc=1, device_id=to, device_id_type=MESH_ID)

        def acquire(self):
            for k in range(len((self.right, self.left, partner))):
                pl.semaphore_wait(credit.at[k], 1)

    def grad_a(j, dst, halves=None, q=None):
        t = off(z, j)

        def rows(h, carry):
            lo = [pl.ds(mo((2 * h + q) * XD + t * ZD, ZD), ZD) for q in HALVES]
            lhs = jnp.concatenate([XV[:, :, :, s].reshape(8 * TB, ZD) for s in lo], axis=1)

            cols, width = (pl.ds(0, K), K) if q is None else (pl.ds(q * ND, ND), ND)
            dst[h, :, :, cols] = dot_tn(lhs, DV[:, :, cols].reshape(8 * TB, width)).reshape(2, ZD, width)
            return carry
        if halves is None:
            loop(2, rows, None)
        else:
            for h in halves:
                rows(h, None)

    def grad_b_first(chips, add):
        cols_l, cols = pl.ds(mo(off(y, OPP) * NK, NK), NK), pl.ds(0, K)
        dst = GPB.at[OPP]
        for t in chips:
            out = dot_tn(AV[t, :, :, cols_l].reshape(T2, NK), GV1[t, :, :, cols].reshape(T2, K)).reshape(2, NK // 2, K)
            dst[:, 0] = dst[:, 0] + out if add else out
            add = True

    def grad_b(gv, j, dst, n=None):
        cols_l = pl.ds(mo(off(y, j) * NK, NK), NK)

        def body(n, carry):
            out = dot_tn(AV[:, :, :, cols_l].reshape(8 * TB, NK), gv[:, :, :, pl.ds(mo(n * K, K), K)].reshape(8 * TB, K))
            dst[:, n] = out.reshape(2, NK // 2, K)
            return carry
        if n is None:
            loop(2, body, None)
        else:
            body(n, None)

    grad_keys = [keys_of(sum(u0u, u0a) + d0a), [d.key for d in ex0 + ex1 + gg1.own + gg1.push] + keys_of(d0b + d0c + [gg1.ring])]

    def grad_key(l):
        return grad_keys[l].pop() if grad_keys[l] else fresh("recv")

    class Reduce4:
        def __init__(self, l, axis, part, recv, stage):
            _, right, left = rings[axis]
            self.part, self.recv, self.stage = part, recv, stage
            self.m = [rcopy(part(*PIECES[k]), recv(k), left if k % 2 else right, grad_key(l))
                      for k in range(ARRIVALS)]
            self.loads = [lcopy(recv(k), stage(k)) for k in range(ARRIVALS)] if stage else None

        def opposite(self):
            self.m[0].start()
            self.m[1].start()

        def sides(self, j):
            self.m[2 if j == NXT else 3].start()

        def fetch(self, k):
            self.m[k].wait_send()
            self.m[k].wait_recv()
            if self.loads:
                self.loads[k].start()

        def absorb(self, k):
            if self.loads:
                self.loads[k].wait()
            dst = self.part(*TARGETS[k])
            add_rows(dst, [(self.stage or self.recv)(k)], dst.shape[1], min(dst.shape[1], 16))

    def arrive(reduces, ks):
        for k in ks:
            for r in reduces:
                r.fetch(k)
        for k in ks:
            for r in reduces:
                r.absorb(k)

    def relay(reduces):
        for k in (0, 1):
            for r in reduces:
                r.fetch(k)
        for k in (0, 1):
            for r in reduces:
                r.absorb(k)
                r.m[4 + k].start()

    hq = DR_ROWS // 2
    own_grads = [(SV.at[pl.ds(0, 2)], SV.at[pl.ds(2, 2)]), (GPA.at[OWN], GPB.at[OWN])]

    def third(k, rows):
        return pl.ds((k // 2) * rows, rows)

    def reduce_a(l, q, chunks):
        own = own_grads[l][0]
        ca = pl.ds(q * (K // chunks), K // chunks)

        def part(j, h):
            return (own if j == OWN else GPA.at[j]).at[h, :, :, ca]

        def part2(j, h):
            return own.at[h, :, pl.ds(mo(off(y, j) * 2 * UR, 2 * UR), 2 * UR), ca]
        if l < q:
            second = lambda k: GPA.at[OWN, k % 2, :, third(k, 2 * UR), ca], None
        else:
            second = lambda k: ra2.at[l, k, :, :, ca], lambda k: STA.at[k % 2, :, :, ca]
        return (Reduce4(l, "z", part, lambda k: ra1.at[l, k, :, :, ca], lambda k: part(*PIECES[k])),
                Reduce4(l, "y", part2, *second))

    def reduce_b(l, q):
        own, nb = own_grads[l][1], pl.ds(q, 1)

        def part(j, h):
            return (own if j == OWN else GPB.at[j]).at[h, nb]

        def part2(j, h):
            t = off(z, j)
            return own.at[t // 2, nb, pl.ds(mo(lax.rem(t, 2) * DR_ROWS + h * hq, hq), hq), :]
        if l < q:
            second = lambda k: GPB.at[OWN, k % 2, nb, third(k, hq), :], None
        else:
            second = lambda k: rb2.at[l, k, nb], lambda k: STB.at[k % 2, nb]
        return (Reduce4(l, "y", part, lambda k: rb1.at[l, k, nb], lambda k: part(*PIECES[k])),
                Reduce4(l, "z", part2, *second))

    def sides(reduces, j):
        for r in reduces:
            r.sides(j)

    def second_start(reduces):
        for r in reduces:
            r.opposite()
            r.sides(NXT)
            r.sides(PRV)

    def up_out(l, q, chunks):
        own = own_grads[l][0]
        ca = pl.ds(q * (K // chunks), K // chunks)

        def rows_of(tx, tc):
            return own.at[tx // 2, lax.rem(tx, 2), pl.ds(mo((2 * y + tc) * UR, UR), UR), ca]
        to = uh.at[l, x, mine, ca]
        sends = [rcopy(rows_of(off(x, dx), cp if dc else c), to, dev(dx=dx, dc=dc), grad_key(l)) for dx, dc in group]
        local = [lcopy(rows_of(x, c), to)]
        for cpy in sends + local:
            cpy.start()
        return sends, local

    def down_out(l, n):
        cpy = lcopy(own_grads[l][1].at[z // 2, n, pl.ds(mo(lax.rem(z, 2) * DR_ROWS, DR_ROWS), DR_ROWS), :],
                    gd_out.at[l, :, pl.ds(n * K, K)])
        cpy.start()
        return [], [cpy]

    def grads_out_finish(state):
        for cpy in state[0]:
            cpy.wait_recv()
            cpy.wait_send()
        for cpy in state[1]:
            cpy.wait()

    r = Reduce8(functools.partial(down_part, AV), 0, SPLIT3)
    r_keys = sorted([d.key for m in r.m for d in m] + [f + j for f in r.first for j in range(RING)])
    hidden0(off(x, OPP))
    hidden0(off(x, NXT))
    do(d0b, "finish")
    r.compute(OPP, 0)
    r.compute(NXT, 0)
    do(d0c, "forward")
    do(d0d, "start")
    r.combine(OPP, 0)
    r.opposite(0)
    do(u0u[2] + u0u[3], "drain")
    hidden0(off(x, PRV))
    r.compute(PRV, 0)
    r.side(NXT, 0)
    do(d1a, "forward")
    hidden0(off(x, OWN))
    r.side(PRV, 0)
    save_s = lcopy(SV, sh0)
    save_s.start()
    save_a0 = lcopy(AV, ah.at[0])
    save_a0.start()
    gg1.sides()
    do(d0c, "finish")
    r.compute_all(1)
    r.relay(0)
    do(d0d, "forward")
    for cpy in ex1:
        cpy.wait_recv()
    own_d1.wait()
    do(u1a, "start")
    r.send(1)
    do(d1a, "finish")
    do(d1b, "start")
    gg1.last()
    save_x.wait()
    do(d0d, "finish")
    do(d0b + d0c, "drain")
    save_d0 = lcopy(W, wdh.at[0])
    save_d0.start()
    r.compute(OPP, 2)
    r.relay(1)
    save_u0.wait()
    do(u1a, "forward")
    r.compute(NXT, 2)
    r.combine(OPP, 2)
    r.opposite(2)
    r.compute(PRV, 2)
    r.side(NXT, 2)
    r.compute(OWN, 2)
    r.side(PRV, 2)
    r.compute(OWN, 0)
    for q in range(len(SPLIT3)):
        r.combine(OWN, q)

    def gather_keys(gathers):
        return [d.key for g in gathers for d in g.ring.d + g.own + g.push]

    def token_gathers(slot, buf):
        def make(q):
            cq = tile_cols(SPLIT2, q)
            return Gather8(lambda h: RES.at[slot, half(h), cq], lambda b, k, h: buf.at[b, k, half(h), cq])
        return [make(0), make(1)]

    keys.extend(gather_keys((gx0,)))
    gx1 = token_gathers(X1, XV)
    do(d1a, "drain")
    do(d1b, "forward")
    for q in HALVES:
        r.finish(q, RES.at[X0], [RES.at[X1], XV.at[x, c]])
    r.relay(2)
    gx1[0].start()
    do(u1a, "finish")
    do(u1b, "start")
    do(u1c, "start_first")
    pair, rest = pl.ds(0, 2), pl.ds(2, 2)
    own_up = [lcopy(up[1].at[pair, z], U.at[pair, z]), lcopy(up[1].at[rest, :, y], U.at[rest, :, y])]
    for cpy in own_up:
        cpy.start()
    gg1.wait_own()
    gg1.wait_push(range(len(gg1.push)))
    own_g.wait()
    save_d0.wait()
    do(d0d + u1a, "drain")
    gg1.drain()
    do(d1b, "finish")
    load_w1d = lcopy(wdh.at[1], W)
    load_w1d.start()
    r.finish(2, RES.at[X0], [RES.at[X1], XV.at[x, c]])
    gx1[1].start()
    save_s.wait()
    do(u1b, "forward")
    do(u1c, "start_rest")
    load_w1d.wait()
    dact1(off(x, OWN))
    gx1[0].forward()
    r.release()
    dact1(off(x, NXT))
    gx1[0].sides()
    dact1(off(x, PRV))
    do(u1c, "forward")
    do(u1b, "finish")
    dact1(off(x, OPP))
    load_w0d_again = lcopy(wdh.at[0], W)
    load_w0d_again.start()
    save_a0.wait()
    do(gx1, "wait_own")
    for cpy in own_up:
        cpy.wait()
    hidden1(off(x, OWN), 0)
    do(gx1[1:], "forward")
    do(gx1[1:], "sides")
    for j in (PRV, NXT):
        for g in gx1:
            g.wait_push(PUSHES[j])
        hidden1(off(x, j), 0)
    gx1[0].last()
    do(u1c, "finish")
    hidden1(off(x, OWN), 1)
    hidden1(off(x, PRV), 1)
    gx1[1].last()
    hidden1(off(x, NXT), 1)
    grad_b_first([off(x, j) for j in (OWN, PRV, NXT)], False)
    for g in gx1:
        g.wait_push(PUSHES[OPP])
    hidden1_tile(off(x, OPP), off(y, OPP))

    (a1, a2), (b1, b2) = zip(*[reduce_a(1, q, 2) for q in HALVES]), zip(*[reduce_b(1, q) for q in HALVES])
    first1, second1 = b1 + a1, b2 + a2
    grad_b_first([off(x, OPP)], True)
    b1[0].opposite()
    for n in (PRV, OWN, NXT):
        hidden1_tile(off(x, OPP), off(y, n))
    for q in HALVES:
        for h in HALVES:
            grad_a(OPP, GPA.at[OPP], (h,), q)
            a1[q].m[h].start()
    load_s0 = lcopy(sh0, SV)
    load_s0.start()
    save_a1 = lcopy(AV, ah.at[1])
    save_a1.start()
    grad_b(GV1, OPP, GPB.at[OPP], 1)
    b1[1].opposite()
    r = Reduce8(dx_part, 1, SPLIT2, r_keys)
    r.acquire()
    r.compute(OPP, 0)
    r.compute(NXT, 0)
    r.combine(OPP, 0)
    r.opposite(0)
    r.compute(PRV, 0)
    r.side(NXT, 0)
    r.side(PRV, 0)
    r.compute_all(1)
    load_w0u_again = lcopy(wuh.at[0], U)
    r.compute(OWN, 0)
    do(u1b + u1c, "drain")
    load_w0u_again.start()
    grad_b(GV1, NXT, GPB.at[NXT])
    sides(b1, NXT)
    grad_b(GV1, PRV, GPB.at[PRV])
    sides(b1, PRV)
    r.relay(0)
    r.send(1)
    grad_a(NXT, GPA.at[NXT])
    sides(a1, NXT)
    grad_a(PRV, GPA.at[PRV])
    sides(a1, PRV)
    r.combine(OWN, 0)
    r.combine(OWN, 1)
    keys.extend(gather_keys(gx1))
    gg0 = token_gathers(G0, GV0)
    r.relay(1)
    r.finish(0, RES.at[G1], [RES.at[G0], GV0.at[x, c]])
    gg0[0].start()
    relay(first1)
    grad_b(GV1, OWN, GPB.at[OWN])
    save_a1.wait()
    load_a0 = lcopy(ah.at[0], AV)
    load_a0.start()
    do(d1b, "drain")
    load_a1 = lcopy(ah.at[1], GV1.at[:, :, :, 0:K])
    load_a1.start()
    r.finish(1, RES.at[G1], [RES.at[G0], GV0.at[x, c]])
    gg0[1].start()
    gg0[0].forward()
    grad_a(OWN, GPA.at[OWN])
    do(gx1, "drain")
    load_x0 = lcopy(xh0, XV)
    load_x0.start()
    gg0[0].sides()
    r.release()
    gg0[1].forward()
    gg0[0].last()
    load_w0d_again.wait()
    load_s0.wait()
    do(gg0, "wait_own")
    dact0(off(x, OWN))
    gg0[1].sides()
    gg0[1].last()
    for g in gg0:
        g.wait_push(PUSHES[PRV])
    dact0(off(x, PRV))
    for g in gg0:
        g.wait_push(PUSHES[NXT])
    dact0(off(x, NXT))
    for g in gg0:
        g.wait_push(PUSHES[OPP])

    (a1n, a2n), (b1n, b2n) = zip(*[reduce_a(0, q, 2) for q in HALVES]), zip(*[reduce_b(0, q) for q in HALVES])
    load_a0.wait()
    grad_b(GV0, OPP, GPB.at[OPP])
    b1n[0].opposite()
    dact0(off(x, OPP))
    load_w1d_again = lcopy(wdh.at[1], W)
    load_w1d_again.start()
    load_x0.wait()
    for h in HALVES:
        grad_a(OPP, GPA.at[OPP], (h,))
        a1n[0].m[h].start()
    arrive(first1, EARLY + LATE)
    second_start(second1)
    load_w0u_again.wait()
    r = Reduce8(dx_part, 2, WHOLE, r_keys)
    r.acquire()
    r.compute_all(0)
    r.send(0)
    grad_b(GV0, NXT, GPB.at[NXT])
    b1n[0].sides(NXT)
    grad_b(GV0, PRV, GPB.at[PRV])
    b1n[0].sides(PRV)
    grad_a(NXT, GPA.at[NXT])
    a1n[0].sides(NXT)
    grad_a(PRV, GPA.at[PRV])
    a1n[0].sides(PRV)
    relay(second1)
    r.relay(0)
    relay((b1n[0], a1n[0]))
    for red in (b1n[1], a1n[1]):
        red.opposite()
        red.sides(NXT)
        red.sides(PRV)
    r.combine(OWN, 0)
    grad_b(GV0, OWN, own_grads[0][1])
    grad_a(OWN, own_grads[0][0])
    r.finish(0, RES.at[G0], [RES.at[X0]])
    r.release()
    write_gi = lcopy(RES.at[X0], gi_out)
    write_gi.start()
    arrive((b1n[0], a1n[0]), EARLY)
    arrive(second1, EARLY)
    arrive(second1, LATE)
    state1 = [up_out(1, q, 2) for q in HALVES] + [down_out(1, n) for n in HALVES]
    load_a1.wait()
    load_w1d_again.wait()
    r = Reduce8(functools.partial(down_part, GV1), 3, WHOLE, r_keys)
    r.acquire()
    r.compute_all(0)
    r.send(0)
    r.combine(OWN, 0)
    arrive((b1n[0], a1n[0]), LATE)
    for state in state1:
        grads_out_finish(state)
    relay((b1n[1], a1n[1]))
    second_start((a2n[0], b2n[0]))
    r.relay(0)
    arrive((b1n[1], a1n[1]), EARLY)

    def start(red):
        red.opposite()
        sides((red,), NXT)
        sides((red,), PRV)
    arrive((b1n[1],), LATE)
    relay((a2n[0],))
    arrive((a1n[1],), LATE)
    start(a2n[1])
    start(b2n[1])
    arrive((a2n[0],), EARLY)
    relay((b2n[0],))
    arrive((a2n[0],), LATE)
    state0 = [up_out(0, 0, 2)]
    relay((a2n[1],))
    arrive((b2n[0],), EARLY)
    relay((b2n[1],))
    arrive((a2n[1],), EARLY)
    arrive((a2n[1],), LATE)
    state0.append(up_out(0, 1, 2))
    arrive((b2n[1],), EARLY)
    for q in HALVES:
        arrive((b2n[q],), LATE)
        state0.append(down_out(0, q))
    r.finish(0, RES.at[X1], [RES.at[G1]])
    write_y = lcopy(RES.at[G1], y_out)
    write_y.start()
    r.drain()
    do(gg0, "drain")
    write_gi.wait()
    write_y.wait()
    for state in state0:
        grads_out_finish(state)
    assert used["recv"] <= N_RECV and used["send"] <= N_SEND and used["local"] <= N_LOCAL


def finish_kernel(y_in, gi_in, gu_in, gd_in, y_out, gi_out, gu_out, gd_out, ybuf, gibuf, gubuf, gdbuf, gushuf, sems):
    layers, ur, ff = gu_out.shape
    s2 = ff // 64
    half = s2 // 2
    pairs = [((gu_in.at[l], gubuf.at[l]), (gushuf.at[l], gu_out.at[l])) for l in range(layers)]
    pairs += [((a, b), (b, o)) for a, b, o in ((gd_in, gdbuf, gd_out), (y_in, ybuf, y_out), (gi_in, gibuf, gi_out))]
    loads = [pltpu.make_async_copy(*p, sems.at[0, k]) for k, (p, _) in enumerate(pairs)]
    stores = [pltpu.make_async_copy(*p, sems.at[1, k]) for k, (_, p) in enumerate(pairs)]
    for cpy in loads:
        cpy.start()
    low = lax.broadcasted_iota(jnp.int32, (ur, s2), 1) < half
    swap = lambda v: pltpu.roll(v, half, 1)
    for l, (load, store) in enumerate(zip(loads, stores)):
        load.wait()
        for b in range(RING if l < layers else 0):
            for yy in range(RING):
                for m in HALVES:
                    cols = pl.ds((yy * 2 + m) * s2, s2)
                    t0, t1 = (gubuf[l, b, pl.ds(k * ur, ur), cols] for k in HALVES)
                    strip = (b * RING + 2 * m) * RING + yy
                    gushuf[l, :, pl.ds(strip * s2, s2)] = jnp.where(low, t0, swap(t1))
                    gushuf[l, :, pl.ds((strip + RING) * s2, s2)] = jnp.where(low, swap(t0), t1)
        store.start()
    for cpy in stores:
        cpy.wait()


def solution(mesh, interpret=None):
    fine = Mesh(np.asarray(mesh.devices).reshape(4, 4, 4, 2), ALL)
    tok_spec = P(ALL, None)
    weight_spec = P(None, ALL, None)

    def device_step(x_loc, up_loc, down_loc, g_loc):
        layers, ur, ff = up_loc.shape
        dr, dm = down_loc.shape[1:]
        tb = x_loc.shape[0]
        k = ff // 8
        zd = dm // 16
        hbm = lambda shape, dt: jax.ShapeDtypeStruct(shape, dt)
        outs = [
            hbm((tb, dm), BF16), hbm((tb, dm), BF16), hbm((layers, dr, dm), F32),
            hbm((RING, CORES, tb, dm), BF16),
            hbm((layers, RING, RING, RING, 2 * ur, k), BF16),
            hbm((layers, RING, RING, dr, dm), BF16),
            hbm((RING, CORES, tb, k), F32), hbm((layers, RING, CORES, tb, k), BF16),
            *[hbm((layers, ARRIVALS, CORES, n, k), F32) for n in (zd, zd, 2 * ur, 2 * ur)],
            hbm((layers, RING, 2 * ur, k), F32),
        ]
        vm = pltpu.VMEM
        scratch = [
            vm((RING, RING, RING, 2 * ur, k), BF16), vm((RING, RING, dr, dm), BF16),
            vm((RING, CORES, tb, dm), BF16), vm((RING, CORES, tb, dm), BF16), vm((RING, CORES, tb, dm), BF16),
            vm((RING, CORES, tb, k), F32), vm((RING, CORES, tb, k), BF16), vm((RING, 2 * tb, k), BF16),
            vm((RING, CORES, CORES, zd, k), F32), vm((RING, CORES, CORES, zd, k), F32),
            vm((RING, CORES, tb, dm), F32), vm((4, tb, dm), F32), vm((6, tb // 2, dm), F32),
            vm((4, tb, dm), BF16), vm((CORES, CORES, 2 * ur, k), F32), vm((CORES, CORES, 2 * ur, k), F32),
            *[pltpu.SemaphoreType.DMA((n,)) for n in (N_SEND, N_RECV, N_LOCAL, len(SPLIT3) * RING)],
            pltpu.SemaphoreType.REGULAR((3,)),
        ]
        anyspec = pl.BlockSpec(memory_space=pl.ANY)
        call = pl.pallas_call(
            functools.partial(kernel, (dm, k, tb, ur, dr)),
            out_shape=outs,
            in_specs=[anyspec] * 4,
            out_specs=[anyspec] * len(outs),
            scratch_shapes=scratch,
            compiler_params=pltpu.CompilerParams(collective_id=0, has_side_effects=True, vmem_limit_bytes=67043328),
            name="mlp_stack",
            **({"interpret": interpret} if interpret else {}),
        )
        y_raw, gi_raw, gd_raw, *_, gu_raw = call(x_loc, up_loc, down_loc, g_loc)
        raws = (y_raw, gi_raw, gu_raw, gd_raw)
        outs = [hbm((tb, dm), BF16), hbm((tb, dm), BF16), hbm((layers, ur, ff), F32), hbm((layers, dr, dm), F32)]
        return tuple(pl.pallas_call(
            finish_kernel, out_shape=outs, in_specs=[anyspec] * len(outs), out_specs=[anyspec] * len(outs),
            scratch_shapes=[vm(v.shape, v.dtype) for v in raws] + [vm(outs[2].shape, F32), pltpu.SemaphoreType.DMA((2, layers + len(outs)))],
            name="write_out")(*raws))

    return jax.shard_map(device_step, mesh=fine, in_specs=(tok_spec, weight_spec, weight_spec, tok_spec),
                         out_specs=(tok_spec, tok_spec, weight_spec, weight_spec), check_vma=False)
```

```python
import functools

import jax
import jax.numpy as jnp
import numpy as np
from jax import lax
from jax.experimental import pallas as pl
from jax.experimental.pallas import tpu as pltpu
from jax.sharding import Mesh, PartitionSpec as P

MESH_ID = pl.DeviceIdType.MESH
ALL = ("x", "z", "y", "c")
F32, BF16 = jnp.float32, jnp.bfloat16
RING, CORES, ARRIVALS = 4, 2, 6
OWN, NXT, OPP, PRV = range(RING)
X0, X1, G1, G0 = range(RING)
HALVES = (0, 1)
WHOLE, SPLIT2, SPLIT3 = (4,), (2, 2), (1, 1, 2)
PIECES = ((OPP, 0), (OPP, 1), (NXT, 1), (PRV, 0), (NXT, 0), (PRV, 1))
TARGETS = ((NXT, 0), (PRV, 1), (OWN, 1), (OWN, 0), (OWN, 0), (OWN, 1))
EARLY, LATE = (2, 3), (4, 5)
PUSHES = {PRV: (0, 2), NXT: (1, 3), OPP: (4, 5)}
N_RECV, N_SEND, N_LOCAL = 192, 102, 19


def gelu_parts(pre_act):
    norm_cdf = 0.5 * (1.0 + lax.erf(pre_act * (2.0 ** -0.5)))
    norm_pdf = jnp.exp(-0.5 * pre_act * pre_act) * ((2.0 * jnp.pi) ** -0.5)
    return pre_act * norm_cdf, norm_cdf + pre_act * norm_pdf


def loop(n, body, init):
    return lax.fori_loop(0, n, body, init)


def dot_nn(left, right):
    return lax.dot_general(left, right, (((1,), (0,)), ((), ())), preferred_element_type=F32)


def dot_nt(left, right):
    return lax.dot_general(left, right, (((1,), (1,)), ((), ())), preferred_element_type=F32)


def dot_tn(left, right):
    return lax.dot_general(left, right, (((0,), (0,)), ((), ())), preferred_element_type=F32)


def kernel(dims, x_in, wu_in, wd_in, g_in,
           y_out, gi_out, gd_out,
           xh0, wuh, wdh, sh0, ah, ra1, rb1, ra2, rb2, uh,
           U, W, XV, GV1, GV0, SV, AV, DV, GPA, GPB, PP, DR, XR, RES, STA, STB,
           ss, rs, ls, ps, credit):
    D, K, TB, UR, DR_ROWS = dims
    HB = TB // 2
    x, z, y, c = (lax.axis_index(a) for a in ALL)
    cp = 1 - c
    S2 = 2 * DR_ROWS
    XD = D // 4
    ZD = D // 16

    def dev(dx=0, dz=0, dy=0, dc=0):
        wrap = lambda v, d, n: v if d == 0 else lax.rem(v + (d % n), n)
        return (wrap(x, dx, 4), wrap(z, dz, 4), wrap(y, dy, 4), wrap(c, dc, 2))

    partner = dev(dc=1)
    rings = {"x": (x, dev(dx=1), dev(dx=-1)), "z": (z, dev(dz=1), dev(dz=-1)), "y": (y, dev(dy=1), dev(dy=-1))}
    off = lambda v, d: v if d == 0 else lax.rem(v + d, 4)

    used = {"recv": 0, "send": 0, "local": 0}
    free = {"send": [], "local": []}
    keys = []

    def fresh(kind):
        if kind == "recv" and keys:
            return keys.pop()
        used[kind] += 1
        return used[kind] - 1

    def take(kind):
        return free[kind].pop() if free[kind] else fresh(kind)

    def remote(src, dst, send, recv, to):
        return pltpu.make_async_remote_copy(src_ref=src, dst_ref=dst, send_sem=send, recv_sem=recv,
                                            device_id=to, device_id_type=MESH_ID)

    class rcopy:
        def __init__(self, src, dst, to, key=None):
            self.args, self.key = (src, dst, to), fresh("recv") if key is None else key

        def start(self):
            src, dst, to = self.args
            self.sem = take("send")
            self.d = remote(src, dst, ss.at[self.sem], rs.at[self.key], to)
            self.d.start()

        def wait_recv(self):
            self.d.wait_recv()

        def wait_send(self):
            self.d.wait_send()
            free["send"].append(self.sem)

    class lcopy:
        def __init__(self, src, dst):
            self.args = src, dst

        def start(self):
            self.sem = take("local")
            self.d = pltpu.make_async_copy(*self.args, ls.at[self.sem])
            self.d.start()

        def wait(self):
            self.d.wait()
            free["local"].append(self.sem)

    def mo(v, m):
        return pl.multiple_of(v, m)

    class Gather4:
        def __init__(self, axis, src, dst):
            i, right, left = rings[axis]
            lft, rgt = off(i, 3), off(i, 1)
            self.d = [rcopy(src(0), dst(i, 0), right), rcopy(src(1), dst(i, 1), right),
                      rcopy(src(0), dst(i, 0), left), rcopy(src(1), dst(i, 1), left),
                      rcopy(dst(lft, 0), dst(lft, 0), right), rcopy(dst(rgt, 1), dst(rgt, 1), left)]

        def start_first(self):
            self.d[0].start()
            self.d[3].start()

        def start_rest(self):
            self.d[1].start()
            self.d[2].start()

        def start(self):
            self.start_first()
            self.start_rest()

        def forward(self):
            for k in HALVES:
                self.d[3 * k].wait_recv()
                self.d[4 + k].start()

        def neighbours(self):
            self.d[1].wait_recv()
            self.d[2].wait_recv()

        def opposite(self):
            self.d[4].wait_recv()
            self.d[5].wait_recv()

        def finish(self):
            self.neighbours()
            self.opposite()

        def drain(self):
            for d in self.d:
                d.wait_send()

    class Gather8:
        def __init__(self, src, dst):
            self.ring = Gather4("x", src, lambda b, h: dst(b, c, h))
            lft, rgt, opp = off(x, PRV), off(x, NXT), off(x, OPP)
            blocks = [(lft, 0), (rgt, 1), (lft, 1), (rgt, 0), (opp, 0), (opp, 1)]
            self.own = [rcopy(src(h), dst(x, c, h), partner) for h in HALVES]
            self.push = [rcopy(dst(b, c, h), dst(b, c, h), partner) for b, h in blocks]

        def start(self):
            self.ring.start()
            for d in self.own:
                d.start()

        def forward(self):
            self.ring.forward()
            self.push[0].start()
            self.push[1].start()

        def sides(self):
            self.ring.d[1].wait_recv()
            self.push[2].start()
            self.ring.d[2].wait_recv()
            self.push[3].start()

        def last(self):
            self.ring.d[4].wait_recv()
            self.push[4].start()
            self.ring.d[5].wait_recv()
            self.push[5].start()

        def wait_own(self):
            for d in self.own:
                d.wait_recv()

        def wait_push(self, ks):
            for k in ks:
                self.push[k].wait_recv()

        def drain(self):
            self.ring.drain()
            for d in self.own + self.push:
                d.wait_send()

    def add_rows(dst, srcs, rows, step):
        def body(r, carry):
            sl = pl.ds(mo(r * step, step), step)
            if len(dst.shape) == 3:
                for q in range(dst.shape[0]):
                    acc = dst[q, sl, :]
                    for s in srcs:
                        acc = acc + s[q, sl, :]
                    dst[q, sl, :] = acc
            else:
                acc = dst[sl, :]
                for s in srcs:
                    acc = acc + s[sl, :]
                dst[sl, :] = acc
            return carry
        loop(rows // step, body, None)

    barrier = pltpu.get_barrier_semaphore()
    group = [(dx, dc) for dx in (OPP, NXT, PRV, OWN) for dc in HALVES if dx or dc]
    peers = [dev(dx=dx, dc=dc) for dx, dc in group] + [rings[a][k] for a in "zy" for k in (1, 2)]
    for p in peers:
        pl.semaphore_signal(barrier, inc=1, device_id=p, device_id_type=MESH_ID)

    load_u = [[lcopy(wu_in.at[l, :, pl.ds(b * D, D)], RES.at[G0, pl.ds((l * RING + b) * UR, UR), :])
               for b in range(RING)] for l in HALVES]
    load_d = [lcopy(wd_in.at[l], RES.at[X1, pl.ds(l * DR_ROWS, DR_ROWS), :]) for l in HALVES]
    load_x = lcopy(x_in, RES.at[X0])
    load_g = lcopy(g_in, RES.at[G1])
    own_x = lcopy(x_in, XV.at[x, c])
    own_g = lcopy(g_in, GV1.at[x, c])
    own_d0 = lcopy(wd_in.at[0], W.at[y, z])
    for cpy in load_u[0] + load_u[1] + load_d + [load_x, own_d0, own_x, load_g, own_g]:
        cpy.start()

    low = lax.broadcasted_iota(jnp.int32, (UR, S2), 1) < DR_ROWS
    swap = lambda v: pltpu.roll(v, DR_ROWS, 1)
    for l in HALVES:
        for cpy in load_u[l]:
            cpy.wait()
        for b in range(RING):
            rows = pl.ds((l * RING + b) * UR, UR)
            for yy in range(RING):
                for m in HALVES:
                    s0 = RES[G0, rows, pl.ds((2 * m * RING + yy) * S2, S2)].astype(F32)
                    s1 = RES[G0, rows, pl.ds(((2 * m + 1) * RING + yy) * S2, S2)].astype(F32)
                    cols = pl.ds((yy * 2 + m) * S2, S2)
                    AV[l, 0, pl.ds(2 * b * UR, UR), cols] = jnp.where(low, s0, swap(s1)).astype(BF16)
                    AV[l, 0, pl.ds((2 * b + 1) * UR, UR), cols] = jnp.where(low, swap(s0), s1).astype(BF16)
    for cpy in load_d + [load_x, own_d0]:
        cpy.wait()
    pl.semaphore_wait(barrier, len(peers))

    half = lambda h: pl.ds(h * HB, HB)

    def tile_cols(split, q):
        return pl.ds(sum(split[:q]) * (D // RING), split[q] * (D // RING))

    gx0 = Gather8(lambda h: RES.at[X0, half(h)], lambda b, k, h: XV.at[b, k, half(h)])
    gg1 = Gather8(lambda h: RES.at[G1, half(h)], lambda b, k, h: GV1.at[b, k, half(h)])
    up = [U, wuh.at[1]]
    down = [W, wdh.at[1]]
    hr = DR_ROWS // 4

    def quarter(q, h):
        return pl.ds((2 * q + h) * hr, hr)

    def down_first(l):
        to = down[l]
        src = lambda q: lambda h: RES.at[X1, pl.ds(l * DR_ROWS + (2 * q + h) * hr, hr)]
        return [Gather4("z", src(0), lambda b, h: to.at[y, b, quarter(0, h)]),
                Gather4("y", src(1), lambda b, h: to.at[b, z, quarter(1, h)])]

    def down_second(l, split, n):
        to, cs = down[l], tile_cols(split, n)
        return [Gather4("y", lambda h: to.at[y, :, quarter(0, h), cs], lambda b, h: to.at[b, :, quarter(0, h), cs]),
                Gather4("z", lambda h: to.at[:, z, quarter(1, h), cs], lambda b, h: to.at[:, b, quarter(1, h), cs])]

    def up_first(to):
        return [Gather4("y", lambda h: to.at[h, z, y], lambda b, h: to.at[h, z, b]),
                Gather4("z", lambda h: to.at[2 + h, z, y], lambda b, h: to.at[2 + h, b, y])]

    def hidden_cols(n):
        return pl.ds(sum(SPLIT2[:n]) * (K // RING), SPLIT2[n] * (K // RING))

    def up_second(n):
        cs, src = hidden_cols(n), up[1]
        return [Gather4("z", lambda h: src.at[h, z, :, :, cs], lambda b, h: U.at[h, b, :, :, cs]),
                Gather4("y", lambda h: src.at[2 + h, :, y, :, cs], lambda b, h: U.at[2 + h, :, b, :, cs])]

    def up_unit(to, j):
        yj, zj = off(y, j), off(z, j)
        return [Gather4("z", lambda h: to.at[h, z, yj], lambda b, h: to.at[h, b, yj]),
                Gather4("y", lambda h: to.at[2 + h, zj, y], lambda b, h: to.at[2 + h, zj, b])]

    def do(gathers, step):
        for g in gathers:
            getattr(g, step)()

    mine = pl.ds(mo(c * UR, UR), UR)

    def up_exchange(l):
        sends = []
        for dx, dc in group:
            tx, tc = off(x, dx), (cp if dc else c)
            src = AV.at[l, 0, pl.ds(mo((tx * 2 + tc) * UR, UR), UR), :]
            sends.append(rcopy(src, up[l].at[x, z, y, mine, :], dev(dx=dx, dc=dc)))
        for cpy in sends:
            cpy.start()
        return sends

    def keys_of(gathers):
        return [d.key for g in gathers for d in g.d]

    d0a, d0b, d0c = down_first(0), down_second(0, SPLIT3, 0), down_second(0, SPLIT3, 1)
    u0a, u0u = up_first(up[0]), [up_unit(up[0], j) for j in (OWN, PRV, NXT, OPP)]
    keys.extend(keys_of(u0a))
    d0d = down_second(0, SPLIT3, 2)
    keys.extend(keys_of(d0a))
    d1a = down_first(1)
    keys.extend(keys_of(sum(u0u, [])))
    d1b, u1a = down_second(1, WHOLE, 0), up_first(up[1])
    u1b, u1c = up_second(0), up_second(1)
    ex0 = up_exchange(0)
    do(d0a, "start")
    gx0.start()
    ex1 = up_exchange(1)
    my_rows = pl.ds(mo((x * 2 + c) * UR, UR), UR)
    own_u1 = lcopy(AV.at[1, 0, my_rows, :], up[1].at[x, z, y, mine, :])
    own_u1.start()
    own_d1 = lcopy(RES.at[X1, pl.ds(DR_ROWS, DR_ROWS), :], down[1].at[y, z])
    own_d1.start()
    U[x, z, y, mine, :] = AV[0, 0, my_rows, :]
    do(d0a, "forward")
    for cpy in ex0:
        cpy.wait_recv()
    do(u0a, "start")
    do(u0u[0], "start")
    do(u0a, "forward")
    gx0.forward()
    load_g.wait()
    gg1.start()
    do(u0a, "neighbours")
    do(u0u[1], "start")
    do(u0u[2], "start")
    do(u0u[0], "forward")
    do(u0a, "opposite")
    do(u0u[3], "start")
    do(d0a, "finish")
    do(d0a + u0a, "drain")
    do(u0u[1], "forward")
    do(u0u[2], "forward")
    do(d0b, "start_first")
    gx0.sides()
    for cpy in ex0 + ex1:
        cpy.wait_send()
    own_u1.wait()
    do(u0u[3], "forward")
    do(u0u[0] + u0u[1], "drain")
    do(d0b, "start_rest")
    do(d0c, "start_first")
    do(d0b, "forward")
    do(d0c, "start_rest")
    do(d1a, "start")
    gg1.forward()
    gx0.last()
    gx0.wait_own()
    gx0.wait_push(range(len(gx0.push)))
    own_x.wait()
    save_x = lcopy(XV, xh0)
    save_x.start()
    for unit in u0u:
        do(unit, "finish")
    save_u0 = lcopy(U, wuh.at[0])
    save_u0.start()

    T2 = 2 * TB
    ND = D // 4
    NK = K // 4

    def up_tile(t, n):
        cols = pl.ds(mo(n * NK, NK), NK)
        return dot_nn(XV[t].reshape(T2, D), U[:, :, :, :, cols].reshape(D, NK)), cols

    def hidden0(t):
        for n in range(RING):
            pre, cols = up_tile(t, n)
            act, slope = gelu_parts(pre)
            AV[t, :, :, cols] = act.astype(BF16).reshape(2, TB, NK)
            SV[t, :, :, cols] = slope.reshape(2, TB, NK)

    def hidden1_tile(t, n):
        pre, cols = up_tile(t, n)
        act, slope = gelu_parts(pre)
        AV[t, :, :, cols] = act.astype(BF16).reshape(2, TB, NK)
        DV[t, :, cols] = (SV[t, :, :, cols].reshape(T2, NK) * slope).astype(BF16)

    def hidden1(t, part):
        for n in range(sum(SPLIT2[:part]), sum(SPLIT2[:part + 1])):
            hidden1_tile(t, n)

    def dact(gv, t, n):
        return dot_nt(gv[t].reshape(T2, D), W[n].reshape(NK, D))

    def dact1(t):
        def body(n, carry):
            SV[t, :, :, pl.ds(mo(n * NK, NK), NK)] = dact(GV1, t, n).reshape(2, TB, NK)
            return carry
        loop(RING, body, None)

    def dact0(t):
        def body(n, carry):
            cols = pl.ds(mo(n * NK, NK), NK)
            DV[t, :, cols] = (dact(GV0, t, n) * SV[t, :, :, cols].reshape(T2, NK)).astype(BF16)
            return carry
        loop(RING, body, None)

    def down_part(act, j, lo, tiles):
        t = lax.rem(x + j, RING)

        def body(n, carry):
            cols = pl.ds(mo((lo + n) * ND, ND), ND)
            PP[j, :, :, cols] = dot_nn(act[t, :, :, 0:K].reshape(T2, K), W[:, :, :, cols].reshape(K, ND)).reshape(2, TB, ND)
            return carry
        loop(tiles, body, None)

    def dx_part(j, lo, tiles):
        t = lax.rem(x + j, RING)

        def body(n, carry):
            cols = pl.ds(mo((lo + n) * ND, ND), ND)
            PP[j, :, :, cols] = dot_nt(DV[t], U[lo + n].reshape(ND, K)).reshape(2, TB, ND)
            return carry
        loop(tiles, body, None)

    class Reduce8:
        def __init__(self, part, index, split, old=()):
            self.part, self.index, self.split = part, index, split
            keys.extend(old)
            _, right, left = rings["x"]
            self.right, self.left = right, left
            self.pair, self.m, self.first = [], [], []
            for q in range(len(split)):
                cq = self.cols(q)
                first = sorted(fresh("recv") for j in range(RING))
                self.pair.append([self.swap(j, q, first[0]) for j in range(RING)])
                self.first.append(first[0])
                src = lambda j, h: PP.at[j, c, half(h), cq]
                self.m.append([rcopy(src(*PIECES[k]), XR.at[k, :, cq], left if k % 2 else right) for k in range(ARRIVALS)])
            keys.clear()

        def cols(self, q):
            return tile_cols(self.split, q)

        def swap(self, j, q, first):
            cq = self.cols(q)
            return remote(PP.at[j, cp, :, cq], DR.at[j, :, cq], ps.at[q * RING + j], rs.at[first + j], partner)

        def compute(self, j, q):
            self.part(j, sum(self.split[:q]), self.split[q])
            self.pair[q][j].start()

        def compute_all(self, q):
            def body(i, carry):
                j = lax.rem(i + 1, RING)
                self.part(j, sum(self.split[:q]), self.split[q])
                self.swap(j, q, self.first[q]).start()
                return carry
            loop(RING, body, None)

        def combine(self, j, q):
            self.pair[q][j].wait_recv()
            add_rows(PP.at[j, c, :, self.cols(q)], [DR.at[j, :, self.cols(q)]], TB, min(TB, 16))

        def opposite(self, q):
            self.m[q][0].start()
            self.m[q][1].start()

        def side(self, j, q):
            self.combine(j, q)
            self.m[q][2 if j == NXT else 3].start()

        def send(self, q):
            self.combine(OPP, q)
            self.opposite(q)
            self.side(NXT, q)
            self.side(PRV, q)

        def relay(self, q):
            for k, j, h in ((0, NXT, 0), (1, PRV, 1)):
                self.m[q][k].wait_recv()
                add_rows(PP.at[j, c, half(h), self.cols(q)], [XR.at[k, :, self.cols(q)]], HB, min(HB, 16))
                self.m[q][4 + k].start()

        def finish(self, q, res, outs):
            for d in self.m[q][2:]:
                d.wait_recv()
            step, cq = min(HB, 16), self.cols(q)
            for h, (kl, kr) in enumerate(((4, 3), (2, 5))):
                def body(r, carry):
                    lo = pl.ds(mo(r * step, step), step)
                    sl = pl.ds(mo(h * HB + r * step, step), step)
                    tot = PP[OWN, c, sl, cq] + (XR[kl, lo, cq] + XR[kr, lo, cq])
                    val = (res[sl, cq].astype(F32) + tot).astype(BF16)
                    for o in outs:
                        o[sl, cq] = val
                    return carry
                loop(HB // step, body, None)

        def drain(self):
            for d in sum(self.pair + self.m, []):
                d.wait_send()

        def release(self):
            self.drain()
            for k, to in enumerate((self.right, self.left, partner)):
                pl.semaphore_signal(credit.at[k], inc=1, device_id=to, device_id_type=MESH_ID)

        def acquire(self):
            for k in range(len((self.right, self.left, partner))):
                pl.semaphore_wait(credit.at[k], 1)

    def grad_a(j, dst, halves=None, q=None):
        t = off(z, j)

        def rows(h, carry):
            lo = [pl.ds(mo((2 * h + q) * XD + t * ZD, ZD), ZD) for q in HALVES]
            lhs = jnp.concatenate([XV[:, :, :, s].reshape(8 * TB, ZD) for s in lo], axis=1)

            cols, width = (pl.ds(0, K), K) if q is None else (pl.ds(q * ND, ND), ND)
            dst[h, :, :, cols] = dot_tn(lhs, DV[:, :, cols].reshape(8 * TB, width)).reshape(2, ZD, width)
            return carry
        if halves is None:
            loop(2, rows, None)
        else:
            for h in halves:
                rows(h, None)

    def grad_b_first(chips, add):
        cols_l, cols = pl.ds(mo(off(y, OPP) * NK, NK), NK), pl.ds(0, K)
        dst = GPB.at[OPP]
        for t in chips:
            out = dot_tn(AV[t, :, :, cols_l].reshape(T2, NK), GV1[t, :, :, cols].reshape(T2, K)).reshape(2, NK // 2, K)
            dst[:, 0] = dst[:, 0] + out if add else out
            add = True

    def grad_b(gv, j, dst, n=None):
        cols_l = pl.ds(mo(off(y, j) * NK, NK), NK)

        def body(n, carry):
            out = dot_tn(AV[:, :, :, cols_l].reshape(8 * TB, NK), gv[:, :, :, pl.ds(mo(n * K, K), K)].reshape(8 * TB, K))
            dst[:, n] = out.reshape(2, NK // 2, K)
            return carry
        if n is None:
            loop(2, body, None)
        else:
            body(n, None)

    grad_keys = [keys_of(sum(u0u, u0a) + d0a), [d.key for d in ex0 + ex1 + gg1.own + gg1.push] + keys_of(d0b + d0c + [gg1.ring])]

    def grad_key(l):
        return grad_keys[l].pop() if grad_keys[l] else fresh("recv")

    class Reduce4:
        def __init__(self, l, axis, part, recv, stage):
            _, right, left = rings[axis]
            self.part, self.recv, self.stage = part, recv, stage
            self.m = [rcopy(part(*PIECES[k]), recv(k), left if k % 2 else right, grad_key(l))
                      for k in range(ARRIVALS)]
            self.loads = [lcopy(recv(k), stage(k)) for k in range(ARRIVALS)] if stage else None

        def opposite(self):
            self.m[0].start()
            self.m[1].start()

        def sides(self, j):
            self.m[2 if j == NXT else 3].start()

        def fetch(self, k):
            self.m[k].wait_send()
            self.m[k].wait_recv()
            if self.loads:
                self.loads[k].start()

        def absorb(self, k):
            if self.loads:
                self.loads[k].wait()
            dst = self.part(*TARGETS[k])
            add_rows(dst, [(self.stage or self.recv)(k)], dst.shape[1], min(dst.shape[1], 16))

    def arrive(reduces, ks):
        for k in ks:
            for r in reduces:
                r.fetch(k)
        for k in ks:
            for r in reduces:
                r.absorb(k)

    def relay(reduces):
        for k in (0, 1):
            for r in reduces:
                r.fetch(k)
        for k in (0, 1):
            for r in reduces:
                r.absorb(k)
                r.m[4 + k].start()

    hq = DR_ROWS // 2
    own_grads = [(SV.at[pl.ds(0, 2)], SV.at[pl.ds(2, 2)]), (GPA.at[OWN], GPB.at[OWN])]

    def third(k, rows):
        return pl.ds((k // 2) * rows, rows)

    def reduce_a(l, q, chunks):
        own = own_grads[l][0]
        ca = pl.ds(q * (K // chunks), K // chunks)

        def part(j, h):
            return (own if j == OWN else GPA.at[j]).at[h, :, :, ca]

        def part2(j, h):
            return own.at[h, :, pl.ds(mo(off(y, j) * 2 * UR, 2 * UR), 2 * UR), ca]
        if l < q:
            second = lambda k: GPA.at[OWN, k % 2, :, third(k, 2 * UR), ca], None
        else:
            second = lambda k: ra2.at[l, k, :, :, ca], lambda k: STA.at[k % 2, :, :, ca]
        return (Reduce4(l, "z", part, lambda k: ra1.at[l, k, :, :, ca], lambda k: part(*PIECES[k])),
                Reduce4(l, "y", part2, *second))

    def reduce_b(l, q):
        own, nb = own_grads[l][1], pl.ds(q, 1)

        def part(j, h):
            return (own if j == OWN else GPB.at[j]).at[h, nb]

        def part2(j, h):
            t = off(z, j)
            return own.at[t // 2, nb, pl.ds(mo(lax.rem(t, 2) * DR_ROWS + h * hq, hq), hq), :]
        if l < q:
            second = lambda k: GPB.at[OWN, k % 2, nb, third(k, hq), :], None
        else:
            second = lambda k: rb2.at[l, k, nb], lambda k: STB.at[k % 2, nb]
        return (Reduce4(l, "y", part, lambda k: rb1.at[l, k, nb], lambda k: part(*PIECES[k])),
                Reduce4(l, "z", part2, *second))

    def sides(reduces, j):
        for r in reduces:
            r.sides(j)

    def second_start(reduces):
        for r in reduces:
            r.opposite()
            r.sides(NXT)
            r.sides(PRV)

    def up_out(l, q, chunks):
        own = own_grads[l][0]
        ca = pl.ds(q * (K // chunks), K // chunks)

        def rows_of(tx, tc):
            return own.at[tx // 2, lax.rem(tx, 2), pl.ds(mo((2 * y + tc) * UR, UR), UR), ca]
        to = uh.at[l, x, mine, ca]
        sends = [rcopy(rows_of(off(x, dx), cp if dc else c), to, dev(dx=dx, dc=dc), grad_key(l)) for dx, dc in group]
        local = [lcopy(rows_of(x, c), to)]
        for cpy in sends + local:
            cpy.start()
        return sends, local

    def down_out(l, n):
        cpy = lcopy(own_grads[l][1].at[z // 2, n, pl.ds(mo(lax.rem(z, 2) * DR_ROWS, DR_ROWS), DR_ROWS), :],
                    gd_out.at[l, :, pl.ds(n * K, K)])
        cpy.start()
        return [], [cpy]

    def grads_out_finish(state):
        for cpy in state[0]:
            cpy.wait_recv()
            cpy.wait_send()
        for cpy in state[1]:
            cpy.wait()

    r = Reduce8(functools.partial(down_part, AV), 0, SPLIT3)
    r_keys = sorted([d.key for m in r.m for d in m] + [f + j for f in r.first for j in range(RING)])
    hidden0(off(x, OPP))
    hidden0(off(x, NXT))
    do(d0b, "finish")
    r.compute(OPP, 0)
    r.compute(NXT, 0)
    do(d0c, "forward")
    do(d0d, "start")
    r.combine(OPP, 0)
    r.opposite(0)
    do(u0u[2] + u0u[3], "drain")
    hidden0(off(x, PRV))
    r.compute(PRV, 0)
    r.side(NXT, 0)
    do(d1a, "forward")
    hidden0(off(x, OWN))
    r.side(PRV, 0)
    save_s = lcopy(SV, sh0)
    save_s.start()
    save_a0 = lcopy(AV, ah.at[0])
    save_a0.start()
    gg1.sides()
    do(d0c, "finish")
    r.compute_all(1)
    r.relay(0)
    do(d0d, "forward")
    for cpy in ex1:
        cpy.wait_recv()
    own_d1.wait()
    do(u1a, "start")
    r.send(1)
    do(d1a, "finish")
    do(d1b, "start")
    gg1.last()
    save_x.wait()
    gx0.drain()
    do(d0d, "finish")
    do(d0b + d0c, "drain")
    save_d0 = lcopy(W, wdh.at[0])
    save_d0.start()
    r.compute(OPP, 2)
    r.relay(1)
    save_u0.wait()
    do(u1a, "forward")
    r.compute(NXT, 2)
    r.combine(OPP, 2)
    r.opposite(2)
    r.compute(PRV, 2)
    r.side(NXT, 2)
    r.compute(OWN, 2)
    r.side(PRV, 2)
    r.compute(OWN, 0)
    for q in range(len(SPLIT3)):
        r.combine(OWN, q)

    def gather_keys(gathers):
        return [d.key for g in gathers for d in g.ring.d + g.own + g.push]

    def token_gathers(slot, buf):
        def make(q):
            cq = tile_cols(SPLIT2, q)
            return Gather8(lambda h: RES.at[slot, half(h), cq], lambda b, k, h: buf.at[b, k, half(h), cq])
        return [make(0), make(1)]

    keys.extend(gather_keys((gx0,)))
    gx1 = token_gathers(X1, XV)
    do(d1a, "drain")
    do(d1b, "forward")
    for q in HALVES:
        r.finish(q, RES.at[X0], [RES.at[X1], XV.at[x, c]])
    r.relay(2)
    gx1[0].start()
    do(u1a, "finish")
    do(u1b, "start")
    do(u1c, "start_first")
    pair, rest = pl.ds(0, 2), pl.ds(2, 2)
    own_up = [lcopy(up[1].at[pair, z], U.at[pair, z]), lcopy(up[1].at[rest, :, y], U.at[rest, :, y])]
    for cpy in own_up:
        cpy.start()
    gg1.wait_own()
    gg1.wait_push(range(len(gg1.push)))
    own_g.wait()
    save_d0.wait()
    do(d0d + u1a, "drain")
    gg1.drain()
    do(d1b, "finish")
    load_w1d = lcopy(wdh.at[1], W)
    load_w1d.start()
    r.finish(2, RES.at[X0], [RES.at[X1], XV.at[x, c]])
    gx1[1].start()
    save_s.wait()
    do(u1b, "forward")
    do(u1c, "start_rest")
    load_w1d.wait()
    dact1(off(x, OWN))
    gx1[0].forward()
    r.release()
    dact1(off(x, NXT))
    gx1[0].sides()
    dact1(off(x, PRV))
    do(u1c, "forward")
    do(u1b, "finish")
    dact1(off(x, OPP))
    load_w0d_again = lcopy(wdh.at[0], W)
    load_w0d_again.start()
    save_a0.wait()
    do(gx1, "wait_own")
    for cpy in own_up:
        cpy.wait()
    hidden1(off(x, OWN), 0)
    do(gx1[1:], "forward")
    do(gx1[1:], "sides")
    for j in (PRV, NXT):
        for g in gx1:
            g.wait_push(PUSHES[j])
        hidden1(off(x, j), 0)
    gx1[0].last()
    do(u1c, "finish")
    hidden1(off(x, OWN), 1)
    hidden1(off(x, PRV), 1)
    gx1[1].last()
    hidden1(off(x, NXT), 1)
    grad_b_first([off(x, j) for j in (OWN, PRV, NXT)], False)
    for g in gx1:
        g.wait_push(PUSHES[OPP])
    hidden1_tile(off(x, OPP), off(y, OPP))

    (a1, a2), (b1, b2) = zip(*[reduce_a(1, q, 2) for q in HALVES]), zip(*[reduce_b(1, q) for q in HALVES])
    first1, second1 = b1 + a1, b2 + a2
    grad_b_first([off(x, OPP)], True)
    b1[0].opposite()
    for q in HALVES:
        hidden1(off(x, OPP), q)
        for h in HALVES:
            grad_a(OPP, GPA.at[OPP], (h,), q)
            a1[q].m[h].start()
    load_s0 = lcopy(sh0, SV)
    load_s0.start()
    save_a1 = lcopy(AV, ah.at[1])
    save_a1.start()
    grad_b(GV1, OPP, GPB.at[OPP], 1)
    b1[1].opposite()
    r = Reduce8(dx_part, 1, SPLIT2, r_keys)
    r.acquire()
    r.compute(OPP, 0)
    r.compute(NXT, 0)
    r.combine(OPP, 0)
    r.opposite(0)
    r.compute(PRV, 0)
    r.side(NXT, 0)
    r.side(PRV, 0)
    r.compute_all(1)
    load_w0u_again = lcopy(wuh.at[0], U)
    r.compute(OWN, 0)
    do(u1b + u1c, "drain")
    load_w0u_again.start()
    grad_b(GV1, NXT, GPB.at[NXT])
    sides(b1, NXT)
    grad_b(GV1, PRV, GPB.at[PRV])
    sides(b1, PRV)
    r.relay(0)
    r.send(1)
    grad_a(NXT, GPA.at[NXT])
    sides(a1, NXT)
    grad_a(PRV, GPA.at[PRV])
    sides(a1, PRV)
    r.combine(OWN, 0)
    r.combine(OWN, 1)
    keys.extend(gather_keys(gx1))
    gg0 = token_gathers(G0, GV0)
    r.relay(1)
    r.finish(0, RES.at[G1], [RES.at[G0], GV0.at[x, c]])
    gg0[0].start()
    relay(first1)
    grad_b(GV1, OWN, GPB.at[OWN])
    save_a1.wait()
    load_a0 = lcopy(ah.at[0], AV)
    load_a0.start()
    do(d1b, "drain")
    load_a1 = lcopy(ah.at[1], GV1.at[:, :, :, 0:K])
    load_a1.start()
    r.finish(1, RES.at[G1], [RES.at[G0], GV0.at[x, c]])
    gg0[1].start()
    gg0[0].forward()
    grad_a(OWN, GPA.at[OWN])
    do(gx1, "drain")
    load_x0 = lcopy(xh0, XV)
    load_x0.start()
    gg0[0].sides()
    r.release()
    gg0[1].forward()
    gg0[0].last()
    load_w0d_again.wait()
    load_s0.wait()
    do(gg0, "wait_own")
    dact0(off(x, OWN))
    gg0[1].sides()
    gg0[1].last()
    for g in gg0:
        g.wait_push(PUSHES[PRV])
    dact0(off(x, PRV))
    for g in gg0:
        g.wait_push(PUSHES[NXT])
    dact0(off(x, NXT))
    for g in gg0:
        g.wait_push(PUSHES[OPP])

    (a1n, a2n), (b1n, b2n) = zip(*[reduce_a(0, q, 2) for q in HALVES]), zip(*[reduce_b(0, q) for q in HALVES])
    load_a0.wait()
    grad_b(GV0, OPP, GPB.at[OPP])
    b1n[0].opposite()
    dact0(off(x, OPP))
    load_w1d_again = lcopy(wdh.at[1], W)
    load_w1d_again.start()
    load_x0.wait()
    for h in HALVES:
        grad_a(OPP, GPA.at[OPP], (h,))
        a1n[0].m[h].start()
    arrive(first1, EARLY + LATE)
    second_start(second1)
    load_w0u_again.wait()
    r = Reduce8(dx_part, 2, WHOLE, r_keys)
    r.acquire()
    r.compute_all(0)
    r.send(0)
    grad_b(GV0, NXT, GPB.at[NXT])
    b1n[0].sides(NXT)
    grad_b(GV0, PRV, GPB.at[PRV])
    b1n[0].sides(PRV)
    grad_a(NXT, GPA.at[NXT])
    a1n[0].sides(NXT)
    grad_a(PRV, GPA.at[PRV])
    a1n[0].sides(PRV)
    relay(second1)
    r.relay(0)
    relay((b1n[0], a1n[0]))
    for red in (b1n[1], a1n[1]):
        red.opposite()
        red.sides(NXT)
        red.sides(PRV)
    r.combine(OWN, 0)
    grad_b(GV0, OWN, own_grads[0][1])
    grad_a(OWN, own_grads[0][0])
    r.finish(0, RES.at[G0], [RES.at[X0]])
    r.release()
    write_gi = lcopy(RES.at[X0], gi_out)
    write_gi.start()
    arrive((b1n[0], a1n[0]), EARLY)
    arrive(second1, EARLY)
    arrive(second1, LATE)
    state1 = [up_out(1, q, 2) for q in HALVES] + [down_out(1, n) for n in HALVES]
    load_a1.wait()
    load_w1d_again.wait()
    r = Reduce8(functools.partial(down_part, GV1), 3, WHOLE, r_keys)
    r.acquire()
    r.compute_all(0)
    r.send(0)
    r.combine(OWN, 0)
    arrive((b1n[0], a1n[0]), LATE)
    for state in state1:
        grads_out_finish(state)
    relay((b1n[1], a1n[1]))
    second_start((a2n[0], b2n[0]))
    r.relay(0)
    arrive((b1n[1], a1n[1]), EARLY)

    def start(red):
        red.opposite()
        sides((red,), NXT)
        sides((red,), PRV)
    arrive((b1n[1],), LATE)
    relay((a2n[0],))
    arrive((a1n[1],), LATE)
    start(a2n[1])
    start(b2n[1])
    arrive((a2n[0],), EARLY)
    relay((b2n[0],))
    arrive((a2n[0],), LATE)
    state0 = [up_out(0, 0, 2)]
    relay((a2n[1],))
    arrive((b2n[0],), EARLY)
    relay((b2n[1],))
    arrive((a2n[1],), EARLY)
    arrive((a2n[1],), LATE)
    state0.append(up_out(0, 1, 2))
    arrive((b2n[1],), EARLY)
    for q in HALVES:
        arrive((b2n[q],), LATE)
        state0.append(down_out(0, q))
    r.finish(0, RES.at[X1], [RES.at[G1]])
    write_y = lcopy(RES.at[G1], y_out)
    write_y.start()
    r.drain()
    do(gg0, "drain")
    write_gi.wait()
    write_y.wait()
    for state in state0:
        grads_out_finish(state)
    assert used["recv"] <= N_RECV and used["send"] <= N_SEND and used["local"] <= N_LOCAL


def finish_kernel(y_in, gi_in, gu_in, gd_in, y_out, gi_out, gu_out, gd_out, ybuf, gibuf, gubuf, gdbuf, gushuf, sems):
    layers, ur, ff = gu_out.shape
    s2 = ff // 64
    half = s2 // 2
    pairs = [((gu_in.at[l], gubuf.at[l]), (gushuf.at[l], gu_out.at[l])) for l in range(layers)]
    pairs += [((a, b), (b, o)) for a, b, o in ((gd_in, gdbuf, gd_out), (y_in, ybuf, y_out), (gi_in, gibuf, gi_out))]
    loads = [pltpu.make_async_copy(*p, sems.at[0, k]) for k, (p, _) in enumerate(pairs)]
    stores = [pltpu.make_async_copy(*p, sems.at[1, k]) for k, (_, p) in enumerate(pairs)]
    for cpy in loads:
        cpy.start()
    low = lax.broadcasted_iota(jnp.int32, (ur, s2), 1) < half
    swap = lambda v: pltpu.roll(v, half, 1)
    for l, (load, store) in enumerate(zip(loads, stores)):
        load.wait()
        for b in range(RING if l < layers else 0):
            for yy in range(RING):
                for m in HALVES:
                    cols = pl.ds((yy * 2 + m) * s2, s2)
                    t0, t1 = (gubuf[l, b, pl.ds(k * ur, ur), cols] for k in HALVES)
                    strip = (b * RING + 2 * m) * RING + yy
                    gushuf[l, :, pl.ds(strip * s2, s2)] = jnp.where(low, t0, swap(t1))
                    gushuf[l, :, pl.ds((strip + RING) * s2, s2)] = jnp.where(low, swap(t0), t1)
        store.start()
    for cpy in stores:
        cpy.wait()


def solution(mesh, interpret=None):
    fine = Mesh(np.asarray(mesh.devices).reshape(4, 4, 4, 2), ALL)
    tok_spec = P(ALL, None)
    weight_spec = P(None, ALL, None)

    def device_step(x_loc, up_loc, down_loc, g_loc):
        layers, ur, ff = up_loc.shape
        dr, dm = down_loc.shape[1:]
        tb = x_loc.shape[0]
        k = ff // 8
        zd = dm // 16
        hbm = lambda shape, dt: jax.ShapeDtypeStruct(shape, dt)
        outs = [
            hbm((tb, dm), BF16), hbm((tb, dm), BF16), hbm((layers, dr, dm), F32),
            hbm((RING, CORES, tb, dm), BF16),
            hbm((layers, RING, RING, RING, 2 * ur, k), BF16),
            hbm((layers, RING, RING, dr, dm), BF16),
            hbm((RING, CORES, tb, k), F32), hbm((layers, RING, CORES, tb, k), BF16),
            *[hbm((layers, ARRIVALS, CORES, n, k), F32) for n in (zd, zd, 2 * ur, 2 * ur)],
            hbm((layers, RING, 2 * ur, k), F32),
        ]
        vm = pltpu.VMEM
        scratch = [
            vm((RING, RING, RING, 2 * ur, k), BF16), vm((RING, RING, dr, dm), BF16),
            vm((RING, CORES, tb, dm), BF16), vm((RING, CORES, tb, dm), BF16), vm((RING, CORES, tb, dm), BF16),
            vm((RING, CORES, tb, k), F32), vm((RING, CORES, tb, k), BF16), vm((RING, 2 * tb, k), BF16),
            vm((RING, CORES, CORES, zd, k), F32), vm((RING, CORES, CORES, zd, k), F32),
            vm((RING, CORES, tb, dm), F32), vm((4, tb, dm), F32), vm((6, tb // 2, dm), F32),
            vm((4, tb, dm), BF16), vm((CORES, CORES, 2 * ur, k), F32), vm((CORES, CORES, 2 * ur, k), F32),
            *[pltpu.SemaphoreType.DMA((n,)) for n in (N_SEND, N_RECV, N_LOCAL, len(SPLIT3) * RING)],
            pltpu.SemaphoreType.REGULAR((3,)),
        ]
        anyspec = pl.BlockSpec(memory_space=pl.ANY)
        call = pl.pallas_call(
            functools.partial(kernel, (dm, k, tb, ur, dr)),
            out_shape=outs,
            in_specs=[anyspec] * 4,
            out_specs=[anyspec] * len(outs),
            scratch_shapes=scratch,
            compiler_params=pltpu.CompilerParams(collective_id=0, has_side_effects=True, vmem_limit_bytes=67043328),
            name="mlp_stack",
            **({"interpret": interpret} if interpret else {}),
        )
        y_raw, gi_raw, gd_raw, *_, gu_raw = call(x_loc, up_loc, down_loc, g_loc)
        raws = (y_raw, gi_raw, gu_raw, gd_raw)
        outs = [hbm((tb, dm), BF16), hbm((tb, dm), BF16), hbm((layers, ur, ff), F32), hbm((layers, dr, dm), F32)]
        return tuple(pl.pallas_call(
            finish_kernel, out_shape=outs, in_specs=[anyspec] * len(outs), out_specs=[anyspec] * len(outs),
            scratch_shapes=[vm(v.shape, v.dtype) for v in raws] + [vm(outs[2].shape, F32), pltpu.SemaphoreType.DMA((2, layers + len(outs)))],
            name="write_out")(*raws))

    return jax.shard_map(device_step, mesh=fine, in_specs=(tok_spec, weight_spec, weight_spec, tok_spec),
                         out_specs=(tok_spec, tok_spec, weight_spec, weight_spec), check_vma=False)
```

```python
import functools

import jax
import jax.numpy as jnp
import numpy as np
from jax import lax
from jax.experimental import pallas as pl
from jax.experimental.pallas import tpu as pltpu
from jax.sharding import Mesh, PartitionSpec as P

MESH_ID = pl.DeviceIdType.MESH
ALL = ("x", "z", "y", "c")
F32, BF16 = jnp.float32, jnp.bfloat16
RING, CORES, ARRIVALS = 4, 2, 6
OWN, NXT, OPP, PRV = range(RING)
X0, X1, G1, G0 = range(RING)
HALVES = (0, 1)
WHOLE, SPLIT2, SPLIT3 = (4,), (2, 2), (1, 1, 2)
PIECES = ((OPP, 0), (OPP, 1), (NXT, 1), (PRV, 0), (NXT, 0), (PRV, 1))
TARGETS = ((NXT, 0), (PRV, 1), (OWN, 1), (OWN, 0), (OWN, 0), (OWN, 1))
EARLY, LATE = (2, 3), (4, 5)
PUSHES = {PRV: (0, 2), NXT: (1, 3), OPP: (4, 5)}
N_RECV, N_SEND, N_LOCAL = 192, 90, 19


def gelu_parts(pre_act):
    norm_cdf = 0.5 * (1.0 + lax.erf(pre_act * (2.0 ** -0.5)))
    norm_pdf = jnp.exp(-0.5 * pre_act * pre_act) * ((2.0 * jnp.pi) ** -0.5)
    return pre_act * norm_cdf, norm_cdf + pre_act * norm_pdf


def loop(n, body, init):
    return lax.fori_loop(0, n, body, init)


def dot_nn(left, right):
    return lax.dot_general(left, right, (((1,), (0,)), ((), ())), preferred_element_type=F32)


def dot_nt(left, right):
    return lax.dot_general(left, right, (((1,), (1,)), ((), ())), preferred_element_type=F32)


def dot_tn(left, right):
    return lax.dot_general(left, right, (((0,), (0,)), ((), ())), preferred_element_type=F32)


def kernel(dims, x_in, wu_in, wd_in, g_in,
           y_out, gi_out, gd_out,
           xh0, wuh, wdh, sh0, ah, ra1, rb1, ra2, rb2, uh,
           U, W, XV, GV1, GV0, SV, AV, DV, GPA, GPB, PP, DR, XR, RES, STA, STB,
           ss, rs, ls, ps, credit):
    D, K, TB, UR, DR_ROWS = dims
    HB = TB // 2
    x, z, y, c = (lax.axis_index(a) for a in ALL)
    cp = 1 - c
    S2 = 2 * DR_ROWS
    XD = D // 4
    ZD = D // 16

    def dev(dx=0, dz=0, dy=0, dc=0):
        wrap = lambda v, d, n: v if d == 0 else lax.rem(v + (d % n), n)
        return (wrap(x, dx, 4), wrap(z, dz, 4), wrap(y, dy, 4), wrap(c, dc, 2))

    partner = dev(dc=1)
    rings = {"x": (x, dev(dx=1), dev(dx=-1)), "z": (z, dev(dz=1), dev(dz=-1)), "y": (y, dev(dy=1), dev(dy=-1))}
    off = lambda v, d: v if d == 0 else lax.rem(v + d, 4)

    used = {"recv": 0, "send": 0, "local": 0}
    free = {"send": [], "local": []}
    keys = []

    def fresh(kind):
        if kind == "recv" and keys:
            return keys.pop()
        used[kind] += 1
        return used[kind] - 1

    def take(kind):
        return free[kind].pop() if free[kind] else fresh(kind)

    def remote(src, dst, send, recv, to):
        return pltpu.make_async_remote_copy(src_ref=src, dst_ref=dst, send_sem=send, recv_sem=recv,
                                            device_id=to, device_id_type=MESH_ID)

    class rcopy:
        def __init__(self, src, dst, to, key=None):
            self.args, self.key = (src, dst, to), fresh("recv") if key is None else key

        def start(self):
            src, dst, to = self.args
            self.sem = take("send")
            self.d = remote(src, dst, ss.at[self.sem], rs.at[self.key], to)
            self.d.start()

        def wait_recv(self):
            self.d.wait_recv()

        def wait_send(self):
            self.d.wait_send()
            free["send"].append(self.sem)

    class lcopy:
        def __init__(self, src, dst):
            self.args = src, dst

        def start(self):
            self.sem = take("local")
            self.d = pltpu.make_async_copy(*self.args, ls.at[self.sem])
            self.d.start()

        def wait(self):
            self.d.wait()
            free["local"].append(self.sem)

    def mo(v, m):
        return pl.multiple_of(v, m)

    class Gather4:
        def __init__(self, axis, src, dst):
            i, right, left = rings[axis]
            lft, rgt = off(i, 3), off(i, 1)
            self.d = [rcopy(src(0), dst(i, 0), right), rcopy(src(1), dst(i, 1), right),
                      rcopy(src(0), dst(i, 0), left), rcopy(src(1), dst(i, 1), left),
                      rcopy(dst(lft, 0), dst(lft, 0), right), rcopy(dst(rgt, 1), dst(rgt, 1), left)]

        def start_first(self):
            self.d[0].start()
            self.d[3].start()

        def start_rest(self):
            self.d[1].start()
            self.d[2].start()

        def start(self):
            self.start_first()
            self.start_rest()

        def forward(self):
            for k in HALVES:
                self.d[3 * k].wait_recv()
                self.d[4 + k].start()

        def neighbours(self):
            self.d[1].wait_recv()
            self.d[2].wait_recv()

        def opposite(self):
            self.d[4].wait_recv()
            self.d[5].wait_recv()

        def finish(self):
            self.neighbours()
            self.opposite()

        def drain(self):
            for d in self.d:
                d.wait_send()

    class Gather8:
        def __init__(self, src, dst):
            self.ring = Gather4("x", src, lambda b, h: dst(b, c, h))
            lft, rgt, opp = off(x, PRV), off(x, NXT), off(x, OPP)
            blocks = [(lft, 0), (rgt, 1), (lft, 1), (rgt, 0), (opp, 0), (opp, 1)]
            self.own = [rcopy(src(h), dst(x, c, h), partner) for h in HALVES]
            self.push = [rcopy(dst(b, c, h), dst(b, c, h), partner) for b, h in blocks]

        def start(self):
            self.ring.start()
            for d in self.own:
                d.start()

        def forward(self):
            self.ring.forward()
            self.push[0].start()
            self.push[1].start()

        def sides(self):
            self.ring.d[1].wait_recv()
            self.push[2].start()
            self.ring.d[2].wait_recv()
            self.push[3].start()

        def last(self):
            self.ring.d[4].wait_recv()
            self.push[4].start()
            self.ring.d[5].wait_recv()
            self.push[5].start()

        def wait_own(self):
            for d in self.own:
                d.wait_recv()

        def wait_push(self, ks):
            for k in ks:
                self.push[k].wait_recv()

        def drain(self):
            self.ring.drain()
            for d in self.own + self.push:
                d.wait_send()

    def add_rows(dst, srcs, rows, step):
        def body(r, carry):
            sl = pl.ds(mo(r * step, step), step)
            if len(dst.shape) == 3:
                for q in range(dst.shape[0]):
                    acc = dst[q, sl, :]
                    for s in srcs:
                        acc = acc + s[q, sl, :]
                    dst[q, sl, :] = acc
            else:
                acc = dst[sl, :]
                for s in srcs:
                    acc = acc + s[sl, :]
                dst[sl, :] = acc
            return carry
        loop(rows // step, body, None)

    barrier = pltpu.get_barrier_semaphore()
    group = [(dx, dc) for dx in (OPP, NXT, PRV, OWN) for dc in HALVES if dx or dc]
    peers = [dev(dx=dx, dc=dc) for dx, dc in group] + [rings[a][k] for a in "zy" for k in (1, 2)]
    for p in peers:
        pl.semaphore_signal(barrier, inc=1, device_id=p, device_id_type=MESH_ID)

    load_u = [[lcopy(wu_in.at[l, :, pl.ds(b * D, D)], RES.at[G0, pl.ds((l * RING + b) * UR, UR), :])
               for b in range(RING)] for l in HALVES]
    load_d = [lcopy(wd_in.at[l], RES.at[X1, pl.ds(l * DR_ROWS, DR_ROWS), :]) for l in HALVES]
    load_x = lcopy(x_in, RES.at[X0])
    load_g = lcopy(g_in, RES.at[G1])
    own_x = lcopy(x_in, XV.at[x, c])
    own_g = lcopy(g_in, GV1.at[x, c])
    own_d0 = lcopy(wd_in.at[0], W.at[y, z])
    for cpy in load_u[0] + load_u[1] + load_d + [load_x, own_d0, own_x, load_g, own_g]:
        cpy.start()

    low = lax.broadcasted_iota(jnp.int32, (UR, S2), 1) < DR_ROWS
    swap = lambda v: pltpu.roll(v, DR_ROWS, 1)
    for l in HALVES:
        for cpy in load_u[l]:
            cpy.wait()
        for b in range(RING):
            rows = pl.ds((l * RING + b) * UR, UR)
            for yy in range(RING):
                for m in HALVES:
                    s0 = RES[G0, rows, pl.ds((2 * m * RING + yy) * S2, S2)].astype(F32)
                    s1 = RES[G0, rows, pl.ds(((2 * m + 1) * RING + yy) * S2, S2)].astype(F32)
                    cols = pl.ds((yy * 2 + m) * S2, S2)
                    AV[l, 0, pl.ds(2 * b * UR, UR), cols] = jnp.where(low, s0, swap(s1)).astype(BF16)
                    AV[l, 0, pl.ds((2 * b + 1) * UR, UR), cols] = jnp.where(low, swap(s0), s1).astype(BF16)
    for cpy in load_d + [load_x, own_d0]:
        cpy.wait()
    pl.semaphore_wait(barrier, len(peers))

    half = lambda h: pl.ds(h * HB, HB)

    def tile_cols(split, q):
        return pl.ds(sum(split[:q]) * (D // RING), split[q] * (D // RING))

    gx0 = Gather8(lambda h: RES.at[X0, half(h)], lambda b, k, h: XV.at[b, k, half(h)])
    gg1 = Gather8(lambda h: RES.at[G1, half(h)], lambda b, k, h: GV1.at[b, k, half(h)])
    up = [U, wuh.at[1]]
    down = [W, wdh.at[1]]
    hr = DR_ROWS // 4

    def quarter(q, h):
        return pl.ds((2 * q + h) * hr, hr)

    def down_first(l):
        to = down[l]
        src = lambda q: lambda h: RES.at[X1, pl.ds(l * DR_ROWS + (2 * q + h) * hr, hr)]
        return [Gather4("z", src(0), lambda b, h: to.at[y, b, quarter(0, h)]),
                Gather4("y", src(1), lambda b, h: to.at[b, z, quarter(1, h)])]

    def down_second(l, split, n):
        to, cs = down[l], tile_cols(split, n)
        return [Gather4("y", lambda h: to.at[y, :, quarter(0, h), cs], lambda b, h: to.at[b, :, quarter(0, h), cs]),
                Gather4("z", lambda h: to.at[:, z, quarter(1, h), cs], lambda b, h: to.at[:, b, quarter(1, h), cs])]

    def up_first(to):
        return [Gather4("y", lambda h: to.at[h, z, y], lambda b, h: to.at[h, z, b]),
                Gather4("z", lambda h: to.at[2 + h, z, y], lambda b, h: to.at[2 + h, b, y])]

    def hidden_cols(n):
        return pl.ds(sum(SPLIT2[:n]) * (K // RING), SPLIT2[n] * (K // RING))

    def up_second(n):
        cs, src = hidden_cols(n), up[1]
        return [Gather4("z", lambda h: src.at[h, z, :, :, cs], lambda b, h: U.at[h, b, :, :, cs]),
                Gather4("y", lambda h: src.at[2 + h, :, y, :, cs], lambda b, h: U.at[2 + h, :, b, :, cs])]

    def up_unit(to, j):
        yj, zj = off(y, j), off(z, j)
        return [Gather4("z", lambda h: to.at[h, z, yj], lambda b, h: to.at[h, b, yj]),
                Gather4("y", lambda h: to.at[2 + h, zj, y], lambda b, h: to.at[2 + h, zj, b])]

    def do(gathers, step):
        for g in gathers:
            getattr(g, step)()

    mine = pl.ds(mo(c * UR, UR), UR)

    def up_exchange(l):
        sends = []
        for dx, dc in group:
            tx, tc = off(x, dx), (cp if dc else c)
            src = AV.at[l, 0, pl.ds(mo((tx * 2 + tc) * UR, UR), UR), :]
            sends.append(rcopy(src, up[l].at[x, z, y, mine, :], dev(dx=dx, dc=dc)))
        for cpy in sends:
            cpy.start()
        return sends

    def keys_of(gathers):
        return [d.key for g in gathers for d in g.d]

    d0a, d0b, d0c = down_first(0), down_second(0, SPLIT3, 0), down_second(0, SPLIT3, 1)
    u0a, u0u = up_first(up[0]), [up_unit(up[0], j) for j in (OWN, PRV, NXT, OPP)]
    keys.extend(keys_of(u0a))
    d0d = down_second(0, SPLIT3, 2)
    keys.extend(keys_of(d0a))
    d1a = down_first(1)
    keys.extend(keys_of(sum(u0u, [])))
    d1b, u1a = down_second(1, WHOLE, 0), up_first(up[1])
    u1b, u1c = up_second(0), up_second(1)
    ex0 = up_exchange(0)
    do(d0a, "start")
    gx0.start()
    ex1 = up_exchange(1)
    my_rows = pl.ds(mo((x * 2 + c) * UR, UR), UR)
    own_u1 = lcopy(AV.at[1, 0, my_rows, :], up[1].at[x, z, y, mine, :])
    own_u1.start()
    own_d1 = lcopy(RES.at[X1, pl.ds(DR_ROWS, DR_ROWS), :], down[1].at[y, z])
    own_d1.start()
    U[x, z, y, mine, :] = AV[0, 0, my_rows, :]
    do(d0a, "forward")
    for cpy in ex0:
        cpy.wait_recv()
    do(u0a, "start")
    do(u0u[0], "start")
    do(u0a, "forward")
    gx0.forward()
    load_g.wait()
    gg1.start()
    do(u0a, "neighbours")
    do(u0u[1], "start")
    do(u0u[2], "start")
    do(u0u[0], "forward")
    do(u0a, "opposite")
    do(u0u[3], "start")
    do(d0a, "finish")
    do(d0a + u0a, "drain")
    do(u0u[1], "forward")
    do(u0u[2], "forward")
    do(d0b, "start_first")
    gx0.sides()
    for cpy in ex0 + ex1:
        cpy.wait_send()
    own_u1.wait()
    do(u0u[3], "forward")
    do(u0u[0] + u0u[1], "drain")
    do(d0b, "start_rest")
    do(d0c, "start_first")
    do(d0b, "forward")
    do(d0c, "start_rest")
    do(d1a, "start")
    gg1.forward()
    gx0.last()
    gx0.wait_own()
    gx0.wait_push(range(len(gx0.push)))
    own_x.wait()
    save_x = lcopy(XV, xh0)
    save_x.start()
    for unit in u0u:
        do(unit, "finish")
    save_u0 = lcopy(U, wuh.at[0])
    save_u0.start()

    T2 = 2 * TB
    ND = D // 4
    NK = K // 4

    def up_tile(t, n):
        cols = pl.ds(mo(n * NK, NK), NK)
        return dot_nn(XV[t].reshape(T2, D), U[:, :, :, :, cols].reshape(D, NK)), cols

    def hidden0(t):
        for n in range(RING):
            pre, cols = up_tile(t, n)
            act, slope = gelu_parts(pre)
            AV[t, :, :, cols] = act.astype(BF16).reshape(2, TB, NK)
            SV[t, :, :, cols] = slope.reshape(2, TB, NK)

    def hidden1_tile(t, n):
        pre, cols = up_tile(t, n)
        act, slope = gelu_parts(pre)
        AV[t, :, :, cols] = act.astype(BF16).reshape(2, TB, NK)
        DV[t, :, cols] = (SV[t, :, :, cols].reshape(T2, NK) * slope).astype(BF16)

    def hidden1(t, part):
        for n in range(sum(SPLIT2[:part]), sum(SPLIT2[:part + 1])):
            hidden1_tile(t, n)

    def dact(gv, t, n):
        return dot_nt(gv[t].reshape(T2, D), W[n].reshape(NK, D))

    def dact1(t):
        def body(n, carry):
            SV[t, :, :, pl.ds(mo(n * NK, NK), NK)] = dact(GV1, t, n).reshape(2, TB, NK)
            return carry
        loop(RING, body, None)

    def dact0(t):
        def body(n, carry):
            cols = pl.ds(mo(n * NK, NK), NK)
            DV[t, :, cols] = (dact(GV0, t, n) * SV[t, :, :, cols].reshape(T2, NK)).astype(BF16)
            return carry
        loop(RING, body, None)

    def down_part(act, j, lo, tiles):
        t = lax.rem(x + j, RING)

        def body(n, carry):
            cols = pl.ds(mo((lo + n) * ND, ND), ND)
            PP[j, :, :, cols] = dot_nn(act[t, :, :, 0:K].reshape(T2, K), W[:, :, :, cols].reshape(K, ND)).reshape(2, TB, ND)
            return carry
        loop(tiles, body, None)

    def dx_part(j, lo, tiles):
        t = lax.rem(x + j, RING)

        def body(n, carry):
            cols = pl.ds(mo((lo + n) * ND, ND), ND)
            PP[j, :, :, cols] = dot_nt(DV[t], U[lo + n].reshape(ND, K)).reshape(2, TB, ND)
            return carry
        loop(tiles, body, None)

    class Reduce8:
        def __init__(self, part, index, split, old=()):
            self.part, self.index, self.split = part, index, split
            keys.extend(old)
            _, right, left = rings["x"]
            self.right, self.left = right, left
            self.pair, self.m, self.first = [], [], []
            for q in range(len(split)):
                cq = self.cols(q)
                first = sorted(fresh("recv") for j in range(RING))
                self.pair.append([self.swap(j, q, first[0]) for j in range(RING)])
                self.first.append(first[0])
                src = lambda j, h: PP.at[j, c, half(h), cq]
                self.m.append([rcopy(src(*PIECES[k]), XR.at[k, :, cq], left if k % 2 else right) for k in range(ARRIVALS)])
            keys.clear()

        def cols(self, q):
            return tile_cols(self.split, q)

        def swap(self, j, q, first):
            cq = self.cols(q)
            return remote(PP.at[j, cp, :, cq], DR.at[j, :, cq], ps.at[q * RING + j], rs.at[first + j], partner)

        def compute(self, j, q):
            self.part(j, sum(self.split[:q]), self.split[q])
            self.pair[q][j].start()

        def compute_all(self, q):
            def body(i, carry):
                j = lax.rem(i + 1, RING)
                self.part(j, sum(self.split[:q]), self.split[q])
                self.swap(j, q, self.first[q]).start()
                return carry
            loop(RING, body, None)

        def combine(self, j, q):
            self.pair[q][j].wait_recv()
            add_rows(PP.at[j, c, :, self.cols(q)], [DR.at[j, :, self.cols(q)]], TB, min(TB, 16))

        def opposite(self, q):
            self.m[q][0].start()
            self.m[q][1].start()

        def side(self, j, q):
            self.combine(j, q)
            self.m[q][2 if j == NXT else 3].start()

        def send(self, q):
            self.combine(OPP, q)
            self.opposite(q)
            self.side(NXT, q)
            self.side(PRV, q)

        def relay(self, q):
            for k, j, h in ((0, NXT, 0), (1, PRV, 1)):
                self.m[q][k].wait_recv()
                add_rows(PP.at[j, c, half(h), self.cols(q)], [XR.at[k, :, self.cols(q)]], HB, min(HB, 16))
                self.m[q][4 + k].start()

        def finish(self, q, res, outs):
            for d in self.m[q][2:]:
                d.wait_recv()
            step, cq = min(HB, 16), self.cols(q)
            for h, (kl, kr) in enumerate(((4, 3), (2, 5))):
                def body(r, carry):
                    lo = pl.ds(mo(r * step, step), step)
                    sl = pl.ds(mo(h * HB + r * step, step), step)
                    tot = PP[OWN, c, sl, cq] + (XR[kl, lo, cq] + XR[kr, lo, cq])
                    val = (res[sl, cq].astype(F32) + tot).astype(BF16)
                    for o in outs:
                        o[sl, cq] = val
                    return carry
                loop(HB // step, body, None)

        def drain(self):
            for d in sum(self.pair + self.m, []):
                d.wait_send()

        def release(self):
            self.drain()
            for k, to in enumerate((self.right, self.left, partner)):
                pl.semaphore_signal(credit.at[k], inc=1, device_id=to, device_id_type=MESH_ID)

        def acquire(self):
            for k in range(len((self.right, self.left, partner))):
                pl.semaphore_wait(credit.at[k], 1)

    def grad_a(j, dst, halves=None, q=None):
        t = off(z, j)

        def rows(h, carry):
            lo = [pl.ds(mo((2 * h + q) * XD + t * ZD, ZD), ZD) for q in HALVES]
            lhs = jnp.concatenate([XV[:, :, :, s].reshape(8 * TB, ZD) for s in lo], axis=1)

            cols, width = (pl.ds(0, K), K) if q is None else (pl.ds(q * ND, ND), ND)
            dst[h, :, :, cols] = dot_tn(lhs, DV[:, :, cols].reshape(8 * TB, width)).reshape(2, ZD, width)
            return carry
        if halves is None:
            loop(2, rows, None)
        else:
            for h in halves:
                rows(h, None)

    def grad_b_first(chips, add):
        cols_l, cols = pl.ds(mo(off(y, OPP) * NK, NK), NK), pl.ds(0, K)
        dst = GPB.at[OPP]
        for t in chips:
            out = dot_tn(AV[t, :, :, cols_l].reshape(T2, NK), GV1[t, :, :, cols].reshape(T2, K)).reshape(2, NK // 2, K)
            dst[:, 0] = dst[:, 0] + out if add else out
            add = True

    def grad_b(gv, j, dst, n=None):
        cols_l = pl.ds(mo(off(y, j) * NK, NK), NK)

        def body(n, carry):
            out = dot_tn(AV[:, :, :, cols_l].reshape(8 * TB, NK), gv[:, :, :, pl.ds(mo(n * K, K), K)].reshape(8 * TB, K))
            dst[:, n] = out.reshape(2, NK // 2, K)
            return carry
        if n is None:
            loop(2, body, None)
        else:
            body(n, None)

    grad_keys = [keys_of(sum(u0u, u0a) + d0a), [d.key for d in ex0 + ex1 + gg1.own + gg1.push] + keys_of(d0b + d0c + [gg1.ring])]

    def grad_key(l):
        return grad_keys[l].pop() if grad_keys[l] else fresh("recv")

    class Reduce4:
        def __init__(self, l, axis, part, recv, stage):
            _, right, left = rings[axis]
            self.part, self.recv, self.stage = part, recv, stage
            self.m = [rcopy(part(*PIECES[k]), recv(k), left if k % 2 else right, grad_key(l))
                      for k in range(ARRIVALS)]
            self.loads = [lcopy(recv(k), stage(k)) for k in range(ARRIVALS)] if stage else None

        def opposite(self):
            self.m[0].start()
            self.m[1].start()

        def sides(self, j):
            self.m[2 if j == NXT else 3].start()

        def fetch(self, k):
            self.m[k].wait_send()
            self.m[k].wait_recv()
            if self.loads:
                self.loads[k].start()

        def absorb(self, k):
            if self.loads:
                self.loads[k].wait()
            dst = self.part(*TARGETS[k])
            add_rows(dst, [(self.stage or self.recv)(k)], dst.shape[1], min(dst.shape[1], 16))

    def arrive(reduces, ks):
        for k in ks:
            for r in reduces:
                r.fetch(k)
        for k in ks:
            for r in reduces:
                r.absorb(k)

    def relay(reduces):
        for k in (0, 1):
            for r in reduces:
                r.fetch(k)
        for k in (0, 1):
            for r in reduces:
                r.absorb(k)
                r.m[4 + k].start()

    hq = DR_ROWS // 2
    own_grads = [(SV.at[pl.ds(0, 2)], SV.at[pl.ds(2, 2)]), (GPA.at[OWN], GPB.at[OWN])]

    def third(k, rows):
        return pl.ds((k // 2) * rows, rows)

    def reduce_a(l, q, chunks):
        own = own_grads[l][0]
        ca = pl.ds(q * (K // chunks), K // chunks)

        def part(j, h):
            return (own if j == OWN else GPA.at[j]).at[h, :, :, ca]

        def part2(j, h):
            return own.at[h, :, pl.ds(mo(off(y, j) * 2 * UR, 2 * UR), 2 * UR), ca]
        if l < q:
            second = lambda k: GPA.at[OWN, k % 2, :, third(k, 2 * UR), ca], None
        else:
            second = lambda k: ra2.at[l, k, :, :, ca], lambda k: STA.at[k % 2, :, :, ca]
        return (Reduce4(l, "z", part, lambda k: ra1.at[l, k, :, :, ca], lambda k: part(*PIECES[k])),
                Reduce4(l, "y", part2, *second))

    def reduce_b(l, q):
        own, nb = own_grads[l][1], pl.ds(q, 1)

        def part(j, h):
            return (own if j == OWN else GPB.at[j]).at[h, nb]

        def part2(j, h):
            t = off(z, j)
            return own.at[t // 2, nb, pl.ds(mo(lax.rem(t, 2) * DR_ROWS + h * hq, hq), hq), :]
        if l < q:
            second = lambda k: GPB.at[OWN, k % 2, nb, third(k, hq), :], None
        else:
            second = lambda k: rb2.at[l, k, nb], lambda k: STB.at[k % 2, nb]
        return (Reduce4(l, "y", part, lambda k: rb1.at[l, k, nb], lambda k: part(*PIECES[k])),
                Reduce4(l, "z", part2, *second))

    def sides(reduces, j):
        for r in reduces:
            r.sides(j)

    def second_start(reduces):
        for r in reduces:
            r.opposite()
            r.sides(NXT)
            r.sides(PRV)

    def up_out(l, q, chunks):
        own = own_grads[l][0]
        ca = pl.ds(q * (K // chunks), K // chunks)

        def rows_of(tx, tc):
            return own.at[tx // 2, lax.rem(tx, 2), pl.ds(mo((2 * y + tc) * UR, UR), UR), ca]
        to = uh.at[l, x, mine, ca]
        sends = [rcopy(rows_of(off(x, dx), cp if dc else c), to, dev(dx=dx, dc=dc), grad_key(l)) for dx, dc in group]
        local = [lcopy(rows_of(x, c), to)]
        for cpy in sends + local:
            cpy.start()
        return sends, local

    def down_out(l, n):
        cpy = lcopy(own_grads[l][1].at[z // 2, n, pl.ds(mo(lax.rem(z, 2) * DR_ROWS, DR_ROWS), DR_ROWS), :],
                    gd_out.at[l, :, pl.ds(n * K, K)])
        cpy.start()
        return [], [cpy]

    def grads_out_finish(state):
        for cpy in state[0]:
            cpy.wait_recv()
            cpy.wait_send()
        for cpy in state[1]:
            cpy.wait()

    r = Reduce8(functools.partial(down_part, AV), 0, SPLIT3)
    r_keys = sorted([d.key for m in r.m for d in m] + [f + j for f in r.first for j in range(RING)])
    hidden0(off(x, OPP))
    hidden0(off(x, NXT))
    do(d0b, "finish")
    r.compute(OPP, 0)
    r.compute(NXT, 0)
    do(d0c, "forward")
    do(d0d, "start")
    r.combine(OPP, 0)
    r.opposite(0)
    do(u0u[2] + u0u[3], "drain")
    hidden0(off(x, PRV))
    r.compute(PRV, 0)
    r.side(NXT, 0)
    do(d1a, "forward")
    hidden0(off(x, OWN))
    r.side(PRV, 0)
    gx0.drain()
    save_s = lcopy(SV, sh0)
    save_s.start()
    save_a0 = lcopy(AV, ah.at[0])
    save_a0.start()
    gg1.sides()
    do(d0c, "finish")
    r.compute_all(1)
    r.relay(0)
    do(d0d, "forward")
    for cpy in ex1:
        cpy.wait_recv()
    own_d1.wait()
    do(u1a, "start")
    r.send(1)
    do(d1a, "finish")
    do(d1b, "start")
    gg1.last()
    save_x.wait()
    do(d0d, "finish")
    do(d0b + d0c, "drain")
    save_d0 = lcopy(W, wdh.at[0])
    save_d0.start()
    r.compute(OPP, 2)
    r.relay(1)
    save_u0.wait()
    do(u1a, "forward")
    r.compute(NXT, 2)
    r.combine(OPP, 2)
    r.opposite(2)
    r.compute(PRV, 2)
    r.side(NXT, 2)
    r.compute(OWN, 2)
    r.side(PRV, 2)
    r.compute(OWN, 0)
    for q in range(len(SPLIT3)):
        r.combine(OWN, q)

    def gather_keys(gathers):
        return [d.key for g in gathers for d in g.ring.d + g.own + g.push]

    def token_gathers(slot, buf):
        def make(q):
            cq = tile_cols(SPLIT2, q)
            return Gather8(lambda h: RES.at[slot, half(h), cq], lambda b, k, h: buf.at[b, k, half(h), cq])
        return [make(0), make(1)]

    keys.extend(gather_keys((gx0,)))
    gx1 = token_gathers(X1, XV)
    do(d1a, "drain")
    do(d1b, "forward")
    for q in HALVES:
        r.finish(q, RES.at[X0], [RES.at[X1], XV.at[x, c]])
    r.relay(2)
    gx1[0].start()
    do(u1a, "finish")
    do(u1b, "start")
    do(u1c, "start_first")
    pair, rest = pl.ds(0, 2), pl.ds(2, 2)
    own_up = [lcopy(up[1].at[pair, z], U.at[pair, z]), lcopy(up[1].at[rest, :, y], U.at[rest, :, y])]
    for cpy in own_up:
        cpy.start()
    gg1.wait_own()
    gg1.wait_push(range(len(gg1.push)))
    own_g.wait()
    save_d0.wait()
    do(d0d + u1a, "drain")
    gg1.drain()
    do(d1b, "finish")
    load_w1d = lcopy(wdh.at[1], W)
    load_w1d.start()
    r.finish(2, RES.at[X0], [RES.at[X1], XV.at[x, c]])
    gx1[1].start()
    save_s.wait()
    do(u1b, "forward")
    do(u1c, "start_rest")
    load_w1d.wait()
    dact1(off(x, OWN))
    gx1[0].forward()
    r.release()
    dact1(off(x, NXT))
    gx1[0].sides()
    dact1(off(x, PRV))
    do(u1c, "forward")
    do(u1b, "finish")
    dact1(off(x, OPP))
    load_w0d_again = lcopy(wdh.at[0], W)
    load_w0d_again.start()
    save_a0.wait()
    do(gx1, "wait_own")
    for cpy in own_up:
        cpy.wait()
    hidden1(off(x, OWN), 0)
    do(gx1[1:], "forward")
    do(gx1[1:], "sides")
    for j in (PRV, NXT):
        for g in gx1:
            g.wait_push(PUSHES[j])
        hidden1(off(x, j), 0)
    gx1[0].last()
    do(u1c, "finish")
    hidden1(off(x, OWN), 1)
    hidden1(off(x, PRV), 1)
    gx1[1].last()
    hidden1(off(x, NXT), 1)
    grad_b_first([off(x, j) for j in (OWN, PRV, NXT)], False)
    for g in gx1:
        g.wait_push(PUSHES[OPP])
    hidden1_tile(off(x, OPP), off(y, OPP))

    (a1, a2), (b1, b2) = zip(*[reduce_a(1, q, 2) for q in HALVES]), zip(*[reduce_b(1, q) for q in HALVES])
    first1, second1 = b1 + a1, b2 + a2
    grad_b_first([off(x, OPP)], True)
    b1[0].opposite()
    for q in HALVES:
        hidden1(off(x, OPP), q)
        for h in HALVES:
            grad_a(OPP, GPA.at[OPP], (h,), q)
            a1[q].m[h].start()
    load_s0 = lcopy(sh0, SV)
    load_s0.start()
    save_a1 = lcopy(AV, ah.at[1])
    save_a1.start()
    grad_b(GV1, OPP, GPB.at[OPP], 1)
    b1[1].opposite()
    r = Reduce8(dx_part, 1, SPLIT2, r_keys)
    r.acquire()
    r.compute(OPP, 0)
    r.compute(NXT, 0)
    r.combine(OPP, 0)
    r.opposite(0)
    r.compute(PRV, 0)
    r.side(NXT, 0)
    r.side(PRV, 0)
    r.compute_all(1)
    load_w0u_again = lcopy(wuh.at[0], U)
    r.compute(OWN, 0)
    do(u1b + u1c, "drain")
    load_w0u_again.start()
    grad_b(GV1, NXT, GPB.at[NXT])
    sides(b1, NXT)
    grad_b(GV1, PRV, GPB.at[PRV])
    sides(b1, PRV)
    r.relay(0)
    r.send(1)
    grad_a(NXT, GPA.at[NXT])
    sides(a1, NXT)
    grad_a(PRV, GPA.at[PRV])
    sides(a1, PRV)
    r.combine(OWN, 0)
    r.combine(OWN, 1)
    keys.extend(gather_keys(gx1))
    gg0 = token_gathers(G0, GV0)
    r.relay(1)
    r.finish(0, RES.at[G1], [RES.at[G0], GV0.at[x, c]])
    gg0[0].start()
    relay(first1)
    grad_b(GV1, OWN, GPB.at[OWN])
    save_a1.wait()
    load_a0 = lcopy(ah.at[0], AV)
    load_a0.start()
    do(d1b, "drain")
    load_a1 = lcopy(ah.at[1], GV1.at[:, :, :, 0:K])
    load_a1.start()
    r.finish(1, RES.at[G1], [RES.at[G0], GV0.at[x, c]])
    gg0[1].start()
    gg0[0].forward()
    grad_a(OWN, GPA.at[OWN])
    do(gx1, "drain")
    load_x0 = lcopy(xh0, XV)
    load_x0.start()
    gg0[0].sides()
    r.release()
    gg0[1].forward()
    gg0[0].last()
    load_w0d_again.wait()
    load_s0.wait()
    do(gg0, "wait_own")
    dact0(off(x, OWN))
    gg0[1].sides()
    gg0[1].last()
    for g in gg0:
        g.wait_push(PUSHES[PRV])
    dact0(off(x, PRV))
    for g in gg0:
        g.wait_push(PUSHES[NXT])
    dact0(off(x, NXT))
    for g in gg0:
        g.wait_push(PUSHES[OPP])

    (a1n, a2n), (b1n, b2n) = zip(*[reduce_a(0, q, 2) for q in HALVES]), zip(*[reduce_b(0, q) for q in HALVES])
    load_a0.wait()
    grad_b(GV0, OPP, GPB.at[OPP])
    b1n[0].opposite()
    dact0(off(x, OPP))
    load_w1d_again = lcopy(wdh.at[1], W)
    load_w1d_again.start()
    load_x0.wait()
    for h in HALVES:
        grad_a(OPP, GPA.at[OPP], (h,))
        a1n[0].m[h].start()
    arrive(first1, EARLY + LATE)
    second_start(second1)
    load_w0u_again.wait()
    r = Reduce8(dx_part, 2, WHOLE, r_keys)
    r.acquire()
    r.compute_all(0)
    r.send(0)
    grad_b(GV0, NXT, GPB.at[NXT])
    b1n[0].sides(NXT)
    grad_b(GV0, PRV, GPB.at[PRV])
    b1n[0].sides(PRV)
    grad_a(NXT, GPA.at[NXT])
    a1n[0].sides(NXT)
    grad_a(PRV, GPA.at[PRV])
    a1n[0].sides(PRV)
    relay(second1)
    r.relay(0)
    relay((b1n[0], a1n[0]))
    for red in (b1n[1], a1n[1]):
        red.opposite()
        red.sides(NXT)
        red.sides(PRV)
    r.combine(OWN, 0)
    grad_b(GV0, OWN, own_grads[0][1])
    grad_a(OWN, own_grads[0][0])
    r.finish(0, RES.at[G0], [RES.at[X0]])
    r.release()
    write_gi = lcopy(RES.at[X0], gi_out)
    write_gi.start()
    arrive((b1n[0], a1n[0]), EARLY)
    arrive(second1, EARLY)
    arrive(second1, LATE)
    state1 = [up_out(1, q, 2) for q in HALVES] + [down_out(1, n) for n in HALVES]
    load_a1.wait()
    load_w1d_again.wait()
    r = Reduce8(functools.partial(down_part, GV1), 3, WHOLE, r_keys)
    r.acquire()
    r.compute_all(0)
    r.send(0)
    r.combine(OWN, 0)
    arrive((b1n[0], a1n[0]), LATE)
    for state in state1:
        grads_out_finish(state)
    relay((b1n[1], a1n[1]))
    second_start((a2n[0], b2n[0]))
    r.relay(0)
    arrive((b1n[1], a1n[1]), EARLY)

    def start(red):
        red.opposite()
        sides((red,), NXT)
        sides((red,), PRV)
    arrive((b1n[1],), LATE)
    relay((a2n[0],))
    arrive((a1n[1],), LATE)
    start(a2n[1])
    start(b2n[1])
    arrive((a2n[0],), EARLY)
    relay((b2n[0],))
    arrive((a2n[0],), LATE)
    state0 = [up_out(0, 0, 2)]
    relay((a2n[1],))
    arrive((b2n[0],), EARLY)
    relay((b2n[1],))
    arrive((a2n[1],), EARLY)
    arrive((a2n[1],), LATE)
    state0.append(up_out(0, 1, 2))
    arrive((b2n[1],), EARLY)
    for q in HALVES:
        arrive((b2n[q],), LATE)
        state0.append(down_out(0, q))
    r.finish(0, RES.at[X1], [RES.at[G1]])
    write_y = lcopy(RES.at[G1], y_out)
    write_y.start()
    r.drain()
    do(gg0, "drain")
    write_gi.wait()
    write_y.wait()
    for state in state0:
        grads_out_finish(state)
    assert used["recv"] <= N_RECV and used["send"] <= N_SEND and used["local"] <= N_LOCAL


def finish_kernel(y_in, gi_in, gu_in, gd_in, y_out, gi_out, gu_out, gd_out, ybuf, gibuf, gubuf, gdbuf, gushuf, sems):
    layers, ur, ff = gu_out.shape
    s2 = ff // 64
    half = s2 // 2
    pairs = [((gu_in.at[l], gubuf.at[l]), (gushuf.at[l], gu_out.at[l])) for l in range(layers)]
    pairs += [((a, b), (b, o)) for a, b, o in ((gd_in, gdbuf, gd_out), (y_in, ybuf, y_out), (gi_in, gibuf, gi_out))]
    loads = [pltpu.make_async_copy(*p, sems.at[0, k]) for k, (p, _) in enumerate(pairs)]
    stores = [pltpu.make_async_copy(*p, sems.at[1, k]) for k, (_, p) in enumerate(pairs)]
    for cpy in loads:
        cpy.start()
    low = lax.broadcasted_iota(jnp.int32, (ur, s2), 1) < half
    swap = lambda v: pltpu.roll(v, half, 1)
    for l, (load, store) in enumerate(zip(loads, stores)):
        load.wait()
        for b in range(RING if l < layers else 0):
            for yy in range(RING):
                for m in HALVES:
                    cols = pl.ds((yy * 2 + m) * s2, s2)
                    t0, t1 = (gubuf[l, b, pl.ds(k * ur, ur), cols] for k in HALVES)
                    strip = (b * RING + 2 * m) * RING + yy
                    gushuf[l, :, pl.ds(strip * s2, s2)] = jnp.where(low, t0, swap(t1))
                    gushuf[l, :, pl.ds((strip + RING) * s2, s2)] = jnp.where(low, swap(t0), t1)
        store.start()
    for cpy in stores:
        cpy.wait()


def solution(mesh, interpret=None):
    fine = Mesh(np.asarray(mesh.devices).reshape(4, 4, 4, 2), ALL)
    tok_spec = P(ALL, None)
    weight_spec = P(None, ALL, None)

    def device_step(x_loc, up_loc, down_loc, g_loc):
        layers, ur, ff = up_loc.shape
        dr, dm = down_loc.shape[1:]
        tb = x_loc.shape[0]
        k = ff // 8
        zd = dm // 16
        hbm = lambda shape, dt: jax.ShapeDtypeStruct(shape, dt)
        outs = [
            hbm((tb, dm), BF16), hbm((tb, dm), BF16), hbm((layers, dr, dm), F32),
            hbm((RING, CORES, tb, dm), BF16),
            hbm((layers, RING, RING, RING, 2 * ur, k), BF16),
            hbm((layers, RING, RING, dr, dm), BF16),
            hbm((RING, CORES, tb, k), F32), hbm((layers, RING, CORES, tb, k), BF16),
            *[hbm((layers, ARRIVALS, CORES, n, k), F32) for n in (zd, zd, 2 * ur, 2 * ur)],
            hbm((layers, RING, 2 * ur, k), F32),
        ]
        vm = pltpu.VMEM
        scratch = [
            vm((RING, RING, RING, 2 * ur, k), BF16), vm((RING, RING, dr, dm), BF16),
            vm((RING, CORES, tb, dm), BF16), vm((RING, CORES, tb, dm), BF16), vm((RING, CORES, tb, dm), BF16),
            vm((RING, CORES, tb, k), F32), vm((RING, CORES, tb, k), BF16), vm((RING, 2 * tb, k), BF16),
            vm((RING, CORES, CORES, zd, k), F32), vm((RING, CORES, CORES, zd, k), F32),
            vm((RING, CORES, tb, dm), F32), vm((4, tb, dm), F32), vm((6, tb // 2, dm), F32),
            vm((4, tb, dm), BF16), vm((CORES, CORES, 2 * ur, k), F32), vm((CORES, CORES, 2 * ur, k), F32),
            *[pltpu.SemaphoreType.DMA((n,)) for n in (N_SEND, N_RECV, N_LOCAL, len(SPLIT3) * RING)],
            pltpu.SemaphoreType.REGULAR((3,)),
        ]
        anyspec = pl.BlockSpec(memory_space=pl.ANY)
        call = pl.pallas_call(
            functools.partial(kernel, (dm, k, tb, ur, dr)),
            out_shape=outs,
            in_specs=[anyspec] * 4,
            out_specs=[anyspec] * len(outs),
            scratch_shapes=scratch,
            compiler_params=pltpu.CompilerParams(collective_id=0, has_side_effects=True, vmem_limit_bytes=67043328),
            name="mlp_stack",
            **({"interpret": interpret} if interpret else {}),
        )
        y_raw, gi_raw, gd_raw, *_, gu_raw = call(x_loc, up_loc, down_loc, g_loc)
        raws = (y_raw, gi_raw, gu_raw, gd_raw)
        outs = [hbm((tb, dm), BF16), hbm((tb, dm), BF16), hbm((layers, ur, ff), F32), hbm((layers, dr, dm), F32)]
        return tuple(pl.pallas_call(
            finish_kernel, out_shape=outs, in_specs=[anyspec] * len(outs), out_specs=[anyspec] * len(outs),
            scratch_shapes=[vm(v.shape, v.dtype) for v in raws] + [vm(outs[2].shape, F32), pltpu.SemaphoreType.DMA((2, layers + len(outs)))],
            name="write_out")(*raws))

    return jax.shard_map(device_step, mesh=fine, in_specs=(tok_spec, weight_spec, weight_spec, tok_spec),
                         out_specs=(tok_spec, tok_spec, weight_spec, weight_spec), check_vma=False)
```
